16 devices in a mesh: fsdp: 16 (over z, y, x, core).
Axes of the slice: x: 2, y: 2, z: 2, core: 2. Of those that a mesh axis runs over, the one named last changes fastest.
Arguments:
- resid_in: bfloat16 [128, 257, 1280], P('fsdp')
- grad_out: bfloat16 [128, 257, 1280], P('fsdp')
- ln1_gain: float32 [1280], P('fsdp')
- ln1_bias: float32 [1280], P('fsdp')
- qkv_weight: float32 [1280, 3840], P('fsdp')
- qkv_bias: float32 [3840], P('fsdp')
- out_weight: float32 [1280, 1280], P('fsdp')
- out_bias: float32 [1280], P('fsdp')
- ln2_gain: float32 [1280], P('fsdp')
- ln2_bias: float32 [1280], P('fsdp')
- fc_weight: float32 [1280, 5120], P('fsdp')
- fc_bias: float32 [5120], P('fsdp')
- proj_weight: float32 [5120, 1280], P('fsdp')
- proj_bias: float32 [1280], P('fsdp')
Outputs:
- output 1: bfloat16 [128, 257, 1280], P('fsdp')
- output 2: bfloat16 [128, 257, 1280], P('fsdp')
- output 3: float32 [1280], P('fsdp')
- output 4: float32 [1280], P('fsdp')
- output 5: float32 [1280, 3840], P('fsdp')
- output 6: float32 [3840], P('fsdp')
- output 7: float32 [1280, 1280], P('fsdp')
- output 8: float32 [1280], P('fsdp')
- output 9: float32 [1280], P('fsdp')
- output 10: float32 [1280], P('fsdp')
- output 11: float32 [1280, 5120], P('fsdp')
- output 12: float32 [5120], P('fsdp')
- output 13: float32 [5120, 1280], P('fsdp')
- output 14: float32 [1280], P('fsdp')
All inputs are finite; a program needn't handle non-finite values.
Results may differ from the reference program's by a relative error of at most 0.02.
Values are sent between devices in bfloat16 or wider.
A program may use at most 1 GiB of HBM per device.

```python
import jax
import jax.numpy as jnp
from jax import lax

WIDTH = 1280
FFN = 5120
HEADS = 16
PATCHES = 256
BATCH = 128

SEQ = PATCHES + 1
HEAD_DIM = WIDTH // HEADS
LN_EPS = 1e-5


def setup_inputs(seed: int = 0) -> dict:
    keys = jax.random.split(jax.random.key(seed), 14)

    def normal(key_index, shape, scale):
        return jax.random.normal(keys[key_index], shape, jnp.float32) * scale

    return {
        "resid_in": normal(0, (BATCH, SEQ, WIDTH), 1.0).astype(jnp.bfloat16),
        "grad_out": normal(1, (BATCH, SEQ, WIDTH), 1.0).astype(jnp.bfloat16),
        "ln1_gain": 1.0 + normal(2, (WIDTH,), 0.6),
        "ln1_bias": normal(3, (WIDTH,), 1.0),
        "qkv_weight": normal(4, (WIDTH, 3 * WIDTH), WIDTH ** -0.5),
        "qkv_bias": normal(5, (3 * WIDTH,), 1.0),
        "out_weight": normal(6, (WIDTH, WIDTH), WIDTH ** -0.5),
        "out_bias": normal(7, (WIDTH,), 1.0),
        "ln2_gain": 1.0 + normal(8, (WIDTH,), 0.6),
        "ln2_bias": normal(9, (WIDTH,), 1.0),
        "fc_weight": normal(10, (WIDTH, FFN), WIDTH ** -0.5),
        "fc_bias": normal(11, (FFN,), 1.0),
        "proj_weight": normal(12, (FFN, WIDTH), FFN ** -0.5),
        "proj_bias": normal(13, (WIDTH,), 1.0),
    }


def layer_norm(values, gain, bias):
    mean_val = jnp.mean(values, axis=-1, keepdims=True)
    centered = values - mean_val
    variance = jnp.mean(centered * centered, axis=-1, keepdims=True)
    return centered * lax.rsqrt(variance + LN_EPS) * gain + bias


def layer_forward(params, tokens):
    (ln1_gain, ln1_bias, qkv_weight, qkv_bias, out_weight, out_bias,
     ln2_gain, ln2_bias, fc_weight, fc_bias, proj_weight, proj_bias) = [param.astype(jnp.bfloat16) for param in params]
    resid = tokens.astype(jnp.float32)
    normed_one = layer_norm(resid, ln1_gain, ln1_bias).astype(jnp.bfloat16)
    qkv_vals = (jnp.dot(normed_one, qkv_weight, preferred_element_type=jnp.float32) + qkv_bias).astype(jnp.bfloat16)
    qkv_vals = qkv_vals.reshape(SEQ, 3, HEADS, HEAD_DIM).astype(jnp.float32)
    scores = jnp.einsum("qhd,khd->hqk", qkv_vals[:, 0], qkv_vals[:, 1]) * (HEAD_DIM ** -0.5)
    attn_probs = jax.nn.softmax(scores, axis=-1).astype(jnp.bfloat16).astype(jnp.float32)
    mixed = jnp.einsum("hqk,khd->qhd", attn_probs, qkv_vals[:, 2]).astype(jnp.bfloat16).reshape(SEQ, WIDTH)
    middle = (resid + jnp.dot(mixed, out_weight, preferred_element_type=jnp.float32) + out_bias).astype(jnp.bfloat16)
    middle_wide = middle.astype(jnp.float32)
    normed_two = layer_norm(middle_wide, ln2_gain, ln2_bias).astype(jnp.bfloat16)
    pre_act = jnp.dot(normed_two, fc_weight, preferred_element_type=jnp.float32) + fc_bias
    hidden = jax.nn.gelu(pre_act, approximate=False).astype(jnp.bfloat16)
    return (middle_wide + jnp.dot(hidden, proj_weight, preferred_element_type=jnp.float32) + proj_bias).astype(jnp.bfloat16)


def reference(resid_in, grad_out, ln1_gain, ln1_bias, qkv_weight, qkv_bias, out_weight, out_bias,
              ln2_gain, ln2_bias, fc_weight, fc_bias, proj_weight, proj_bias):
    params = (ln1_gain, ln1_bias, qkv_weight, qkv_bias, out_weight, out_bias,
              ln2_gain, ln2_bias, fc_weight, fc_bias, proj_weight, proj_bias)

    def per_image(grad_sum, pair):
        tokens, cotangent = pair
        image_out, pullback = jax.vjp(layer_forward, params, tokens)
        param_grads, token_grad = pullback(cotangent)
        grad_sum = jax.tree.map(lambda total, fresh: total + fresh, grad_sum, param_grads)
        return grad_sum, (image_out, token_grad)

    start_sum = jax.tree.map(jnp.zeros_like, params)
    grad_sum, (resid_out, grad_in) = lax.scan(per_image, start_sum, (resid_in, grad_out))
    (grad_ln1_gain, grad_ln1_bias, grad_qkv_weight, grad_qkv_bias, grad_out_weight, grad_out_bias,
     grad_ln2_gain, grad_ln2_bias, grad_fc_weight, grad_fc_bias, grad_proj_weight, grad_proj_bias) = grad_sum
    return (resid_out, grad_in, grad_ln1_gain, grad_ln1_bias, grad_qkv_weight, grad_qkv_bias,
            grad_out_weight, grad_out_bias, grad_ln2_gain, grad_ln2_bias, grad_fc_weight, grad_fc_bias,
            grad_proj_weight, grad_proj_bias)
```

```python
import math
import jax, jax.numpy as jnp
from jax import lax
from jax.experimental import pallas as pl
from jax.experimental.pallas import tpu as pltpu
from jax.sharding import PartitionSpec as P

BF, F32 = jnp.bfloat16, jnp.float32
IMAGES, SEQ, WIDTH, FFN, HEADS, HEAD = 8, 257, 1280, 5120, 16, 80
MAIN = SEQ - 1
TOKENS = IMAGES * SEQ
TAIL = IMAGES * MAIN
LN_EPS = 1e-5
VMEM_MAX = 67043328
LANES = WIDTH // 128
ROWS = 32


def dot(a, b):
    return jnp.dot(a, b, preferred_element_type=F32)


def dot_nt(a, b):
    return lax.dot_general(a, b, (((1,), (1,)), ((), ())), preferred_element_type=F32)


def dot_tn(a, b):
    return lax.dot_general(a, b, (((0,), (0,)), ((), ())), preferred_element_type=F32)


def col_sum(v):
    return jnp.sum(v, axis=0, keepdims=True)


def col_max(v):
    return jnp.max(v, axis=0, keepdims=True)


def row_sum(v):
    return jnp.sum(v, axis=-1, keepdims=True)


def whole(*shape, **kw):
    return pl.BlockSpec(shape, lambda *i: (0,) * len(shape), **kw)


def norm_stats(values):
    mean = row_sum(values) * (1.0 / WIDTH)
    centered = values - mean
    inv = lax.rsqrt(row_sum(centered * centered) * (1.0 / WIDTH) + LN_EPS)
    return centered * inv, inv


def row_tiles(body, step=128):
    def loop(i, carry):
        body(pl.multiple_of(i * step, step), step)
        return carry
    lax.fori_loop(0, TAIL // step, loop, 0)
    body(TAIL, IMAGES)


def to_image_order(wide, place, step=128):
    per = MAIN // step
    def loop(i, carry):
        first = (i % per) * (step * IMAGES) + i // per
        rows = [wide[c, pl.ds(first, step, stride=IMAGES), :] for c in range(LANES)]
        place(pl.multiple_of(i * step, step), step, jnp.concatenate(rows, axis=1))
        return carry
    lax.fori_loop(0, IMAGES * per, loop, 0)
    place(TAIL, IMAGES, joined(wide, TAIL, IMAGES))


def from_image_order(values, wide):
    def loop(i, carry):
        rows = values[pl.ds(pl.multiple_of(i * 128, 128), 128), :]
        for c in range(LANES):
            wide[c, pl.ds((i % 2) * (128 * IMAGES) + i // 2, 128, stride=IMAGES), :] = rows[:, c * 128:(c + 1) * 128]
        return carry
    lax.fori_loop(0, 2 * IMAGES, loop, 0)
    put(wide, TAIL, IMAGES, values[pl.ds(TAIL, IMAGES), :])


def joined(wide, r, n):
    return jnp.concatenate([wide[c, pl.ds(r, n), :] for c in range(LANES)], axis=1)


def put(wide, r, n, values):
    for c in range(LANES):
        wide[c, pl.ds(r, n), :] = values[:, c * 128:(c + 1) * 128]


QKV_N = 768


def qkv_kernel(x_ref, gain_ref, bias_ref, w_ref, wb_ref, xim_ref, h_ref, qkv_ref, wide):
    @pl.when(pl.program_id(0) == 0)
    def _():
        def widen(r, n):
            put(wide, r, n, x_ref[pl.ds(r, n), :].astype(F32))
        row_tiles(widen)
        gain, bias = gain_ref[...], bias_ref[...]

        def place(r, n, values):
            xim_ref[pl.ds(r, n), :] = values.astype(BF)
            hat, _ = norm_stats(values)
            h_ref[pl.ds(r, n), :] = (hat * gain + bias).astype(BF)
        to_image_order(wide, place, ROWS)
    qkv_ref[...] = (dot(h_ref[...], w_ref[...]) + wb_ref[...]).astype(BF)


def qkv_call(x, gain, bias, w, wb):
    full = whole(TOKENS, WIDTH)
    vec = whole(1, WIDTH)
    return pl.pallas_call(
        qkv_kernel,
        grid=(3 * WIDTH // QKV_N,),
        in_specs=[whole(TOKENS, WIDTH, pipeline_mode=pl.Buffered(1)), vec, vec,
                  pl.BlockSpec((WIDTH, QKV_N), lambda i: (0, i)), pl.BlockSpec((1, QKV_N), lambda i: (0, i))],
        out_specs=[full, full, pl.BlockSpec((TOKENS, QKV_N), lambda i: (0, i))],
        out_shape=[jax.ShapeDtypeStruct((TOKENS, WIDTH), BF), jax.ShapeDtypeStruct((TOKENS, WIDTH), BF),
                   jax.ShapeDtypeStruct((TOKENS, 3 * WIDTH), BF)],
        scratch_shapes=[pltpu.VMEM((LANES, TOKENS, 128), F32)],
        compiler_params=pltpu.CompilerParams(dimension_semantics=("arbitrary",), vmem_limit_bytes=VMEM_MAX),
        cost_estimate=pl.CostEstimate(flops=2 * TOKENS * WIDTH * 3 * WIDTH, bytes_accessed=60_000_000, transcendentals=0),
        name="qkv",
    )(x, gain, bias, w, wb)


MLP_F = 256
CDF_P = 0.33
CDF_C = (0.1326322871417956, 0.11939570820799192, 0.18103829560051796, -0.08904113226212501,
         0.33075919469138065, -0.22023738432274684, 0.0454530347223348)


def gelu_pair(u):
    bell = jnp.exp(u * u * -0.5)
    t = 1.0 / (1.0 + CDF_P * jnp.abs(u))
    poly = CDF_C[6]
    for c in CDF_C[5::-1]:
        poly = poly * t + c
    tail = poly * t * bell
    cdf = jnp.where(u < 0.0, tail, 1.0 - tail)
    return u * cdf, cdf + u * bell * ((2.0 * math.pi) ** -0.5)


def mlp_kernel(r_hbm, dy_hbm, gain_ref, bias_ref, pb_ref, fc_ref, proj_ref, fcb_ref,
               y_hbm, dr_hbm, dr16_hbm, dfc_ref, dproj_ref, dfcb_ref, small_ref,
               n2, dy, y_acc, dn_acc, g, du, ua, ub, da, db, sem):
    step, last = pl.program_id(0), pl.num_programs(0) - 1

    @pl.when(step == 0)
    def _():
        cp = pltpu.make_async_copy(dy_hbm, n2, sem)
        cp.start()
        cp.wait()

        def widen(r, n):
            put(dn_acc, r, n, n2[pl.ds(r, n), :].astype(F32))
        row_tiles(widen)
        cp = pltpu.make_async_copy(r_hbm, n2, sem)
        cp.start()

        def place(r, n, values):
            dy[pl.ds(r, n), :] = values.astype(BF)
        to_image_order(dn_acc, place)
        cp.wait()
        gain, bias = gain_ref[...], bias_ref[...]

        def norm(r, n):
            hat, _ = norm_stats(n2[pl.ds(r, n), :].astype(F32))
            n2[pl.ds(r, n), :] = (hat * gain + bias).astype(BF)
            y_acc[pl.ds(r, n), :] = jnp.zeros((n, WIDTH), F32)
            put(dn_acc, r, n, jnp.zeros((n, WIDTH), F32))
        row_tiles(norm, ROWS)

    fcb = fcb_ref[...]
    bias_sum = jnp.zeros((8, MLP_F), F32)
    tiles = [(b * MAIN, MAIN) for b in range(IMAGES - 1)] + [((IMAGES - 1) * MAIN, MAIN + IMAGES)]
    pairs = ((ua, da), (ub, db))

    def products(k):
        r, n = tiles[k]
        u_s, d_s = pairs[k % 2]
        u_s[0:n, :] = dot(n2[r:r + n, :], fc_ref[...])
        d_s[0:n, :] = dot_nt(dy[r:r + n, :], proj_ref[...])

    def pointwise(k, total):
        r, n = tiles[k]
        u_s, d_s = pairs[k % 2]
        value, slope = gelu_pair(u_s[0:n, :] + fcb)
        g[r:r + n, :] = value.astype(BF)
        grad = d_s[0:n, :] * slope
        du[r:r + n, :] = grad.astype(BF)
        return total + jnp.sum(grad.reshape(n // 8, 8, MLP_F), axis=0)

    products(0)
    for k in range(1, IMAGES):
        products(k)
        bias_sum = pointwise(k - 1, bias_sum)
    bias_sum = pointwise(IMAGES - 1, bias_sum)
    dfcb_ref[...] = col_sum(bias_sum)
    y_acc[...] += dot(g[...], proj_ref[...])
    for c in range(LANES // 2):
        part = dot_nt(du[...], fc_ref[c * 256:(c + 1) * 256, :])
        dn_acc[2 * c] += part[:, :128]
        dn_acc[2 * c + 1] += part[:, 128:]
    dproj_ref[...] = dot_tn(g[...], dy[...])
    dfc_ref[...] = dot_tn(n2[...], du[...])

    @pl.when(step == last)
    def _():
        cp = pltpu.make_async_copy(r_hbm, n2, sem)
        cp.start()
        cp.wait()
        gain, pb = gain_ref[...], pb_ref[...]
        small_ref[...] = jnp.zeros_like(small_ref)

        def rows_sum(v):
            return jnp.sum(v.reshape(v.shape[0] // 8, 8, WIDTH), axis=0)

        def back(r, n):
            wide_r = n2[pl.ds(r, n), :].astype(F32)
            hat, inv = norm_stats(wide_r)
            dn = joined(dn_acc, r, n)
            wide_dy = dy[pl.ds(r, n), :].astype(F32)
            small_ref[0:8, :] += rows_sum(dn * hat)
            small_ref[8:16, :] += rows_sum(dn)
            small_ref[16:24, :] += rows_sum(wide_dy)
            dhat = dn * gain
            m1 = row_sum(dhat) * (1.0 / WIDTH)
            m2 = row_sum(dhat * hat) * (1.0 / WIDTH)
            dr = wide_dy + inv * (dhat - m1 - hat * m2)
            put(dn_acc, r, n, dr)
            small_ref[24:32, :] += rows_sum(dr)
            y_acc[pl.ds(r, n), :] += wide_r + pb
            n2[pl.ds(r, n), :] = dr.astype(BF)
        row_tiles(back, ROWS)
        copies = [pltpu.make_async_copy(dn_acc, dr_hbm, sem), pltpu.make_async_copy(n2, dr16_hbm, sem)]
        for cp in copies:
            cp.start()
        for cp in copies:
            cp.wait()
        from_image_order(y_acc, dn_acc)

        def narrow(r, n):
            dy[pl.ds(r, n), :] = joined(dn_acc, r, n).astype(BF)
        row_tiles(narrow)
        cp = pltpu.make_async_copy(dy, y_hbm, sem)
        cp.start()
        cp.wait()


def mlp_call(r, dy, gain, bias, pb, fc, proj, fcb):
    hbm = pl.BlockSpec(memory_space=pl.ANY)
    vec = whole(1, WIDTH)
    n = fc.shape[1]
    return pl.pallas_call(
        mlp_kernel,
        grid=(n // MLP_F,),
        in_specs=[hbm, hbm, vec, vec, vec, pl.BlockSpec((WIDTH, MLP_F), lambda i: (0, i)),
                  pl.BlockSpec((MLP_F, WIDTH), lambda i: (i, 0)), pl.BlockSpec((1, MLP_F), lambda i: (0, i))],
        out_specs=[hbm, hbm, hbm, pl.BlockSpec((WIDTH, MLP_F), lambda i: (0, i)), pl.BlockSpec((MLP_F, WIDTH), lambda i: (i, 0)),
                   pl.BlockSpec((1, MLP_F), lambda i: (0, i)), whole(32, WIDTH)],
        out_shape=[jax.ShapeDtypeStruct((TOKENS, WIDTH), BF), jax.ShapeDtypeStruct((LANES, TOKENS, 128), F32),
                   jax.ShapeDtypeStruct((TOKENS, WIDTH), BF), jax.ShapeDtypeStruct((WIDTH, n), F32), jax.ShapeDtypeStruct((n, WIDTH), F32),
                   jax.ShapeDtypeStruct((1, n), F32), jax.ShapeDtypeStruct((32, WIDTH), F32)],
        scratch_shapes=[pltpu.VMEM((TOKENS, WIDTH), BF), pltpu.VMEM((TOKENS, WIDTH), BF),
                        pltpu.VMEM((TOKENS, WIDTH), F32), pltpu.VMEM((LANES, TOKENS, 128), F32),
                        pltpu.VMEM((TOKENS, MLP_F), BF), pltpu.VMEM((TOKENS, MLP_F), BF)]
                       + [pltpu.VMEM((MAIN + IMAGES, MLP_F), F32)] * 4 + [pltpu.SemaphoreType.DMA],
        compiler_params=pltpu.CompilerParams(dimension_semantics=("arbitrary",), vmem_limit_bytes=VMEM_MAX),
        cost_estimate=pl.CostEstimate(flops=12 * TOKENS * WIDTH * n, bytes_accessed=150_000_000, transcendentals=TOKENS * n),
        name="mlp",
    )(r, dy, gain, bias, pb, fc, proj, fcb)


SCALE = HEAD ** -0.5


def window(h):
    first = min(HEAD * h // 128 * 128, WIDTH - 256)
    wide = 128 if HEAD * h + HEAD <= first + 128 else 256
    return first, wide, HEAD * h - first


def lane_mask(h):
    first, wide, off = window(h)
    lane = lax.broadcasted_iota(jnp.int32, (MAIN, wide), 1)
    return (lane >= off) & (lane < off + HEAD)


def head_rows():
    lane = lax.broadcasted_iota(jnp.int32, (HEADS, WIDTH), 1)
    row = lax.broadcasted_iota(jnp.int32, (HEADS, WIDTH), 0)
    return jnp.where((lane >= row * HEAD) & (lane < row * HEAD + HEAD), 1.0, 0.0).astype(F32)


def tail_softmax(s, s_self):
    m = jnp.maximum(jnp.max(s, axis=1, keepdims=True), s_self)
    e = jnp.exp((s - m) * SCALE)
    e_self = jnp.exp((s_self - m) * SCALE)
    inv = 1.0 / (row_sum(e) + e_self)
    return e * inv, e_self * inv


def attn_kernel(qkv_ref, qkvt_ref, x_ref, xt_ref, w_ref, wb_ref, o_hbm, r_hbm, max_ref, inv_ref,
                tails, o_tail, o_t, ptail, o_buf, r_buf, sems):
    b, last = pl.program_id(0), pl.num_programs(0) - 1
    slot = b % 2

    @pl.when(b == 0)
    def _():
        tails[...] = qkvt_ref[...].astype(F32)

    heads = head_rows()
    q_t = heads * tails[pl.ds(b, 1), 0:WIDTH]
    k_t = heads * tails[pl.ds(b, 1), WIDTH:2 * WIDTH]
    v_t = heads * tails[pl.ds(b, 1), 2 * WIDTH:3 * WIDTH]
    q, k, v = qkv_ref[:, 0:WIDTH], qkv_ref[:, WIDTH:2 * WIDTH], qkv_ref[:, 2 * WIDTH:3 * WIDTH]

    p, p_self = tail_softmax(dot_nt(q_t.astype(BF), k), row_sum(q_t * k_t))
    mixed = dot(p.astype(BF), v) * heads + p_self.astype(BF).astype(F32) * v_t
    o_tail[pl.ds(b, 1), :] = col_sum(mixed)

    s_tail = dot_nt(k_t.astype(BF), q)
    v_turned = v.T
    for h in range(HEADS):
        first, wide, _ = window(h)
        q_h = jnp.where(lane_mask(h), qkv_ref[:, first:first + wide], jnp.zeros((), BF))
        s = dot_nt(qkv_ref[:, WIDTH + first:WIDTH + first + wide], q_h)
        top = jnp.maximum(col_max(s), s_tail[h:h + 1, :])
        e = jnp.exp((s - top) * SCALE)
        e_tail = jnp.exp((s_tail[h:h + 1, :] - top) * SCALE)
        inv = 1.0 / (col_sum(e) + e_tail)
        max_ref[0, h:h + 1, :] = top
        inv_ref[0, h:h + 1, :] = inv
        ptail[h:h + 1, :] = e_tail * inv
        o_t[HEAD * h:HEAD * h + HEAD, :] = dot(v_turned[HEAD * h:HEAD * h + HEAD, :], (e * inv).astype(BF))

    @pl.when(b >= 2)
    def _():
        out_copy(o_buf, o_hbm, slot, b - 2, sems, 0).wait()
        out_copy(r_buf, r_hbm, slot, b - 2, sems, 1).wait()

    o = (o_t[...].T + dot_tn(ptail[...].astype(BF), v_t.astype(BF))).astype(BF)
    o_buf[slot] = o
    r_buf[slot] = (x_ref[...].astype(F32) + dot(o, w_ref[...]) + wb_ref[...]).astype(BF)
    out_copy(o_buf, o_hbm, slot, b, sems, 0).start()
    out_copy(r_buf, r_hbm, slot, b, sems, 1).start()

    @pl.when(b == last)
    def _():
        for buf, hbm, n in ((o_buf, o_hbm, 0), (r_buf, r_hbm, 1)):
            out_copy(buf, hbm, 1 - slot, b - 1, sems, n).wait()
        o = o_tail[...].astype(BF)
        o_buf[1 - slot, 0:IMAGES, :] = o
        r_buf[1 - slot, 0:IMAGES, :] = (xt_ref[...].astype(F32) + dot(o, w_ref[...]) + wb_ref[...]).astype(BF)
        copies = [pltpu.make_async_copy(buf.at[1 - slot, pl.ds(0, IMAGES)], hbm.at[pl.ds(TAIL, IMAGES)], sems.at[n, 1 - slot])
                  for buf, hbm, n in ((o_buf, o_hbm, 0), (r_buf, r_hbm, 1))]
        for cp in copies:
            cp.start()
        for cp in copies:
            cp.wait()
        for buf, hbm, n in ((o_buf, o_hbm, 0), (r_buf, r_hbm, 1)):
            out_copy(buf, hbm, slot, b, sems, n).wait()


def out_copy(buf, hbm, slot, b, sems, n):
    return pltpu.make_async_copy(buf.at[slot], hbm.at[pl.ds(pl.multiple_of(b * MAIN, MAIN), MAIN)], sems.at[n, slot])


def attn_call(qkv, xim, w, wb):
    hbm = pl.BlockSpec(memory_space=pl.ANY)
    main = lambda n: pl.BlockSpec((MAIN, n), lambda i: (i, 0))
    tail = lambda n: pl.BlockSpec((IMAGES, n), lambda i: (TAIL // IMAGES, 0))
    stat = pl.BlockSpec((1, HEADS, MAIN), lambda i: (i, 0, 0))
    return pl.pallas_call(
        attn_kernel,
        grid=(IMAGES,),
        in_specs=[main(3 * WIDTH), tail(3 * WIDTH), main(WIDTH), tail(WIDTH),
                  whole(WIDTH, WIDTH), whole(1, WIDTH)],
        out_specs=[hbm, hbm, stat, stat],
        out_shape=[jax.ShapeDtypeStruct((TOKENS, WIDTH), BF), jax.ShapeDtypeStruct((TOKENS, WIDTH), BF),
                   jax.ShapeDtypeStruct((IMAGES, HEADS, MAIN), F32), jax.ShapeDtypeStruct((IMAGES, HEADS, MAIN), F32)],
        scratch_shapes=[pltpu.VMEM((IMAGES, 3 * WIDTH), F32), pltpu.VMEM((IMAGES, WIDTH), F32),
                        pltpu.VMEM((WIDTH, MAIN), F32), pltpu.VMEM((HEADS, MAIN), F32),
                        pltpu.VMEM((2, MAIN, WIDTH), BF), pltpu.VMEM((2, MAIN, WIDTH), BF), pltpu.SemaphoreType.DMA((2, 2))],
        compiler_params=pltpu.CompilerParams(dimension_semantics=("arbitrary",), vmem_limit_bytes=VMEM_MAX),
        cost_estimate=pl.CostEstimate(flops=30_000_000_000, bytes_accessed=50_000_000, transcendentals=8_400_000),
        name="attn",
    )(qkv, qkv, xim, xim, w, wb)


def outb_kernel(dr_ref, o_ref, w_ref, do_ref, dw_ref):
    n = 256
    c = pl.program_id(0)
    do_ref[...] = dot_nt(dr_ref[...], w_ref[...]).astype(BF)
    dw_ref[...] = dot_tn(o_ref[...], dr_ref[:, pl.ds(pl.multiple_of(c * n, n), n)])


def outb_call(dr, o, w):
    n = 256
    full = whole(TOKENS, WIDTH)
    return pl.pallas_call(
        outb_kernel,
        grid=(WIDTH // n,),
        in_specs=[full, full, pl.BlockSpec((n, WIDTH), lambda i: (i, 0))],
        out_specs=[pl.BlockSpec((TOKENS, n), lambda i: (0, i)), pl.BlockSpec((WIDTH, n), lambda i: (0, i))],
        out_shape=[jax.ShapeDtypeStruct((TOKENS, WIDTH), BF), jax.ShapeDtypeStruct((WIDTH, WIDTH), F32)],
        compiler_params=pltpu.CompilerParams(dimension_semantics=("arbitrary",), vmem_limit_bytes=VMEM_MAX),
        cost_estimate=pl.CostEstimate(flops=4 * TOKENS * WIDTH * WIDTH, bytes_accessed=30_000_000, transcendentals=0),
        name="outb",
    )(dr, o, w)


def attn_back_kernel(qkv_ref, qkvt_ref, do_ref, dot_ref, max_ref, inv_ref, dqkv_hbm, dwb_ref,
                     tails, do_tails, grad_tails, dq_t, dk, dv, ds_tail, buf, sems):
    b, last = pl.program_id(0), pl.num_programs(0) - 1
    slot = b % 2

    @pl.when(b == 0)
    def _():
        tails[...] = qkvt_ref[...].astype(F32)
        do_tails[...] = dot_ref[...].astype(F32)
        dwb_ref[...] = jnp.zeros_like(dwb_ref)

    heads = head_rows()
    q_t = heads * tails[pl.ds(b, 1), 0:WIDTH]
    k_t = heads * tails[pl.ds(b, 1), WIDTH:2 * WIDTH]
    v_t = heads * tails[pl.ds(b, 1), 2 * WIDTH:3 * WIDTH]
    do_t = heads * do_tails[pl.ds(b, 1), :]
    q, k, v = qkv_ref[:, 0:WIDTH], qkv_ref[:, WIDTH:2 * WIDTH], qkv_ref[:, 2 * WIDTH:3 * WIDTH]
    do = do_ref[...]
    q_t16, k_t16, v_t16, do_t16 = (z.astype(BF) for z in (q_t, k_t, v_t, do_t))

    p, p_self = tail_softmax(dot_nt(q_t16, k), row_sum(q_t * k_t))
    dp, dp_self = dot_nt(do_t16, v), row_sum(do_t * v_t)
    inner = row_sum(p * dp) + p_self * dp_self
    ds16 = (p * (dp - inner) * SCALE).astype(BF)
    ds_self = (p_self * (dp_self - inner) * SCALE).astype(BF).astype(F32)
    grad_q = col_sum(dot(ds16, k) * heads + ds_self * k_t)
    grad_k = ds_self * q_t
    grad_v = p_self.astype(BF).astype(F32) * do_t
    dk[...] = dot_tn(ds16, q_t16)
    dv[...] = dot_tn(p.astype(BF), do_t16)

    p_tail = jnp.exp((dot_nt(k_t16, q) - max_ref[0]) * SCALE) * inv_ref[0]
    dp_tail = dot_nt(v_t16, do)
    inner_tail = p_tail * dp_tail

    k_turned = k.T
    for h in range(HEADS):
        first, wide, _ = window(h)
        here = slice(first, first + wide)
        mask = lane_mask(h)
        q_h = jnp.where(mask, qkv_ref[:, here], jnp.zeros((), BF))
        do_h = jnp.where(mask, do_ref[:, here], jnp.zeros((), BF))
        s = dot_nt(qkv_ref[:, WIDTH + first:WIDTH + first + wide], q_h)
        dp = dot_nt(qkv_ref[:, 2 * WIDTH + first:2 * WIDTH + first + wide], do_h)
        p = jnp.exp((s - max_ref[0, h:h + 1, :]) * SCALE) * inv_ref[0, h:h + 1, :]
        inner = col_sum(p * dp) + inner_tail[h:h + 1, :]
        ds = (p * (dp - inner) * SCALE).astype(BF)
        dv[:, here] += dot(p.astype(BF), do_h)
        dk[:, here] += dot(ds, q_h)
        dq_t[HEAD * h:HEAD * h + HEAD, :] = dot(k_turned[HEAD * h:HEAD * h + HEAD, :], ds)
        ds_tail[h:h + 1, :] = p_tail[h:h + 1, :] * (dp_tail[h:h + 1, :] - inner) * SCALE

    ds_tail16 = ds_tail[...].astype(BF)
    grad_k = col_sum(grad_k + dot(ds_tail16, q) * heads)
    grad_v = col_sum(grad_v + dot(p_tail.astype(BF), do) * heads)

    @pl.when(b >= 2)
    def _():
        out_copy(buf, dqkv_hbm, slot, b - 2, sems, 0).wait()

    grad = dq_t[...].T + dot_tn(ds_tail16, k_t16)
    for n, (main, tail) in enumerate(((grad, grad_q), (dk[...], grad_k), (dv[...], grad_v))):
        here = slice(n * WIDTH, (n + 1) * WIDTH)
        buf[slot, :, here] = main.astype(BF)
        grad_tails[pl.ds(b, 1), here] = tail
        dwb_ref[:, here] += col_sum(main) + tail
    out_copy(buf, dqkv_hbm, slot, b, sems, 0).start()

    @pl.when(b == last)
    def _():
        out_copy(buf, dqkv_hbm, 1 - slot, b - 1, sems, 0).wait()
        buf[1 - slot, 0:IMAGES, :] = grad_tails[...].astype(BF)
        cp = pltpu.make_async_copy(buf.at[1 - slot, pl.ds(0, IMAGES)], dqkv_hbm.at[pl.ds(TAIL, IMAGES)], sems.at[0, 1 - slot])
        cp.start()
        cp.wait()
        out_copy(buf, dqkv_hbm, slot, b, sems, 0).wait()


def attn_back_call(qkv, do, top, inv):
    hbm = pl.BlockSpec(memory_space=pl.ANY)
    main = lambda n: pl.BlockSpec((MAIN, n), lambda i: (i, 0))
    tail = lambda n: pl.BlockSpec((IMAGES, n), lambda i: (TAIL // IMAGES, 0))
    stat = pl.BlockSpec((1, HEADS, MAIN), lambda i: (i, 0, 0))
    return pl.pallas_call(
        attn_back_kernel,
        grid=(IMAGES,),
        in_specs=[main(3 * WIDTH), tail(3 * WIDTH), main(WIDTH), tail(WIDTH), stat, stat],
        out_specs=[hbm, whole(1, 3 * WIDTH)],
        out_shape=[jax.ShapeDtypeStruct((TOKENS, 3 * WIDTH), BF), jax.ShapeDtypeStruct((1, 3 * WIDTH), F32)],
        scratch_shapes=[pltpu.VMEM((IMAGES, 3 * WIDTH), F32), pltpu.VMEM((IMAGES, WIDTH), F32),
                        pltpu.VMEM((IMAGES, 3 * WIDTH), F32), pltpu.VMEM((WIDTH, MAIN), F32),
                        pltpu.VMEM((MAIN, WIDTH), F32), pltpu.VMEM((MAIN, WIDTH), F32), pltpu.VMEM((HEADS, MAIN), F32),
                        pltpu.VMEM((2, MAIN, 3 * WIDTH), BF), pltpu.SemaphoreType.DMA((1, 2))],
        compiler_params=pltpu.CompilerParams(dimension_semantics=("arbitrary",), vmem_limit_bytes=VMEM_MAX),
        cost_estimate=pl.CostEstimate(flops=60_000_000_000, bytes_accessed=50_000_000, transcendentals=8_400_000),
        name="attn_back",
    )(qkv, qkv, do, do, top, inv)


def qkvb_kernel(xim_hbm, dr_hbm, gain_ref, h_ref, dqkv_ref, w_ref, dx_hbm, dw_ref, small_ref, acc, dr, xd, sems):
    c, last = pl.program_id(0), pl.num_programs(0) - 1
    loads = [pltpu.make_async_copy(dr_hbm, dr, sems.at[0]), pltpu.make_async_copy(xim_hbm, xd, sems.at[1])]

    @pl.when(c == 0)
    def _():
        for cp in loads:
            cp.start()
        acc[...] = jnp.zeros_like(acc)
    acc[...] += dot_nt(dqkv_ref[...], w_ref[...])
    dw_ref[...] = dot_tn(h_ref[...], dqkv_ref[...])

    @pl.when(c == last)
    def _():
        for cp in loads:
            cp.wait()
        gain = gain_ref[...]
        small_ref[...] = jnp.zeros_like(small_ref)

        def back(r, n):
            hat, inv = norm_stats(xd[pl.ds(r, n), :].astype(F32))
            dn = acc[pl.ds(r, n), :]
            small_ref[0:8, :] += jnp.sum((dn * hat).reshape(n // 8, 8, WIDTH), axis=0)
            small_ref[8:16, :] += jnp.sum(dn.reshape(n // 8, 8, WIDTH), axis=0)
            dhat = dn * gain
            m1 = row_sum(dhat) * (1.0 / WIDTH)
            m2 = row_sum(dhat * hat) * (1.0 / WIDTH)
            acc[pl.ds(r, n), :] = joined(dr, r, n) + inv * (dhat - m1 - hat * m2)
        row_tiles(back, ROWS)
        from_image_order(acc, dr)

        def narrow(r, n):
            xd[pl.ds(r, n), :] = joined(dr, r, n).astype(BF)
        row_tiles(narrow)
        cp = pltpu.make_async_copy(xd, dx_hbm, sems.at[1])
        cp.start()
        cp.wait()


def qkvb_call(xim, dr, gain, h, dqkv, w):
    hbm = pl.BlockSpec(memory_space=pl.ANY)
    return pl.pallas_call(
        qkvb_kernel,
        grid=(3 * WIDTH // QKV_N,),
        in_specs=[hbm, hbm, whole(1, WIDTH),
                  whole(TOKENS, WIDTH, pipeline_mode=pl.Buffered(1)),
                  pl.BlockSpec((TOKENS, QKV_N), lambda i: (0, i)), pl.BlockSpec((WIDTH, QKV_N), lambda i: (0, i))],
        out_specs=[hbm, pl.BlockSpec((WIDTH, QKV_N), lambda i: (0, i)), whole(16, WIDTH)],
        out_shape=[jax.ShapeDtypeStruct((TOKENS, WIDTH), BF), jax.ShapeDtypeStruct((WIDTH, 3 * WIDTH), F32),
                   jax.ShapeDtypeStruct((16, WIDTH), F32)],
        scratch_shapes=[pltpu.VMEM((TOKENS, WIDTH), F32), pltpu.VMEM((LANES, TOKENS, 128), F32), pltpu.VMEM((TOKENS, WIDTH), BF),
                        pltpu.SemaphoreType.DMA((2,))],
        compiler_params=pltpu.CompilerParams(dimension_semantics=("arbitrary",), vmem_limit_bytes=VMEM_MAX),
        cost_estimate=pl.CostEstimate(flops=4 * TOKENS * WIDTH * 3 * WIDTH, bytes_accessed=80_000_000, transcendentals=0),
        name="qkvb",
    )(xim, dr, gain, h, dqkv, w)


PARTS = 16
VECTORS = (80, 80, 240, 80, 80, 80, 320, 80)


def solution(mesh):
    specs = (P("fsdp"),) * 14

    def gather(shard):
        return lax.all_gather(shard.astype(BF), "fsdp", axis=0, tiled=True)

    def scatter(grad):
        return lax.psum_scatter(grad, "fsdp", scatter_dimension=0, tiled=True)

    def device_step(resid_in, grad_out, ln1_gain, ln1_bias, qkv_weight, qkv_bias, out_weight, out_bias,
                    ln2_gain, ln2_bias, fc_weight, fc_bias, proj_weight, proj_bias):
        wq, wo, wf, wp = (gather(w) for w in (qkv_weight, out_weight, fc_weight, proj_weight))
        packed = jnp.concatenate([ln1_gain, ln1_bias, qkv_bias, out_bias, ln2_gain, ln2_bias, fc_bias, proj_bias])
        packed = gather(packed[None]).astype(F32)
        cuts = [sum(VECTORS[:i]) for i in range(len(VECTORS) + 1)]
        g1, b1, bq, bo, g2, b2, bf, bp = (packed[:, a:b].reshape(1, -1) for a, b in zip(cuts, cuts[1:]))

        x = resid_in.transpose(1, 0, 2).reshape(TOKENS, WIDTH)
        dy = grad_out.transpose(1, 0, 2).reshape(TOKENS, WIDTH)
        xim, h, qkv = qkv_call(x, g1, b1, wq, bq)
        o, r, top, inv = attn_call(qkv, xim, wo, bo)
        y, dr, dr16, dwf, dwp, dbf, small2 = mlp_call(r, dy, g2, b2, bp, wf, wp, bf)
        do, dwo = outb_call(dr16, o, wo)
        dqkv, dbq = attn_back_call(qkv, do, top, inv)
        dx, dwq, small1 = qkvb_call(xim, dr, g1, h, dqkv, wq)

        turned = dwp.reshape(PARTS, 4, 80, WIDTH).transpose(0, 2, 1, 3).reshape(WIDTH, 4 * WIDTH)
        s1 = scatter(dwf[:, :3 * WIDTH])
        s2 = scatter(jnp.concatenate([dwf[:, 3 * WIDTH:], turned[:, :2 * WIDTH]], axis=1))
        s3 = scatter(jnp.concatenate([turned[:, 2 * WIDTH:], dwo], axis=1))
        dwf = jnp.concatenate([s1, s2[:, :WIDTH]], axis=1)
        dwp = jnp.concatenate([s2[:, WIDTH:], s3[:, :2 * WIDTH]], axis=1).reshape(80, 4, WIDTH).transpose(1, 0, 2).reshape(320, WIDTH)
        dwo = s3[:, 2 * WIDTH:]
        dwq = scatter(dwq)
        rows = lambda a, i: jnp.sum(a[8 * i:8 * i + 8], axis=0)
        vectors = (rows(small1, 0), rows(small1, 1), dbq[0], rows(small2, 3), rows(small2, 0), rows(small2, 1), dbf[0], rows(small2, 2))
        packed = jnp.concatenate([v.reshape(PARTS, -1) for v in vectors], axis=1)
        packed = scatter(packed)[0]
        dg1, db1, dbq, dbo, dg2, db2, dbf, dbp = (packed[a:b] for a, b in zip(cuts, cuts[1:]))
        unturn = lambda t: t.reshape(SEQ, IMAGES, WIDTH).transpose(1, 0, 2)
        return (unturn(y), unturn(dx), dg1, db1, dwq, dbq, dwo, dbo, dg2, db2, dwf, dbf, dwp, dbp)

    return jax.shard_map(device_step, mesh=mesh, in_specs=specs, out_specs=specs, check_vma=False)
```

```python
import itertools
import math
import jax, jax.numpy as jnp
from jax import lax
from jax.experimental import pallas as pl
from jax.experimental.pallas import tpu as pltpu
from jax.sharding import PartitionSpec as P

BF, F32 = jnp.bfloat16, jnp.float32
IMAGES, SEQ, WIDTH, FFN, HEADS, HEAD = 8, 257, 1280, 5120, 16, 80
MAIN = SEQ - 1
TOKENS = IMAGES * SEQ
TAIL = IMAGES * MAIN
LN_EPS = 1e-5
VMEM_MAX = 67043328
LANES = WIDTH // 128
ROWS = 32


def dot(a, b):
    return jnp.dot(a, b, preferred_element_type=F32)


def dot_nt(a, b):
    return lax.dot_general(a, b, (((1,), (1,)), ((), ())), preferred_element_type=F32)


def dot_tn(a, b):
    return lax.dot_general(a, b, (((0,), (0,)), ((), ())), preferred_element_type=F32)


def col_sum(v):
    return jnp.sum(v, axis=0, keepdims=True)


def col_max(v):
    return jnp.max(v, axis=0, keepdims=True)


def row_sum(v):
    return jnp.sum(v, axis=-1, keepdims=True)


def eights(v):
    return jnp.sum(v.reshape(v.shape[0] // 8, 8, v.shape[1]), axis=0)


def whole(*shape, **kw):
    return pl.BlockSpec(shape, lambda *i: (0,) * len(shape), **kw)


def by_cols(rows, cols, at=lambda i: i):
    return pl.BlockSpec((rows, cols), lambda i: (0, at(i)))


def by_rows(rows, cols, at=lambda i: i):
    return pl.BlockSpec((rows, cols), lambda i: (at(i), 0))


def steps(first, wide):
    return slice(first * wide, (first + 1) * wide)


def norm_stats(values):
    mean = row_sum(values) * (1.0 / WIDTH)
    centered = values - mean
    inv = lax.rsqrt(row_sum(centered * centered) * (1.0 / WIDTH) + LN_EPS)
    return centered * inv, inv


def row_tiles(body, step=128):
    def loop(i, carry):
        body(pl.multiple_of(i * step, step), step)
        return carry
    lax.fori_loop(0, TAIL // step, loop, 0)
    body(TAIL, IMAGES)


def to_image_order(wide, place, step=128):
    per = MAIN // step
    def loop(i, carry):
        first = (i % per) * (step * IMAGES) + i // per
        rows = [wide[c, pl.ds(first, step, stride=IMAGES), :] for c in range(LANES)]
        place(pl.multiple_of(i * step, step), step, jnp.concatenate(rows, axis=1))
        return carry
    lax.fori_loop(0, IMAGES * per, loop, 0)
    place(TAIL, IMAGES, joined(wide, TAIL, IMAGES))


def from_image_order(values, wide):
    def loop(i, carry):
        rows = values[pl.ds(pl.multiple_of(i * 128, 128), 128), :]
        for c in range(LANES):
            wide[c, pl.ds((i % 2) * (128 * IMAGES) + i // 2, 128, stride=IMAGES), :] = rows[:, steps(c, 128)]
        return carry
    lax.fori_loop(0, 2 * IMAGES, loop, 0)
    put(wide, TAIL, IMAGES, values[pl.ds(TAIL, IMAGES), :])


def joined(wide, r, n):
    return jnp.concatenate([wide[c, pl.ds(r, n), :] for c in range(LANES)], axis=1)


def put(wide, r, n, values):
    for c in range(LANES):
        wide[c, pl.ds(r, n), :] = values[:, steps(c, 128)]


def norm_back(dn, hat, inv, gain):
    dhat = dn * gain
    m1 = row_sum(dhat) * (1.0 / WIDTH)
    m2 = row_sum(dhat * hat) * (1.0 / WIDTH)
    return inv * (dhat - m1 - hat * m2)


SLOTS = 3
ORDERS = ((2, 1, 0), (1, 0, 2), (0, 2, 1))


class Exchange:
    def __init__(self, rows, cols, cuts, along):
        self.rows, self.cols = rows, cols
        self.blocks = (2, 2, 2, 2, rows, cols)
        self.parts = [((slice(a, b), slice(None)) if along == 0 else (slice(None), slice(a, b))) for a, b in zip(cuts, cuts[1:])]
        self.shapes = [((b - a, cols) if along == 0 else (rows, b - a)) for a, b in zip(cuts, cuts[1:])]

    def scratch(self):
        two = (2, 2, 2)
        out = [pltpu.VMEM((2, *self.blocks), F32), pltpu.VMEM((SLOTS, *two, self.rows, self.cols), F32)]
        for axes in (2, 1, 0):
            out += [pltpu.VMEM((SLOTS, *two[:axes], *shape), F32) for shape in self.shapes]
        return out + [pltpu.SemaphoreType.DMA((10, SLOTS)), pltpu.SemaphoreType.DMA((10, SLOTS))]

    COUNT = 13

    def bind(self, refs):
        self.local, self.pair = refs[0], refs[1]
        self.held = [None, refs[2:5], refs[5:8], refs[8:11]]
        self.send, self.recv = refs[11], refs[12]
        me = lax.axis_index("fsdp")
        self.core = me % 2
        self.at = (me // 8, (me // 4) % 2, (me // 2) % 2)
        self.other_core = me + 1 - 2 * self.core
        self.other = [me + step - 2 * step * place for step, place in zip((8, 4, 2), self.at)]
        return self

    def neighbours(self):
        return (self.other_core, *self.other)

    def remote(self, src, dst, sem, slot, device):
        return pltpu.make_async_remote_copy(src_ref=src, dst_ref=dst, send_sem=self.send.at[sem, slot], recv_sem=self.recv.at[sem, slot],
                                            device_id=(device,), device_id_type=pl.DeviceIdType.MESH)

    def index(self, stage, part, side, rest=None):
        order = ORDERS[part]
        left = [a for a in range(3) if a not in order[:stage - 1]]
        axis = order[stage - 1]
        where = self.at[axis] if side else 1 - self.at[axis]
        return tuple(where if a == axis else slice(None) for a in left)

    def copy(self, stage, part, c):
        slot = c % SLOTS
        if stage == 0:
            return self.remote(self.local.at[c % 2, :, :, :, 1 - self.core], self.pair.at[slot], 0, slot, self.other_core)
        source = self.pair if stage == 1 else self.held[stage - 1][part]
        tail = self.parts[part] if stage == 1 else ()
        return self.remote(source.at[(slot, *self.index(stage, part, False), *tail)], self.held[stage][part].at[slot],
                           3 * stage - 2 + part, slot, self.other[ORDERS[part][stage - 1]])

    def start(self, stage, c):
        for part in range(1 if stage == 0 else 3):
            self.copy(stage, part, c).start()

    def wait(self, stage, c):
        for part in range(1 if stage == 0 else 3):
            self.copy(stage, part, c).wait()

    def add(self, stage, c):
        slot = c % SLOTS
        if stage == 0:
            for chip in itertools.product(range(2), repeat=3):
                self.pair[(slot, *chip)] += self.local[(c % 2, *chip, self.core)]
            return
        for part in range(3):
            source = self.pair if stage == 1 else self.held[stage - 1][part]
            tail = self.parts[part] if stage == 1 else ()
            for place in itertools.product(range(2), repeat=3 - stage):
                free = iter(place)
                kept = tuple(next(free) if isinstance(i, slice) else i for i in self.index(stage, part, True))
                self.held[stage][part][(slot, *place)] += source[(slot, *kept, *tail)]

    def result(self, c, out_ref):
        for part in range(3):
            out_ref[self.parts[part]] = self.held[3][part][c % SLOTS]


def meet(exchange):
    barrier = pltpu.get_barrier_semaphore()
    for device in exchange.neighbours():
        pl.semaphore_signal(barrier, inc=1, device_id=(device,), device_id_type=pl.DeviceIdType.MESH)
    pl.semaphore_wait(barrier, 4)


def advance(exchanges, t, chunks, outs):
    for stage in (3, 2, 1, 0):
        c = t - 2 - stage

        @pl.when((c >= 0) & (c < chunks))
        def _():
            for exchange, out in zip(exchanges, outs):
                exchange.wait(stage, c)
                exchange.add(stage, c)
                if stage < 3:
                    exchange.start(stage + 1, c)
                else:
                    exchange.result(c, out)

    @pl.when((t >= 1) & (t <= chunks))
    def _():
        for exchange in exchanges:
            exchange.start(0, t - 1)


DRAIN = 5


QKV_N = 768


def qkv_kernel(x_ref, gain_ref, bias_ref, w_ref, wb_ref, xim_ref, h_ref, qkv_ref, wide):
    @pl.when(pl.program_id(0) == 0)
    def _():
        def widen(r, n):
            put(wide, r, n, x_ref[pl.ds(r, n), :].astype(F32))
        row_tiles(widen)
        gain, bias = gain_ref[...], bias_ref[...]

        def place(r, n, values):
            xim_ref[pl.ds(r, n), :] = values.astype(BF)
            hat, _ = norm_stats(values)
            h_ref[pl.ds(r, n), :] = (hat * gain + bias).astype(BF)
        to_image_order(wide, place, ROWS)
    qkv_ref[...] = (dot(h_ref[...], w_ref[...]) + wb_ref[...]).astype(BF)


def qkv_call(x, gain, bias, w, wb):
    full = whole(TOKENS, WIDTH)
    vec = whole(1, WIDTH)
    return pl.pallas_call(
        qkv_kernel,
        grid=(3 * WIDTH // QKV_N,),
        in_specs=[whole(TOKENS, WIDTH, pipeline_mode=pl.Buffered(1)), vec, vec,
                  by_cols(WIDTH, QKV_N), by_cols(1, QKV_N)],
        out_specs=[full, full, by_cols(TOKENS, QKV_N)],
        out_shape=[jax.ShapeDtypeStruct((TOKENS, WIDTH), BF), jax.ShapeDtypeStruct((TOKENS, WIDTH), BF),
                   jax.ShapeDtypeStruct((TOKENS, 3 * WIDTH), BF)],
        scratch_shapes=[pltpu.VMEM((LANES, TOKENS, 128), F32)],
        compiler_params=pltpu.CompilerParams(dimension_semantics=("arbitrary",), vmem_limit_bytes=VMEM_MAX),
        cost_estimate=pl.CostEstimate(flops=2 * TOKENS * WIDTH * 3 * WIDTH, bytes_accessed=60_000_000, transcendentals=0),
        name="qkv",
    )(x, gain, bias, w, wb)


PARTS = 16
MLP_F = 256
UNITS = MLP_F // PARTS
MLP_STEPS = FFN // MLP_F
FC_SUM = Exchange(WIDTH // PARTS, MLP_F, (0, 24, 48, 80), 0)
PROJ_SUM = Exchange(UNITS, WIDTH, (0, 512, 896, 1280), 1)
CDF_P = 0.33
CDF_C = (0.1326322871417956, 0.11939570820799192, 0.18103829560051796, -0.08904113226212501,
         0.33075919469138065, -0.22023738432274684, 0.0454530347223348)


def gelu_pair(u):
    bell = jnp.exp(u * u * -0.5)
    t = 1.0 / (1.0 + CDF_P * jnp.abs(u))
    poly = CDF_C[6]
    for c in CDF_C[5::-1]:
        poly = poly * t + c
    tail = poly * t * bell
    cdf = jnp.where(u < 0.0, tail, 1.0 - tail)
    return u * cdf, cdf + u * bell * ((2.0 * math.pi) ** -0.5)


def mlp_kernel(r_hbm, dy_hbm, gain_ref, bias_ref, pb_ref, fc_ref, proj_ref, fcb_ref,
               y_hbm, dr_hbm, dr16_hbm, dfc_ref, dproj_ref, dfcb_ref, small_ref,
               n2, dy, y_acc, dn_acc, g, du, ua, ub, da, db, sem, *comm):
    step = pl.program_id(0)
    by_row, by_col = FC_SUM.bind(comm[:Exchange.COUNT]), PROJ_SUM.bind(comm[Exchange.COUNT:])

    @pl.when(step == 0)
    def _():
        meet(by_row)
        cp = pltpu.make_async_copy(dy_hbm, n2, sem)
        cp.start()
        cp.wait()

        def widen(r, n):
            put(dn_acc, r, n, n2[pl.ds(r, n), :].astype(F32))
        row_tiles(widen)
        cp = pltpu.make_async_copy(r_hbm, n2, sem)
        cp.start()

        def place(r, n, values):
            dy[pl.ds(r, n), :] = values.astype(BF)
        to_image_order(dn_acc, place, ROWS)
        cp.wait()
        gain, bias, pb = gain_ref[...], bias_ref[...], pb_ref[...]

        def norm(r, n):
            wide_r = n2[pl.ds(r, n), :].astype(F32)
            hat, _ = norm_stats(wide_r)
            n2[pl.ds(r, n), :] = (hat * gain + bias).astype(BF)
            y_acc[pl.ds(r, n), :] = wide_r + pb
            put(dn_acc, r, n, jnp.zeros((n, WIDTH), F32))
        row_tiles(norm, ROWS)
        small_ref[...] = jnp.zeros_like(small_ref)

    advance((by_row, by_col), step, MLP_STEPS, (dfc_ref, dproj_ref))

    @pl.when(step < MLP_STEPS)
    def _():
        fcb = fcb_ref[...]
        fc, proj = fc_ref[...], proj_ref[...].reshape(MLP_F, WIDTH)
        bias_sum = jnp.zeros((8, MLP_F), F32)
        tiles = [(b * MAIN, MAIN) for b in range(IMAGES - 1)] + [((IMAGES - 1) * MAIN, MAIN + IMAGES)]
        pairs = ((ua, da), (ub, db))

        def products(k):
            r, n = tiles[k]
            u_s, d_s = pairs[k % 2]
            u_s[0:n, :] = dot(n2[r:r + n, :], fc)
            d_s[0:n, :] = dot_nt(dy[r:r + n, :], proj)

        def pointwise(k, total):
            r, n = tiles[k]
            u_s, d_s = pairs[k % 2]
            value, slope = gelu_pair(u_s[0:n, :] + fcb)
            g[r:r + n, :] = value.astype(BF)
            grad = d_s[0:n, :] * slope
            du[r:r + n, :] = grad.astype(BF)
            return total + eights(grad)

        products(0)
        for k in range(1, IMAGES):
            products(k)
            bias_sum = pointwise(k - 1, bias_sum)
        bias_sum = pointwise(IMAGES - 1, bias_sum)
        dfcb_ref[...] = col_sum(bias_sum)
        y_acc[...] += dot(g[...], proj)
        for c in range(LANES // 2):
            part = dot_nt(du[...], fc_ref[steps(c, 256), :])
            dn_acc[2 * c] += part[:, :128]
            dn_acc[2 * c + 1] += part[:, 128:]
        by_col.local[step % 2] = dot_tn(g[...], dy[...]).reshape(by_col.blocks)
        by_row.local[step % 2] = dot_tn(n2[...], du[...]).reshape(by_row.blocks)

    out_copies = [pltpu.make_async_copy(dn_acc, dr_hbm, sem), pltpu.make_async_copy(n2, dr16_hbm, sem)]
    y_copy = pltpu.make_async_copy(dy, y_hbm, sem)

    @pl.when(step == MLP_STEPS)
    def _():
        cp = pltpu.make_async_copy(r_hbm, n2, sem)
        cp.start()
        cp.wait()
        gain = gain_ref[...]

        def back(r, n):
            hat, inv = norm_stats(n2[pl.ds(r, n), :].astype(F32))
            dn = joined(dn_acc, r, n)
            wide_dy = dy[pl.ds(r, n), :].astype(F32)
            dr = wide_dy + norm_back(dn, hat, inv, gain)
            put(dn_acc, r, n, dr)
            n2[pl.ds(r, n), :] = dr.astype(BF)
            for i, v in enumerate((dn * hat, dn, wide_dy, dr)):
                small_ref[steps(i, 8), :] += eights(v)
        row_tiles(back, ROWS)
        for cp in out_copies:
            cp.start()

    @pl.when(step == MLP_STEPS + 1)
    def _():
        for cp in out_copies:
            cp.wait()
        from_image_order(y_acc, dn_acc)

    @pl.when(step == MLP_STEPS + 2)
    def _():
        def narrow(r, n):
            dy[pl.ds(r, n), :] = joined(dn_acc, r, n).astype(BF)
        row_tiles(narrow)
        y_copy.start()

    @pl.when(step == MLP_STEPS + 3)
    def _():
        y_copy.wait()


def mlp_call(r, dy, gain, bias, pb, fc, proj, fcb):
    hbm = pl.BlockSpec(memory_space=pl.ANY)
    vec = whole(1, WIDTH)
    now = lambda i: jnp.minimum(i, MLP_STEPS - 1)
    done = lambda i: jnp.maximum(i - DRAIN, 0)
    return pl.pallas_call(
        mlp_kernel,
        grid=(MLP_STEPS + DRAIN,),
        in_specs=[hbm, hbm, vec, vec, vec, by_cols(WIDTH, MLP_F, now),
                  pl.BlockSpec((PARTS, None, UNITS, WIDTH), lambda i: (0, now(i), 0, 0)),
                  by_cols(1, MLP_F, now)],
        out_specs=[hbm, hbm, hbm, by_cols(WIDTH // PARTS, MLP_F, done),
                   by_rows(UNITS, WIDTH, done),
                   by_cols(1, MLP_F, now), whole(32, WIDTH)],
        out_shape=[jax.ShapeDtypeStruct((TOKENS, WIDTH), BF), jax.ShapeDtypeStruct((LANES, TOKENS, 128), F32),
                   jax.ShapeDtypeStruct((TOKENS, WIDTH), BF), jax.ShapeDtypeStruct((WIDTH // PARTS, FFN), F32),
                   jax.ShapeDtypeStruct((FFN // PARTS, WIDTH), F32),
                   jax.ShapeDtypeStruct((1, FFN), F32), jax.ShapeDtypeStruct((32, WIDTH), F32)],
        scratch_shapes=[pltpu.VMEM((TOKENS, WIDTH), BF), pltpu.VMEM((TOKENS, WIDTH), BF),
                        pltpu.VMEM((TOKENS, WIDTH), F32), pltpu.VMEM((LANES, TOKENS, 128), F32),
                        pltpu.VMEM((TOKENS, MLP_F), BF), pltpu.VMEM((TOKENS, MLP_F), BF)]
                       + [pltpu.VMEM((MAIN + IMAGES, MLP_F), F32)] * 4 + [pltpu.SemaphoreType.DMA]
                       + FC_SUM.scratch() + PROJ_SUM.scratch(),
        compiler_params=pltpu.CompilerParams(dimension_semantics=("arbitrary",), vmem_limit_bytes=VMEM_MAX, collective_id=0,
                                             has_side_effects=True),
        cost_estimate=pl.CostEstimate(flops=12 * TOKENS * WIDTH * FFN, bytes_accessed=150_000_000, transcendentals=TOKENS * FFN),
        name="mlp",
    )(r, dy, gain, bias, pb, fc, proj.reshape(PARTS, MLP_STEPS, UNITS, WIDTH), fcb)


SCALE = HEAD ** -0.5


def window(h):
    first = min(HEAD * h // 128 * 128, WIDTH - 256)
    wide = 128 if HEAD * h + HEAD <= first + 128 else 256
    return first, wide, HEAD * h - first


def lane_mask(h):
    first, wide, off = window(h)
    lane = lax.broadcasted_iota(jnp.int32, (MAIN, wide), 1)
    return (lane >= off) & (lane < off + HEAD)


def head_rows():
    lane = lax.broadcasted_iota(jnp.int32, (HEADS, WIDTH), 1)
    row = lax.broadcasted_iota(jnp.int32, (HEADS, WIDTH), 0)
    return jnp.where((lane >= row * HEAD) & (lane < row * HEAD + HEAD), 1.0, 0.0).astype(F32)


def tail_softmax(s, s_self):
    m = jnp.maximum(jnp.max(s, axis=1, keepdims=True), s_self)
    e = jnp.exp((s - m) * SCALE)
    e_self = jnp.exp((s_self - m) * SCALE)
    inv = 1.0 / (row_sum(e) + e_self)
    return e * inv, e_self * inv


def attn_kernel(qkv_ref, qkvt_ref, x_ref, xt_ref, w_ref, wb_ref, o_hbm, r_hbm, max_ref, inv_ref,
                tails, o_tail, o_t, ptail, o_buf, r_buf, sems):
    b, last = pl.program_id(0), pl.num_programs(0) - 1
    slot = b % 2

    @pl.when(b == 0)
    def _():
        tails[...] = qkvt_ref[...].astype(F32)

    heads = head_rows()
    q_t, k_t, v_t = (heads * tails[pl.ds(b, 1), steps(i, WIDTH)] for i in range(3))
    q, k, v = (qkv_ref[:, steps(i, WIDTH)] for i in range(3))

    p, p_self = tail_softmax(dot_nt(q_t.astype(BF), k), row_sum(q_t * k_t))
    mixed = dot(p.astype(BF), v) * heads + p_self.astype(BF).astype(F32) * v_t
    o_tail[pl.ds(b, 1), :] = col_sum(mixed)

    s_tail = dot_nt(k_t.astype(BF), q)
    v_turned = v.T
    for h in range(HEADS):
        first, wide, _ = window(h)
        q_h = jnp.where(lane_mask(h), qkv_ref[:, first:first + wide], jnp.zeros((), BF))
        s = dot_nt(qkv_ref[:, WIDTH + first:WIDTH + first + wide], q_h)
        top = jnp.maximum(col_max(s), s_tail[h:h + 1, :])
        e = jnp.exp((s - top) * SCALE)
        e_tail = jnp.exp((s_tail[h:h + 1, :] - top) * SCALE)
        inv = 1.0 / (col_sum(e) + e_tail)
        max_ref[0, h:h + 1, :] = top
        inv_ref[0, h:h + 1, :] = inv
        ptail[h:h + 1, :] = e_tail * inv
        o_t[steps(h, HEAD), :] = dot(v_turned[steps(h, HEAD), :], (e * inv).astype(BF))

    @pl.when(b >= 2)
    def _():
        out_copy(o_buf, o_hbm, slot, b - 2, sems, 0).wait()
        out_copy(r_buf, r_hbm, slot, b - 2, sems, 1).wait()

    o = (o_t[...].T + dot_tn(ptail[...].astype(BF), v_t.astype(BF))).astype(BF)
    o_buf[slot] = o
    r_buf[slot] = (x_ref[...].astype(F32) + dot(o, w_ref[...]) + wb_ref[...]).astype(BF)
    out_copy(o_buf, o_hbm, slot, b, sems, 0).start()
    out_copy(r_buf, r_hbm, slot, b, sems, 1).start()

    @pl.when(b == last)
    def _():
        for buf, hbm, n in ((o_buf, o_hbm, 0), (r_buf, r_hbm, 1)):
            out_copy(buf, hbm, 1 - slot, b - 1, sems, n).wait()
        o = o_tail[...].astype(BF)
        o_buf[1 - slot, 0:IMAGES, :] = o
        r_buf[1 - slot, 0:IMAGES, :] = (xt_ref[...].astype(F32) + dot(o, w_ref[...]) + wb_ref[...]).astype(BF)
        copies = [pltpu.make_async_copy(buf.at[1 - slot, pl.ds(0, IMAGES)], hbm.at[pl.ds(TAIL, IMAGES)], sems.at[n, 1 - slot])
                  for buf, hbm, n in ((o_buf, o_hbm, 0), (r_buf, r_hbm, 1))]
        for cp in copies:
            cp.start()
        for cp in copies:
            cp.wait()
        for buf, hbm, n in ((o_buf, o_hbm, 0), (r_buf, r_hbm, 1)):
            out_copy(buf, hbm, slot, b, sems, n).wait()


def out_copy(buf, hbm, slot, b, sems, n):
    return pltpu.make_async_copy(buf.at[slot], hbm.at[pl.ds(pl.multiple_of(b * MAIN, MAIN), MAIN)], sems.at[n, slot])


def attn_call(qkv, xim, w, wb):
    hbm = pl.BlockSpec(memory_space=pl.ANY)
    main = lambda n: by_rows(MAIN, n)
    tail = lambda n: by_rows(IMAGES, n, lambda i: TAIL // IMAGES)
    stat = pl.BlockSpec((1, HEADS, MAIN), lambda i: (i, 0, 0))
    return pl.pallas_call(
        attn_kernel,
        grid=(IMAGES,),
        in_specs=[main(3 * WIDTH), tail(3 * WIDTH), main(WIDTH), tail(WIDTH),
                  whole(WIDTH, WIDTH), whole(1, WIDTH)],
        out_specs=[hbm, hbm, stat, stat],
        out_shape=[jax.ShapeDtypeStruct((TOKENS, WIDTH), BF), jax.ShapeDtypeStruct((TOKENS, WIDTH), BF),
                   jax.ShapeDtypeStruct((IMAGES, HEADS, MAIN), F32), jax.ShapeDtypeStruct((IMAGES, HEADS, MAIN), F32)],
        scratch_shapes=[pltpu.VMEM((IMAGES, 3 * WIDTH), F32), pltpu.VMEM((IMAGES, WIDTH), F32),
                        pltpu.VMEM((WIDTH, MAIN), F32), pltpu.VMEM((HEADS, MAIN), F32),
                        pltpu.VMEM((2, MAIN, WIDTH), BF), pltpu.VMEM((2, MAIN, WIDTH), BF), pltpu.SemaphoreType.DMA((2, 2))],
        compiler_params=pltpu.CompilerParams(dimension_semantics=("arbitrary",), vmem_limit_bytes=VMEM_MAX),
        cost_estimate=pl.CostEstimate(flops=30_000_000_000, bytes_accessed=50_000_000, transcendentals=8_400_000),
        name="attn",
    )(qkv, qkv, xim, xim, w, wb)


def outb_kernel(dr_ref, o_ref, w_ref, do_ref, dw_ref):
    n = 256
    c = pl.program_id(0)
    do_ref[...] = dot_nt(dr_ref[...], w_ref[...]).astype(BF)
    dw_ref[...] = dot_tn(o_ref[...], dr_ref[:, pl.ds(pl.multiple_of(c * n, n), n)])


def outb_call(dr, o, w):
    n = 256
    full = whole(TOKENS, WIDTH)
    return pl.pallas_call(
        outb_kernel,
        grid=(WIDTH // n,),
        in_specs=[full, full, by_rows(n, WIDTH)],
        out_specs=[by_cols(TOKENS, n), by_cols(WIDTH, n)],
        out_shape=[jax.ShapeDtypeStruct((TOKENS, WIDTH), BF), jax.ShapeDtypeStruct((WIDTH, WIDTH), F32)],
        compiler_params=pltpu.CompilerParams(dimension_semantics=("arbitrary",), vmem_limit_bytes=VMEM_MAX),
        cost_estimate=pl.CostEstimate(flops=4 * TOKENS * WIDTH * WIDTH, bytes_accessed=30_000_000, transcendentals=0),
        name="outb",
    )(dr, o, w)


def attn_back_kernel(qkv_ref, qkvt_ref, do_ref, dot_ref, max_ref, inv_ref, dqkv_hbm, dwb_ref,
                     tails, do_tails, grad_tails, dq_t, dk, dv, ds_tail, buf, sems):
    b, last = pl.program_id(0), pl.num_programs(0) - 1
    slot = b % 2

    @pl.when(b == 0)
    def _():
        tails[...] = qkvt_ref[...].astype(F32)
        do_tails[...] = dot_ref[...].astype(F32)
        dwb_ref[...] = jnp.zeros_like(dwb_ref)

    heads = head_rows()
    q_t, k_t, v_t = (heads * tails[pl.ds(b, 1), steps(i, WIDTH)] for i in range(3))
    do_t = heads * do_tails[pl.ds(b, 1), :]
    q, k, v = (qkv_ref[:, steps(i, WIDTH)] for i in range(3))
    do = do_ref[...]
    q_t16, k_t16, v_t16, do_t16 = (z.astype(BF) for z in (q_t, k_t, v_t, do_t))

    p, p_self = tail_softmax(dot_nt(q_t16, k), row_sum(q_t * k_t))
    dp, dp_self = dot_nt(do_t16, v), row_sum(do_t * v_t)
    inner = row_sum(p * dp) + p_self * dp_self
    ds16 = (p * (dp - inner) * SCALE).astype(BF)
    ds_self = (p_self * (dp_self - inner) * SCALE).astype(BF).astype(F32)
    grad_q = col_sum(dot(ds16, k) * heads + ds_self * k_t)
    grad_k = ds_self * q_t
    grad_v = p_self.astype(BF).astype(F32) * do_t
    dk[...] = dot_tn(ds16, q_t16)
    dv[...] = dot_tn(p.astype(BF), do_t16)

    p_tail = jnp.exp((dot_nt(k_t16, q) - max_ref[0]) * SCALE) * inv_ref[0]
    dp_tail = dot_nt(v_t16, do)
    inner_tail = p_tail * dp_tail

    k_turned = k.T
    for h in range(HEADS):
        first, wide, _ = window(h)
        here = slice(first, first + wide)
        mask = lane_mask(h)
        q_h = jnp.where(mask, qkv_ref[:, here], jnp.zeros((), BF))
        do_h = jnp.where(mask, do_ref[:, here], jnp.zeros((), BF))
        s = dot_nt(qkv_ref[:, WIDTH + first:WIDTH + first + wide], q_h)
        dp = dot_nt(qkv_ref[:, 2 * WIDTH + first:2 * WIDTH + first + wide], do_h)
        p = jnp.exp((s - max_ref[0, h:h + 1, :]) * SCALE) * inv_ref[0, h:h + 1, :]
        inner = col_sum(p * dp) + inner_tail[h:h + 1, :]
        ds = (p * (dp - inner) * SCALE).astype(BF)
        dv[:, here] += dot(p.astype(BF), do_h)
        dk[:, here] += dot(ds, q_h)
        dq_t[steps(h, HEAD), :] = dot(k_turned[steps(h, HEAD), :], ds)
        ds_tail[h:h + 1, :] = p_tail[h:h + 1, :] * (dp_tail[h:h + 1, :] - inner) * SCALE

    ds_tail16 = ds_tail[...].astype(BF)
    grad_k = col_sum(grad_k + dot(ds_tail16, q) * heads)
    grad_v = col_sum(grad_v + dot(p_tail.astype(BF), do) * heads)

    @pl.when(b >= 2)
    def _():
        out_copy(buf, dqkv_hbm, slot, b - 2, sems, 0).wait()

    grad = dq_t[...].T + dot_tn(ds_tail16, k_t16)
    for n, (main, tail) in enumerate(((grad, grad_q), (dk[...], grad_k), (dv[...], grad_v))):
        here = steps(n, WIDTH)
        buf[slot, :, here] = main.astype(BF)
        grad_tails[pl.ds(b, 1), here] = tail
        dwb_ref[:, here] += col_sum(main) + tail
    out_copy(buf, dqkv_hbm, slot, b, sems, 0).start()

    @pl.when(b == last)
    def _():
        out_copy(buf, dqkv_hbm, 1 - slot, b - 1, sems, 0).wait()
        buf[1 - slot, 0:IMAGES, :] = grad_tails[...].astype(BF)
        cp = pltpu.make_async_copy(buf.at[1 - slot, pl.ds(0, IMAGES)], dqkv_hbm.at[pl.ds(TAIL, IMAGES)], sems.at[0, 1 - slot])
        cp.start()
        cp.wait()
        out_copy(buf, dqkv_hbm, slot, b, sems, 0).wait()


def attn_back_call(qkv, do, top, inv):
    hbm = pl.BlockSpec(memory_space=pl.ANY)
    main = lambda n: by_rows(MAIN, n)
    tail = lambda n: by_rows(IMAGES, n, lambda i: TAIL // IMAGES)
    stat = pl.BlockSpec((1, HEADS, MAIN), lambda i: (i, 0, 0))
    return pl.pallas_call(
        attn_back_kernel,
        grid=(IMAGES,),
        in_specs=[main(3 * WIDTH), tail(3 * WIDTH), main(WIDTH), tail(WIDTH), stat, stat],
        out_specs=[hbm, whole(1, 3 * WIDTH)],
        out_shape=[jax.ShapeDtypeStruct((TOKENS, 3 * WIDTH), BF), jax.ShapeDtypeStruct((1, 3 * WIDTH), F32)],
        scratch_shapes=[pltpu.VMEM((IMAGES, 3 * WIDTH), F32), pltpu.VMEM((IMAGES, WIDTH), F32),
                        pltpu.VMEM((IMAGES, 3 * WIDTH), F32), pltpu.VMEM((WIDTH, MAIN), F32),
                        pltpu.VMEM((MAIN, WIDTH), F32), pltpu.VMEM((MAIN, WIDTH), F32), pltpu.VMEM((HEADS, MAIN), F32),
                        pltpu.VMEM((2, MAIN, 3 * WIDTH), BF), pltpu.SemaphoreType.DMA((1, 2))],
        compiler_params=pltpu.CompilerParams(dimension_semantics=("arbitrary",), vmem_limit_bytes=VMEM_MAX),
        cost_estimate=pl.CostEstimate(flops=60_000_000_000, bytes_accessed=50_000_000, transcendentals=8_400_000),
        name="attn_back",
    )(qkv, qkv, do, do, top, inv)


def qkvb_kernel(xim_hbm, dr_hbm, gain_ref, h_ref, dqkv_ref, w_ref, dx_hbm, dw_ref, small_ref, acc, dr, xd, sems):
    c, last = pl.program_id(0), pl.num_programs(0) - 1
    loads = [pltpu.make_async_copy(dr_hbm, dr, sems.at[0]), pltpu.make_async_copy(xim_hbm, xd, sems.at[1])]

    @pl.when(c == 0)
    def _():
        for cp in loads:
            cp.start()
        acc[...] = jnp.zeros_like(acc)
    acc[...] += dot_nt(dqkv_ref[...], w_ref[...])
    dw_ref[...] = dot_tn(h_ref[...], dqkv_ref[...])

    @pl.when(c == last)
    def _():
        for cp in loads:
            cp.wait()
        gain = gain_ref[...]
        small_ref[...] = jnp.zeros_like(small_ref)

        def back(r, n):
            hat, inv = norm_stats(xd[pl.ds(r, n), :].astype(F32))
            dn = acc[pl.ds(r, n), :]
            for i, v in enumerate((dn * hat, dn)):
                small_ref[steps(i, 8), :] += eights(v)
            acc[pl.ds(r, n), :] = joined(dr, r, n) + norm_back(dn, hat, inv, gain)
        row_tiles(back, ROWS)
        from_image_order(acc, dr)

        def narrow(r, n):
            xd[pl.ds(r, n), :] = joined(dr, r, n).astype(BF)
        row_tiles(narrow)
        cp = pltpu.make_async_copy(xd, dx_hbm, sems.at[1])
        cp.start()
        cp.wait()


def qkvb_call(xim, dr, gain, h, dqkv, w):
    hbm = pl.BlockSpec(memory_space=pl.ANY)
    return pl.pallas_call(
        qkvb_kernel,
        grid=(3 * WIDTH // QKV_N,),
        in_specs=[hbm, hbm, whole(1, WIDTH),
                  whole(TOKENS, WIDTH, pipeline_mode=pl.Buffered(1)),
                  by_cols(TOKENS, QKV_N), by_cols(WIDTH, QKV_N)],
        out_specs=[hbm, by_cols(WIDTH, QKV_N), whole(16, WIDTH)],
        out_shape=[jax.ShapeDtypeStruct((TOKENS, WIDTH), BF), jax.ShapeDtypeStruct((WIDTH, 3 * WIDTH), F32),
                   jax.ShapeDtypeStruct((16, WIDTH), F32)],
        scratch_shapes=[pltpu.VMEM((TOKENS, WIDTH), F32), pltpu.VMEM((LANES, TOKENS, 128), F32), pltpu.VMEM((TOKENS, WIDTH), BF),
                        pltpu.SemaphoreType.DMA((2,))],
        compiler_params=pltpu.CompilerParams(dimension_semantics=("arbitrary",), vmem_limit_bytes=VMEM_MAX),
        cost_estimate=pl.CostEstimate(flops=4 * TOKENS * WIDTH * 3 * WIDTH, bytes_accessed=80_000_000, transcendentals=0),
        name="qkvb",
    )(xim, dr, gain, h, dqkv, w)


VECTORS = (80, 80, 240, 80, 80, 80, 320, 80)


def to_steps(v):
    rows = v.shape[0]
    return v.reshape(rows, PARTS, MLP_STEPS, UNITS).swapaxes(1, 2).reshape(rows, FFN)


def from_steps(v):
    rows = v.shape[0]
    return v.reshape(rows, MLP_STEPS, PARTS, UNITS).swapaxes(1, 2).reshape(rows, FFN)


def solution(mesh):
    specs = (P("fsdp"),) * 14

    def gather(shard):
        return lax.all_gather(shard.astype(BF), "fsdp", axis=0, tiled=True)

    def scatter(grad):
        return lax.psum_scatter(grad, "fsdp", scatter_dimension=0, tiled=True)

    def device_step(resid_in, grad_out, ln1_gain, ln1_bias, qkv_weight, qkv_bias, out_weight, out_bias,
                    ln2_gain, ln2_bias, fc_weight, fc_bias, proj_weight, proj_bias):
        wq, wo, wf, wp = (gather(w) for w in (qkv_weight, out_weight, to_steps(fc_weight.astype(BF)), proj_weight))
        packed = jnp.concatenate([ln1_gain, ln1_bias, qkv_bias, out_bias, ln2_gain, ln2_bias, fc_bias, proj_bias])
        packed = gather(packed[None]).astype(F32)
        cuts = [sum(VECTORS[:i]) for i in range(len(VECTORS) + 1)]
        g1, b1, bq, bo, g2, b2, bf, bp = (packed[:, a:b].reshape(1, -1) for a, b in zip(cuts, cuts[1:]))

        x = resid_in.transpose(1, 0, 2).reshape(TOKENS, WIDTH)
        dy = grad_out.transpose(1, 0, 2).reshape(TOKENS, WIDTH)
        xim, h, qkv = qkv_call(x, g1, b1, wq, bq)
        o, r, top, inv = attn_call(qkv, xim, wo, bo)
        y, dr, dr16, dwf, dwp, dbf, small2 = mlp_call(r, dy, g2, b2, bp, wf, wp, to_steps(bf))
        do, dwo = outb_call(dr16, o, wo)
        dqkv, dbq = attn_back_call(qkv, do, top, inv)
        dx, dwq, small1 = qkvb_call(xim, dr, g1, h, dqkv, wq)

        dwf, dbf = from_steps(dwf), from_steps(dbf)
        dwo = scatter(dwo)
        dwq = scatter(dwq)
        fold = lambda a: list(jnp.sum(a.reshape(-1, 8, WIDTH), axis=1))
        small1 = fold(small1)
        *ln2_sums, proj_bias_sum, out_bias_sum = fold(small2)
        vectors = (*small1, dbq, out_bias_sum, *ln2_sums, dbf, proj_bias_sum)
        packed = jnp.concatenate([v.reshape(PARTS, -1) for v in vectors], axis=1)
        packed = scatter(packed)[0]
        dg1, db1, dbq, dbo, dg2, db2, dbf, dbp = (packed[a:b] for a, b in zip(cuts, cuts[1:]))
        unturn = lambda t: t.reshape(SEQ, IMAGES, WIDTH).transpose(1, 0, 2)
        return (unturn(y), unturn(dx), dg1, db1, dwq, dbq, dwo, dbo, dg2, db2, dwf, dbf, dwp, dbp)

    return jax.shard_map(device_step, mesh=mesh, in_specs=specs, out_specs=specs, check_vma=False)
```

```python
import itertools
import math
import jax, jax.numpy as jnp
from jax import lax
from jax.experimental import pallas as pl
from jax.experimental.pallas import tpu as pltpu
from jax.sharding import PartitionSpec as P

BF, F32 = jnp.bfloat16, jnp.float32
IMAGES, SEQ, WIDTH, FFN, HEADS, HEAD = 8, 257, 1280, 5120, 16, 80
MAIN = SEQ - 1
TOKENS = IMAGES * SEQ
TAIL = IMAGES * MAIN
LN_EPS = 1e-5
VMEM_MAX = 67043328
LANE, SUBLANE, QUAD, QKV = 128, 8, 4, 3 * WIDTH
LANES = WIDTH // LANE
ROWS = 32


def dot(a, b):
    return jnp.dot(a, b, preferred_element_type=F32)


def dot_nt(a, b):
    return lax.dot_general(a, b, (((1,), (1,)), ((), ())), preferred_element_type=F32)


def dot_tn(a, b):
    return lax.dot_general(a, b, (((0,), (0,)), ((), ())), preferred_element_type=F32)


def col_sum(v):
    return jnp.sum(v, axis=0, keepdims=True)


def col_max(v):
    return jnp.max(v, axis=0, keepdims=True)


def row_sum(v):
    return jnp.sum(v, axis=-1, keepdims=True)


def row_mean(v):
    return row_sum(v) * (1.0 / WIDTH)


def clear(*refs):
    for ref in refs:
        ref[...] = jnp.zeros_like(ref)


def step_id():
    return pl.program_id(0)


def cost(flops, bytes_accessed, transcendentals=0):
    return pl.CostEstimate(flops=flops, bytes_accessed=bytes_accessed, transcendentals=transcendentals)


def eights(v):
    return jnp.sum(v.reshape(v.shape[0] // SUBLANE, SUBLANE, v.shape[1]), axis=0)


def whole(*shape, **kw):
    return pl.BlockSpec(shape, lambda *i: (0,) * len(shape), **kw)


def by_cols(rows, cols, at=lambda i: i):
    return pl.BlockSpec((rows, cols), lambda i: (0, at(i)))


def by_rows(rows, cols, at=lambda i: i):
    return pl.BlockSpec((rows, cols), lambda i: (at(i), 0))


def steps(first, wide):
    return slice(first * wide, (first + 1) * wide)


def norm_stats(values):
    mean = row_mean(values)
    centered = values - mean
    inv = lax.rsqrt(row_mean(centered * centered) + LN_EPS)
    return centered * inv, inv


def row_tiles(body, step=LANE):
    def loop(i, carry):
        body(pl.multiple_of(i * step, step), step)
        return carry
    lax.fori_loop(0, TAIL // step, loop, 0)
    body(TAIL, IMAGES)


def to_image_order(wide, place, step=LANE):
    per = MAIN // step
    def loop(i, carry):
        first = (i % per) * (step * IMAGES) + i // per
        rows = [wide[c, pl.ds(first, step, stride=IMAGES), :] for c in range(LANES)]
        place(pl.multiple_of(i * step, step), step, jnp.concatenate(rows, axis=1))
        return carry
    lax.fori_loop(0, IMAGES * per, loop, 0)
    place(TAIL, IMAGES, joined(wide, TAIL, IMAGES))


def from_image_order(values, wide):
    def loop(i, carry):
        rows = values[pl.ds(pl.multiple_of(i * LANE, LANE), LANE), :]
        for c in range(LANES):
            wide[c, pl.ds((i % 2) * (LANE * IMAGES) + i // 2, LANE, stride=IMAGES), :] = rows[:, steps(c, LANE)]
        return carry
    lax.fori_loop(0, 2 * IMAGES, loop, 0)
    put(wide, TAIL, IMAGES, values[pl.ds(TAIL, IMAGES), :])


def joined(wide, r, n):
    return jnp.concatenate([wide[c, pl.ds(r, n), :] for c in range(LANES)], axis=1)


def put(wide, r, n, values):
    for c in range(LANES):
        wide[c, pl.ds(r, n), :] = values[:, steps(c, LANE)]


def norm_back(dn, hat, inv, gain):
    dhat = dn * gain
    m1 = row_mean(dhat)
    m2 = row_mean(dhat * hat)
    return inv * (dhat - m1 - hat * m2)


ORDERS = ((2, 1, 0), (1, 0, 2), (0, 2, 1))


class Links:
    def find(self, send, recv):
        self.send, self.recv = send, recv
        me = lax.axis_index("fsdp")
        self.core = me % 2
        self.at = (me // SUBLANE, (me // QUAD) % 2, (me // 2) % 2)
        self.other_core = me + 1 - 2 * self.core
        self.other = [me + step - 2 * step * place for step, place in zip((SUBLANE, QUAD, 2), self.at)]
        return self

    def meet(self):
        barrier = pltpu.get_barrier_semaphore()
        devices = (self.other_core, *self.other)
        for device in devices:
            pl.semaphore_signal(barrier, inc=1, device_id=(device,), device_id_type=pl.DeviceIdType.MESH)
        pl.semaphore_wait(barrier, len(devices))

    def remote(self, src, dst, sem, device):
        return pltpu.make_async_remote_copy(src_ref=src, dst_ref=dst, send_sem=self.send.at[sem], recv_sem=self.recv.at[sem],
                                            device_id=(device,), device_id_type=pl.DeviceIdType.MESH)


class Gather(Links):
    COUNT = 2

    def __init__(self, rows, cols, cuts):
        self.rows, self.cols, self.cuts = rows, cols, cuts
        self.full_shape = jax.ShapeDtypeStruct((2, 2, 2, 2, rows, cols), BF)

    def scratch(self):
        return [pltpu.SemaphoreType.DMA((SEMS,))] * self.COUNT

    def bind(self, own, full, sems):
        self.own, self.full = own, full
        return self.find(*sems)

    def region(self, part, known, arrived=False):
        done = ORDERS[part][:known]
        place = [slice(None) if a in done else self.at[a] for a in range(3)]
        if arrived:
            place[done[-1]] = 1 - self.at[done[-1]]
        return (*place, self.core, slice(None), pl.ds(self.cuts[part], self.cuts[part + 1] - self.cuts[part]))

    def hop(self, stage, part):
        where = self.full.at[self.region(part, stage - 1)]
        source = self.own.at[self.region(part, 0)[-2:]] if stage == 1 else where
        return self.remote(source, where, QUAD * stage + part, self.other[ORDERS[part][stage - 1]])

    def forward(self, stage, part):
        if stage == 0:
            return self.remote(self.own, self.full.at[(*self.at, self.core)], 0, self.other_core)
        where = self.full.at[self.region(part, stage, True)]
        return self.remote(where, where, QUAD * (stage + 3) + part, self.other_core)

    def keep(self):
        return pltpu.make_async_copy(self.own, self.full.at[(*self.at, self.core)], self.send.at[1])

    def begin(self):
        for part in range(3):
            self.hop(1, part).start()
        self.forward(0, 0).start()
        self.keep().start()

    def turn(self, stage):
        if stage == 1:
            self.keep().wait()
        for part in range(3):
            self.hop(stage, part).wait()
            if stage < 3:
                self.hop(stage + 1, part).start()
        for part in range(3):
            self.forward(stage, part).start()

    def end(self):
        self.forward(0, 0).wait()
        for stage in range(1, QUAD):
            for part in range(3):
                self.forward(stage, part).wait()


SEMS = 28


class Exchange(Links):
    def __init__(self, rows, cols, cuts, along, stride=1, spare=0):
        self.rows, self.cols, self.stride = rows, cols, stride
        self.slots, self.locals = 3 * stride + spare, 1 + stride
        self.blocks = (2, 2, 2, 2, rows, cols)
        self.parts = [((slice(a, b), slice(None)) if along == 0 else (slice(None), slice(a, b))) for a, b in zip(cuts, cuts[1:])]
        self.shapes = [((b - a, cols) if along == 0 else (rows, b - a)) for a, b in zip(cuts, cuts[1:])]

    def scratch(self):
        two = (2, 2, 2)
        out = [pltpu.VMEM((self.locals, *self.blocks), F32), pltpu.VMEM((self.slots, *two, self.rows, self.cols), F32)]
        for axes in (2, 1, 0):
            out += [pltpu.VMEM((self.slots, *two[:axes], *shape), F32) for shape in self.shapes]
        return out + [pltpu.SemaphoreType.DMA((10, self.slots))] * 2

    COUNT = 13

    def bind(self, refs):
        self.local, self.pair = refs[0], refs[1]
        self.held = [None, refs[2:5], refs[5:SUBLANE], refs[SUBLANE:11]]
        return self.find(*refs[11:])

    def index(self, stage, part, side):
        order = ORDERS[part]
        left = [a for a in range(3) if a not in order[:stage - 1]]
        axis = order[stage - 1]
        where = self.at[axis] if side else 1 - self.at[axis]
        return tuple(where if a == axis else slice(None) for a in left)

    def copy(self, stage, part, c):
        slot = c % self.slots
        if stage == 0:
            return self.remote(self.local.at[c % self.locals, :, :, :, 1 - self.core], self.pair.at[slot], (0, slot), self.other_core)
        source = self.pair if stage == 1 else self.held[stage - 1][part]
        tail = self.parts[part] if stage == 1 else ()
        return self.remote(source.at[(slot, *self.index(stage, part, False), *tail)], self.held[stage][part].at[slot],
                           (3 * stage - 2 + part, slot), self.other[ORDERS[part][stage - 1]])

    def start(self, stage, c):
        for part in range(1 if stage == 0 else 3):
            self.copy(stage, part, c).start()

    def wait(self, stage, c):
        for part in range(1 if stage == 0 else 3):
            self.copy(stage, part, c).wait()

    def add(self, stage, c):
        slot = c % self.slots
        if stage == 0:
            for chip in itertools.product(range(2), repeat=3):
                self.pair[(slot, *chip)] += self.local[(c % self.locals, *chip, self.core)]
            return
        for part in range(3):
            source = self.pair if stage == 1 else self.held[stage - 1][part]
            tail = self.parts[part] if stage == 1 else ()
            for place in itertools.product(range(2), repeat=3 - stage):
                free = iter(place)
                kept = tuple(next(free) if isinstance(i, slice) else i for i in self.index(stage, part, True))
                self.held[stage][part][(slot, *place)] += source[(slot, *kept, *tail)]

    def result(self, c, out_ref):
        for part in range(3):
            out_ref[self.parts[part]] = self.held[3][part][c % self.slots]

    def put_local(self, c, values):
        self.local[c % self.locals] = values.reshape(self.blocks)


def comm_params(n):
    return pltpu.CompilerParams(dimension_semantics=("arbitrary",), vmem_limit_bytes=VMEM_MAX, collective_id=n, has_side_effects=True)


def advance(exchanges, t, exists, emit):
    for stage in (3, 2, 1, 0):
        c = t - 1 - (stage + 1) * exchanges[0].stride

        @pl.when(exists(c))
        def _():
            for n, exchange in enumerate(exchanges):
                exchange.wait(stage, c)
                exchange.add(stage, c)
                if stage < 3:
                    exchange.start(stage + 1, c)
                else:
                    emit(n, exchange, c)

    @pl.when(exists(t - 1))
    def _():
        for exchange in exchanges:
            exchange.start(0, t - 1)


def first_chunks(n):
    return lambda c: (c >= 0) & (c < n)


DRAIN = 5


QKV_N = 768


def qkv_kernel(x_ref, gain_ref, bias_ref, w_ref, wb_ref, xim_ref, ht_ref, qkv_ref, wide, h_ref):
    @pl.when(step_id() == 0)
    def _():
        def widen(r, n):
            put(wide, r, n, x_ref[pl.ds(r, n), :].astype(F32))
        row_tiles(widen)
        gain, bias = gain_ref[...], bias_ref[...]

        def place(r, n, values):
            xim_ref[pl.ds(r, n), :] = values.astype(BF)
            hat, _ = norm_stats(values)
            h_ref[pl.ds(r, n), :] = (hat * gain + bias).astype(BF)
        to_image_order(wide, place, ROWS)
        for b in range(IMAGES):
            ht_ref[:, steps(b, MAIN)] = h_ref[steps(b, MAIN), :].T
        ht_ref[:, TAIL:TOKENS] = h_ref[TAIL:TOKENS, :].T
    qkv_ref[...] = (dot(h_ref[...], w_ref[...]) + wb_ref[...]).astype(BF)


def qkv_call(x, gain, bias, w, wb):
    full = whole(TOKENS, WIDTH)
    vec = whole(1, WIDTH)
    return pl.pallas_call(
        qkv_kernel,
        grid=(QKV // QKV_N,),
        in_specs=[whole(TOKENS, WIDTH, pipeline_mode=pl.Buffered(1)), vec, vec,
                  by_cols(WIDTH, QKV_N), by_cols(1, QKV_N)],
        out_specs=[full, whole(WIDTH, TOKENS), by_cols(TOKENS, QKV_N)],
        out_shape=[jax.ShapeDtypeStruct((TOKENS, WIDTH), BF), jax.ShapeDtypeStruct((WIDTH, TOKENS), BF),
                   jax.ShapeDtypeStruct((TOKENS, QKV), BF)],
        scratch_shapes=[pltpu.VMEM((LANES, TOKENS, LANE), F32), pltpu.VMEM((TOKENS, WIDTH), BF)],
        compiler_params=pltpu.CompilerParams(dimension_semantics=("arbitrary",), vmem_limit_bytes=VMEM_MAX),
        cost_estimate=cost(2 * TOKENS * WIDTH * QKV, 60_000_000),
        name="qkv",
    )(x, gain, bias, w, wb)


PARTS = 16
MLP_F = MAIN
UNITS = MLP_F // PARTS
MLP_STEPS = FFN // MLP_F
ROW_CUTS = (0, 24, 48, 80)
FC_SUM = Exchange(WIDTH // PARTS, MLP_F, ROW_CUTS, 0)
PROJ_SUM = Exchange(UNITS, WIDTH, (0, 512, 896, 1280), 1)
CDF_P = 0.33
CDF_C = (0.1326322871417956, 0.11939570820799192, 0.18103829560051796, -0.08904113226212501,
         0.33075919469138065, -0.22023738432274684, 0.0454530347223348)


def gelu_pair(u):
    bell = jnp.exp(u * u * -0.5)
    t = 1.0 / (1.0 + CDF_P * jnp.abs(u))
    poly = CDF_C[6]
    for c in CDF_C[5::-1]:
        poly = poly * t + c
    tail = poly * t * bell
    cdf = jnp.where(u < 0.0, tail, 1.0 - tail)
    return u * cdf, cdf + u * bell * ((2.0 * math.pi) ** -0.5)


def mlp_kernel(r_hbm, dy_hbm, gain_ref, bias_ref, pb_ref, fc_ref, proj_ref, fcb_ref,
               y_hbm, dr_hbm, dr16_hbm, dfc_ref, dproj_ref, dfcb_ref, small_ref,
               n2, dy, y_acc, dn_acc, g, du, ua, ub, da, db, sem, *comm):
    step = step_id()
    by_row, by_col = FC_SUM.bind(comm[:Exchange.COUNT]), PROJ_SUM.bind(comm[Exchange.COUNT:])

    @pl.when(step == 0)
    def _():
        by_row.meet()
        cp = pltpu.make_async_copy(dy_hbm, n2, sem)
        cp.start()
        cp.wait()

        def widen(r, n):
            put(dn_acc, r, n, n2[pl.ds(r, n), :].astype(F32))
        row_tiles(widen)
        cp = pltpu.make_async_copy(r_hbm, n2, sem)
        cp.start()

        def place(r, n, values):
            dy[pl.ds(r, n), :] = values.astype(BF)
        to_image_order(dn_acc, place, ROWS)
        cp.wait()
        gain, bias, pb = gain_ref[...], bias_ref[...], pb_ref[...]

        def norm(r, n):
            wide_r = n2[pl.ds(r, n), :].astype(F32)
            hat, _ = norm_stats(wide_r)
            n2[pl.ds(r, n), :] = (hat * gain + bias).astype(BF)
            y_acc[pl.ds(r, n), :] = wide_r + pb
            put(dn_acc, r, n, jnp.zeros((n, WIDTH), F32))
        row_tiles(norm, ROWS)
        clear(small_ref)

    outs = (dfc_ref, dproj_ref)
    advance((by_row, by_col), step, first_chunks(MLP_STEPS), lambda n, exchange, c: exchange.result(c, outs[n]))

    @pl.when(step < MLP_STEPS)
    def _():
        fcb = fcb_ref[...]
        fc, proj = fc_ref[...], proj_ref[...].reshape(MLP_F, WIDTH)
        bias_sum = jnp.zeros((SUBLANE, MLP_F), F32)
        tiles = [(b * MAIN, MAIN) for b in range(IMAGES - 1)] + [((IMAGES - 1) * MAIN, MAIN + IMAGES)]
        pairs = ((ua, da), (ub, db))

        def products(k):
            r, n = tiles[k]
            u_s, d_s = pairs[k % 2]
            u_s[0:n, :] = dot(n2[r:r + n, :], fc)
            d_s[0:n, :] = dot_nt(dy[r:r + n, :], proj)

        def pointwise(k, total):
            r, n = tiles[k]
            u_s, d_s = pairs[k % 2]
            value, slope = gelu_pair(u_s[0:n, :] + fcb)
            g[r:r + n, :] = value.astype(BF)
            grad = d_s[0:n, :] * slope
            du[r:r + n, :] = grad.astype(BF)
            return total + eights(grad)

        products(0)
        for k in range(1, IMAGES):
            products(k)
            bias_sum = pointwise(k - 1, bias_sum)
        bias_sum = pointwise(IMAGES - 1, bias_sum)
        dfcb_ref[...] = col_sum(bias_sum)
        y_acc[...] += dot(g[...], proj)
        for c in range(LANES // 2):
            part = dot_nt(du[...], fc_ref[steps(c, MAIN), :])
            dn_acc[2 * c] += part[:, :LANE]
            dn_acc[2 * c + 1] += part[:, LANE:]
        by_col.put_local(step, dot_tn(g[...], dy[...]))
        by_row.put_local(step, dot_tn(n2[...], du[...]))

    out_copies = [pltpu.make_async_copy(dn_acc, dr_hbm, sem), pltpu.make_async_copy(n2, dr16_hbm, sem)]
    y_copy = pltpu.make_async_copy(dy, y_hbm, sem)

    @pl.when(step == MLP_STEPS)
    def _():
        cp = pltpu.make_async_copy(r_hbm, n2, sem)
        cp.start()
        cp.wait()
        gain = gain_ref[...]

        def back(r, n):
            hat, inv = norm_stats(n2[pl.ds(r, n), :].astype(F32))
            dn = joined(dn_acc, r, n)
            wide_dy = dy[pl.ds(r, n), :].astype(F32)
            dr = wide_dy + norm_back(dn, hat, inv, gain)
            put(dn_acc, r, n, dr)
            n2[pl.ds(r, n), :] = dr.astype(BF)
            for i, v in enumerate((dn * hat, dn, wide_dy, dr)):
                small_ref[steps(i, SUBLANE), :] += eights(v)
        row_tiles(back, ROWS)
        for cp in out_copies:
            cp.start()

    @pl.when(step == MLP_STEPS + 1)
    def _():
        for cp in out_copies:
            cp.wait()
        from_image_order(y_acc, dn_acc)

    @pl.when(step == MLP_STEPS + 2)
    def _():
        def narrow(r, n):
            dy[pl.ds(r, n), :] = joined(dn_acc, r, n).astype(BF)
        row_tiles(narrow)
        y_copy.start()

    @pl.when(step == MLP_STEPS + 3)
    def _():
        y_copy.wait()


def mlp_call(r, dy, gain, bias, pb, fc, proj, fcb):
    hbm = pl.BlockSpec(memory_space=pl.ANY)
    vec = whole(1, WIDTH)
    now = lambda i: jnp.minimum(i, MLP_STEPS - 1)
    done = lambda i: jnp.maximum(i - DRAIN, 0)
    return pl.pallas_call(
        mlp_kernel,
        grid=(MLP_STEPS + DRAIN,),
        in_specs=[hbm, hbm, vec, vec, vec, by_cols(WIDTH, MLP_F, now),
                  pl.BlockSpec((PARTS, None, UNITS, WIDTH), lambda i: (0, now(i), 0, 0)),
                  by_cols(1, MLP_F, now)],
        out_specs=[hbm, hbm, hbm, by_cols(WIDTH // PARTS, MLP_F, done),
                   by_rows(UNITS, WIDTH, done),
                   by_cols(1, MLP_F, now), whole(32, WIDTH)],
        out_shape=[jax.ShapeDtypeStruct((TOKENS, WIDTH), BF), jax.ShapeDtypeStruct((LANES, TOKENS, LANE), F32),
                   jax.ShapeDtypeStruct((TOKENS, WIDTH), BF), jax.ShapeDtypeStruct((WIDTH // PARTS, FFN), F32),
                   jax.ShapeDtypeStruct((FFN // PARTS, WIDTH), F32),
                   jax.ShapeDtypeStruct((1, FFN), F32), jax.ShapeDtypeStruct((32, WIDTH), F32)],
        scratch_shapes=[pltpu.VMEM((TOKENS, WIDTH), BF), pltpu.VMEM((TOKENS, WIDTH), BF),
                        pltpu.VMEM((TOKENS, WIDTH), F32), pltpu.VMEM((LANES, TOKENS, LANE), F32),
                        pltpu.VMEM((TOKENS, MLP_F), BF), pltpu.VMEM((TOKENS, MLP_F), BF)]
                       + [pltpu.VMEM((MAIN + IMAGES, MLP_F), F32)] * QUAD + [pltpu.SemaphoreType.DMA]
                       + FC_SUM.scratch() + PROJ_SUM.scratch(),
        compiler_params=comm_params(0),
        cost_estimate=cost(12 * TOKENS * WIDTH * FFN, 150_000_000, TOKENS * FFN),
        name="mlp",
    )(r, dy, gain, bias, pb, fc, proj.reshape(PARTS, MLP_STEPS, UNITS, WIDTH), fcb)


SCALE = HEAD ** -0.5


def window(h):
    first = min(HEAD * h // LANE * LANE, WIDTH - MAIN)
    wide = LANE if HEAD * h + HEAD <= first + LANE else MAIN
    return first, wide, HEAD * h - first


def lane_mask(h):
    first, wide, off = window(h)
    lane = lax.broadcasted_iota(jnp.int32, (MAIN, wide), 1)
    return (lane >= off) & (lane < off + HEAD)


def thirds(ref, rows=slice(None)):
    return [ref[rows, steps(i, WIDTH)] for i in range(3)]


def head_rows():
    lane = lax.broadcasted_iota(jnp.int32, (HEADS, WIDTH), 1)
    row = lax.broadcasted_iota(jnp.int32, (HEADS, WIDTH), 0)
    return (lane // HEAD == row).astype(F32)


def tail_softmax(s, s_self):
    m = jnp.maximum(jnp.max(s, axis=1, keepdims=True), s_self)
    e = jnp.exp((s - m) * SCALE)
    e_self = jnp.exp((s_self - m) * SCALE)
    inv = 1.0 / (row_sum(e) + e_self)
    return e * inv, e_self * inv


def attn_kernel(qkv_ref, qkvt_ref, x_ref, xt_ref, w_ref, wb_ref, o_hbm, r_hbm, max_ref, inv_ref,
                tails, o_tail, o_t, ptail, o_buf, r_buf, sems):
    b, last = step_id(), pl.num_programs(0) - 1
    slot = b % 2

    @pl.when(b == 0)
    def _():
        tails[...] = qkvt_ref[...].astype(F32)

    heads = head_rows()
    q_t, k_t, v_t = (heads * z for z in thirds(tails, pl.ds(b, 1)))
    q, k, v = thirds(qkv_ref)

    p, p_self = tail_softmax(dot_nt(q_t.astype(BF), k), row_sum(q_t * k_t))
    mixed = dot(p.astype(BF), v) * heads + p_self.astype(BF).astype(F32) * v_t
    o_tail[pl.ds(b, 1), :] = col_sum(mixed)

    s_tail = dot_nt(k_t.astype(BF), q)
    v_turned = v.T
    for h in range(HEADS):
        first, wide, _ = window(h)
        q_h = jnp.where(lane_mask(h), qkv_ref[:, first:first + wide], jnp.zeros((), BF))
        s = dot_nt(qkv_ref[:, pl.ds(WIDTH + first, wide)], q_h)
        top = jnp.maximum(col_max(s), s_tail[steps(h, 1), :])
        e = jnp.exp((s - top) * SCALE)
        e_tail = jnp.exp((s_tail[steps(h, 1), :] - top) * SCALE)
        inv = 1.0 / (col_sum(e) + e_tail)
        max_ref[0, steps(h, 1), :] = top
        inv_ref[0, steps(h, 1), :] = inv
        ptail[steps(h, 1), :] = e_tail * inv
        o_t[steps(h, HEAD), :] = dot(v_turned[steps(h, HEAD), :], (e * inv).astype(BF))

    @pl.when(b >= 2)
    def _():
        out_copy(o_buf, o_hbm, slot, b - 2, sems, 0).wait()
        out_copy(r_buf, r_hbm, slot, b - 2, sems, 1).wait()

    o = (o_t[...].T + dot_tn(ptail[...].astype(BF), v_t.astype(BF))).astype(BF)
    o_buf[slot] = o
    r_buf[slot] = (x_ref[...].astype(F32) + dot(o, w_ref[...]) + wb_ref[...]).astype(BF)
    out_copy(o_buf, o_hbm, slot, b, sems, 0).start()
    out_copy(r_buf, r_hbm, slot, b, sems, 1).start()

    @pl.when(b == last)
    def _():
        for buf, hbm, n in ((o_buf, o_hbm, 0), (r_buf, r_hbm, 1)):
            out_copy(buf, hbm, 1 - slot, b - 1, sems, n).wait()
        o = o_tail[...].astype(BF)
        o_buf[1 - slot, 0:IMAGES, :] = o
        r_buf[1 - slot, 0:IMAGES, :] = (xt_ref[...].astype(F32) + dot(o, w_ref[...]) + wb_ref[...]).astype(BF)
        copies = [pltpu.make_async_copy(buf.at[1 - slot, pl.ds(0, IMAGES)], hbm.at[pl.ds(TAIL, IMAGES)], sems.at[n, 1 - slot])
                  for buf, hbm, n in ((o_buf, o_hbm, 0), (r_buf, r_hbm, 1))]
        for cp in copies:
            cp.start()
        for cp in copies:
            cp.wait()
        for buf, hbm, n in ((o_buf, o_hbm, 0), (r_buf, r_hbm, 1)):
            out_copy(buf, hbm, slot, b, sems, n).wait()


def out_copy(buf, hbm, slot, b, sems, n):
    return pltpu.make_async_copy(buf.at[slot], hbm.at[pl.ds(pl.multiple_of(b * MAIN, MAIN), MAIN)], sems.at[n, slot])


def attn_call(qkv, xim, w, wb):
    hbm = pl.BlockSpec(memory_space=pl.ANY)
    main = lambda n: by_rows(MAIN, n)
    tail = lambda n: by_rows(IMAGES, n, lambda i: TAIL // IMAGES)
    stat = pl.BlockSpec((1, HEADS, MAIN), lambda i: (i, 0, 0))
    return pl.pallas_call(
        attn_kernel,
        grid=(IMAGES,),
        in_specs=[main(QKV), tail(QKV), main(WIDTH), tail(WIDTH),
                  whole(WIDTH, WIDTH), whole(1, WIDTH)],
        out_specs=[hbm, hbm, stat, stat],
        out_shape=[jax.ShapeDtypeStruct((TOKENS, WIDTH), BF), jax.ShapeDtypeStruct((TOKENS, WIDTH), BF),
                   jax.ShapeDtypeStruct((IMAGES, HEADS, MAIN), F32), jax.ShapeDtypeStruct((IMAGES, HEADS, MAIN), F32)],
        scratch_shapes=[pltpu.VMEM((IMAGES, QKV), F32), pltpu.VMEM((IMAGES, WIDTH), F32),
                        pltpu.VMEM((WIDTH, MAIN), F32), pltpu.VMEM((HEADS, MAIN), F32),
                        pltpu.VMEM((2, MAIN, WIDTH), BF), pltpu.VMEM((2, MAIN, WIDTH), BF), pltpu.SemaphoreType.DMA((2, 2))],
        compiler_params=pltpu.CompilerParams(dimension_semantics=("arbitrary",), vmem_limit_bytes=VMEM_MAX),
        cost_estimate=cost(30_000_000_000, 50_000_000, 8_400_000),
        name="attn",
    )(qkv, qkv, xim, xim, w, wb)


def outb_kernel(dr_ref, o_ref, w_ref, do_ref, dw_ref):
    n = MAIN
    c = step_id()
    do_ref[...] = dot_nt(dr_ref[...], w_ref[...]).astype(BF)
    dw_ref[...] = dot_tn(o_ref[...], dr_ref[:, pl.ds(pl.multiple_of(c * n, n), n)])


def outb_call(dr, o, w):
    n = MAIN
    full = whole(TOKENS, WIDTH)
    return pl.pallas_call(
        outb_kernel,
        grid=(WIDTH // n,),
        in_specs=[full, full, by_rows(n, WIDTH)],
        out_specs=[by_cols(TOKENS, n), by_cols(WIDTH, n)],
        out_shape=[jax.ShapeDtypeStruct((TOKENS, WIDTH), BF), jax.ShapeDtypeStruct((WIDTH, WIDTH), F32)],
        compiler_params=pltpu.CompilerParams(dimension_semantics=("arbitrary",), vmem_limit_bytes=VMEM_MAX),
        cost_estimate=cost(QUAD * TOKENS * WIDTH * WIDTH, 30_000_000),
        name="outb",
    )(dr, o, w)


def attn_back_kernel(qkv_ref, qkvt_ref, do_ref, dot_ref, max_ref, inv_ref, dw_ref, dqkv_hbm, dwb_ref, dwout_ref,
                     tails, do_tails, grad_tails, dq_t, dk, dv, ds_tail, buf, sems, *comm):
    b = step_id()
    by_row = FC_SUM.bind(comm)

    @pl.when(b == 0)
    def _():
        by_row.meet()
    advance((by_row,), b, first_chunks(OUT_STEPS), lambda n, exchange, c: exchange.result(c, dwout_ref))

    @pl.when(b < OUT_STEPS)
    def _():
        by_row.put_local(b, dw_ref[...])

    @pl.when(b < IMAGES)
    def _():
        image_back(b, qkv_ref, qkvt_ref, do_ref, dot_ref, max_ref, inv_ref, dqkv_hbm, dwb_ref,
                   tails, do_tails, grad_tails, dq_t, dk, dv, ds_tail, buf, sems)


OUT_STEPS = WIDTH // MAIN


def image_back(b, qkv_ref, qkvt_ref, do_ref, dot_ref, max_ref, inv_ref, dqkv_hbm, dwb_ref,
               tails, do_tails, grad_tails, dq_t, dk, dv, ds_tail, buf, sems):
    last = IMAGES - 1
    slot = b % 2

    @pl.when(b == 0)
    def _():
        tails[...] = qkvt_ref[...].astype(F32)
        do_tails[...] = dot_ref[...].astype(F32)
        clear(dwb_ref)

    heads = head_rows()
    q_t, k_t, v_t = (heads * z for z in thirds(tails, pl.ds(b, 1)))
    do_t = heads * do_tails[pl.ds(b, 1), :]
    q, k, v = thirds(qkv_ref)
    do = do_ref[...]
    q_t16, k_t16, v_t16, do_t16 = (z.astype(BF) for z in (q_t, k_t, v_t, do_t))

    p, p_self = tail_softmax(dot_nt(q_t16, k), row_sum(q_t * k_t))
    dp, dp_self = dot_nt(do_t16, v), row_sum(do_t * v_t)
    inner = row_sum(p * dp) + p_self * dp_self
    ds16 = (p * (dp - inner) * SCALE).astype(BF)
    ds_self = (p_self * (dp_self - inner) * SCALE).astype(BF).astype(F32)
    grad_q = col_sum(dot(ds16, k) * heads + ds_self * k_t)
    grad_k = ds_self * q_t
    grad_v = p_self.astype(BF).astype(F32) * do_t
    dk[...] = dot_tn(ds16, q_t16)
    dv[...] = dot_tn(p.astype(BF), do_t16)

    p_tail = jnp.exp((dot_nt(k_t16, q) - max_ref[0]) * SCALE) * inv_ref[0]
    dp_tail = dot_nt(v_t16, do)
    inner_tail = p_tail * dp_tail

    k_turned = k.T
    for h in range(HEADS):
        first, wide, _ = window(h)
        here = slice(first, first + wide)
        mask = lane_mask(h)
        q_h = jnp.where(mask, qkv_ref[:, here], jnp.zeros((), BF))
        do_h = jnp.where(mask, do_ref[:, here], jnp.zeros((), BF))
        s = dot_nt(qkv_ref[:, pl.ds(WIDTH + first, wide)], q_h)
        dp = dot_nt(qkv_ref[:, pl.ds(2 * WIDTH + first, wide)], do_h)
        p = jnp.exp((s - max_ref[0, steps(h, 1), :]) * SCALE) * inv_ref[0, steps(h, 1), :]
        inner = col_sum(p * dp) + inner_tail[steps(h, 1), :]
        ds = (p * (dp - inner) * SCALE).astype(BF)
        dv[:, here] += dot(p.astype(BF), do_h)
        dk[:, here] += dot(ds, q_h)
        dq_t[steps(h, HEAD), :] = dot(k_turned[steps(h, HEAD), :], ds)
        ds_tail[steps(h, 1), :] = p_tail[steps(h, 1), :] * (dp_tail[steps(h, 1), :] - inner) * SCALE

    ds_tail16 = ds_tail[...].astype(BF)
    grad_k = col_sum(grad_k + dot(ds_tail16, q) * heads)
    grad_v = col_sum(grad_v + dot(p_tail.astype(BF), do) * heads)

    @pl.when(b >= 2)
    def _():
        out_copy(buf, dqkv_hbm, slot, b - 2, sems, 0).wait()

    grad = dq_t[...].T + dot_tn(ds_tail16, k_t16)
    for n, (main, tail) in enumerate(((grad, grad_q), (dk[...], grad_k), (dv[...], grad_v))):
        here = steps(n, WIDTH)
        buf[slot, :, here] = main.astype(BF)
        grad_tails[pl.ds(b, 1), here] = tail
        dwb_ref[:, here] += col_sum(main) + tail
    out_copy(buf, dqkv_hbm, slot, b, sems, 0).start()

    @pl.when(b == last)
    def _():
        out_copy(buf, dqkv_hbm, 1 - slot, b - 1, sems, 0).wait()
        buf[1 - slot, 0:IMAGES, :] = grad_tails[...].astype(BF)
        cp = pltpu.make_async_copy(buf.at[1 - slot, pl.ds(0, IMAGES)], dqkv_hbm.at[pl.ds(TAIL, IMAGES)], sems.at[0, 1 - slot])
        cp.start()
        cp.wait()
        out_copy(buf, dqkv_hbm, slot, b, sems, 0).wait()


def attn_back_call(qkv, do, top, inv, dw):
    hbm = pl.BlockSpec(memory_space=pl.ANY)
    image = lambda i: jnp.minimum(i, IMAGES - 1)
    main = lambda n: by_rows(MAIN, n, image)
    tail = lambda n: by_rows(IMAGES, n, lambda i: TAIL // IMAGES)
    stat = pl.BlockSpec((1, HEADS, MAIN), lambda i: (image(i), 0, 0))
    return pl.pallas_call(
        attn_back_kernel,
        grid=(OUT_STEPS + DRAIN,),
        in_specs=[main(QKV), tail(QKV), main(WIDTH), tail(WIDTH), stat, stat,
                  by_cols(WIDTH, MAIN, lambda i: jnp.minimum(i, OUT_STEPS - 1))],
        out_specs=[hbm, whole(1, QKV), by_cols(WIDTH // PARTS, MAIN, lambda i: jnp.maximum(i - DRAIN, 0))],
        out_shape=[jax.ShapeDtypeStruct((TOKENS, QKV), BF), jax.ShapeDtypeStruct((1, QKV), F32),
                   jax.ShapeDtypeStruct((WIDTH // PARTS, WIDTH), F32)],
        scratch_shapes=[pltpu.VMEM((IMAGES, QKV), F32), pltpu.VMEM((IMAGES, WIDTH), F32),
                        pltpu.VMEM((IMAGES, QKV), F32), pltpu.VMEM((WIDTH, MAIN), F32),
                        pltpu.VMEM((MAIN, WIDTH), F32), pltpu.VMEM((MAIN, WIDTH), F32), pltpu.VMEM((HEADS, MAIN), F32),
                        pltpu.VMEM((2, MAIN, QKV), BF), pltpu.SemaphoreType.DMA((1, 2))] + FC_SUM.scratch(),
        compiler_params=comm_params(1),
        cost_estimate=cost(60_000_000_000, 50_000_000, 8_400_000),
        name="attn_back",
    )(qkv, qkv, do, do, top, inv, dw)


QB_N = MAIN
QB_STEPS = QKV // QB_N
QKV_SUM = Exchange(WIDTH // PARTS, QB_N, ROW_CUTS, 0, 2, 1)
VECTOR_CHUNK = QB_STEPS + 2
QB_GRID = VECTOR_CHUNK + 2 + QUAD * QKV_SUM.stride
VECTOR_ROWS = 16


def qkvb_kernel(xim_hbm, dr_hbm, gain_ref, vec_ref, ht_ref, dqkv_ref, w_ref, dx_hbm, dw_ref, out_vec_ref,
                acc, dr, xd, vec, vec_out, sums, sems, *comm):
    t = step_id()
    by_row = QKV_SUM.bind(comm)
    loads = [pltpu.make_async_copy(dr_hbm, dr, sems.at[0]), pltpu.make_async_copy(xim_hbm, xd, sems.at[1])]
    store = pltpu.make_async_copy(xd, dx_hbm, sems.at[1])

    @pl.when(t == 0)
    def _():
        by_row.meet()
        for cp in loads:
            cp.start()
        clear(acc, sums, vec)
        vec[:VECTOR_ROWS, :] = vec_ref[...]

    def emit(n, exchange, c):
        @pl.when(c < QB_STEPS)
        def _():
            exchange.result(c, dw_ref)

        @pl.when(c == VECTOR_CHUNK)
        def _():
            exchange.result(c, vec_out)
            out_vec_ref[...] = vec_out[:, :LANE].T[:VECTOR_ROWS, :]
    advance((by_row,), t, lambda c: ((c >= 0) & (c < QB_STEPS)) | (c == VECTOR_CHUNK), emit)

    @pl.when(t < QB_STEPS)
    def _():
        by_row.put_local(t, dot(ht_ref[...], dqkv_ref[...]))
        acc[...] += dot_nt(dqkv_ref[...], w_ref[...])

    @pl.when(t == QB_STEPS)
    def _():
        for cp in loads:
            cp.wait()

    def back(r, n):
        hat, inv = norm_stats(xd[pl.ds(r, n), :].astype(F32))
        dn = acc[pl.ds(r, n), :]
        for i, v in enumerate((dn * hat, dn)):
            sums[steps(i, SUBLANE), :] += eights(v)
        acc[pl.ds(r, n), :] = joined(dr, r, n) + norm_back(dn, hat, inv, gain_ref[...])

    @pl.when((t >= QB_STEPS) & (t <= VECTOR_CHUNK))
    def _():
        part = (t - QB_STEPS) * BACK_TILES

        def loop(i, carry):
            @pl.when(part + i < TAIL // ROWS)
            def _():
                back(pl.multiple_of((part + i) * ROWS, ROWS), ROWS)
            return carry
        lax.fori_loop(0, BACK_TILES, loop, 0)

    @pl.when(t == VECTOR_CHUNK)
    def _():
        back(TAIL, IMAGES)
        for i in range(2):
            vec[VECTOR_ROWS - 2 + i:VECTOR_ROWS - 1 + i, :] = col_sum(sums[steps(i, SUBLANE), :])
        turned = vec[...].T
        by_row.put_local(t, jnp.concatenate([turned, jnp.zeros_like(turned)], axis=1))

    @pl.when(t == VECTOR_CHUNK + 1)
    def _():
        from_image_order(acc, dr)

    @pl.when(t == VECTOR_CHUNK + 2)
    def _():
        def narrow(r, n):
            xd[pl.ds(r, n), :] = joined(dr, r, n).astype(BF)
        row_tiles(narrow)
        store.start()

    @pl.when(t == QB_GRID - 1)
    def _():
        store.wait()


BACK_TILES = -(-TAIL // ROWS // 3)


def qkvb_call(xim, dr, gain, vec, ht, dqkv, w):
    hbm = pl.BlockSpec(memory_space=pl.ANY)
    now = lambda i: jnp.minimum(i, QB_STEPS - 1)
    return pl.pallas_call(
        qkvb_kernel,
        grid=(QB_GRID,),
        in_specs=[hbm, hbm, whole(1, WIDTH), whole(VECTOR_ROWS, WIDTH),
                  whole(WIDTH, TOKENS, pipeline_mode=pl.Buffered(1)), by_cols(TOKENS, QB_N, now), by_cols(WIDTH, QB_N, now)],
        out_specs=[hbm, by_cols(WIDTH // PARTS, QB_N, lambda i: jnp.clip(i - 1 - QUAD * QKV_SUM.stride, 0, QB_STEPS - 1)),
                   whole(VECTOR_ROWS, WIDTH // PARTS)],
        out_shape=[jax.ShapeDtypeStruct((TOKENS, WIDTH), BF), jax.ShapeDtypeStruct((WIDTH // PARTS, QKV), F32),
                   jax.ShapeDtypeStruct((VECTOR_ROWS, WIDTH // PARTS), F32)],
        scratch_shapes=[pltpu.VMEM((TOKENS, WIDTH), F32), pltpu.VMEM((LANES, TOKENS, LANE), F32), pltpu.VMEM((TOKENS, WIDTH), BF),
                        pltpu.VMEM((LANE, WIDTH), F32), pltpu.VMEM((WIDTH // PARTS, QB_N), F32), pltpu.VMEM((16, WIDTH), F32), pltpu.SemaphoreType.DMA((2,))]
                       + QKV_SUM.scratch(),
        compiler_params=comm_params(2),
        cost_estimate=cost(QUAD * TOKENS * WIDTH * QKV, 80_000_000),
        name="qkvb",
    )(xim, dr, gain, vec, ht, dqkv, w)


VECTORS = (80, 80, 240, 80, 80, 80, 320, 80)


def to_steps(v):
    rows = v.shape[0]
    return v.reshape(rows, PARTS, MLP_STEPS, UNITS).swapaxes(1, 2).reshape(rows, FFN)


def from_steps(v):
    rows = v.shape[0]
    return v.reshape(rows, MLP_STEPS, PARTS, UNITS).swapaxes(1, 2).reshape(rows, FFN)


def solution(mesh):
    specs = (P("fsdp"),) * 14

    def gather(shard):
        return lax.all_gather(shard.astype(BF), "fsdp", axis=0, tiled=True)

    def device_step(resid_in, grad_out, ln1_gain, ln1_bias, qkv_weight, qkv_bias, out_weight, out_bias,
                    ln2_gain, ln2_bias, fc_weight, fc_bias, proj_weight, proj_bias):
        wq, wo, wf, wp = (gather(w) for w in (qkv_weight, out_weight, to_steps(fc_weight.astype(BF)), proj_weight))
        packed = jnp.concatenate([ln1_gain, ln1_bias, qkv_bias, out_bias, ln2_gain, ln2_bias, fc_bias, proj_bias])
        packed = gather(packed[None]).astype(F32)
        cuts = [sum(VECTORS[:i]) for i in range(len(VECTORS) + 1)]
        g1, b1, bq, bo, g2, b2, bf, bp = (packed[:, a:b].reshape(1, -1) for a, b in zip(cuts, cuts[1:]))

        x = resid_in.transpose(1, 0, 2).reshape(TOKENS, WIDTH)
        dy = grad_out.transpose(1, 0, 2).reshape(TOKENS, WIDTH)
        xim, ht, qkv = qkv_call(x, g1, b1, wq, bq)
        o, r, top, inv = attn_call(qkv, xim, wo, bo)
        y, dr, dr16, dwf, dwp, dbf, small = mlp_call(r, dy, g2, b2, bp, wf, wp, to_steps(bf))
        do, dwo = outb_call(dr16, o, wo)
        dqkv, dbq, dwo = attn_back_call(qkv, do, top, inv, dwo)
        owned = lambda v: v.reshape(PARTS, -1, WIDTH // PARTS).swapaxes(0, 1).reshape(-1, WIDTH)
        vec = jnp.concatenate([jnp.sum(small.reshape(4, 8, WIDTH), axis=1), owned(dbq), owned(from_steps(dbf))])
        vec = jnp.pad(vec, ((0, VECTOR_ROWS - len(vec)), (0, 0)))
        dx, dwq, vec = qkvb_call(xim, dr, g1, vec, ht, dqkv, wq)
        dg2, db2, dbp, dbo = vec[:4]
        dbq, dbf = vec[4:7].reshape(-1), vec[7:11].reshape(-1)
        dg1, db1 = vec[VECTOR_ROWS - 2:]
        dwf = from_steps(dwf)
        unturn = lambda t: t.reshape(SEQ, IMAGES, WIDTH).transpose(1, 0, 2)
        return (unturn(y), unturn(dx), dg1, db1, dwq, dbq, dwo, dbo, dg2, db2, dwf, dbf, dwp, dbp)

    return jax.shard_map(device_step, mesh=mesh, in_specs=specs, out_specs=specs, check_vma=False)
```

```python
import itertools
import math
import jax, jax.numpy as jnp
from jax import lax
from jax.experimental import pallas as pl
from jax.experimental.pallas import tpu as pltpu
from jax.sharding import PartitionSpec as P

BF, F32 = jnp.bfloat16, jnp.float32
IMAGES, SEQ, WIDTH, FFN, HEADS, HEAD = 8, 257, 1280, 5120, 16, 80
MAIN = SEQ - 1
TOKENS = IMAGES * SEQ
TAIL = IMAGES * MAIN
LN_EPS = 1e-5
VMEM_MAX = 67043328
LANE, SUBLANE, QUAD, QKV = 128, 8, 4, 3 * WIDTH
ALL = ...
LANES = WIDTH // LANE
ROWS = 32


def dot(a, b):
    return jnp.dot(a, b, preferred_element_type=F32)


def dot_nt(a, b):
    return lax.dot_general(a, b, (((1,), (1,)), ((), ())), preferred_element_type=F32)


def dot_tn(a, b):
    return lax.dot_general(a, b, (((0,), (0,)), ((), ())), preferred_element_type=F32)


def col_sum(v):
    return jnp.sum(v, axis=0, keepdims=True)


def col_max(v):
    return jnp.max(v, axis=0, keepdims=True)


def row_sum(v):
    return jnp.sum(v, axis=-1, keepdims=True)


def row_mean(v):
    return row_sum(v) * (1.0 / WIDTH)


def clear(*refs):
    for ref in refs:
        ref[ALL] = jnp.zeros_like(ref)


def step_id():
    return pl.program_id(0)


def cost(flops, bytes_accessed, transcendentals=0):
    return pl.CostEstimate(flops=flops, bytes_accessed=bytes_accessed, transcendentals=transcendentals)


def eights(v):
    return jnp.sum(v.reshape(v.shape[0] // SUBLANE, SUBLANE, v.shape[1]), axis=0)


def whole(*shape, **kw):
    return pl.BlockSpec(shape, lambda *i: (0,) * len(shape), **kw)


def by_cols(rows, cols, at=lambda i: i):
    return pl.BlockSpec((rows, cols), lambda i: (0, at(i)))


def by_rows(rows, cols, at=lambda i: i):
    return pl.BlockSpec((rows, cols), lambda i: (at(i), 0))


def steps(first, wide):
    return slice(first * wide, (first + 1) * wide)


def norm_stats(values):
    mean = row_mean(values)
    centered = values - mean
    inv = lax.rsqrt(row_mean(centered * centered) + LN_EPS)
    return centered * inv, inv


BLOCKS = [slice(a, b) for a, b in ((0, 512), (512, 1024), (1024, 1536), (1536, TOKENS))]


def row_tiles(body, step=LANE):
    def loop(i, carry):
        body(pl.multiple_of(i * step, step), step)
        return carry
    lax.fori_loop(0, TAIL // step, loop, 0)
    body(TAIL, IMAGES)


def to_image_order(wide, place, step=LANE):
    per = MAIN // step
    def loop(i, carry):
        first = (i % per) * (step * IMAGES) + i // per
        rows = [wide[c, pl.ds(first, step, stride=IMAGES), :] for c in range(LANES)]
        place(pl.multiple_of(i * step, step), step, jnp.concatenate(rows, axis=1))
        return carry
    lax.fori_loop(0, IMAGES * per, loop, 0)
    place(TAIL, IMAGES, joined(wide, TAIL, IMAGES))


def from_image_order(values, wide):
    def loop(i, carry):
        rows = values[pl.ds(pl.multiple_of(i * LANE, LANE), LANE), :]
        for c in range(LANES):
            wide[c, pl.ds((i % 2) * (LANE * IMAGES) + i // 2, LANE, stride=IMAGES), :] = rows[:, steps(c, LANE)]
        return carry
    lax.fori_loop(0, 2 * IMAGES, loop, 0)
    put(wide, TAIL, IMAGES, values[pl.ds(TAIL, IMAGES), :])


def joined(wide, r, n):
    return jnp.concatenate([wide[c, pl.ds(r, n), :] for c in range(LANES)], axis=1)


def put(wide, r, n, values):
    for c in range(LANES):
        wide[c, pl.ds(r, n), :] = values[:, steps(c, LANE)]


def norm_back(dn, hat, inv, gain):
    dhat = dn * gain
    m1 = row_mean(dhat)
    m2 = row_mean(dhat * hat)
    return inv * (dhat - m1 - hat * m2)


ORDERS = ((2, 1, 0), (1, 0, 2), (0, 2, 1))


class Links:
    def find(self, send, recv):
        self.send, self.recv = send, recv
        me = lax.axis_index("fsdp")
        self.core = me % 2
        self.at = (me // SUBLANE, (me // QUAD) % 2, (me // 2) % 2)
        self.other_core = me + 1 - 2 * self.core
        self.other = [me + step - 2 * step * place for step, place in zip((SUBLANE, QUAD, 2), self.at)]
        return self

    def meet(self):
        barrier = pltpu.get_barrier_semaphore()
        devices = (self.other_core, *self.other)
        for device in devices:
            pl.semaphore_signal(barrier, inc=1, device_id=(device,), device_id_type=pl.DeviceIdType.MESH)
        pl.semaphore_wait(barrier, len(devices))

    def remote(self, src, dst, sem, device):
        return pltpu.make_async_remote_copy(src_ref=src, dst_ref=dst, send_sem=self.send.at[sem], recv_sem=self.recv.at[sem],
                                            device_id=(device,), device_id_type=pl.DeviceIdType.MESH)


class Gather(Links):
    COUNT = 2

    def __init__(self, rows, cols, cuts):
        self.rows, self.cols, self.cuts = rows, cols, cuts
        self.parts = range(len(cuts) - 1)
        self.full_shape = jax.ShapeDtypeStruct((2, 2, 2, 2, rows, cols), BF)

    def scratch(self):
        return [pltpu.SemaphoreType.DMA((SEMS,))] * self.COUNT

    def bind(self, own, full, sems):
        self.own, self.full = own, full
        return self.find(*sems)

    def region(self, part, known, arrived=False):
        done = ORDERS[part][:known]
        place = [slice(None) if a in done else self.at[a] for a in range(3)]
        if arrived:
            place[done[-1]] = 1 - self.at[done[-1]]
        return (*place, self.core, slice(None), pl.ds(self.cuts[part], self.cuts[part + 1] - self.cuts[part]))

    def hop(self, stage, part):
        where = self.full.at[self.region(part, stage - 1)]
        source = self.own.at[self.region(part, 0)[-2:]] if stage == 1 else where
        return self.remote(source, where, QUAD * stage + part, self.other[ORDERS[part][stage - 1]])

    def forward(self, stage, part):
        if stage == 0:
            return self.remote(self.own, self.full.at[(*self.at, self.core)], 0, self.other_core)
        where = self.full.at[self.region(part, stage, True)]
        return self.remote(where, where, QUAD * (stage + 3) + part, self.other_core)

    def keep(self):
        return pltpu.make_async_copy(self.own, self.full.at[(*self.at, self.core)], self.send.at[1])

    def begin(self):
        for part in self.parts:
            self.hop(1, part).start()
        self.forward(0, 0).start()
        self.keep().start()

    def turn(self, stage):
        if stage == 1:
            self.keep().wait()
        for part in self.parts:
            self.hop(stage, part).wait()
            if stage < 3:
                self.hop(stage + 1, part).start()
        for part in self.parts:
            self.forward(stage, part).start()

    def end(self):
        self.forward(0, 0).wait()
        for stage in range(1, QUAD):
            for part in self.parts:
                self.forward(stage, part).wait()


SEMS = 28


class Exchange(Links):
    def __init__(self, rows, cols, cuts, along, stride=1, spare=0):
        self.rows, self.cols, self.stride = rows, cols, stride
        self.slots, self.locals = 3 * stride + spare, 1 + stride
        self.blocks = (2, 2, 2, 2, rows, cols)
        self.parts = [((slice(a, b), slice(None)) if along == 0 else (slice(None), slice(a, b))) for a, b in zip(cuts, cuts[1:])]
        self.shapes = [((b - a, cols) if along == 0 else (rows, b - a)) for a, b in zip(cuts, cuts[1:])]

    def scratch(self):
        two = (2, 2, 2)
        out = [pltpu.VMEM((self.locals, *self.blocks), F32), pltpu.VMEM((self.slots, *two, self.rows, self.cols), F32)]
        for axes in (2, 1, 0):
            out += [pltpu.VMEM((self.slots, *two[:axes], *shape), F32) for shape in self.shapes]
        return out + [pltpu.SemaphoreType.DMA((10, self.slots))] * 2

    COUNT = 13

    def bind(self, refs):
        self.local, self.pair = refs[0], refs[1]
        self.held = [None, refs[2:5], refs[5:SUBLANE], refs[SUBLANE:11]]
        return self.find(*refs[11:])

    def index(self, stage, part, side):
        order = ORDERS[part]
        left = [a for a in range(3) if a not in order[:stage - 1]]
        axis = order[stage - 1]
        where = self.at[axis] if side else 1 - self.at[axis]
        return tuple(where if a == axis else slice(None) for a in left)

    def copy(self, stage, part, c):
        slot = c % self.slots
        if stage == 0:
            return self.remote(self.local.at[c % self.locals, :, :, :, 1 - self.core], self.pair.at[slot], (0, slot), self.other_core)
        source = self.pair if stage == 1 else self.held[stage - 1][part]
        tail = self.parts[part] if stage == 1 else ()
        return self.remote(source.at[(slot, *self.index(stage, part, False), *tail)], self.held[stage][part].at[slot],
                           (3 * stage - 2 + part, slot), self.other[ORDERS[part][stage - 1]])

    def start(self, stage, c):
        for part in range(1 if stage == 0 else 3):
            self.copy(stage, part, c).start()

    def wait(self, stage, c):
        for part in range(1 if stage == 0 else 3):
            self.copy(stage, part, c).wait()

    def add(self, stage, c):
        slot = c % self.slots
        if stage == 0:
            for chip in itertools.product(range(2), repeat=3):
                self.pair[(slot, *chip)] += self.local[(c % self.locals, *chip, self.core)]
            return
        for part in range(3):
            source = self.pair if stage == 1 else self.held[stage - 1][part]
            tail = self.parts[part] if stage == 1 else ()
            for place in itertools.product(range(2), repeat=3 - stage):
                free = iter(place)
                kept = tuple(next(free) if isinstance(i, slice) else i for i in self.index(stage, part, True))
                self.held[stage][part][(slot, *place)] += source[(slot, *kept, *tail)]

    def result(self, c, out_ref):
        for part in range(3):
            out_ref[self.parts[part]] = self.held[3][part][c % self.slots]

    def put_local(self, c, values):
        self.local[c % self.locals] = values.reshape(self.blocks)


def comm_params(n):
    return pltpu.CompilerParams(dimension_semantics=("arbitrary",), vmem_limit_bytes=VMEM_MAX, collective_id=n, has_side_effects=True)


def advance(exchanges, t, exists, emit):
    for stage in (3, 2, 1, 0):
        c = t - 1 - (stage + 1) * exchanges[0].stride

        @pl.when(exists(c))
        def _():
            for n, exchange in enumerate(exchanges):
                exchange.wait(stage, c)
                exchange.add(stage, c)
                if stage < 3:
                    exchange.start(stage + 1, c)
                else:
                    emit(n, exchange, c)

    @pl.when(exists(t - 1))
    def _():
        for exchange in exchanges:
            exchange.start(0, t - 1)


def first_chunks(n):
    return lambda c: (c >= 0) & (c < n)


DRAIN = 5


PARTS = 16
SHARD = WIDTH // PARTS
VECTOR_ROWS = 16
QKV_ALL = Gather(SHARD, QKV, (0, 1280, 2560, 3840))
OUT_ALL = Gather(SHARD, WIDTH, (0, 384, 768, 1280))
FC_ALL = Gather(SHARD, FFN, (0, 1664, 3328, 5120))
PROJ_ALL = Gather(FFN // PARTS, WIDTH, (0, 384, 896, 1280))
VECTOR_ALL = Gather(SHARD, LANE, (0, LANE))


def open_kernel(x_hbm, rows_ref, wq_ref, wo_ref, xim_hbm, h_hbm, ht_hbm, vec_ref, wq_full, wo_full,
                x, wide, h, ht, rows, vec_own, vec_full, wq_own, wo_own, sems, *comm):
    loads = pltpu.make_async_copy(x_hbm, x, sems.at[0])
    loads.start()
    clear(rows)
    rows[:VECTOR_ROWS, :] = rows_ref[ALL]
    vec_own[ALL] = rows[ALL].T[:SHARD, :].astype(BF)
    wq_own[ALL] = wq_ref[ALL].astype(BF)
    wo_own[ALL] = wo_ref[ALL].astype(BF)
    pairs = [comm[2 * i:2 * i + 2] for i in range(3)]
    vectors = VECTOR_ALL.bind(vec_own, vec_full, pairs[0])
    weights = QKV_ALL.bind(wq_own, wq_full, pairs[1]), OUT_ALL.bind(wo_own, wo_full, pairs[2])
    gathers = (vectors, *weights)
    vectors.meet()
    for gather in gathers:
        gather.begin()
    loads.wait()

    def widen(r, n):
        put(wide, r, n, x[pl.ds(r, n), :].astype(F32))
    row_tiles(widen)
    for gather in gathers:
        gather.turn(1)

    def place(r, n, values):
        x[pl.ds(r, n), :] = values.astype(BF)
    to_image_order(wide, place)
    for gather in gathers:
        gather.turn(2)
    vectors.turn(3)
    vectors.end()
    vec_ref[ALL] = vec_full[ALL].reshape(WIDTH, LANE).astype(F32).T[:VECTOR_ROWS, :]
    gain, bias = vec_ref[0:1, :], vec_ref[1:2, :]

    def norm(r, n):
        hat, _ = norm_stats(x[pl.ds(r, n), :].astype(F32))
        h[pl.ds(r, n), :] = (hat * gain + bias).astype(BF)
    row_tiles(norm, ROWS)
    for b in range(IMAGES):
        ht[:, steps(b, MAIN)] = h[steps(b, MAIN), :].T
    ht[:, TAIL:TOKENS] = h[TAIL:TOKENS, :].T
    stores = [pltpu.make_async_copy(src, dst, sems.at[i]) for i, (src, dst) in enumerate(((x, xim_hbm), (h, h_hbm), (ht, ht_hbm)))]
    for cp in stores:
        cp.start()
    for gather in weights:
        gather.turn(3)
    for gather in weights:
        gather.end()
    for cp in stores:
        cp.wait()


def open_call(x, rows, wq, wo):
    hbm, vmem = pl.BlockSpec(memory_space=pl.ANY), pl.BlockSpec(memory_space=pltpu.VMEM)
    return pl.pallas_call(
        open_kernel,
        in_specs=[hbm, vmem, vmem, vmem],
        out_specs=[hbm, hbm, hbm, vmem, hbm, hbm],
        out_shape=[jax.ShapeDtypeStruct((TOKENS, WIDTH), BF), jax.ShapeDtypeStruct((TOKENS, WIDTH), BF),
                   jax.ShapeDtypeStruct((WIDTH, TOKENS), BF), jax.ShapeDtypeStruct((VECTOR_ROWS, WIDTH), F32),
                   QKV_ALL.full_shape, OUT_ALL.full_shape],
        scratch_shapes=[pltpu.VMEM((TOKENS, WIDTH), BF), pltpu.VMEM((LANES, TOKENS, LANE), F32), pltpu.VMEM((TOKENS, WIDTH), BF),
                        pltpu.VMEM((WIDTH, TOKENS), BF), pltpu.VMEM((LANE, LANE), F32), pltpu.VMEM((SHARD, LANE), BF),
                        pltpu.VMEM(VECTOR_ALL.full_shape.shape, BF), pltpu.VMEM((SHARD, QKV), BF), pltpu.VMEM((SHARD, WIDTH), BF),
                        pltpu.SemaphoreType.DMA((3,))] + VECTOR_ALL.scratch() + QKV_ALL.scratch() + OUT_ALL.scratch(),
        compiler_params=pltpu.CompilerParams(vmem_limit_bytes=VMEM_MAX, collective_id=3, has_side_effects=True),
        cost_estimate=cost(1_000_000_000, 60_000_000),
        name="open",
    )(x, rows, wq, wo)


QKV_N = 768


def qkv_kernel(h_ref, w_ref, wb_ref, own_ref, qkv_ref, full, *sems):
    t, last = step_id(), pl.num_programs(0) - 1
    gather = FC_ALL.bind(own_ref, full, sems)

    @pl.when(t == 0)
    def _():
        gather.meet()
        gather.begin()

    @pl.when(t == 1)
    def _():
        gather.turn(1)

    @pl.when(t == 3)
    def _():
        gather.turn(2)
    for rows in BLOCKS:
        qkv_ref[rows, :] = (dot(h_ref[rows, :], w_ref[ALL]) + wb_ref[ALL]).astype(BF)

    @pl.when(t == last)
    def _():
        gather.turn(3)
        gather.end()


def qkv_call(h, w, wb, own):
    hbm = pl.BlockSpec(memory_space=pl.ANY)
    return pl.pallas_call(
        qkv_kernel,
        grid=(QKV // QKV_N,),
        in_specs=[whole(TOKENS, WIDTH, pipeline_mode=pl.Buffered(1)), by_cols(WIDTH, QKV_N), by_cols(1, QKV_N), whole(SHARD, FFN)],
        out_specs=[by_cols(TOKENS, QKV_N), hbm],
        out_shape=[jax.ShapeDtypeStruct((TOKENS, QKV), BF), FC_ALL.full_shape],
        scratch_shapes=FC_ALL.scratch(),
        compiler_params=comm_params(QUAD),
        cost_estimate=cost(2 * TOKENS * WIDTH * QKV, 60_000_000),
        name="qkv",
    )(h, w, wb, own)


MLP_F = MAIN
UNITS = MLP_F // PARTS
MLP_STEPS = FFN // MLP_F
ROW_CUTS = (0, 24, 48, 80)
FC_SUM = Exchange(WIDTH // PARTS, MLP_F, ROW_CUTS, 0)
PROJ_SUM = Exchange(UNITS, WIDTH, (0, 512, 896, 1280), 1)
CDF_P = 0.33
CDF_C = (0.1326322871417956, 0.11939570820799192, 0.18103829560051796, -0.08904113226212501,
         0.33075919469138065, -0.22023738432274684, 0.0454530347223348)


def gelu_pair(u):
    bell = jnp.exp(u * u * -0.5)
    t = 1.0 / (1.0 + CDF_P * jnp.abs(u))
    poly = CDF_C[6]
    for c in CDF_C[5::-1]:
        poly = poly * t + c
    tail = poly * t * bell
    cdf = jnp.where(u < 0.0, tail, 1.0 - tail)
    return u * cdf, cdf + u * bell * ((2.0 * math.pi) ** -0.5)


def mlp_kernel(r_hbm, dy_hbm, gain_ref, bias_ref, pb_ref, fc_ref, proj_ref, fcb_ref,
               y_hbm, dr_hbm, dr16_hbm, dfc_ref, dproj_ref, dfcb_ref, small_ref,
               n2, dy, y_acc, dn_acc, g, du, ua, ub, da, db, sem, *comm):
    step = step_id()
    by_row, by_col = FC_SUM.bind(comm[:Exchange.COUNT]), PROJ_SUM.bind(comm[Exchange.COUNT:])

    @pl.when(step == 0)
    def _():
        by_row.meet()
        cp = pltpu.make_async_copy(dy_hbm, n2, sem)
        cp.start()
        cp.wait()

        def widen(r, n):
            put(dn_acc, r, n, n2[pl.ds(r, n), :].astype(F32))
        row_tiles(widen)
        cp = pltpu.make_async_copy(r_hbm, n2, sem)
        cp.start()

        def place(r, n, values):
            dy[pl.ds(r, n), :] = values.astype(BF)
        to_image_order(dn_acc, place, ROWS)
        cp.wait()
        gain, bias, pb = gain_ref[ALL], bias_ref[ALL], pb_ref[ALL]

        def norm(r, n):
            wide_r = n2[pl.ds(r, n), :].astype(F32)
            hat, _ = norm_stats(wide_r)
            n2[pl.ds(r, n), :] = (hat * gain + bias).astype(BF)
            y_acc[pl.ds(r, n), :] = wide_r + pb
            put(dn_acc, r, n, jnp.zeros((n, WIDTH), F32))
        row_tiles(norm, ROWS)
        clear(small_ref)

    outs = (dfc_ref, dproj_ref)
    advance((by_row, by_col), step, first_chunks(MLP_STEPS), lambda n, exchange, c: exchange.result(c, outs[n]))

    @pl.when(step < MLP_STEPS)
    def _():
        fcb = fcb_ref[ALL]
        fc, proj = fc_ref[ALL], proj_ref[ALL].reshape(MLP_F, WIDTH)
        bias_sum = jnp.zeros((SUBLANE, MLP_F), F32)
        tiles = [(b * MAIN, MAIN) for b in range(IMAGES - 1)] + [((IMAGES - 1) * MAIN, MAIN + IMAGES)]
        pairs = ((ua, da), (ub, db))

        def products(k):
            r, n = tiles[k]
            u_s, d_s = pairs[k % 2]
            u_s[0:n, :] = dot(n2[r:r + n, :], fc)
            d_s[0:n, :] = dot_nt(dy[r:r + n, :], proj)

        def pointwise(k, total):
            r, n = tiles[k]
            u_s, d_s = pairs[k % 2]
            value, slope = gelu_pair(u_s[0:n, :] + fcb)
            g[r:r + n, :] = value.astype(BF)
            grad = d_s[0:n, :] * slope
            du[r:r + n, :] = grad.astype(BF)
            return total + eights(grad)

        products(0)
        for k in range(1, IMAGES):
            products(k)
            bias_sum = pointwise(k - 1, bias_sum)
        bias_sum = pointwise(IMAGES - 1, bias_sum)
        dfcb_ref[ALL] = col_sum(bias_sum)
        y_acc[ALL] += dot(g[ALL], proj)
        for c in range(LANES // 2):
            part = dot_nt(du[ALL], fc_ref[steps(c, MAIN), :])
            dn_acc[2 * c] += part[:, :LANE]
            dn_acc[2 * c + 1] += part[:, LANE:]
        by_col.put_local(step, dot_tn(g[ALL], dy[ALL]))
        by_row.put_local(step, dot_tn(n2[ALL], du[ALL]))

    out_copies = [pltpu.make_async_copy(dn_acc, dr_hbm, sem), pltpu.make_async_copy(n2, dr16_hbm, sem)]
    y_copy = pltpu.make_async_copy(dy, y_hbm, sem)

    @pl.when(step == MLP_STEPS)
    def _():
        cp = pltpu.make_async_copy(r_hbm, n2, sem)
        cp.start()
        cp.wait()
        gain = gain_ref[ALL]

        def back(r, n):
            hat, inv = norm_stats(n2[pl.ds(r, n), :].astype(F32))
            dn = joined(dn_acc, r, n)
            wide_dy = dy[pl.ds(r, n), :].astype(F32)
            dr = wide_dy + norm_back(dn, hat, inv, gain)
            put(dn_acc, r, n, dr)
            n2[pl.ds(r, n), :] = dr.astype(BF)
            for i, v in enumerate((dn * hat, dn, wide_dy, dr)):
                small_ref[steps(i, SUBLANE), :] += eights(v)
        row_tiles(back, ROWS)
        for cp in out_copies:
            cp.start()

    @pl.when(step == MLP_STEPS + 1)
    def _():
        for cp in out_copies:
            cp.wait()
        from_image_order(y_acc, dn_acc)

    @pl.when(step == MLP_STEPS + 2)
    def _():
        def narrow(r, n):
            dy[pl.ds(r, n), :] = joined(dn_acc, r, n).astype(BF)
        row_tiles(narrow)
        y_copy.start()

    @pl.when(step == MLP_STEPS + 3)
    def _():
        y_copy.wait()


def mlp_call(r, dy, gain, bias, pb, fc, proj, fcb):
    hbm = pl.BlockSpec(memory_space=pl.ANY)
    vec = whole(1, WIDTH)
    now = lambda i: jnp.minimum(i, MLP_STEPS - 1)
    done = lambda i: jnp.maximum(i - DRAIN, 0)
    return pl.pallas_call(
        mlp_kernel,
        grid=(MLP_STEPS + DRAIN,),
        in_specs=[hbm, hbm, vec, vec, vec, by_cols(WIDTH, MLP_F, now),
                  pl.BlockSpec((PARTS, None, UNITS, WIDTH), lambda i: (0, now(i), 0, 0)),
                  by_cols(1, MLP_F, now)],
        out_specs=[hbm, hbm, hbm, by_cols(WIDTH // PARTS, MLP_F, done),
                   by_rows(UNITS, WIDTH, done),
                   by_cols(1, MLP_F, now), whole(32, WIDTH)],
        out_shape=[jax.ShapeDtypeStruct((TOKENS, WIDTH), BF), jax.ShapeDtypeStruct((LANES, TOKENS, LANE), F32),
                   jax.ShapeDtypeStruct((TOKENS, WIDTH), BF), jax.ShapeDtypeStruct((WIDTH // PARTS, FFN), F32),
                   jax.ShapeDtypeStruct((FFN // PARTS, WIDTH), F32),
                   jax.ShapeDtypeStruct((1, FFN), F32), jax.ShapeDtypeStruct((32, WIDTH), F32)],
        scratch_shapes=[pltpu.VMEM((TOKENS, WIDTH), BF), pltpu.VMEM((TOKENS, WIDTH), BF),
                        pltpu.VMEM((TOKENS, WIDTH), F32), pltpu.VMEM((LANES, TOKENS, LANE), F32),
                        pltpu.VMEM((TOKENS, MLP_F), BF), pltpu.VMEM((TOKENS, MLP_F), BF)]
                       + [pltpu.VMEM((MAIN + IMAGES, MLP_F), F32)] * QUAD + [pltpu.SemaphoreType.DMA]
                       + FC_SUM.scratch() + PROJ_SUM.scratch(),
        compiler_params=comm_params(0),
        cost_estimate=cost(12 * TOKENS * WIDTH * FFN, 150_000_000, TOKENS * FFN),
        name="mlp",
    )(r, dy, gain, bias, pb, fc, proj.reshape(PARTS, MLP_STEPS, UNITS, WIDTH), fcb)


SCALE = HEAD ** -0.5


def window(h):
    first = min(HEAD * h // LANE * LANE, WIDTH - MAIN)
    wide = LANE if HEAD * h + HEAD <= first + LANE else MAIN
    return first, wide, HEAD * h - first


def lane_mask(h):
    first, wide, off = window(h)
    lane = lax.broadcasted_iota(jnp.int32, (MAIN, wide), 1)
    return (lane >= off) & (lane < off + HEAD)


def thirds(ref, rows=slice(None)):
    return [ref[rows, steps(i, WIDTH)] for i in range(3)]


def head_rows():
    lane = lax.broadcasted_iota(jnp.int32, (HEADS, WIDTH), 1)
    row = lax.broadcasted_iota(jnp.int32, (HEADS, WIDTH), 0)
    return (lane // HEAD == row).astype(F32)


def tail_softmax(s, s_self):
    m = jnp.maximum(jnp.max(s, axis=1, keepdims=True), s_self)
    e = jnp.exp((s - m) * SCALE)
    e_self = jnp.exp((s_self - m) * SCALE)
    inv = 1.0 / (row_sum(e) + e_self)
    return e * inv, e_self * inv


def attn_kernel(qkv_ref, qkvt_ref, x_ref, xt_ref, w_ref, wb_ref, proj_ref, o_hbm, r_hbm, max_ref, inv_ref, full,
                tails, o_tail, o_t, ptail, o_buf, r_buf, sems, own, *comm):
    b, last = step_id(), pl.num_programs(0) - 1
    slot = b % 2
    gather = PROJ_ALL.bind(own, full, comm)

    @pl.when(b == 0)
    def _():
        tails[ALL] = qkvt_ref[ALL].astype(F32)
        own[ALL] = proj_ref[ALL].astype(BF)
        gather.meet()
        gather.begin()

    @pl.when(b == 1)
    def _():
        gather.turn(1)

    @pl.when(b == 3)
    def _():
        gather.turn(2)

    @pl.when(b == last)
    def _():
        gather.turn(3)

    heads = head_rows()
    q_t, k_t, v_t = (heads * z for z in thirds(tails, pl.ds(b, 1)))
    q, k, v = thirds(qkv_ref)

    p, p_self = tail_softmax(dot_nt(q_t.astype(BF), k), row_sum(q_t * k_t))
    mixed = dot(p.astype(BF), v) * heads + p_self.astype(BF).astype(F32) * v_t
    o_tail[pl.ds(b, 1), :] = col_sum(mixed)

    s_tail = dot_nt(k_t.astype(BF), q)
    v_turned = v.T
    for h in range(HEADS):
        first, wide, _ = window(h)
        q_h = jnp.where(lane_mask(h), qkv_ref[:, first:first + wide], jnp.zeros((), BF))
        s = dot_nt(qkv_ref[:, pl.ds(WIDTH + first, wide)], q_h)
        top = jnp.maximum(col_max(s), s_tail[steps(h, 1), :])
        e = jnp.exp((s - top) * SCALE)
        e_tail = jnp.exp((s_tail[steps(h, 1), :] - top) * SCALE)
        inv = 1.0 / (col_sum(e) + e_tail)
        max_ref[0, steps(h, 1), :] = top
        inv_ref[0, steps(h, 1), :] = inv
        ptail[steps(h, 1), :] = e_tail * inv
        o_t[steps(h, HEAD), :] = dot(v_turned[steps(h, HEAD), :], (e * inv).astype(BF))

    @pl.when(b >= 2)
    def _():
        out_copy(o_buf, o_hbm, slot, b - 2, sems, 0).wait()
        out_copy(r_buf, r_hbm, slot, b - 2, sems, 1).wait()

    o = (o_t[ALL].T + dot_tn(ptail[ALL].astype(BF), v_t.astype(BF))).astype(BF)
    o_buf[slot] = o
    r_buf[slot] = (x_ref[ALL].astype(F32) + dot(o, w_ref[ALL]) + wb_ref[ALL]).astype(BF)
    out_copy(o_buf, o_hbm, slot, b, sems, 0).start()
    out_copy(r_buf, r_hbm, slot, b, sems, 1).start()

    @pl.when(b == last)
    def _():
        for buf, hbm, n in ((o_buf, o_hbm, 0), (r_buf, r_hbm, 1)):
            out_copy(buf, hbm, 1 - slot, b - 1, sems, n).wait()
        o = o_tail[ALL].astype(BF)
        o_buf[1 - slot, 0:IMAGES, :] = o
        r_buf[1 - slot, 0:IMAGES, :] = (xt_ref[ALL].astype(F32) + dot(o, w_ref[ALL]) + wb_ref[ALL]).astype(BF)
        copies = [pltpu.make_async_copy(buf.at[1 - slot, pl.ds(0, IMAGES)], hbm.at[pl.ds(TAIL, IMAGES)], sems.at[n, 1 - slot])
                  for buf, hbm, n in ((o_buf, o_hbm, 0), (r_buf, r_hbm, 1))]
        for cp in copies:
            cp.start()
        for cp in copies:
            cp.wait()
        for buf, hbm, n in ((o_buf, o_hbm, 0), (r_buf, r_hbm, 1)):
            out_copy(buf, hbm, slot, b, sems, n).wait()
        gather.end()


def out_copy(buf, hbm, slot, b, sems, n):
    return pltpu.make_async_copy(buf.at[slot], hbm.at[pl.ds(pl.multiple_of(b * MAIN, MAIN), MAIN)], sems.at[n, slot])


def attn_call(qkv, xim, w, wb, proj):
    hbm = pl.BlockSpec(memory_space=pl.ANY)
    main = lambda n: by_rows(MAIN, n)
    tail = lambda n: by_rows(IMAGES, n, lambda i: TAIL // IMAGES)
    stat = pl.BlockSpec((1, HEADS, MAIN), lambda i: (i, 0, 0))
    return pl.pallas_call(
        attn_kernel,
        grid=(IMAGES,),
        in_specs=[main(QKV), tail(QKV), main(WIDTH), tail(WIDTH),
                  whole(WIDTH, WIDTH), whole(1, WIDTH), whole(*proj.shape)],
        out_specs=[hbm, hbm, stat, stat, hbm],
        out_shape=[jax.ShapeDtypeStruct((TOKENS, WIDTH), BF), jax.ShapeDtypeStruct((TOKENS, WIDTH), BF),
                   jax.ShapeDtypeStruct((IMAGES, HEADS, MAIN), F32), jax.ShapeDtypeStruct((IMAGES, HEADS, MAIN), F32),
                   PROJ_ALL.full_shape],
        scratch_shapes=[pltpu.VMEM((IMAGES, QKV), F32), pltpu.VMEM((IMAGES, WIDTH), F32),
                        pltpu.VMEM((WIDTH, MAIN), F32), pltpu.VMEM((HEADS, MAIN), F32),
                        pltpu.VMEM((2, MAIN, WIDTH), BF), pltpu.VMEM((2, MAIN, WIDTH), BF), pltpu.SemaphoreType.DMA((2, 2)),
                        pltpu.VMEM(proj.shape, BF)] + PROJ_ALL.scratch(),
        compiler_params=comm_params(5),
        cost_estimate=cost(30_000_000_000, 50_000_000, 8_400_000),
        name="attn",
    )(qkv, qkv, xim, xim, w, wb, proj)


def outb_kernel(dr_ref, o_ref, w_ref, do_ref, dw_ref):
    n = MAIN
    c = step_id()
    do_ref[ALL] = dot_nt(dr_ref[ALL], w_ref[ALL]).astype(BF)
    dw_ref[ALL] = dot_tn(o_ref[ALL], dr_ref[:, pl.ds(pl.multiple_of(c * n, n), n)])


def outb_call(dr, o, w):
    n = MAIN
    full = whole(TOKENS, WIDTH)
    return pl.pallas_call(
        outb_kernel,
        grid=(WIDTH // n,),
        in_specs=[full, full, by_rows(n, WIDTH)],
        out_specs=[by_cols(TOKENS, n), by_cols(WIDTH, n)],
        out_shape=[jax.ShapeDtypeStruct((TOKENS, WIDTH), BF), jax.ShapeDtypeStruct((WIDTH, WIDTH), F32)],
        compiler_params=pltpu.CompilerParams(dimension_semantics=("arbitrary",), vmem_limit_bytes=VMEM_MAX),
        cost_estimate=cost(QUAD * TOKENS * WIDTH * WIDTH, 30_000_000),
        name="outb",
    )(dr, o, w)


def attn_back_kernel(qkv_ref, qkvt_ref, do_ref, dot_ref, max_ref, inv_ref, dw_ref, dqkv_hbm, dwb_ref, dwout_ref,
                     tails, do_tails, grad_tails, dq_t, dk, dv, ds_tail, buf, sems, *comm):
    b = step_id()
    by_row = FC_SUM.bind(comm)

    @pl.when(b == 0)
    def _():
        by_row.meet()
    advance((by_row,), b, first_chunks(OUT_STEPS), lambda n, exchange, c: exchange.result(c, dwout_ref))

    @pl.when(b < OUT_STEPS)
    def _():
        by_row.put_local(b, dw_ref[ALL])

    @pl.when(b < IMAGES)
    def _():
        image_back(b, qkv_ref, qkvt_ref, do_ref, dot_ref, max_ref, inv_ref, dqkv_hbm, dwb_ref,
                   tails, do_tails, grad_tails, dq_t, dk, dv, ds_tail, buf, sems)


OUT_STEPS = WIDTH // MAIN


def image_back(b, qkv_ref, qkvt_ref, do_ref, dot_ref, max_ref, inv_ref, dqkv_hbm, dwb_ref,
               tails, do_tails, grad_tails, dq_t, dk, dv, ds_tail, buf, sems):
    last = IMAGES - 1
    slot = b % 2

    @pl.when(b == 0)
    def _():
        tails[ALL] = qkvt_ref[ALL].astype(F32)
        do_tails[ALL] = dot_ref[ALL].astype(F32)
        clear(dwb_ref)

    heads = head_rows()
    q_t, k_t, v_t = (heads * z for z in thirds(tails, pl.ds(b, 1)))
    do_t = heads * do_tails[pl.ds(b, 1), :]
    q, k, v = thirds(qkv_ref)
    do = do_ref[ALL]
    q_t16, k_t16, v_t16, do_t16 = (z.astype(BF) for z in (q_t, k_t, v_t, do_t))

    p, p_self = tail_softmax(dot_nt(q_t16, k), row_sum(q_t * k_t))
    dp, dp_self = dot_nt(do_t16, v), row_sum(do_t * v_t)
    inner = row_sum(p * dp) + p_self * dp_self
    ds16 = (p * (dp - inner) * SCALE).astype(BF)
    ds_self = (p_self * (dp_self - inner) * SCALE).astype(BF).astype(F32)
    grad_q = col_sum(dot(ds16, k) * heads + ds_self * k_t)
    grad_k = ds_self * q_t
    grad_v = p_self.astype(BF).astype(F32) * do_t
    dk[ALL] = dot_tn(ds16, q_t16)
    dv[ALL] = dot_tn(p.astype(BF), do_t16)

    p_tail = jnp.exp((dot_nt(k_t16, q) - max_ref[0]) * SCALE) * inv_ref[0]
    dp_tail = dot_nt(v_t16, do)
    inner_tail = p_tail * dp_tail

    k_turned = k.T
    for h in range(HEADS):
        first, wide, _ = window(h)
        here = slice(first, first + wide)
        mask = lane_mask(h)
        q_h = jnp.where(mask, qkv_ref[:, here], jnp.zeros((), BF))
        do_h = jnp.where(mask, do_ref[:, here], jnp.zeros((), BF))
        s = dot_nt(qkv_ref[:, pl.ds(WIDTH + first, wide)], q_h)
        dp = dot_nt(qkv_ref[:, pl.ds(2 * WIDTH + first, wide)], do_h)
        p = jnp.exp((s - max_ref[0, steps(h, 1), :]) * SCALE) * inv_ref[0, steps(h, 1), :]
        inner = col_sum(p * dp) + inner_tail[steps(h, 1), :]
        ds = (p * (dp - inner) * SCALE).astype(BF)
        dv[:, here] += dot(p.astype(BF), do_h)
        dk[:, here] += dot(ds, q_h)
        dq_t[steps(h, HEAD), :] = dot(k_turned[steps(h, HEAD), :], ds)
        ds_tail[steps(h, 1), :] = p_tail[steps(h, 1), :] * (dp_tail[steps(h, 1), :] - inner) * SCALE

    ds_tail16 = ds_tail[ALL].astype(BF)
    grad_k = col_sum(grad_k + dot(ds_tail16, q) * heads)
    grad_v = col_sum(grad_v + dot(p_tail.astype(BF), do) * heads)

    @pl.when(b >= 2)
    def _():
        out_copy(buf, dqkv_hbm, slot, b - 2, sems, 0).wait()

    grad = dq_t[ALL].T + dot_tn(ds_tail16, k_t16)
    for n, (main, tail) in enumerate(((grad, grad_q), (dk[ALL], grad_k), (dv[ALL], grad_v))):
        here = steps(n, WIDTH)
        buf[slot, :, here] = main.astype(BF)
        grad_tails[pl.ds(b, 1), here] = tail
        dwb_ref[:, here] += col_sum(main) + tail
    out_copy(buf, dqkv_hbm, slot, b, sems, 0).start()

    @pl.when(b == last)
    def _():
        out_copy(buf, dqkv_hbm, 1 - slot, b - 1, sems, 0).wait()
        buf[1 - slot, 0:IMAGES, :] = grad_tails[ALL].astype(BF)
        cp = pltpu.make_async_copy(buf.at[1 - slot, pl.ds(0, IMAGES)], dqkv_hbm.at[pl.ds(TAIL, IMAGES)], sems.at[0, 1 - slot])
        cp.start()
        cp.wait()
        out_copy(buf, dqkv_hbm, slot, b, sems, 0).wait()


def attn_back_call(qkv, do, top, inv, dw):
    hbm = pl.BlockSpec(memory_space=pl.ANY)
    image = lambda i: jnp.minimum(i, IMAGES - 1)
    main = lambda n: by_rows(MAIN, n, image)
    tail = lambda n: by_rows(IMAGES, n, lambda i: TAIL // IMAGES)
    stat = pl.BlockSpec((1, HEADS, MAIN), lambda i: (image(i), 0, 0))
    return pl.pallas_call(
        attn_back_kernel,
        grid=(OUT_STEPS + DRAIN,),
        in_specs=[main(QKV), tail(QKV), main(WIDTH), tail(WIDTH), stat, stat,
                  by_cols(WIDTH, MAIN, lambda i: jnp.minimum(i, OUT_STEPS - 1))],
        out_specs=[hbm, whole(1, QKV), by_cols(WIDTH // PARTS, MAIN, lambda i: jnp.maximum(i - DRAIN, 0))],
        out_shape=[jax.ShapeDtypeStruct((TOKENS, QKV), BF), jax.ShapeDtypeStruct((1, QKV), F32),
                   jax.ShapeDtypeStruct((WIDTH // PARTS, WIDTH), F32)],
        scratch_shapes=[pltpu.VMEM((IMAGES, QKV), F32), pltpu.VMEM((IMAGES, WIDTH), F32),
                        pltpu.VMEM((IMAGES, QKV), F32), pltpu.VMEM((WIDTH, MAIN), F32),
                        pltpu.VMEM((MAIN, WIDTH), F32), pltpu.VMEM((MAIN, WIDTH), F32), pltpu.VMEM((HEADS, MAIN), F32),
                        pltpu.VMEM((2, MAIN, QKV), BF), pltpu.SemaphoreType.DMA((1, 2))] + FC_SUM.scratch(),
        compiler_params=comm_params(1),
        cost_estimate=cost(60_000_000_000, 50_000_000, 8_400_000),
        name="attn_back",
    )(qkv, qkv, do, do, top, inv, dw)


QB_N = MAIN
QB_STEPS = QKV // QB_N
QKV_SUM = Exchange(WIDTH // PARTS, QB_N, ROW_CUTS, 0, 2, 1)
VECTOR_CHUNK = QB_STEPS + 2
QB_GRID = VECTOR_CHUNK + 2 + QUAD * QKV_SUM.stride


def qkvb_kernel(xim_hbm, dr_hbm, gain_ref, vec_ref, ht_ref, dqkv_ref, w_ref, dx_hbm, dw_ref, out_vec_ref,
                acc, dr, xd, vec, vec_out, sums, sems, *comm):
    t = step_id()
    by_row = QKV_SUM.bind(comm)
    loads = [pltpu.make_async_copy(dr_hbm, dr, sems.at[0]), pltpu.make_async_copy(xim_hbm, xd, sems.at[1])]
    store = pltpu.make_async_copy(xd, dx_hbm, sems.at[1])

    @pl.when(t == 0)
    def _():
        by_row.meet()
        for cp in loads:
            cp.start()
        clear(acc, sums, vec)
        vec[:VECTOR_ROWS, :] = vec_ref[ALL]

    def emit(n, exchange, c):
        @pl.when(c < QB_STEPS)
        def _():
            exchange.result(c, dw_ref)

        @pl.when(c == VECTOR_CHUNK)
        def _():
            exchange.result(c, vec_out)
            out_vec_ref[ALL] = vec_out[:, :LANE].T[:VECTOR_ROWS, :]
    advance((by_row,), t, lambda c: ((c >= 0) & (c < QB_STEPS)) | (c == VECTOR_CHUNK), emit)

    @pl.when(t < QB_STEPS)
    def _():
        by_row.put_local(t, dot(ht_ref[ALL], dqkv_ref[ALL]))
        acc[ALL] += dot_nt(dqkv_ref[ALL], w_ref[ALL])

    @pl.when(t == QB_STEPS)
    def _():
        for cp in loads:
            cp.wait()

    def back(r, n):
        hat, inv = norm_stats(xd[pl.ds(r, n), :].astype(F32))
        dn = acc[pl.ds(r, n), :]
        for i, v in enumerate((dn * hat, dn)):
            sums[steps(i, SUBLANE), :] += eights(v)
        acc[pl.ds(r, n), :] = joined(dr, r, n) + norm_back(dn, hat, inv, gain_ref[ALL])

    @pl.when((t >= QB_STEPS) & (t <= VECTOR_CHUNK))
    def _():
        part = (t - QB_STEPS) * BACK_TILES

        def loop(i, carry):
            @pl.when(part + i < TAIL // ROWS)
            def _():
                back(pl.multiple_of((part + i) * ROWS, ROWS), ROWS)
            return carry
        lax.fori_loop(0, BACK_TILES, loop, 0)

    @pl.when(t == VECTOR_CHUNK)
    def _():
        back(TAIL, IMAGES)
        for i in range(2):
            vec[VECTOR_ROWS - 2 + i:VECTOR_ROWS - 1 + i, :] = col_sum(sums[steps(i, SUBLANE), :])
        turned = vec[ALL].T
        by_row.put_local(t, jnp.concatenate([turned, jnp.zeros_like(turned)], axis=1))

    @pl.when(t == VECTOR_CHUNK + 1)
    def _():
        from_image_order(acc, dr)

    @pl.when(t == VECTOR_CHUNK + 2)
    def _():
        def narrow(r, n):
            xd[pl.ds(r, n), :] = joined(dr, r, n).astype(BF)
        row_tiles(narrow)
        store.start()

    @pl.when(t == QB_GRID - 1)
    def _():
        store.wait()


BACK_TILES = -(-TAIL // ROWS // 3)


def qkvb_call(xim, dr, gain, vec, ht, dqkv, w):
    hbm = pl.BlockSpec(memory_space=pl.ANY)
    now = lambda i: jnp.minimum(i, QB_STEPS - 1)
    return pl.pallas_call(
        qkvb_kernel,
        grid=(QB_GRID,),
        in_specs=[hbm, hbm, whole(1, WIDTH), whole(VECTOR_ROWS, WIDTH),
                  whole(WIDTH, TOKENS, pipeline_mode=pl.Buffered(1)), by_cols(TOKENS, QB_N, now), by_cols(WIDTH, QB_N, now)],
        out_specs=[hbm, by_cols(WIDTH // PARTS, QB_N, lambda i: jnp.clip(i - 1 - QUAD * QKV_SUM.stride, 0, QB_STEPS - 1)),
                   whole(VECTOR_ROWS, WIDTH // PARTS)],
        out_shape=[jax.ShapeDtypeStruct((TOKENS, WIDTH), BF), jax.ShapeDtypeStruct((WIDTH // PARTS, QKV), F32),
                   jax.ShapeDtypeStruct((VECTOR_ROWS, WIDTH // PARTS), F32)],
        scratch_shapes=[pltpu.VMEM((TOKENS, WIDTH), F32), pltpu.VMEM((LANES, TOKENS, LANE), F32), pltpu.VMEM((TOKENS, WIDTH), BF),
                        pltpu.VMEM((LANE, WIDTH), F32), pltpu.VMEM((WIDTH // PARTS, QB_N), F32), pltpu.VMEM((16, WIDTH), F32), pltpu.SemaphoreType.DMA((2,))]
                       + QKV_SUM.scratch(),
        compiler_params=comm_params(2),
        cost_estimate=cost(QUAD * TOKENS * WIDTH * QKV, 80_000_000),
        name="qkvb",
    )(xim, dr, gain, vec, ht, dqkv, w)


def to_steps(v):
    rows = v.shape[0]
    return v.reshape(rows, PARTS, MLP_STEPS, UNITS).swapaxes(1, 2).reshape(rows, FFN)


def from_steps(v):
    rows = v.shape[0]
    return v.reshape(rows, MLP_STEPS, PARTS, UNITS).swapaxes(1, 2).reshape(rows, FFN)


def solution(mesh):
    specs = (P("fsdp"),) * 14

    def device_step(resid_in, grad_out, ln1_gain, ln1_bias, qkv_weight, qkv_bias, out_weight, out_bias,
                    ln2_gain, ln2_bias, fc_weight, fc_bias, proj_weight, proj_bias):
        rows = jnp.concatenate([ln1_gain, ln1_bias, qkv_bias, out_bias, ln2_gain, ln2_bias, fc_bias, proj_bias]).reshape(-1, SHARD)
        rows = jnp.pad(rows, ((0, VECTOR_ROWS - len(rows)), (0, LANE - SHARD)))
        x = resid_in.transpose(1, 0, 2).reshape(TOKENS, WIDTH)
        dy = grad_out.transpose(1, 0, 2).reshape(TOKENS, WIDTH)
        xim, h, ht, rows, wq, wo = open_call(x, rows, qkv_weight, out_weight)
        wq, wo = wq.reshape(WIDTH, QKV), wo.reshape(WIDTH, WIDTH)
        bo, g2, b2 = rows[5:6], rows[6:7], rows[7:8]
        joint = lambda v: v.reshape(-1, PARTS, SHARD).swapaxes(0, 1).reshape(1, -1)
        qkv, wf = qkv_call(h, wq, joint(rows[2:5]), to_steps(fc_weight.astype(BF)))
        o, r, top, inv, wp = attn_call(qkv, xim, wo, bo, proj_weight)
        y, dr, dr16, dwf, dwp, dbf, small = mlp_call(r, dy, g2, b2, rows[12:13], wf.reshape(WIDTH, FFN), wp, to_steps(joint(rows[8:12])))
        do, dwo = outb_call(dr16, o, wo)
        dqkv, dbq, dwo = attn_back_call(qkv, do, top, inv, dwo)
        owned = lambda v: v.reshape(PARTS, -1, WIDTH // PARTS).swapaxes(0, 1).reshape(-1, WIDTH)
        vec = jnp.concatenate([jnp.sum(small.reshape(4, 8, WIDTH), axis=1), owned(dbq), owned(from_steps(dbf))])
        vec = jnp.pad(vec, ((0, VECTOR_ROWS - len(vec)), (0, 0)))
        dx, dwq, vec = qkvb_call(xim, dr, rows[:1], vec, ht, dqkv, wq)
        dg2, db2, dbp, dbo = vec[:4]
        dbq, dbf = vec[4:7].reshape(-1), vec[7:11].reshape(-1)
        dg1, db1 = vec[VECTOR_ROWS - 2:]
        dwf = from_steps(dwf)
        unturn = lambda t: t.reshape(SEQ, IMAGES, WIDTH).transpose(1, 0, 2)
        return (unturn(y), unturn(dx), dg1, db1, dwq, dbq, dwo, dbo, dg2, db2, dwf, dbf, dwp, dbp)

    return jax.shard_map(device_step, mesh=mesh, in_specs=specs, out_specs=specs, check_vma=False)
```

```python
import itertools
import math
import jax, jax.numpy as jnp
from jax import lax
from jax.experimental import pallas as pl
from jax.experimental.pallas import tpu as pltpu
from jax.sharding import PartitionSpec as P

BF, F32 = jnp.bfloat16, jnp.float32
IMAGES, SEQ, WIDTH, FFN, HEADS, HEAD = 8, 257, 1280, 5120, 16, 80
MAIN = SEQ - 1
TOKENS = IMAGES * SEQ
TAIL = IMAGES * MAIN
LN_EPS = 1e-5
VMEM_MAX = 67043328
LANE, SUBLANE, QUAD, QKV = 128, 8, 4, 3 * WIDTH
ALL = ...
LANES = WIDTH // LANE
ROWS = 32


def dot(a, b):
    return jnp.dot(a, b, preferred_element_type=F32)


def dot_nt(a, b):
    return lax.dot_general(a, b, (((1,), (1,)), ((), ())), preferred_element_type=F32)


def dot_tn(a, b):
    return lax.dot_general(a, b, (((0,), (0,)), ((), ())), preferred_element_type=F32)


def col_sum(v):
    return jnp.sum(v, axis=0, keepdims=True)


def col_max(v):
    return jnp.max(v, axis=0, keepdims=True)


def row_sum(v):
    return jnp.sum(v, axis=-1, keepdims=True)


def row_mean(v):
    return row_sum(v) * (1.0 / WIDTH)


def clear(*refs):
    for ref in refs:
        ref[ALL] = jnp.zeros_like(ref)


def step_id():
    return pl.program_id(0)


def cost(flops, bytes_accessed, transcendentals=0):
    return pl.CostEstimate(flops=flops, bytes_accessed=bytes_accessed, transcendentals=transcendentals)


def eights(v):
    return jnp.sum(v.reshape(v.shape[0] // SUBLANE, SUBLANE, v.shape[1]), axis=0)


def whole(*shape, **kw):
    return pl.BlockSpec(shape, lambda *i: (0,) * len(shape), **kw)


def by_cols(rows, cols, at=lambda i: i):
    return pl.BlockSpec((rows, cols), lambda i: (0, at(i)))


def by_rows(rows, cols, at=lambda i: i):
    return pl.BlockSpec((rows, cols), lambda i: (at(i), 0))


def steps(first, wide):
    return slice(first * wide, (first + 1) * wide)


def norm_stats(values):
    mean = row_mean(values)
    centered = values - mean
    inv = lax.rsqrt(row_mean(centered * centered) + LN_EPS)
    return centered * inv, inv


BLOCKS = [slice(a, b) for a, b in ((0, 512), (512, 1024), (1024, 1536), (1536, TOKENS))]


def row_tiles(body, step=LANE):
    def loop(i, carry):
        body(pl.multiple_of(i * step, step), step)
        return carry
    lax.fori_loop(0, TAIL // step, loop, 0)
    body(TAIL, IMAGES)


def to_image_order(wide, place, step=LANE):
    per = MAIN // step
    def loop(i, carry):
        first = (i % per) * (step * IMAGES) + i // per
        rows = [wide[c, pl.ds(first, step, stride=IMAGES), :] for c in range(LANES)]
        place(pl.multiple_of(i * step, step), step, jnp.concatenate(rows, axis=1))
        return carry
    lax.fori_loop(0, IMAGES * per, loop, 0)
    place(TAIL, IMAGES, joined(wide, TAIL, IMAGES))


def from_image_order(values, wide):
    def loop(i, carry):
        rows = values[pl.ds(pl.multiple_of(i * LANE, LANE), LANE), :]
        for c in range(LANES):
            wide[c, pl.ds((i % 2) * (LANE * IMAGES) + i // 2, LANE, stride=IMAGES), :] = rows[:, steps(c, LANE)]
        return carry
    lax.fori_loop(0, 2 * IMAGES, loop, 0)
    put(wide, TAIL, IMAGES, values[pl.ds(TAIL, IMAGES), :])


def joined(wide, r, n):
    return jnp.concatenate([wide[c, pl.ds(r, n), :] for c in range(LANES)], axis=1)


def put(wide, r, n, values):
    for c in range(LANES):
        wide[c, pl.ds(r, n), :] = values[:, steps(c, LANE)]


def norm_back(dn, hat, inv, gain):
    dhat = dn * gain
    m1 = row_mean(dhat)
    m2 = row_mean(dhat * hat)
    return inv * (dhat - m1 - hat * m2)


ORDERS = ((2, 1, 0), (1, 0, 2), (0, 2, 1))


class Links:
    def find(self, send, recv):
        self.send, self.recv = send, recv
        me = lax.axis_index("fsdp")
        self.core = me % 2
        self.at = (me // SUBLANE, (me // QUAD) % 2, (me // 2) % 2)
        self.other_core = me + 1 - 2 * self.core
        self.other = [me + step - 2 * step * place for step, place in zip((SUBLANE, QUAD, 2), self.at)]
        return self

    def meet(self):
        barrier = pltpu.get_barrier_semaphore()
        devices = (self.other_core, *self.other)
        for device in devices:
            pl.semaphore_signal(barrier, inc=1, device_id=(device,), device_id_type=pl.DeviceIdType.MESH)
        pl.semaphore_wait(barrier, len(devices))

    def remote(self, src, dst, sem, device):
        return pltpu.make_async_remote_copy(src_ref=src, dst_ref=dst, send_sem=self.send.at[sem], recv_sem=self.recv.at[sem],
                                            device_id=(device,), device_id_type=pl.DeviceIdType.MESH)


class Gather(Links):
    COUNT = 2

    def __init__(self, rows, cols, cuts):
        self.rows, self.cols, self.cuts = rows, cols, cuts
        self.parts = range(len(cuts) - 1)
        self.full_shape = jax.ShapeDtypeStruct((2, 2, 2, 2, rows, cols), BF)

    def scratch(self):
        return [pltpu.SemaphoreType.DMA((SEMS,))] * self.COUNT

    def bind(self, own, full, sems):
        self.own, self.full = own, full
        return self.find(*sems)

    def region(self, part, known, arrived=False):
        done = ORDERS[part][:known]
        place = [slice(None) if a in done else self.at[a] for a in range(3)]
        if arrived:
            place[done[-1]] = 1 - self.at[done[-1]]
        return (*place, self.core, slice(None), pl.ds(self.cuts[part], self.cuts[part + 1] - self.cuts[part]))

    def hop(self, stage, part):
        where = self.full.at[self.region(part, stage - 1)]
        source = self.own.at[self.region(part, 0)[-2:]] if stage == 1 else where
        return self.remote(source, where, QUAD * stage + part, self.other[ORDERS[part][stage - 1]])

    def forward(self, stage, part):
        if stage == 0:
            return self.remote(self.own, self.full.at[(*self.at, self.core)], 0, self.other_core)
        where = self.full.at[self.region(part, stage, True)]
        return self.remote(where, where, QUAD * (stage + 3) + part, self.other_core)

    def keep(self):
        return pltpu.make_async_copy(self.own, self.full.at[(*self.at, self.core)], self.send.at[1])

    def begin(self):
        for part in self.parts:
            self.hop(1, part).start()
        self.forward(0, 0).start()
        self.keep().start()

    def turn(self, stage):
        if stage == 1:
            self.keep().wait()
        for part in self.parts:
            self.hop(stage, part).wait()
            if stage < 3:
                self.hop(stage + 1, part).start()
        for part in self.parts:
            self.forward(stage, part).start()

    def end(self):
        self.forward(0, 0).wait()
        for stage in range(1, QUAD):
            for part in self.parts:
                self.forward(stage, part).wait()


SEMS = 28


class Exchange(Links):
    def __init__(self, rows, cols, cuts, along, stride=1, spare=0):
        self.rows, self.cols, self.stride = rows, cols, stride
        self.slots, self.locals = 3 * stride + spare, 1 + stride
        self.blocks = (2, 2, 2, 2, rows, cols)
        self.parts = [((slice(a, b), slice(None)) if along == 0 else (slice(None), slice(a, b))) for a, b in zip(cuts, cuts[1:])]
        self.shapes = [((b - a, cols) if along == 0 else (rows, b - a)) for a, b in zip(cuts, cuts[1:])]

    def scratch(self):
        two = (2, 2, 2)
        out = [pltpu.VMEM((self.locals, *self.blocks), F32), pltpu.VMEM((self.slots, *two, self.rows, self.cols), F32)]
        for axes in (2, 1, 0):
            out += [pltpu.VMEM((self.slots, *two[:axes], *shape), F32) for shape in self.shapes]
        return out + [pltpu.SemaphoreType.DMA((10, self.slots))] * 2

    COUNT = 13

    def bind(self, refs):
        self.local, self.pair = refs[0], refs[1]
        self.held = [None, refs[2:5], refs[5:SUBLANE], refs[SUBLANE:11]]
        return self.find(*refs[11:])

    def index(self, stage, part, side):
        order = ORDERS[part]
        left = [a for a in range(3) if a not in order[:stage - 1]]
        axis = order[stage - 1]
        where = self.at[axis] if side else 1 - self.at[axis]
        return tuple(where if a == axis else slice(None) for a in left)

    def copy(self, stage, part, c):
        slot = c % self.slots
        if stage == 0:
            return self.remote(self.local.at[c % self.locals, :, :, :, 1 - self.core], self.pair.at[slot], (0, slot), self.other_core)
        source = self.pair if stage == 1 else self.held[stage - 1][part]
        tail = self.parts[part] if stage == 1 else ()
        return self.remote(source.at[(slot, *self.index(stage, part, False), *tail)], self.held[stage][part].at[slot],
                           (3 * stage - 2 + part, slot), self.other[ORDERS[part][stage - 1]])

    def start(self, stage, c):
        for part in range(1 if stage == 0 else 3):
            self.copy(stage, part, c).start()

    def wait(self, stage, c):
        for part in range(1 if stage == 0 else 3):
            self.copy(stage, part, c).wait()

    def add(self, stage, c):
        slot = c % self.slots
        if stage == 0:
            for chip in itertools.product(range(2), repeat=3):
                self.pair[(slot, *chip)] += self.local[(c % self.locals, *chip, self.core)]
            return
        for part in range(3):
            source = self.pair if stage == 1 else self.held[stage - 1][part]
            tail = self.parts[part] if stage == 1 else ()
            for place in itertools.product(range(2), repeat=3 - stage):
                free = iter(place)
                kept = tuple(next(free) if isinstance(i, slice) else i for i in self.index(stage, part, True))
                self.held[stage][part][(slot, *place)] += source[(slot, *kept, *tail)]

    def result(self, c, out_ref):
        for part in range(3):
            out_ref[self.parts[part]] = self.held[3][part][c % self.slots]

    def put_local(self, c, values):
        self.local[c % self.locals] = values.reshape(self.blocks)


def comm_params(n):
    return pltpu.CompilerParams(dimension_semantics=("arbitrary",), vmem_limit_bytes=VMEM_MAX, collective_id=n, has_side_effects=True)


def advance(exchanges, t, exists, emit):
    for stage in (3, 2, 1, 0):
        c = t - 1 - (stage + 1) * exchanges[0].stride

        @pl.when(exists(c))
        def _():
            for n, exchange in enumerate(exchanges):
                exchange.wait(stage, c)
                exchange.add(stage, c)
                if stage < 3:
                    exchange.start(stage + 1, c)
                else:
                    emit(n, exchange, c)

    @pl.when(exists(t - 1))
    def _():
        for exchange in exchanges:
            exchange.start(0, t - 1)


def first_chunks(n):
    return lambda c: (c >= 0) & (c < n)


DRAIN = 5


PARTS = 16
SHARD = WIDTH // PARTS
VECTOR_ROWS = PARTS
MLP_F = MAIN
UNITS = MLP_F // PARTS
MLP_STEPS = FFN // MLP_F
QKV_ALL = Gather(SHARD, QKV, (0, WIDTH, 2 * WIDTH, QKV))
WIDTH_CUTS = (0, 384, 896, WIDTH)
EARLY = 10
FC_ALL = Gather(SHARD, EARLY * MLP_F, (0, 768, 1664, EARLY * MLP_F))
PROJ_ALL = Gather(EARLY * UNITS, WIDTH, WIDTH_CUTS)
FC_STEP = Gather(SHARD, MLP_F, (0, LANE, MLP_F))
PROJ_STEP = Gather(UNITS, WIDTH, WIDTH_CUTS)
OUT_ALL = Gather(SHARD, WIDTH, WIDTH_CUTS)
VECTOR_ALL = Gather(SHARD, LANE, (0, LANE))


def open_kernel(x_hbm, rows_ref, wq_ref, xim_hbm, h_hbm, ht_hbm, vec_ref, wq_full,
                x, wide, h, ht, rows, vec_own, vec_full, wq_own, sems, *comm):
    loads = pltpu.make_async_copy(x_hbm, x, sems.at[0])
    loads.start()
    clear(rows)
    rows[:VECTOR_ROWS, :] = rows_ref[ALL]
    vec_own[ALL] = rows[ALL].T[:SHARD, :].astype(BF)
    wq_own[ALL] = wq_ref[ALL].astype(BF)
    vectors, weights = VECTOR_ALL.bind(vec_own, vec_full, comm[:2]), QKV_ALL.bind(wq_own, wq_full, comm[2:])
    gathers = (vectors, weights)
    vectors.meet()
    for gather in gathers:
        gather.begin()
    loads.wait()

    def widen(r, n):
        put(wide, r, n, x[pl.ds(r, n), :].astype(F32))
    row_tiles(widen)
    for gather in gathers:
        gather.turn(1)

    def place(r, n, values):
        x[pl.ds(r, n), :] = values.astype(BF)
    to_image_order(wide, place)
    for gather in gathers:
        gather.turn(2)
    vectors.turn(3)
    vectors.end()
    vec_ref[ALL] = vec_full[ALL].reshape(WIDTH, LANE).astype(F32).T[:VECTOR_ROWS, :]
    gain, bias = vec_ref[0:1, :], vec_ref[1:2, :]

    def norm(r, n):
        hat, _ = norm_stats(x[pl.ds(r, n), :].astype(F32))
        h[pl.ds(r, n), :] = (hat * gain + bias).astype(BF)
    row_tiles(norm, ROWS)
    for b in range(IMAGES):
        ht[:, steps(b, MAIN)] = h[steps(b, MAIN), :].T
    ht[:, TAIL:TOKENS] = h[TAIL:TOKENS, :].T
    stores = [pltpu.make_async_copy(src, dst, sems.at[i]) for i, (src, dst) in enumerate(((x, xim_hbm), (h, h_hbm), (ht, ht_hbm)))]
    for cp in stores:
        cp.start()
    weights.turn(3)
    weights.end()
    for cp in stores:
        cp.wait()


def open_call(x, rows, wq):
    hbm, vmem = pl.BlockSpec(memory_space=pl.ANY), pl.BlockSpec(memory_space=pltpu.VMEM)
    return pl.pallas_call(
        open_kernel,
        in_specs=[hbm, vmem, vmem],
        out_specs=[hbm, hbm, hbm, vmem, hbm],
        out_shape=[jax.ShapeDtypeStruct((TOKENS, WIDTH), BF), jax.ShapeDtypeStruct((TOKENS, WIDTH), BF),
                   jax.ShapeDtypeStruct((WIDTH, TOKENS), BF), jax.ShapeDtypeStruct((VECTOR_ROWS, WIDTH), F32),
                   QKV_ALL.full_shape],
        scratch_shapes=[pltpu.VMEM((TOKENS, WIDTH), BF), pltpu.VMEM((LANES, TOKENS, LANE), F32), pltpu.VMEM((TOKENS, WIDTH), BF),
                        pltpu.VMEM((WIDTH, TOKENS), BF), pltpu.VMEM((LANE, LANE), F32), pltpu.VMEM((SHARD, LANE), BF),
                        pltpu.VMEM(VECTOR_ALL.full_shape.shape, BF), pltpu.VMEM((SHARD, QKV), BF),
                        pltpu.SemaphoreType.DMA((3,))] + VECTOR_ALL.scratch() + QKV_ALL.scratch(),
        compiler_params=pltpu.CompilerParams(vmem_limit_bytes=VMEM_MAX, collective_id=3, has_side_effects=True),
        cost_estimate=cost(1_000_000_000, 60_000_000),
        name="open",
    )(x, rows, wq)


QKV_N = 768


def qkv_kernel(h_ref, w_ref, wb_ref, fc_ref, out_ref, qkv_ref, fc_full, out_full, out_own, *sems):
    t, last = step_id(), pl.num_programs(0) - 1
    gathers = OUT_ALL.bind(out_own, out_full, sems[:2]), FC_ALL.bind(fc_ref, fc_full, sems[2:])

    @pl.when(t == 0)
    def _():
        out_own[ALL] = out_ref[ALL].astype(BF)
        gathers[0].meet()
        for gather in gathers:
            gather.begin()

    for stage in (1, 2):
        @pl.when(t == stage)
        def _():
            for gather in gathers:
                gather.turn(stage)
    for rows in BLOCKS:
        qkv_ref[rows, :] = (dot(h_ref[rows, :], w_ref[ALL]) + wb_ref[ALL]).astype(BF)

    @pl.when(t == last)
    def _():
        for gather in gathers:
            gather.turn(3)
        for gather in gathers:
            gather.end()


def qkv_call(h, w, wb, fc, out):
    hbm = pl.BlockSpec(memory_space=pl.ANY)
    return pl.pallas_call(
        qkv_kernel,
        grid=(QKV // QKV_N,),
        in_specs=[whole(TOKENS, WIDTH, pipeline_mode=pl.Buffered(1)), by_cols(WIDTH, QKV_N), by_cols(1, QKV_N),
                  whole(*fc.shape), whole(*out.shape)],
        out_specs=[by_cols(TOKENS, QKV_N), hbm, hbm],
        out_shape=[jax.ShapeDtypeStruct((TOKENS, QKV), BF), FC_ALL.full_shape, OUT_ALL.full_shape],
        scratch_shapes=[pltpu.VMEM(out.shape, BF)] + OUT_ALL.scratch() + FC_ALL.scratch(),
        compiler_params=comm_params(QUAD),
        cost_estimate=cost(2 * TOKENS * WIDTH * QKV, 60_000_000),
        name="qkv",
    )(h, w, wb, fc, out)


ROW_CUTS = (0, 24, 48, 80)
FC_SUM = Exchange(SHARD, MLP_F, ROW_CUTS, 0)
PROJ_SUM = Exchange(UNITS, WIDTH, WIDTH_CUTS, 1)
CDF_P = 0.33
CDF_C = (0.1326322871417956, 0.11939570820799192, 0.18103829560051796, -0.08904113226212501,
         0.33075919469138065, -0.22023738432274684, 0.0454530347223348)


def gelu_pair(u):
    bell = jnp.exp(u * u * -0.5)
    t = 1.0 / (1.0 + CDF_P * jnp.abs(u))
    poly = CDF_C[6]
    for c in CDF_C[5::-1]:
        poly = poly * t + c
    tail = poly * t * bell
    cdf = jnp.where(u < 0.0, tail, 1.0 - tail)
    return u * cdf, cdf + u * bell * ((2.0 * math.pi) ** -0.5)


def late_weights(step, own, full, now, sems, *comm):
    def gathers(c):
        slot = c % GATHER_SLOTS
        return [kind.bind(own[i].at[c - EARLY], full[i].at[c - EARLY], [sem.at[slot] for sem in comm[2 * i:2 * i + 2]])
                for i, kind in enumerate((FC_STEP, PROJ_STEP))]

    def fetches(c):
        return [pltpu.make_async_copy(full[i].at[c - EARLY], now[i].at[c % 2], sems.at[i]) for i in range(2)]

    @pl.when((step >= EARLY) & (step < MLP_STEPS))
    def _():
        for cp in fetches(step):
            cp.wait()
    for ahead in range(1, 6):
        c = step + ahead

        @pl.when((c >= EARLY) & (c < MLP_STEPS))
        def _():
            for gather in gathers(c):
                if ahead == 1:
                    gather.end()
                elif ahead == 5:
                    gather.begin()
                else:
                    gather.turn(5 - ahead)
            if ahead == 1:
                for cp in fetches(c):
                    cp.start()


GATHER_SLOTS = 6


def mlp_kernel(r_hbm, dy_hbm, gain_ref, bias_ref, pb_ref, fc_ref, proj_ref, fcb_ref, fc_own, proj_own,
               y_hbm, dr_hbm, dr16_hbm, dfc_ref, dproj_ref, dfcb_ref, small_ref, fc_full, proj_full,
               n2, dy, y_acc, dn_acc, g, du, fc_now, proj_now, ua, ub, da, db, sem, sems, *comm):
    step = step_id()
    by_row, by_col = FC_SUM.bind(comm[:Exchange.COUNT]), PROJ_SUM.bind(comm[Exchange.COUNT:2 * Exchange.COUNT])

    @pl.when(step == 0)
    def _():
        by_row.meet()
        cp = pltpu.make_async_copy(dy_hbm, n2, sem)
        cp.start()
        cp.wait()

        def widen(r, n):
            put(dn_acc, r, n, n2[pl.ds(r, n), :].astype(F32))
        row_tiles(widen)
        cp = pltpu.make_async_copy(r_hbm, n2, sem)
        cp.start()

        def place(r, n, values):
            dy[pl.ds(r, n), :] = values.astype(BF)
        to_image_order(dn_acc, place, ROWS)
        cp.wait()
        gain, bias, pb = gain_ref[ALL], bias_ref[ALL], pb_ref[ALL]

        def norm(r, n):
            wide_r = n2[pl.ds(r, n), :].astype(F32)
            hat, _ = norm_stats(wide_r)
            n2[pl.ds(r, n), :] = (hat * gain + bias).astype(BF)
            y_acc[pl.ds(r, n), :] = wide_r + pb
            put(dn_acc, r, n, jnp.zeros((n, WIDTH), F32))
        row_tiles(norm, ROWS)
        clear(small_ref)

    outs = (dfc_ref, dproj_ref)
    late_weights(step, (fc_own, proj_own), (fc_full, proj_full), (fc_now, proj_now), sems, *comm[2 * Exchange.COUNT:])
    advance((by_row, by_col), step, first_chunks(MLP_STEPS), lambda n, exchange, c: exchange.result(c, outs[n]))

    @pl.when(step < MLP_STEPS)
    def _():
        slot = step % 2

        @pl.when(step < EARLY)
        def _():
            fc_now[slot] = fc_ref[ALL].reshape(FC_STEP.full_shape.shape)
            proj_now[slot] = proj_ref[ALL].reshape(PROJ_STEP.full_shape.shape)
        fcb = fcb_ref[ALL]
        fc, proj = fc_now[slot].reshape(WIDTH, MLP_F), proj_now[slot].reshape(MLP_F, WIDTH)
        bias_sum = jnp.zeros((SUBLANE, MLP_F), F32)
        tiles = [(b * MAIN, MAIN) for b in range(IMAGES - 1)] + [((IMAGES - 1) * MAIN, MAIN + IMAGES)]
        pairs = ((ua, da), (ub, db))

        def products(k):
            r, n = tiles[k]
            u_s, d_s = pairs[k % 2]
            u_s[0:n, :] = dot(n2[r:r + n, :], fc)
            d_s[0:n, :] = dot_nt(dy[r:r + n, :], proj)

        def pointwise(k, total):
            r, n = tiles[k]
            u_s, d_s = pairs[k % 2]
            value, slope = gelu_pair(u_s[0:n, :] + fcb)
            g[r:r + n, :] = value.astype(BF)
            grad = d_s[0:n, :] * slope
            du[r:r + n, :] = grad.astype(BF)
            return total + eights(grad)

        products(0)
        for k in range(1, IMAGES):
            products(k)
            bias_sum = pointwise(k - 1, bias_sum)
        bias_sum = pointwise(IMAGES - 1, bias_sum)
        dfcb_ref[ALL] = col_sum(bias_sum)
        y_acc[ALL] += dot(g[ALL], proj)
        for c in range(LANES // 2):
            part = dot_nt(du[ALL], fc[steps(c, MAIN), :])
            dn_acc[2 * c] += part[:, :LANE]
            dn_acc[2 * c + 1] += part[:, LANE:]
        by_col.put_local(step, dot_tn(g[ALL], dy[ALL]))
        by_row.put_local(step, dot_tn(n2[ALL], du[ALL]))

    out_copies = [pltpu.make_async_copy(dn_acc, dr_hbm, sem), pltpu.make_async_copy(n2, dr16_hbm, sem)]
    y_copy = pltpu.make_async_copy(dy, y_hbm, sem)

    @pl.when(step == MLP_STEPS)
    def _():
        cp = pltpu.make_async_copy(r_hbm, n2, sem)
        cp.start()
        cp.wait()
        gain = gain_ref[ALL]

        def back(r, n):
            hat, inv = norm_stats(n2[pl.ds(r, n), :].astype(F32))
            dn = joined(dn_acc, r, n)
            wide_dy = dy[pl.ds(r, n), :].astype(F32)
            dr = wide_dy + norm_back(dn, hat, inv, gain)
            put(dn_acc, r, n, dr)
            n2[pl.ds(r, n), :] = dr.astype(BF)
            for i, v in enumerate((dn * hat, dn, wide_dy, dr)):
                small_ref[steps(i, SUBLANE), :] += eights(v)
        row_tiles(back, ROWS)
        for cp in out_copies:
            cp.start()

    @pl.when(step == MLP_STEPS + 1)
    def _():
        for cp in out_copies:
            cp.wait()
        from_image_order(y_acc, dn_acc)

    @pl.when(step == MLP_STEPS + 2)
    def _():
        def narrow(r, n):
            dy[pl.ds(r, n), :] = joined(dn_acc, r, n).astype(BF)
        row_tiles(narrow)
        y_copy.start()

    @pl.when(step == MLP_STEPS + 3)
    def _():
        y_copy.wait()


def mlp_call(r, dy, gain, bias, pb, fc, proj, fcb, fc_own, proj_own):
    hbm = pl.BlockSpec(memory_space=pl.ANY)
    vec = whole(1, WIDTH)
    now = lambda i: jnp.minimum(i, MLP_STEPS - 1)
    early = lambda i: jnp.minimum(i, EARLY - 1)
    done = lambda i: jnp.maximum(i - DRAIN, 0)
    return pl.pallas_call(
        mlp_kernel,
        grid=(MLP_STEPS + DRAIN,),
        in_specs=[hbm, hbm, vec, vec, vec, by_cols(WIDTH, MLP_F, early),
                  pl.BlockSpec((PARTS, None, UNITS, WIDTH), lambda i: (0, early(i), 0, 0)),
                  by_cols(1, MLP_F, now), whole(*fc_own.shape, pipeline_mode=pl.Buffered(1)),
                  whole(*proj_own.shape, pipeline_mode=pl.Buffered(1))],
        out_specs=[hbm, hbm, hbm, by_cols(SHARD, MLP_F, done),
                   by_rows(UNITS, WIDTH, done),
                   by_cols(1, MLP_F, now), whole(32, WIDTH), hbm, hbm],
        out_shape=[jax.ShapeDtypeStruct((TOKENS, WIDTH), BF), jax.ShapeDtypeStruct((LANES, TOKENS, LANE), F32),
                   jax.ShapeDtypeStruct((TOKENS, WIDTH), BF), jax.ShapeDtypeStruct((SHARD, FFN), F32),
                   jax.ShapeDtypeStruct((FFN // PARTS, WIDTH), F32),
                   jax.ShapeDtypeStruct((1, FFN), F32), jax.ShapeDtypeStruct((32, WIDTH), F32),
                   *(jax.ShapeDtypeStruct((MLP_STEPS - EARLY, *kind.full_shape.shape), BF) for kind in (FC_STEP, PROJ_STEP))],
        scratch_shapes=[pltpu.VMEM((TOKENS, WIDTH), BF), pltpu.VMEM((TOKENS, WIDTH), BF),
                        pltpu.VMEM((TOKENS, WIDTH), F32), pltpu.VMEM((LANES, TOKENS, LANE), F32),
                        pltpu.VMEM((TOKENS, MLP_F), BF), pltpu.VMEM((TOKENS, MLP_F), BF),
                        *(pltpu.VMEM((2, *kind.full_shape.shape), BF) for kind in (FC_STEP, PROJ_STEP))]
                       + [pltpu.VMEM((MAIN + IMAGES, MLP_F), F32)] * QUAD + [pltpu.SemaphoreType.DMA, pltpu.SemaphoreType.DMA((2,))]
                       + FC_SUM.scratch() + PROJ_SUM.scratch() + [pltpu.SemaphoreType.DMA((GATHER_SLOTS, SEMS))] * QUAD,
        compiler_params=comm_params(0),
        cost_estimate=cost(12 * TOKENS * WIDTH * FFN, 150_000_000, TOKENS * FFN),
        name="mlp",
    )(r, dy, gain, bias, pb, fc, proj.reshape(PARTS, EARLY, UNITS, WIDTH), fcb, fc_own, proj_own)


SCALE = HEAD ** -0.5
ATTN_COST = cost(40_000_000_000, 50_000_000, 8_400_000)


def window(h):
    first = min(HEAD * h // LANE * LANE, WIDTH - MAIN)
    wide = LANE if HEAD * h + HEAD <= first + LANE else MAIN
    return first, wide, HEAD * h - first


def lane_mask(h):
    first, wide, off = window(h)
    lane = lax.broadcasted_iota(jnp.int32, (MAIN, wide), 1)
    return (lane >= off) & (lane < off + HEAD)


def thirds(ref, rows=slice(None)):
    return [ref[rows, steps(i, WIDTH)] for i in range(3)]


def head_rows():
    lane = lax.broadcasted_iota(jnp.int32, (HEADS, WIDTH), 1)
    row = lax.broadcasted_iota(jnp.int32, (HEADS, WIDTH), 0)
    return (lane // HEAD == row).astype(F32)


def tail_softmax(s, s_self):
    m = jnp.maximum(jnp.max(s, axis=1, keepdims=True), s_self)
    e = jnp.exp((s - m) * SCALE)
    e_self = jnp.exp((s_self - m) * SCALE)
    inv = 1.0 / (row_sum(e) + e_self)
    return e * inv, e_self * inv


def attn_kernel(qkv_ref, qkvt_ref, x_ref, xt_ref, w_ref, wb_ref, proj_ref, o_hbm, r_hbm, max_ref, inv_ref, full,
                tails, o_tail, o_t, ptail, o_buf, r_buf, sems, own, *comm):
    b, last = step_id(), pl.num_programs(0) - 1
    slot = b % 2
    gather = PROJ_ALL.bind(own, full, comm)

    @pl.when(b == 0)
    def _():
        tails[ALL] = qkvt_ref[ALL].astype(F32)
        own[ALL] = proj_ref[ALL].astype(BF)
        gather.meet()
        gather.begin()

    @pl.when(b == 1)
    def _():
        gather.turn(1)

    @pl.when(b == 2)
    def _():
        gather.turn(2)

    @pl.when(b == QUAD)
    def _():
        gather.turn(3)

    heads = head_rows()
    q_t, k_t, v_t = (heads * z for z in thirds(tails, pl.ds(b, 1)))
    q, k, v = thirds(qkv_ref)

    p, p_self = tail_softmax(dot_nt(q_t.astype(BF), k), row_sum(q_t * k_t))
    mixed = dot(p.astype(BF), v) * heads + p_self.astype(BF).astype(F32) * v_t
    o_tail[pl.ds(b, 1), :] = col_sum(mixed)

    s_tail = dot_nt(k_t.astype(BF), q)
    v_turned = v.T
    for h in range(HEADS):
        first, wide, _ = window(h)
        q_h = jnp.where(lane_mask(h), qkv_ref[:, first:first + wide], jnp.zeros((), BF))
        s = dot_nt(qkv_ref[:, pl.ds(WIDTH + first, wide)], q_h)
        top = jnp.maximum(col_max(s), s_tail[steps(h, 1), :])
        e = jnp.exp((s - top) * SCALE)
        e_tail = jnp.exp((s_tail[steps(h, 1), :] - top) * SCALE)
        inv = 1.0 / (col_sum(e) + e_tail)
        max_ref[0, steps(h, 1), :] = top
        inv_ref[0, steps(h, 1), :] = inv
        ptail[steps(h, 1), :] = e_tail * inv
        o_t[steps(h, HEAD), :] = dot(v_turned[steps(h, HEAD), :], (e * inv).astype(BF))

    @pl.when(b >= 2)
    def _():
        out_copy(o_buf, o_hbm, slot, b - 2, sems, 0).wait()
        out_copy(r_buf, r_hbm, slot, b - 2, sems, 1).wait()

    o = (o_t[ALL].T + dot_tn(ptail[ALL].astype(BF), v_t.astype(BF))).astype(BF)
    o_buf[slot] = o
    r_buf[slot] = (x_ref[ALL].astype(F32) + dot(o, w_ref[ALL]) + wb_ref[ALL]).astype(BF)
    out_copy(o_buf, o_hbm, slot, b, sems, 0).start()
    out_copy(r_buf, r_hbm, slot, b, sems, 1).start()

    @pl.when(b == last)
    def _():
        for buf, hbm, n in ((o_buf, o_hbm, 0), (r_buf, r_hbm, 1)):
            out_copy(buf, hbm, 1 - slot, b - 1, sems, n).wait()
        o = o_tail[ALL].astype(BF)
        o_buf[1 - slot, 0:IMAGES, :] = o
        r_buf[1 - slot, 0:IMAGES, :] = (xt_ref[ALL].astype(F32) + dot(o, w_ref[ALL]) + wb_ref[ALL]).astype(BF)
        copies = [pltpu.make_async_copy(buf.at[1 - slot, pl.ds(0, IMAGES)], hbm.at[pl.ds(TAIL, IMAGES)], sems.at[n, 1 - slot])
                  for buf, hbm, n in ((o_buf, o_hbm, 0), (r_buf, r_hbm, 1))]
        for cp in copies:
            cp.start()
        for cp in copies:
            cp.wait()
        for buf, hbm, n in ((o_buf, o_hbm, 0), (r_buf, r_hbm, 1)):
            out_copy(buf, hbm, slot, b, sems, n).wait()
        gather.end()


def out_copy(buf, hbm, slot, b, sems, n):
    return pltpu.make_async_copy(buf.at[slot], hbm.at[pl.ds(pl.multiple_of(b * MAIN, MAIN), MAIN)], sems.at[n, slot])


def attn_call(qkv, xim, w, wb, proj):
    hbm = pl.BlockSpec(memory_space=pl.ANY)
    main = lambda n: by_rows(MAIN, n)
    tail = lambda n: by_rows(IMAGES, n, lambda i: TAIL // IMAGES)
    stat = pl.BlockSpec((1, HEADS, MAIN), lambda i: (i, 0, 0))
    return pl.pallas_call(
        attn_kernel,
        grid=(IMAGES,),
        in_specs=[main(QKV), tail(QKV), main(WIDTH), tail(WIDTH),
                  whole(WIDTH, WIDTH), whole(1, WIDTH), whole(*proj.shape)],
        out_specs=[hbm, hbm, stat, stat, hbm],
        out_shape=[jax.ShapeDtypeStruct((TOKENS, WIDTH), BF), jax.ShapeDtypeStruct((TOKENS, WIDTH), BF),
                   jax.ShapeDtypeStruct((IMAGES, HEADS, MAIN), F32), jax.ShapeDtypeStruct((IMAGES, HEADS, MAIN), F32),
                   PROJ_ALL.full_shape],
        scratch_shapes=[pltpu.VMEM((IMAGES, QKV), F32), pltpu.VMEM((IMAGES, WIDTH), F32),
                        pltpu.VMEM((WIDTH, MAIN), F32), pltpu.VMEM((HEADS, MAIN), F32),
                        pltpu.VMEM((2, MAIN, WIDTH), BF), pltpu.VMEM((2, MAIN, WIDTH), BF), pltpu.SemaphoreType.DMA((2, 2)),
                        pltpu.VMEM(proj.shape, BF)] + PROJ_ALL.scratch(),
        compiler_params=comm_params(5),
        cost_estimate=ATTN_COST,
        name="attn",
    )(qkv, qkv, xim, xim, w, wb, proj)


def outb_kernel(dr_ref, o_ref, w_ref, do_ref, dw_ref):
    n = MAIN
    c = step_id()
    do_ref[ALL] = dot_nt(dr_ref[ALL], w_ref[ALL]).astype(BF)
    dw_ref[ALL] = dot_tn(o_ref[ALL], dr_ref[:, pl.ds(pl.multiple_of(c * n, n), n)])


def outb_call(dr, o, w):
    n = MAIN
    full = whole(TOKENS, WIDTH)
    return pl.pallas_call(
        outb_kernel,
        grid=(WIDTH // n,),
        in_specs=[full, full, by_rows(n, WIDTH)],
        out_specs=[by_cols(TOKENS, n), by_cols(WIDTH, n)],
        out_shape=[jax.ShapeDtypeStruct((TOKENS, WIDTH), BF), jax.ShapeDtypeStruct((WIDTH, WIDTH), F32)],
        compiler_params=pltpu.CompilerParams(dimension_semantics=("arbitrary",), vmem_limit_bytes=VMEM_MAX),
        cost_estimate=cost(QUAD * TOKENS * WIDTH * WIDTH, 30_000_000),
        name="outb",
    )(dr, o, w)


def attn_back_kernel(qkv_ref, qkvt_ref, do_ref, dot_ref, max_ref, inv_ref, dw_ref, dqkv_hbm, dwb_ref, dwout_ref,
                     tails, do_tails, grad_tails, dq_t, dk, dv, ds_tail, buf, sems, *comm):
    b = step_id()
    by_row = FC_SUM.bind(comm)

    @pl.when(b == 0)
    def _():
        by_row.meet()
    advance((by_row,), b, first_chunks(OUT_STEPS), lambda n, exchange, c: exchange.result(c, dwout_ref))

    @pl.when(b < OUT_STEPS)
    def _():
        by_row.put_local(b, dw_ref[ALL])

    @pl.when(b < IMAGES)
    def _():
        image_back(b, qkv_ref, qkvt_ref, do_ref, dot_ref, max_ref, inv_ref, dqkv_hbm, dwb_ref,
                   tails, do_tails, grad_tails, dq_t, dk, dv, ds_tail, buf, sems)


OUT_STEPS = WIDTH // MAIN


def image_back(b, qkv_ref, qkvt_ref, do_ref, dot_ref, max_ref, inv_ref, dqkv_hbm, dwb_ref,
               tails, do_tails, grad_tails, dq_t, dk, dv, ds_tail, buf, sems):
    last = IMAGES - 1
    slot = b % 2

    @pl.when(b == 0)
    def _():
        tails[ALL] = qkvt_ref[ALL].astype(F32)
        do_tails[ALL] = dot_ref[ALL].astype(F32)
        clear(dwb_ref)

    heads = head_rows()
    q_t, k_t, v_t = (heads * z for z in thirds(tails, pl.ds(b, 1)))
    do_t = heads * do_tails[pl.ds(b, 1), :]
    q, k, v = thirds(qkv_ref)
    do = do_ref[ALL]
    q_t16, k_t16, v_t16, do_t16 = (z.astype(BF) for z in (q_t, k_t, v_t, do_t))

    p, p_self = tail_softmax(dot_nt(q_t16, k), row_sum(q_t * k_t))
    dp, dp_self = dot_nt(do_t16, v), row_sum(do_t * v_t)
    inner = row_sum(p * dp) + p_self * dp_self
    ds16 = (p * (dp - inner) * SCALE).astype(BF)
    ds_self = (p_self * (dp_self - inner) * SCALE).astype(BF).astype(F32)
    grad_q = col_sum(dot(ds16, k) * heads + ds_self * k_t)
    grad_k = ds_self * q_t
    grad_v = p_self.astype(BF).astype(F32) * do_t
    dk[ALL] = dot_tn(ds16, q_t16)
    dv[ALL] = dot_tn(p.astype(BF), do_t16)

    p_tail = jnp.exp((dot_nt(k_t16, q) - max_ref[0]) * SCALE) * inv_ref[0]
    dp_tail = dot_nt(v_t16, do)
    inner_tail = p_tail * dp_tail

    k_turned = k.T
    for h in range(HEADS):
        first, wide, _ = window(h)
        here = slice(first, first + wide)
        mask = lane_mask(h)
        q_h = jnp.where(mask, qkv_ref[:, here], jnp.zeros((), BF))
        do_h = jnp.where(mask, do_ref[:, here], jnp.zeros((), BF))
        s = dot_nt(qkv_ref[:, pl.ds(WIDTH + first, wide)], q_h)
        dp = dot_nt(qkv_ref[:, pl.ds(2 * WIDTH + first, wide)], do_h)
        p = jnp.exp((s - max_ref[0, steps(h, 1), :]) * SCALE) * inv_ref[0, steps(h, 1), :]
        inner = col_sum(p * dp) + inner_tail[steps(h, 1), :]
        ds = (p * (dp - inner) * SCALE).astype(BF)
        dv[:, here] += dot(p.astype(BF), do_h)
        dk[:, here] += dot(ds, q_h)
        dq_t[steps(h, HEAD), :] = dot(k_turned[steps(h, HEAD), :], ds)
        ds_tail[steps(h, 1), :] = p_tail[steps(h, 1), :] * (dp_tail[steps(h, 1), :] - inner) * SCALE

    ds_tail16 = ds_tail[ALL].astype(BF)
    grad_k = col_sum(grad_k + dot(ds_tail16, q) * heads)
    grad_v = col_sum(grad_v + dot(p_tail.astype(BF), do) * heads)

    @pl.when(b >= 2)
    def _():
        out_copy(buf, dqkv_hbm, slot, b - 2, sems, 0).wait()

    grad = dq_t[ALL].T + dot_tn(ds_tail16, k_t16)
    for n, (main, tail) in enumerate(((grad, grad_q), (dk[ALL], grad_k), (dv[ALL], grad_v))):
        here = steps(n, WIDTH)
        buf[slot, :, here] = main.astype(BF)
        grad_tails[pl.ds(b, 1), here] = tail
        dwb_ref[:, here] += col_sum(main) + tail
    out_copy(buf, dqkv_hbm, slot, b, sems, 0).start()

    @pl.when(b == last)
    def _():
        out_copy(buf, dqkv_hbm, 1 - slot, b - 1, sems, 0).wait()
        buf[1 - slot, 0:IMAGES, :] = grad_tails[ALL].astype(BF)
        cp = pltpu.make_async_copy(buf.at[1 - slot, pl.ds(0, IMAGES)], dqkv_hbm.at[pl.ds(TAIL, IMAGES)], sems.at[0, 1 - slot])
        cp.start()
        cp.wait()
        out_copy(buf, dqkv_hbm, slot, b, sems, 0).wait()


def attn_back_call(qkv, do, top, inv, dw):
    hbm = pl.BlockSpec(memory_space=pl.ANY)
    image = lambda i: jnp.minimum(i, IMAGES - 1)
    main = lambda n: by_rows(MAIN, n, image)
    tail = lambda n: by_rows(IMAGES, n, lambda i: TAIL // IMAGES)
    stat = pl.BlockSpec((1, HEADS, MAIN), lambda i: (image(i), 0, 0))
    return pl.pallas_call(
        attn_back_kernel,
        grid=(OUT_STEPS + DRAIN,),
        in_specs=[main(QKV), tail(QKV), main(WIDTH), tail(WIDTH), stat, stat,
                  by_cols(WIDTH, MAIN, lambda i: jnp.minimum(i, OUT_STEPS - 1))],
        out_specs=[hbm, whole(1, QKV), by_cols(SHARD, MAIN, lambda i: jnp.maximum(i - DRAIN, 0))],
        out_shape=[jax.ShapeDtypeStruct((TOKENS, QKV), BF), jax.ShapeDtypeStruct((1, QKV), F32),
                   jax.ShapeDtypeStruct((SHARD, WIDTH), F32)],
        scratch_shapes=[pltpu.VMEM((IMAGES, QKV), F32), pltpu.VMEM((IMAGES, WIDTH), F32),
                        pltpu.VMEM((IMAGES, QKV), F32), pltpu.VMEM((WIDTH, MAIN), F32),
                        pltpu.VMEM((MAIN, WIDTH), F32), pltpu.VMEM((MAIN, WIDTH), F32), pltpu.VMEM((HEADS, MAIN), F32),
                        pltpu.VMEM((2, MAIN, QKV), BF), pltpu.SemaphoreType.DMA((1, 2))] + FC_SUM.scratch(),
        compiler_params=comm_params(1),
        cost_estimate=ATTN_COST,
        name="attn_back",
    )(qkv, qkv, do, do, top, inv, dw)


QB_N = MAIN
QB_STEPS = QKV // QB_N
QKV_SUM = Exchange(SHARD, QB_N, ROW_CUTS, 0, 2)
VECTOR_SUM = Exchange(3 * SUBLANE, LANE, (0, SUBLANE, 2 * SUBLANE, 3 * SUBLANE), 0)
VECTOR_STEP = QB_STEPS + 2
QB_GRID = QB_STEPS + 1 + QUAD * QKV_SUM.stride


def qkvb_kernel(xim_hbm, dr_hbm, gain_ref, vec_ref, ht_ref, dqkv_ref, w_ref, dx_hbm, dw_ref, out_vec_ref,
                acc, dr, xd, vec, sums, sems, *comm):
    t = step_id()
    by_row, by_vector = QKV_SUM.bind(comm[:Exchange.COUNT]), VECTOR_SUM.bind(comm[Exchange.COUNT:])
    loads = [pltpu.make_async_copy(dr_hbm, dr, sems.at[0]), pltpu.make_async_copy(xim_hbm, xd, sems.at[1])]
    store = pltpu.make_async_copy(xd, dx_hbm, sems.at[1])

    @pl.when(t == 0)
    def _():
        by_row.meet()
        for cp in loads:
            cp.start()
        clear(acc, sums)
        by_vector.local[0] = jnp.zeros(by_vector.blocks, F32)
        vec[ALL] = vec_ref[ALL]

    def emit_vectors(n, exchange, c):
        for part, (rows, _) in enumerate(exchange.parts[:2]):
            out_vec_ref[rows, :] = exchange.held[3][part][0, :, :SHARD]
    advance((by_row,), t, first_chunks(QB_STEPS), lambda n, exchange, c: exchange.result(c, dw_ref))
    advance((by_vector,), t - VECTOR_STEP, first_chunks(1), emit_vectors)

    @pl.when(t < QB_STEPS)
    def _():
        by_row.put_local(t, dot(ht_ref[ALL], dqkv_ref[ALL]))
        acc[ALL] += dot_nt(dqkv_ref[ALL], w_ref[ALL])

    @pl.when(t == QB_STEPS)
    def _():
        for cp in loads:
            cp.wait()

    def back(r, n):
        hat, inv = norm_stats(xd[pl.ds(r, n), :].astype(F32))
        dn = acc[pl.ds(r, n), :]
        for i, v in enumerate((dn * hat, dn)):
            sums[steps(i, SUBLANE), :] += eights(v)
        acc[pl.ds(r, n), :] = joined(dr, r, n) + norm_back(dn, hat, inv, gain_ref[ALL])

    @pl.when((t >= QB_STEPS) & (t <= VECTOR_STEP))
    def _():
        part = (t - QB_STEPS) * BACK_TILES

        def loop(i, carry):
            @pl.when(part + i < TAIL // ROWS)
            def _():
                back(pl.multiple_of((part + i) * ROWS, ROWS), ROWS)
            return carry
        lax.fori_loop(0, BACK_TILES, loop, 0)

    @pl.when(t == VECTOR_STEP)
    def _():
        back(TAIL, IMAGES)
        for i in range(2):
            vec[steps(VECTOR_ROWS - 2 + i, 1), :] = col_sum(sums[steps(i, SUBLANE), :])
        for d, place in enumerate(itertools.product(range(2), repeat=QUAD)):
            by_vector.local[(0, *place, pl.ds(0, VECTOR_ROWS), pl.ds(0, SHARD))] = vec[:, steps(d, SHARD)]

    @pl.when(t == VECTOR_STEP + 1)
    def _():
        from_image_order(acc, dr)

    @pl.when(t == VECTOR_STEP + 2)
    def _():
        def narrow(r, n):
            xd[pl.ds(r, n), :] = joined(dr, r, n).astype(BF)
        row_tiles(narrow)
        store.start()

    @pl.when(t == QB_GRID - 1)
    def _():
        store.wait()


BACK_TILES = -(-TAIL // ROWS // 3)


def qkvb_call(xim, dr, gain, vec, ht, dqkv, w):
    hbm = pl.BlockSpec(memory_space=pl.ANY)
    now = lambda i: jnp.minimum(i, QB_STEPS - 1)
    return pl.pallas_call(
        qkvb_kernel,
        grid=(QB_GRID,),
        in_specs=[hbm, hbm, whole(1, WIDTH), whole(VECTOR_ROWS, WIDTH),
                  whole(WIDTH, TOKENS, pipeline_mode=pl.Buffered(1)), by_cols(TOKENS, QB_N, now), by_cols(WIDTH, QB_N, now)],
        out_specs=[hbm, by_cols(SHARD, QB_N, lambda i: jnp.clip(i - 1 - QUAD * QKV_SUM.stride, 0, QB_STEPS - 1)),
                   whole(VECTOR_ROWS, SHARD)],
        out_shape=[jax.ShapeDtypeStruct((TOKENS, WIDTH), BF), jax.ShapeDtypeStruct((SHARD, QKV), F32),
                   jax.ShapeDtypeStruct((VECTOR_ROWS, SHARD), F32)],
        scratch_shapes=[pltpu.VMEM((TOKENS, WIDTH), F32), pltpu.VMEM((LANES, TOKENS, LANE), F32), pltpu.VMEM((TOKENS, WIDTH), BF),
                        pltpu.VMEM((VECTOR_ROWS, WIDTH), F32), pltpu.VMEM((2 * SUBLANE, WIDTH), F32), pltpu.SemaphoreType.DMA((2,))]
                       + QKV_SUM.scratch() + VECTOR_SUM.scratch(),
        compiler_params=comm_params(2),
        cost_estimate=cost(QUAD * TOKENS * WIDTH * QKV, 80_000_000),
        name="qkvb",
    )(xim, dr, gain, vec, ht, dqkv, w)


def to_steps(v):
    rows = v.shape[0]
    return v.reshape(rows, PARTS, MLP_STEPS, UNITS).swapaxes(1, 2).reshape(rows, FFN)


def from_steps(v):
    rows = v.shape[0]
    return v.reshape(rows, MLP_STEPS, PARTS, UNITS).swapaxes(1, 2).reshape(rows, FFN)


def solution(mesh):
    specs = (P("fsdp"),) * 14

    def device_step(resid_in, grad_out, ln1_gain, ln1_bias, qkv_weight, qkv_bias, out_weight, out_bias,
                    ln2_gain, ln2_bias, fc_weight, fc_bias, proj_weight, proj_bias):
        rows = jnp.concatenate([ln1_gain, ln1_bias, qkv_bias, out_bias, ln2_gain, ln2_bias, fc_bias, proj_bias]).reshape(-1, SHARD)
        rows = jnp.pad(rows, ((0, VECTOR_ROWS - len(rows)), (0, LANE - SHARD)))
        x = resid_in.swapaxes(0, 1).reshape(TOKENS, WIDTH)
        dy = grad_out.swapaxes(0, 1).reshape(TOKENS, WIDTH)
        xim, h, ht, rows, wq = open_call(x, rows, qkv_weight)
        wq = wq.reshape(WIDTH, QKV)
        bo, g2, b2 = rows[5:6], rows[6:7], rows[7:8]
        joint = lambda v: v.reshape(-1, PARTS, SHARD).swapaxes(0, 1).reshape(1, -1)
        fc, proj = to_steps(fc_weight.astype(BF)), proj_weight.astype(BF)
        cut = EARLY * UNITS
        qkv, wf, wo = qkv_call(h, wq, joint(rows[2:5]), fc[:, :EARLY * MLP_F], out_weight)
        wo = wo.reshape(WIDTH, WIDTH)
        o, r, top, inv, wp = attn_call(qkv, xim, wo, bo, proj_weight[:cut])
        y, dr, dr16, dwf, dwp, dbf, small, _, _ = mlp_call(
            r, dy, g2, b2, rows[12:13], wf.reshape(WIDTH, -1), wp, to_steps(joint(rows[8:12])),
            fc[:, EARLY * MLP_F:].reshape(SHARD, -1, MLP_F).swapaxes(0, 1), proj[cut:].reshape(-1, UNITS, WIDTH))
        do, dwo = outb_call(dr16, o, wo)
        dqkv, dbq, dwo = attn_back_call(qkv, do, top, inv, dwo)
        owned = lambda v: v.reshape(PARTS, -1, WIDTH // PARTS).swapaxes(0, 1).reshape(-1, WIDTH)
        vec = jnp.concatenate([jnp.sum(small.reshape(4, 8, WIDTH), axis=1), owned(dbq), owned(from_steps(dbf))])
        vec = jnp.pad(vec, ((0, VECTOR_ROWS - len(vec)), (0, 0)))
        dx, dwq, vec = qkvb_call(xim, dr, rows[:1], vec, ht, dqkv, wq)
        dg2, db2, dbp, dbo = vec[:4]
        dbq, dbf = vec[4:7].reshape(-1), vec[7:11].reshape(-1)
        dg1, db1 = vec[VECTOR_ROWS - 2:]
        dwf = from_steps(dwf)
        unturn = lambda t: t.reshape(SEQ, IMAGES, WIDTH).swapaxes(0, 1)
        return (unturn(y), unturn(dx), dg1, db1, dwq, dbq, dwo, dbo, dg2, db2, dwf, dbf, dwp, dbp)

    return jax.shard_map(device_step, mesh=mesh, in_specs=specs, out_specs=specs, check_vma=False)
```

```python
import itertools
import math
import jax, jax.numpy as jnp
from jax import lax
from jax.experimental import pallas as pl
from jax.experimental.pallas import tpu as pltpu
from jax.sharding import PartitionSpec as P

BF, F32 = jnp.bfloat16, jnp.float32
IMAGES, SEQ, WIDTH, FFN, HEADS, HEAD = 8, 257, 1280, 5120, 16, 80
MAIN = SEQ - 1
TOKENS = IMAGES * SEQ
TAIL = IMAGES * MAIN
LN_EPS = 1e-5
VMEM_MAX = 67043328
LANE, SUBLANE, QUAD, QKV = 128, 8, 4, 3 * WIDTH
ALL = ...
LANES = WIDTH // LANE
ROWS = 32


def dot(a, b):
    return jnp.dot(a, b, preferred_element_type=F32)


def dot_nt(a, b):
    return lax.dot_general(a, b, (((1,), (1,)), ((), ())), preferred_element_type=F32)


def dot_tn(a, b):
    return lax.dot_general(a, b, (((0,), (0,)), ((), ())), preferred_element_type=F32)


def col_sum(v):
    return jnp.sum(v, axis=0, keepdims=True)


def col_max(v):
    return jnp.max(v, axis=0, keepdims=True)


def row_sum(v):
    return jnp.sum(v, axis=-1, keepdims=True)


def row_mean(v):
    return row_sum(v) * (1.0 / WIDTH)


def clear(*refs):
    for ref in refs:
        ref[ALL] = jnp.zeros_like(ref)


def step_id():
    return pl.program_id(0)


def cost(flops, bytes_accessed, transcendentals=0):
    return pl.CostEstimate(flops=flops, bytes_accessed=bytes_accessed, transcendentals=transcendentals)


def eights(v):
    return jnp.sum(v.reshape(v.shape[0] // SUBLANE, SUBLANE, v.shape[1]), axis=0)


def whole(*shape, **kw):
    return pl.BlockSpec(shape, lambda *i: (0,) * len(shape), **kw)


def by_cols(rows, cols, at=lambda i: i):
    return pl.BlockSpec((rows, cols), lambda i: (0, at(i)))


def by_rows(rows, cols, at=lambda i: i):
    return pl.BlockSpec((rows, cols), lambda i: (at(i), 0))


def steps(first, wide):
    return slice(first * wide, (first + 1) * wide)


def norm_stats(values):
    mean = row_mean(values)
    centered = values - mean
    inv = lax.rsqrt(row_mean(centered * centered) + LN_EPS)
    return centered * inv, inv


BLOCKS = [slice(a, b) for a, b in ((0, 512), (512, 1024), (1024, 1536), (1536, TOKENS))]


def row_tiles(body, step=LANE):
    def loop(i, carry):
        body(pl.multiple_of(i * step, step), step)
        return carry
    lax.fori_loop(0, TAIL // step, loop, 0)
    body(TAIL, IMAGES)


def back_part(body, part):
    tiles = -(-TAIL // ROWS // 3)

    def loop(i, carry):
        tile = part * tiles + i

        @pl.when(tile < TAIL // ROWS)
        def _():
            body(pl.multiple_of(tile * ROWS, ROWS), ROWS)
        return carry
    lax.fori_loop(0, tiles, loop, 0)


def to_image_order(wide, place, step=LANE):
    per = MAIN // step
    def loop(i, carry):
        first = (i % per) * (step * IMAGES) + i // per
        rows = [wide[c, pl.ds(first, step, stride=IMAGES), :] for c in range(LANES)]
        place(pl.multiple_of(i * step, step), step, jnp.concatenate(rows, axis=1))
        return carry
    lax.fori_loop(0, IMAGES * per, loop, 0)
    place(TAIL, IMAGES, joined(wide, TAIL, IMAGES))


def from_image_order(values, wide):
    def loop(i, carry):
        rows = values[pl.ds(pl.multiple_of(i * LANE, LANE), LANE), :]
        for c in range(LANES):
            wide[c, pl.ds((i % 2) * (LANE * IMAGES) + i // 2, LANE, stride=IMAGES), :] = rows[:, steps(c, LANE)]
        return carry
    lax.fori_loop(0, 2 * IMAGES, loop, 0)
    put(wide, TAIL, IMAGES, values[pl.ds(TAIL, IMAGES), :])


def joined(wide, r, n):
    return jnp.concatenate([wide[c, pl.ds(r, n), :] for c in range(LANES)], axis=1)


def put(wide, r, n, values):
    for c in range(LANES):
        wide[c, pl.ds(r, n), :] = values[:, steps(c, LANE)]


def norm_back(dn, hat, inv, gain):
    dhat = dn * gain
    m1 = row_mean(dhat)
    m2 = row_mean(dhat * hat)
    return inv * (dhat - m1 - hat * m2)


ORDERS = ((2, 1, 0), (1, 0, 2), (0, 2, 1))


class Links:
    def find(self, send, recv):
        self.send, self.recv = send, recv
        me = lax.axis_index("fsdp")
        self.core = me % 2
        self.at = (me // SUBLANE, (me // QUAD) % 2, (me // 2) % 2)
        self.other_core = me + 1 - 2 * self.core
        self.other = [me + step - 2 * step * place for step, place in zip((SUBLANE, QUAD, 2), self.at)]
        return self

    def meet(self):
        barrier = pltpu.get_barrier_semaphore()
        devices = (self.other_core, *self.other)
        for device in devices:
            pl.semaphore_signal(barrier, inc=1, device_id=(device,), device_id_type=pl.DeviceIdType.MESH)
        pl.semaphore_wait(barrier, len(devices))

    def remote(self, src, dst, sem, device):
        return pltpu.make_async_remote_copy(src_ref=src, dst_ref=dst, send_sem=self.send.at[sem], recv_sem=self.recv.at[sem],
                                            device_id=(device,), device_id_type=pl.DeviceIdType.MESH)


class Gather(Links):
    COUNT = 2

    def __init__(self, rows, cols, cuts):
        self.rows, self.cols, self.cuts = rows, cols, cuts
        self.parts = range(len(cuts) - 1)
        self.full_shape = jax.ShapeDtypeStruct((2, 2, 2, 2, rows, cols), BF)

    def scratch(self):
        return [pltpu.SemaphoreType.DMA((SEMS,))] * self.COUNT

    def bind(self, own, full, sems):
        self.own, self.full = own, full
        return self.find(*sems)

    def region(self, part, known, arrived=False):
        done = ORDERS[part][:known]
        place = [slice(None) if a in done else self.at[a] for a in range(3)]
        if arrived:
            place[done[-1]] = 1 - self.at[done[-1]]
        return (*place, self.core, slice(None), pl.ds(self.cuts[part], self.cuts[part + 1] - self.cuts[part]))

    def hop(self, stage, part):
        where = self.full.at[self.region(part, stage - 1)]
        source = self.own.at[self.region(part, 0)[-2:]] if stage == 1 else where
        return self.remote(source, where, QUAD * stage + part, self.other[ORDERS[part][stage - 1]])

    def forward(self, stage, part):
        if stage == 0:
            return self.remote(self.own, self.full.at[(*self.at, self.core)], 0, self.other_core)
        where = self.full.at[self.region(part, stage, True)]
        return self.remote(where, where, QUAD * (stage + 3) + part, self.other_core)

    def keep(self):
        return pltpu.make_async_copy(self.own, self.full.at[(*self.at, self.core)], self.send.at[1])

    def begin(self):
        for part in self.parts:
            self.hop(1, part).start()
        self.forward(0, 0).start()
        self.keep().start()

    def turn(self, stage):
        if stage == 1:
            self.keep().wait()
        for part in self.parts:
            self.hop(stage, part).wait()
            if stage < 3:
                self.hop(stage + 1, part).start()
        for part in self.parts:
            self.forward(stage, part).start()

    def end(self):
        self.forward(0, 0).wait()
        for stage in range(1, QUAD):
            for part in self.parts:
                self.forward(stage, part).wait()


SEMS = 28


class Exchange(Links):
    def __init__(self, rows, cols, cuts, along, stride=1, spare=0):
        self.rows, self.cols, self.stride = rows, cols, stride
        self.slots, self.locals = 3 * stride + spare, 1 + stride
        self.blocks = (2, 2, 2, 2, rows, cols)
        self.parts = [((slice(a, b), slice(None)) if along == 0 else (slice(None), slice(a, b))) for a, b in zip(cuts, cuts[1:])]
        self.shapes = [((b - a, cols) if along == 0 else (rows, b - a)) for a, b in zip(cuts, cuts[1:])]

    def scratch(self):
        two = (2, 2, 2)
        out = [pltpu.VMEM((self.locals, *self.blocks), F32), pltpu.VMEM((self.slots, *two, self.rows, self.cols), F32)]
        for axes in (2, 1, 0):
            out += [pltpu.VMEM((self.slots, *two[:axes], *shape), F32) for shape in self.shapes]
        return out + [pltpu.SemaphoreType.DMA((10, self.slots))] * 2

    COUNT = 13

    def bind(self, refs):
        self.local, self.pair = refs[0], refs[1]
        self.held = [None, refs[2:5], refs[5:SUBLANE], refs[SUBLANE:11]]
        return self.find(*refs[11:])

    def index(self, stage, part, side):
        order = ORDERS[part]
        left = [a for a in range(3) if a not in order[:stage - 1]]
        axis = order[stage - 1]
        where = self.at[axis] if side else 1 - self.at[axis]
        return tuple(where if a == axis else slice(None) for a in left)

    def copy(self, stage, part, c):
        slot = c % self.slots
        if stage == 0:
            return self.remote(self.local.at[c % self.locals, :, :, :, 1 - self.core], self.pair.at[slot], (0, slot), self.other_core)
        source = self.pair if stage == 1 else self.held[stage - 1][part]
        tail = self.parts[part] if stage == 1 else ()
        return self.remote(source.at[(slot, *self.index(stage, part, False), *tail)], self.held[stage][part].at[slot],
                           (3 * stage - 2 + part, slot), self.other[ORDERS[part][stage - 1]])

    def start(self, stage, c):
        for part in range(1 if stage == 0 else 3):
            self.copy(stage, part, c).start()

    def wait(self, stage, c):
        for part in range(1 if stage == 0 else 3):
            self.copy(stage, part, c).wait()

    def add(self, stage, c):
        slot = c % self.slots
        if stage == 0:
            for chip in itertools.product(range(2), repeat=3):
                self.pair[(slot, *chip)] += self.local[(c % self.locals, *chip, self.core)]
            return
        for part in range(3):
            source = self.pair if stage == 1 else self.held[stage - 1][part]
            tail = self.parts[part] if stage == 1 else ()
            for place in itertools.product(range(2), repeat=3 - stage):
                free = iter(place)
                kept = tuple(next(free) if isinstance(i, slice) else i for i in self.index(stage, part, True))
                self.held[stage][part][(slot, *place)] += source[(slot, *kept, *tail)]

    def result(self, c, out_ref):
        for part in range(3):
            out_ref[self.parts[part]] = self.held[3][part][c % self.slots]

    def put_local(self, c, values):
        self.local[c % self.locals] = values.reshape(self.blocks)


def comm_params(n):
    return pltpu.CompilerParams(dimension_semantics=("arbitrary",), vmem_limit_bytes=VMEM_MAX, collective_id=n, has_side_effects=True)


def advance(exchanges, t, exists, emit):
    for stage in (3, 2, 1, 0):
        c = t - 1 - (stage + 1) * exchanges[0].stride

        @pl.when(exists(c))
        def _():
            for n, exchange in enumerate(exchanges):
                exchange.wait(stage, c)
                exchange.add(stage, c)
                if stage < 3:
                    exchange.start(stage + 1, c)
                else:
                    emit(n, exchange, c)

    @pl.when(exists(t - 1))
    def _():
        for exchange in exchanges:
            exchange.start(0, t - 1)


def first_chunks(n):
    return lambda c: (c >= 0) & (c < n)


DRAIN = 5


PARTS = 16
SHARD = WIDTH // PARTS
VECTOR_ROWS = PARTS
MLP_F = MAIN
UNITS = MLP_F // PARTS
MLP_STEPS = FFN // MLP_F
WIDTH_CUTS = (0, 384, 896, WIDTH)
QKV_ALL = Gather(SHARD, QKV, (0, WIDTH, 2 * WIDTH, QKV))
OUT_ALL = Gather(SHARD, WIDTH, WIDTH_CUTS)
FC_ALL = Gather(SHARD, FFN, (0, 1664, 3328, 5120))
PROJ_ALL = Gather(FFN // PARTS, WIDTH, WIDTH_CUTS)
VECTOR_ALL = Gather(SHARD, LANE, (0, LANE))


def open_kernel(x_hbm, dy_hbm, rows_ref, wq_ref, wo_ref, xim_hbm, dyim_hbm, h_hbm, ht_hbm, vec_ref, wq_full, wo_full,
                x, dy, wide, h, ht, rows, vec_own, vec_full, wq_own, wo_own, sems, *comm):
    loads = [pltpu.make_async_copy(src, dst, sems.at[i]) for i, (src, dst) in enumerate(((x_hbm, x), (dy_hbm, dy)))]
    for cp in loads:
        cp.start()
    clear(rows)
    rows[:VECTOR_ROWS, :] = rows_ref[ALL]
    vec_own[ALL] = rows[ALL].T[:SHARD, :].astype(BF)
    wq_own[ALL] = wq_ref[ALL].astype(BF)
    wo_own[ALL] = wo_ref[ALL].astype(BF)
    pairs = [comm[2 * i:2 * i + 2] for i in range(3)]
    vectors = VECTOR_ALL.bind(vec_own, vec_full, pairs[0])
    weights = QKV_ALL.bind(wq_own, wq_full, pairs[1]), OUT_ALL.bind(wo_own, wo_full, pairs[2])
    gathers = (vectors, *weights)
    vectors.meet()
    for gather in gathers:
        gather.begin()
    for cp in loads:
        cp.wait()

    def reorder(tokens):
        def widen(r, n):
            put(wide, r, n, tokens[pl.ds(r, n), :].astype(F32))
        row_tiles(widen)

        def place(r, n, values):
            tokens[pl.ds(r, n), :] = values.astype(BF)
        to_image_order(wide, place)
    reorder(x)
    for gather in gathers:
        gather.turn(1)
    reorder(dy)
    for gather in gathers:
        gather.turn(2)
    vectors.turn(3)
    vectors.end()
    vec_ref[ALL] = vec_full[ALL].reshape(WIDTH, LANE).astype(F32).T[:VECTOR_ROWS, :]
    gain, bias = vec_ref[0:1, :], vec_ref[1:2, :]

    def norm(r, n):
        hat, _ = norm_stats(x[pl.ds(r, n), :].astype(F32))
        h[pl.ds(r, n), :] = (hat * gain + bias).astype(BF)
    row_tiles(norm, ROWS)
    for b in range(IMAGES):
        ht[:, steps(b, MAIN)] = h[steps(b, MAIN), :].T
    ht[:, TAIL:] = h[TAIL:, :].T
    stores = [pltpu.make_async_copy(src, dst, sems.at[i]) for i, (src, dst) in enumerate(((x, xim_hbm), (dy, dyim_hbm), (h, h_hbm), (ht, ht_hbm)))]
    for cp in stores:
        cp.start()
    for gather in weights:
        gather.turn(3)
    for gather in weights:
        gather.end()
    for cp in stores:
        cp.wait()


def open_call(x, dy, rows, wq, wo):
    hbm, vmem = pl.BlockSpec(memory_space=pl.ANY), pl.BlockSpec(memory_space=pltpu.VMEM)
    return pl.pallas_call(
        open_kernel,
        in_specs=[hbm, hbm, vmem, vmem, vmem],
        out_specs=[hbm, hbm, hbm, hbm, vmem, hbm, hbm],
        out_shape=[*[jax.ShapeDtypeStruct((TOKENS, WIDTH), BF)] * 3,
                   jax.ShapeDtypeStruct((WIDTH, TOKENS), BF), jax.ShapeDtypeStruct((VECTOR_ROWS, WIDTH), F32),
                   QKV_ALL.full_shape, OUT_ALL.full_shape],
        scratch_shapes=[pltpu.VMEM((TOKENS, WIDTH), BF), pltpu.VMEM((TOKENS, WIDTH), BF), pltpu.VMEM((LANES, TOKENS, LANE), F32),
                        pltpu.VMEM((TOKENS, WIDTH), BF), pltpu.VMEM((WIDTH, TOKENS), BF), pltpu.VMEM((LANE, LANE), F32), pltpu.VMEM((SHARD, LANE), BF),
                        pltpu.VMEM(VECTOR_ALL.full_shape.shape, BF), pltpu.VMEM((SHARD, QKV), BF), pltpu.VMEM((SHARD, WIDTH), BF),
                        pltpu.SemaphoreType.DMA((QUAD,))] + VECTOR_ALL.scratch() + QKV_ALL.scratch() + OUT_ALL.scratch(),
        compiler_params=pltpu.CompilerParams(vmem_limit_bytes=VMEM_MAX, collective_id=3, has_side_effects=True),
        cost_estimate=cost(1_000_000_000, 60_000_000),
        name="open",
    )(x, dy, rows, wq, wo)


QKV_N = 768


def qkv_kernel(h_ref, w_ref, wb_ref, own_ref, qkv_ref, full, *sems):
    t, last = step_id(), pl.num_programs(0) - 1
    gather = FC_ALL.bind(own_ref, full, sems)

    @pl.when(t == 0)
    def _():
        gather.meet()
        gather.begin()

    @pl.when(t == 1)
    def _():
        gather.turn(1)

    @pl.when(t == 3)
    def _():
        gather.turn(2)
    for rows in BLOCKS:
        qkv_ref[rows, :] = (dot(h_ref[rows, :], w_ref[ALL]) + wb_ref[ALL]).astype(BF)

    @pl.when(t == last)
    def _():
        gather.turn(3)
        gather.end()


def qkv_call(h, w, wb, own):
    hbm = pl.BlockSpec(memory_space=pl.ANY)
    return pl.pallas_call(
        qkv_kernel,
        grid=(QKV // QKV_N,),
        in_specs=[whole(TOKENS, WIDTH, pipeline_mode=pl.Buffered(1)), by_cols(WIDTH, QKV_N), by_cols(1, QKV_N), whole(SHARD, FFN)],
        out_specs=[by_cols(TOKENS, QKV_N), hbm],
        out_shape=[jax.ShapeDtypeStruct((TOKENS, QKV), BF), FC_ALL.full_shape],
        scratch_shapes=FC_ALL.scratch(),
        compiler_params=comm_params(QUAD),
        cost_estimate=cost(2 * TOKENS * WIDTH * QKV, 60_000_000),
        name="qkv",
    )(h, w, wb, own)


ROW_CUTS = (0, 24, 48, 80)
FC_SUM = Exchange(SHARD, MLP_F, ROW_CUTS, 0)
PROJ_SUM = Exchange(UNITS, WIDTH, WIDTH_CUTS, 1)
CDF_P = 0.33
CDF_C = (0.1326322871417956, 0.11939570820799192, 0.18103829560051796, -0.08904113226212501,
         0.33075919469138065, -0.22023738432274684, 0.0454530347223348)


def gelu_pair(u):
    bell = jnp.exp(u * u * -0.5)
    t = 1.0 / (1.0 + CDF_P * jnp.abs(u))
    poly = CDF_C[6]
    for c in CDF_C[5::-1]:
        poly = poly * t + c
    tail = poly * t * bell
    cdf = jnp.where(u < 0.0, tail, 1.0 - tail)
    return u * cdf, cdf + u * bell * ((2.0 * math.pi) ** -0.5)


def mlp_kernel(r_hbm, n_hbm, dy_hbm, gain_ref, pb_ref, fc_ref, proj_ref, fcb_ref,
               y_hbm, dr_hbm, dr16_hbm, dfc_ref, dproj_ref, dfcb_ref, small_ref,
               n2, dy, y_acc, dn_acc, g, du, ua, ub, da, db, sem, *comm):
    step = step_id()
    by_row, by_col = FC_SUM.bind(comm[:Exchange.COUNT]), PROJ_SUM.bind(comm[Exchange.COUNT:])

    @pl.when(step == 0)
    def _():
        loads = [pltpu.make_async_copy(n_hbm, n2, sem), pltpu.make_async_copy(dy_hbm, dy, sem)]
        for cp in loads:
            cp.start()
        by_row.meet()
        clear(small_ref, y_acc, dn_acc)
        for cp in loads:
            cp.wait()

    outs = (dfc_ref, dproj_ref)
    advance((by_row, by_col), step, first_chunks(MLP_STEPS), lambda n, exchange, c: exchange.result(c, outs[n]))

    @pl.when(step < MLP_STEPS)
    def _():
        fcb = fcb_ref[ALL]
        fc, proj = fc_ref[ALL], proj_ref[ALL].reshape(MLP_F, WIDTH)
        bias_sum = jnp.zeros((SUBLANE, MLP_F), F32)
        tiles = [(b * MAIN, MAIN) for b in range(IMAGES - 1)] + [((IMAGES - 1) * MAIN, MAIN + IMAGES)]
        pairs = ((ua, da), (ub, db))

        def products(k):
            r, n = tiles[k]
            u_s, d_s = pairs[k % 2]
            u_s[0:n, :] = dot(n2[r:r + n, :], fc)
            d_s[0:n, :] = dot_nt(dy[r:r + n, :], proj)

        def pointwise(k, total):
            r, n = tiles[k]
            u_s, d_s = pairs[k % 2]
            value, slope = gelu_pair(u_s[0:n, :] + fcb)
            g[r:r + n, :] = value.astype(BF)
            grad = d_s[0:n, :] * slope
            du[r:r + n, :] = grad.astype(BF)
            return total + eights(grad)

        products(0)
        for k in range(1, IMAGES):
            products(k)
            bias_sum = pointwise(k - 1, bias_sum)
        bias_sum = pointwise(IMAGES - 1, bias_sum)
        dfcb_ref[ALL] = col_sum(bias_sum)
        y_acc[ALL] += dot(g[ALL], proj)
        for c in range(LANES // 2):
            part = dot_nt(du[ALL], fc_ref[steps(c, MAIN), :])
            dn_acc[2 * c] += part[:, :LANE]
            dn_acc[2 * c + 1] += part[:, LANE:]
        by_col.put_local(step, dot_tn(g[ALL], dy[ALL]))
        by_row.put_local(step, dot_tn(n2[ALL], du[ALL]))

    after = step - MLP_STEPS
    r_copy = pltpu.make_async_copy(r_hbm, n2, sem)
    out_copies = [pltpu.make_async_copy(dn_acc, dr_hbm, sem), pltpu.make_async_copy(n2, dr16_hbm, sem)]
    y_copy = pltpu.make_async_copy(dy, y_hbm, sem)

    def back(r, n):
        wide_r = n2[pl.ds(r, n), :].astype(F32)
        hat, inv = norm_stats(wide_r)
        dn = joined(dn_acc, r, n)
        wide_dy = dy[pl.ds(r, n), :].astype(F32)
        dr = wide_dy + norm_back(dn, hat, inv, gain_ref[ALL])
        put(dn_acc, r, n, dr)
        n2[pl.ds(r, n), :] = dr.astype(BF)
        y_acc[pl.ds(r, n), :] += wide_r + pb_ref[ALL]
        for i, v in enumerate((dn * hat, dn, wide_dy, dr)):
            small_ref[steps(i, SUBLANE), :] += eights(v)

    @pl.when(after == 0)
    def _():
        r_copy.start()
        r_copy.wait()
        back(TAIL, IMAGES)

    @pl.when((after >= 0) & (after < 3))
    def _():
        back_part(back, after)

    @pl.when(after == 2)
    def _():
        for cp in out_copies:
            cp.start()

    @pl.when(after == 3)
    def _():
        for cp in out_copies:
            cp.wait()
        from_image_order(y_acc, dn_acc)

        def narrow(r, n):
            dy[pl.ds(r, n), :] = joined(dn_acc, r, n).astype(BF)
        row_tiles(narrow)
        y_copy.start()

    @pl.when(after == QUAD)
    def _():
        y_copy.wait()


def mlp_call(r, n2, dy, gain, pb, fc, proj, fcb):
    hbm = pl.BlockSpec(memory_space=pl.ANY)
    vec = whole(1, WIDTH)
    now = lambda i: jnp.minimum(i, MLP_STEPS - 1)
    done = lambda i: jnp.maximum(i - DRAIN, 0)
    return pl.pallas_call(
        mlp_kernel,
        grid=(MLP_STEPS + DRAIN,),
        in_specs=[hbm, hbm, hbm, vec, vec, by_cols(WIDTH, MLP_F, now),
                  pl.BlockSpec((PARTS, None, UNITS, WIDTH), lambda i: (0, now(i), 0, 0)),
                  by_cols(1, MLP_F, now)],
        out_specs=[hbm, hbm, hbm, by_cols(SHARD, MLP_F, done),
                   by_rows(UNITS, WIDTH, done),
                   by_cols(1, MLP_F, now), whole(32, WIDTH)],
        out_shape=[jax.ShapeDtypeStruct((TOKENS, WIDTH), BF), jax.ShapeDtypeStruct((LANES, TOKENS, LANE), F32),
                   jax.ShapeDtypeStruct((TOKENS, WIDTH), BF), jax.ShapeDtypeStruct((SHARD, FFN), F32),
                   jax.ShapeDtypeStruct((FFN // PARTS, WIDTH), F32),
                   jax.ShapeDtypeStruct((1, FFN), F32), jax.ShapeDtypeStruct((32, WIDTH), F32)],
        scratch_shapes=[pltpu.VMEM((TOKENS, WIDTH), BF), pltpu.VMEM((TOKENS, WIDTH), BF),
                        pltpu.VMEM((TOKENS, WIDTH), F32), pltpu.VMEM((LANES, TOKENS, LANE), F32),
                        pltpu.VMEM((TOKENS, MLP_F), BF), pltpu.VMEM((TOKENS, MLP_F), BF)]
                       + [pltpu.VMEM((MAIN + IMAGES, MLP_F), F32)] * QUAD + [pltpu.SemaphoreType.DMA]
                       + FC_SUM.scratch() + PROJ_SUM.scratch(),
        compiler_params=comm_params(0),
        cost_estimate=cost(12 * TOKENS * WIDTH * FFN, 150_000_000, TOKENS * FFN),
        name="mlp",
    )(r, n2, dy, gain, pb, fc, proj.reshape(PARTS, MLP_STEPS, UNITS, WIDTH), fcb)


SCALE = HEAD ** -0.5
ATTN_COST = cost(40_000_000_000, 50_000_000, 8_400_000)


def window(h):
    first = min(HEAD * h // LANE * LANE, WIDTH - MAIN)
    wide = LANE if HEAD * h + HEAD <= first + LANE else MAIN
    return first, wide, HEAD * h - first


def lane_mask(h):
    first, wide, off = window(h)
    lane = lax.broadcasted_iota(jnp.int32, (MAIN, wide), 1)
    return (lane >= off) & (lane < off + HEAD)


def thirds(ref, rows=slice(None)):
    return [ref[rows, steps(i, WIDTH)] for i in range(3)]


def head_rows():
    lane = lax.broadcasted_iota(jnp.int32, (HEADS, WIDTH), 1)
    row = lax.broadcasted_iota(jnp.int32, (HEADS, WIDTH), 0)
    return (lane // HEAD == row).astype(F32)


def tail_softmax(s, s_self):
    m = jnp.maximum(jnp.max(s, axis=1, keepdims=True), s_self)
    e = jnp.exp((s - m) * SCALE)
    e_self = jnp.exp((s_self - m) * SCALE)
    inv = 1.0 / (row_sum(e) + e_self)
    return e * inv, e_self * inv


def attn_kernel(qkv_ref, qkvt_ref, x_ref, xt_ref, w_ref, wb_ref, gain_ref, bias_ref, proj_ref, o_hbm, r_hbm, n_hbm,
                max_ref, inv_ref, full,
                tails, o_tail, o_t, ptail, o_buf, r_buf, n_buf, sa, sb, sems, own, *comm):
    b, last = step_id(), pl.num_programs(0) - 1
    slot = b % 2
    gather = PROJ_ALL.bind(own, full, comm)

    @pl.when(b == 0)
    def _():
        tails[ALL] = qkvt_ref[ALL].astype(F32)
        own[ALL] = proj_ref[ALL].astype(BF)
        gather.meet()
        gather.begin()

    @pl.when(b == 1)
    def _():
        gather.turn(1)

    @pl.when(b == 3)
    def _():
        gather.turn(2)

    @pl.when(b == last)
    def _():
        gather.turn(3)

    heads = head_rows()
    q_t, k_t, v_t = (heads * z for z in thirds(tails, pl.ds(b, 1)))
    q, k, v = thirds(qkv_ref)

    p, p_self = tail_softmax(dot_nt(q_t.astype(BF), k), row_sum(q_t * k_t))
    mixed = dot(p.astype(BF), v) * heads + p_self.astype(BF).astype(F32) * v_t
    o_tail[pl.ds(b, 1), :] = col_sum(mixed)

    s_tail = dot_nt(k_t.astype(BF), q)
    v_turned = v.T
    scores = sa, sb

    def next_scores(h):
        first, wide, _ = window(h)
        q_h = jnp.where(lane_mask(h), qkv_ref[:, pl.ds(first, wide)], jnp.zeros((), BF))
        scores[h % 2][ALL] = dot_nt(qkv_ref[:, pl.ds(WIDTH + first, wide)], q_h)
    next_scores(0)
    for h in range(HEADS):
        if h + 1 < HEADS:
            next_scores(h + 1)
        s, mine = scores[h % 2], steps(h, 1)
        top = jnp.maximum(col_max(s[ALL]), s_tail[mine, :])
        e = jnp.exp((s[ALL] - top) * SCALE)
        e_tail = jnp.exp((s_tail[mine, :] - top) * SCALE)
        inv = 1.0 / (col_sum(e) + e_tail)
        max_ref[0, mine, :] = top
        inv_ref[0, mine, :] = inv
        ptail[mine, :] = e_tail * inv
        o_t[steps(h, HEAD), :] = dot(v_turned[steps(h, HEAD), :], (e * inv).astype(BF))

    outs = (o_buf, o_hbm), (r_buf, r_hbm), (n_buf, n_hbm)

    def write(slot, rows, o, x):
        o_buf[slot, rows, :] = o
        r = (x.astype(F32) + dot(o, w_ref[ALL]) + wb_ref[ALL]).astype(BF)
        r_buf[slot, rows, :] = r
        hat, _ = norm_stats(r.astype(F32))
        n_buf[slot, rows, :] = (hat * gain_ref[ALL] + bias_ref[ALL]).astype(BF)

    @pl.when(b >= 2)
    def _():
        for n, (buf, hbm) in enumerate(outs):
            out_copy(buf, hbm, slot, b - 2, sems, n).wait()

    o = (o_t[ALL].T + dot_tn(ptail[ALL].astype(BF), v_t.astype(BF))).astype(BF)
    write(slot, slice(None), o, x_ref[ALL])
    for n, (buf, hbm) in enumerate(outs):
        out_copy(buf, hbm, slot, b, sems, n).start()

    @pl.when(b == last)
    def _():
        for n, (buf, hbm) in enumerate(outs):
            out_copy(buf, hbm, 1 - slot, b - 1, sems, n).wait()
        write(1 - slot, slice(IMAGES), o_tail[ALL].astype(BF), xt_ref[ALL])
        copies = [pltpu.make_async_copy(buf.at[1 - slot, pl.ds(0, IMAGES)], hbm.at[pl.ds(TAIL, IMAGES)], sems.at[n, 1 - slot])
                  for n, (buf, hbm) in enumerate(outs)]
        for cp in copies:
            cp.start()
        for cp in copies:
            cp.wait()
        for n, (buf, hbm) in enumerate(outs):
            out_copy(buf, hbm, slot, b, sems, n).wait()
        gather.end()


def out_copy(buf, hbm, slot, b, sems, n):
    return pltpu.make_async_copy(buf.at[slot], hbm.at[pl.ds(pl.multiple_of(b * MAIN, MAIN), MAIN)], sems.at[n, slot])


def attn_call(qkv, xim, w, wb, gain, bias, proj):
    hbm = pl.BlockSpec(memory_space=pl.ANY)
    main = lambda n: by_rows(MAIN, n)
    tail = lambda n: by_rows(IMAGES, n, lambda i: TAIL // IMAGES)
    stat = pl.BlockSpec((1, HEADS, MAIN), lambda i: (i, 0, 0))
    return pl.pallas_call(
        attn_kernel,
        grid=(IMAGES,),
        in_specs=[main(QKV), tail(QKV), main(WIDTH), tail(WIDTH),
                  whole(WIDTH, WIDTH), *[whole(1, WIDTH)] * 3, whole(*proj.shape)],
        out_specs=[hbm, hbm, hbm, stat, stat, hbm],
        out_shape=[*[jax.ShapeDtypeStruct((TOKENS, WIDTH), BF)] * 3,
                   jax.ShapeDtypeStruct((IMAGES, HEADS, MAIN), F32), jax.ShapeDtypeStruct((IMAGES, HEADS, MAIN), F32),
                   PROJ_ALL.full_shape],
        scratch_shapes=[pltpu.VMEM((IMAGES, QKV), F32), pltpu.VMEM((IMAGES, WIDTH), F32),
                        pltpu.VMEM((WIDTH, MAIN), F32), pltpu.VMEM((HEADS, MAIN), F32),
                        *[pltpu.VMEM((2, MAIN, WIDTH), BF)] * 3, *[pltpu.VMEM((MAIN, MAIN), F32)] * 2, pltpu.SemaphoreType.DMA((3, 2)),
                        pltpu.VMEM(proj.shape, BF)] + PROJ_ALL.scratch(),
        compiler_params=comm_params(5),
        cost_estimate=ATTN_COST,
        name="attn",
    )(qkv, qkv, xim, xim, w, wb, gain, bias, proj)


def outb_kernel(dr_ref, o_ref, w_ref, do_ref, dw_ref):
    n = MAIN
    c = step_id()
    do_ref[ALL] = dot_nt(dr_ref[ALL], w_ref[ALL]).astype(BF)
    dw_ref[ALL] = dot_tn(o_ref[ALL], dr_ref[:, pl.ds(pl.multiple_of(c * n, n), n)])


def outb_call(dr, o, w):
    n = MAIN
    full = whole(TOKENS, WIDTH)
    return pl.pallas_call(
        outb_kernel,
        grid=(WIDTH // n,),
        in_specs=[full, full, by_rows(n, WIDTH)],
        out_specs=[by_cols(TOKENS, n), by_cols(WIDTH, n)],
        out_shape=[jax.ShapeDtypeStruct((TOKENS, WIDTH), BF), jax.ShapeDtypeStruct((WIDTH, WIDTH), F32)],
        compiler_params=pltpu.CompilerParams(dimension_semantics=("arbitrary",), vmem_limit_bytes=VMEM_MAX),
        cost_estimate=cost(QUAD * TOKENS * WIDTH * WIDTH, 30_000_000),
        name="outb",
    )(dr, o, w)


def attn_back_kernel(qkv_ref, qkvt_ref, do_ref, dot_ref, max_ref, inv_ref, dw_ref, dqkv_hbm, dwb_ref, dwout_ref,
                     tails, do_tails, grad_tails, dq_t, dk, dv, ds_tail, sa, da, sb, db, buf, sems, *comm):
    b = step_id()
    by_row = FC_SUM.bind(comm)

    @pl.when(b == 0)
    def _():
        by_row.meet()
    advance((by_row,), b, first_chunks(OUT_STEPS), lambda n, exchange, c: exchange.result(c, dwout_ref))

    @pl.when(b < OUT_STEPS)
    def _():
        by_row.put_local(b, dw_ref[ALL])

    @pl.when(b < IMAGES)
    def _():
        image_back(b, qkv_ref, qkvt_ref, do_ref, dot_ref, max_ref, inv_ref, dqkv_hbm, dwb_ref,
                   tails, do_tails, grad_tails, dq_t, dk, dv, ds_tail, ((sa, da), (sb, db)), buf, sems)


OUT_STEPS = WIDTH // MAIN


def image_back(b, qkv_ref, qkvt_ref, do_ref, dot_ref, max_ref, inv_ref, dqkv_hbm, dwb_ref,
               tails, do_tails, grad_tails, dq_t, dk, dv, ds_tail, ahead, buf, sems):
    last = IMAGES - 1
    slot = b % 2

    @pl.when(b == 0)
    def _():
        tails[ALL] = qkvt_ref[ALL].astype(F32)
        do_tails[ALL] = dot_ref[ALL].astype(F32)
        clear(dwb_ref)

    heads = head_rows()
    q_t, k_t, v_t = (heads * z for z in thirds(tails, pl.ds(b, 1)))
    do_t = heads * do_tails[pl.ds(b, 1), :]
    q, k, v = thirds(qkv_ref)
    do = do_ref[ALL]
    q_t16, k_t16, v_t16, do_t16 = (z.astype(BF) for z in (q_t, k_t, v_t, do_t))

    p, p_self = tail_softmax(dot_nt(q_t16, k), row_sum(q_t * k_t))
    dp, dp_self = dot_nt(do_t16, v), row_sum(do_t * v_t)
    inner = row_sum(p * dp) + p_self * dp_self
    ds16 = (p * (dp - inner) * SCALE).astype(BF)
    ds_self = (p_self * (dp_self - inner) * SCALE).astype(BF).astype(F32)
    grad_q = col_sum(dot(ds16, k) * heads + ds_self * k_t)
    grad_k = ds_self * q_t
    grad_v = p_self.astype(BF).astype(F32) * do_t
    dk[ALL] = dot_tn(ds16, q_t16)
    dv[ALL] = dot_tn(p.astype(BF), do_t16)

    p_tail = jnp.exp((dot_nt(k_t16, q) - max_ref[0]) * SCALE) * inv_ref[0]
    dp_tail = dot_nt(v_t16, do)
    inner_tail = p_tail * dp_tail

    k_turned = k.T

    def masked(h):
        first, wide, _ = window(h)
        here, mask = pl.ds(first, wide), lane_mask(h)
        return here, jnp.where(mask, qkv_ref[:, here], jnp.zeros((), BF)), jnp.where(mask, do_ref[:, here], jnp.zeros((), BF))

    def next_products(h):
        first, wide, _ = window(h)
        _, q_h, do_h = masked(h)
        ahead[h % 2][0][ALL] = dot_nt(qkv_ref[:, pl.ds(WIDTH + first, wide)], q_h)
        ahead[h % 2][1][ALL] = dot_nt(qkv_ref[:, pl.ds(2 * WIDTH + first, wide)], do_h)
    next_products(0)
    for h in range(HEADS):
        if h + 1 < HEADS:
            next_products(h + 1)
        here, q_h, do_h = masked(h)
        mine = steps(h, 1)
        s, dp = (ref[ALL] for ref in ahead[h % 2])
        p = jnp.exp((s - max_ref[0, mine, :]) * SCALE) * inv_ref[0, mine, :]
        inner = col_sum(p * dp) + inner_tail[mine, :]
        ds = (p * (dp - inner) * SCALE).astype(BF)
        dv[:, here] += dot(p.astype(BF), do_h)
        dk[:, here] += dot(ds, q_h)
        dq_t[steps(h, HEAD), :] = dot(k_turned[steps(h, HEAD), :], ds)
        ds_tail[mine, :] = p_tail[mine, :] * (dp_tail[mine, :] - inner) * SCALE

    ds_tail16 = ds_tail[ALL].astype(BF)
    grad_k = col_sum(grad_k + dot(ds_tail16, q) * heads)
    grad_v = col_sum(grad_v + dot(p_tail.astype(BF), do) * heads)

    @pl.when(b >= 2)
    def _():
        out_copy(buf, dqkv_hbm, slot, b - 2, sems, 0).wait()

    grad = dq_t[ALL].T + dot_tn(ds_tail16, k_t16)
    for n, (main, tail) in enumerate(((grad, grad_q), (dk[ALL], grad_k), (dv[ALL], grad_v))):
        here = steps(n, WIDTH)
        buf[slot, :, here] = main.astype(BF)
        grad_tails[pl.ds(b, 1), here] = tail
        dwb_ref[:, here] += col_sum(main) + tail
    out_copy(buf, dqkv_hbm, slot, b, sems, 0).start()

    @pl.when(b == last)
    def _():
        out_copy(buf, dqkv_hbm, 1 - slot, b - 1, sems, 0).wait()
        buf[1 - slot, 0:IMAGES, :] = grad_tails[ALL].astype(BF)
        cp = pltpu.make_async_copy(buf.at[1 - slot, pl.ds(0, IMAGES)], dqkv_hbm.at[pl.ds(TAIL, IMAGES)], sems.at[0, 1 - slot])
        cp.start()
        cp.wait()
        out_copy(buf, dqkv_hbm, slot, b, sems, 0).wait()


def attn_back_call(qkv, do, top, inv, dw):
    hbm = pl.BlockSpec(memory_space=pl.ANY)
    image = lambda i: jnp.minimum(i, IMAGES - 1)
    main = lambda n: by_rows(MAIN, n, image)
    tail = lambda n: by_rows(IMAGES, n, lambda i: TAIL // IMAGES)
    stat = pl.BlockSpec((1, HEADS, MAIN), lambda i: (image(i), 0, 0))
    return pl.pallas_call(
        attn_back_kernel,
        grid=(OUT_STEPS + DRAIN,),
        in_specs=[main(QKV), tail(QKV), main(WIDTH), tail(WIDTH), stat, stat,
                  by_cols(WIDTH, MAIN, lambda i: jnp.minimum(i, OUT_STEPS - 1))],
        out_specs=[hbm, whole(1, QKV), by_cols(SHARD, MAIN, lambda i: jnp.maximum(i - DRAIN, 0))],
        out_shape=[jax.ShapeDtypeStruct((TOKENS, QKV), BF), jax.ShapeDtypeStruct((1, QKV), F32),
                   jax.ShapeDtypeStruct((SHARD, WIDTH), F32)],
        scratch_shapes=[pltpu.VMEM((IMAGES, QKV), F32), pltpu.VMEM((IMAGES, WIDTH), F32),
                        pltpu.VMEM((IMAGES, QKV), F32), pltpu.VMEM((WIDTH, MAIN), F32),
                        pltpu.VMEM((MAIN, WIDTH), F32), pltpu.VMEM((MAIN, WIDTH), F32), pltpu.VMEM((HEADS, MAIN), F32),
                        *[pltpu.VMEM((MAIN, MAIN), F32)] * QUAD, pltpu.VMEM((2, MAIN, QKV), BF), pltpu.SemaphoreType.DMA((1, 2))] + FC_SUM.scratch(),
        compiler_params=comm_params(1),
        cost_estimate=ATTN_COST,
        name="attn_back",
    )(qkv, qkv, do, do, top, inv, dw)


QB_N = MAIN
QB_STEPS = QKV // QB_N
QKV_SUM = Exchange(SHARD, QB_N, ROW_CUTS, 0, 2)
VECTOR_SUM = Exchange(3 * SUBLANE, LANE, (0, SUBLANE, 2 * SUBLANE, 3 * SUBLANE), 0)
VECTOR_STEP = QB_STEPS + 2
QB_GRID = QB_STEPS + 1 + QUAD * QKV_SUM.stride


def qkvb_kernel(xim_hbm, dr_hbm, gain_ref, vec_ref, ht_ref, dqkv_ref, w_ref, dx_hbm, dw_ref, out_vec_ref,
                acc, dr, xd, vec, sums, sems, *comm):
    t = step_id()
    by_row, by_vector = QKV_SUM.bind(comm[:Exchange.COUNT]), VECTOR_SUM.bind(comm[Exchange.COUNT:])
    loads = [pltpu.make_async_copy(dr_hbm, dr, sems.at[0]), pltpu.make_async_copy(xim_hbm, xd, sems.at[1])]
    store = pltpu.make_async_copy(xd, dx_hbm, sems.at[1])

    @pl.when(t == 0)
    def _():
        by_row.meet()
        for cp in loads:
            cp.start()
        clear(acc, sums)
        by_vector.local[0] = jnp.zeros(by_vector.blocks, F32)
        vec[ALL] = vec_ref[ALL]

    def emit_vectors(n, exchange, c):
        for part, (rows, _) in enumerate(exchange.parts[:2]):
            out_vec_ref[rows, :] = exchange.held[3][part][0, :, :SHARD]
    advance((by_row,), t, first_chunks(QB_STEPS), lambda n, exchange, c: exchange.result(c, dw_ref))
    advance((by_vector,), t - VECTOR_STEP, first_chunks(1), emit_vectors)

    @pl.when(t < QB_STEPS)
    def _():
        by_row.put_local(t, dot(ht_ref[ALL], dqkv_ref[ALL]))
        acc[ALL] += dot_nt(dqkv_ref[ALL], w_ref[ALL])

    @pl.when(t == QB_STEPS)
    def _():
        for cp in loads:
            cp.wait()

    def back(r, n):
        hat, inv = norm_stats(xd[pl.ds(r, n), :].astype(F32))
        dn = acc[pl.ds(r, n), :]
        for i, v in enumerate((dn * hat, dn)):
            sums[steps(i, SUBLANE), :] += eights(v)
        acc[pl.ds(r, n), :] = joined(dr, r, n) + norm_back(dn, hat, inv, gain_ref[ALL])

    @pl.when((t >= QB_STEPS) & (t <= VECTOR_STEP))
    def _():
        back_part(back, t - QB_STEPS)

    @pl.when(t == VECTOR_STEP)
    def _():
        back(TAIL, IMAGES)
        for i in range(2):
            vec[steps(VECTOR_ROWS - 2 + i, 1), :] = col_sum(sums[steps(i, SUBLANE), :])
        for d, place in enumerate(itertools.product(range(2), repeat=QUAD)):
            by_vector.local[(0, *place, pl.ds(0, VECTOR_ROWS), pl.ds(0, SHARD))] = vec[:, steps(d, SHARD)]

    @pl.when(t == VECTOR_STEP + 1)
    def _():
        from_image_order(acc, dr)

    @pl.when(t == VECTOR_STEP + 2)
    def _():
        def narrow(r, n):
            xd[pl.ds(r, n), :] = joined(dr, r, n).astype(BF)
        row_tiles(narrow)
        store.start()

    @pl.when(t == QB_GRID - 1)
    def _():
        store.wait()


def qkvb_call(xim, dr, gain, vec, ht, dqkv, w):
    hbm = pl.BlockSpec(memory_space=pl.ANY)
    now = lambda i: jnp.minimum(i, QB_STEPS - 1)
    return pl.pallas_call(
        qkvb_kernel,
        grid=(QB_GRID,),
        in_specs=[hbm, hbm, whole(1, WIDTH), whole(VECTOR_ROWS, WIDTH),
                  whole(WIDTH, TOKENS, pipeline_mode=pl.Buffered(1)), by_cols(TOKENS, QB_N, now), by_cols(WIDTH, QB_N, now)],
        out_specs=[hbm, by_cols(SHARD, QB_N, lambda i: jnp.clip(i - 1 - QUAD * QKV_SUM.stride, 0, QB_STEPS - 1)),
                   whole(VECTOR_ROWS, SHARD)],
        out_shape=[jax.ShapeDtypeStruct((TOKENS, WIDTH), BF), jax.ShapeDtypeStruct((SHARD, QKV), F32),
                   jax.ShapeDtypeStruct((VECTOR_ROWS, SHARD), F32)],
        scratch_shapes=[pltpu.VMEM((TOKENS, WIDTH), F32), pltpu.VMEM((LANES, TOKENS, LANE), F32), pltpu.VMEM((TOKENS, WIDTH), BF),
                        pltpu.VMEM((VECTOR_ROWS, WIDTH), F32), pltpu.VMEM((2 * SUBLANE, WIDTH), F32), pltpu.SemaphoreType.DMA((2,))]
                       + QKV_SUM.scratch() + VECTOR_SUM.scratch(),
        compiler_params=comm_params(2),
        cost_estimate=cost(QUAD * TOKENS * WIDTH * QKV, 80_000_000),
        name="qkvb",
    )(xim, dr, gain, vec, ht, dqkv, w)


def to_steps(v):
    rows = v.shape[0]
    return v.reshape(rows, PARTS, MLP_STEPS, UNITS).swapaxes(1, 2).reshape(rows, FFN)


def from_steps(v):
    rows = v.shape[0]
    return v.reshape(rows, MLP_STEPS, PARTS, UNITS).swapaxes(1, 2).reshape(rows, FFN)


def solution(mesh):
    specs = (P("fsdp"),) * 14

    def device_step(resid_in, grad_out, ln1_gain, ln1_bias, qkv_weight, qkv_bias, out_weight, out_bias,
                    ln2_gain, ln2_bias, fc_weight, fc_bias, proj_weight, proj_bias):
        rows = jnp.concatenate([ln1_gain, ln1_bias, qkv_bias, out_bias, ln2_gain, ln2_bias, fc_bias, proj_bias]).reshape(-1, SHARD)
        rows = jnp.pad(rows, ((0, VECTOR_ROWS - len(rows)), (0, LANE - SHARD)))
        x = resid_in.swapaxes(0, 1).reshape(TOKENS, WIDTH)
        dy = grad_out.swapaxes(0, 1).reshape(TOKENS, WIDTH)
        xim, dyim, h, ht, rows, wq, wo = open_call(x, dy, rows, qkv_weight, out_weight)
        wq, wo = wq.reshape(WIDTH, QKV), wo.reshape(WIDTH, WIDTH)
        bo, g2, b2 = rows[5:6], rows[6:7], rows[7:8]
        joint = lambda v: v.reshape(-1, PARTS, SHARD).swapaxes(0, 1).reshape(1, -1)
        qkv, wf = qkv_call(h, wq, joint(rows[2:5]), to_steps(fc_weight.astype(BF)))
        o, r, n2, top, inv, wp = attn_call(qkv, xim, wo, bo, g2, b2, proj_weight)
        y, dr, dr16, dwf, dwp, dbf, small = mlp_call(r, n2, dyim, g2, rows[12:13], wf.reshape(WIDTH, FFN), wp, to_steps(joint(rows[8:12])))
        do, dwo = outb_call(dr16, o, wo)
        dqkv, dbq, dwo = attn_back_call(qkv, do, top, inv, dwo)
        owned = lambda v: v.reshape(PARTS, -1, WIDTH // PARTS).swapaxes(0, 1).reshape(-1, WIDTH)
        vec = jnp.concatenate([jnp.sum(small.reshape(4, 8, WIDTH), axis=1), owned(dbq), owned(from_steps(dbf))])
        vec = jnp.pad(vec, ((0, VECTOR_ROWS - len(vec)), (0, 0)))
        dx, dwq, vec = qkvb_call(xim, dr, rows[:1], vec, ht, dqkv, wq)
        dg2, db2, dbp, dbo = vec[:4]
        dbq, dbf = vec[4:7].reshape(-1), vec[7:11].reshape(-1)
        dg1, db1 = vec[VECTOR_ROWS - 2:]
        dwf = from_steps(dwf)
        unturn = lambda t: t.reshape(SEQ, IMAGES, WIDTH).swapaxes(0, 1)
        return (unturn(y), unturn(dx), dg1, db1, dwq, dbq, dwo, dbo, dg2, db2, dwf, dbf, dwp, dbp)

    return jax.shard_map(device_step, mesh=mesh, in_specs=specs, out_specs=specs, check_vma=False)
```

```python
import itertools
import math
import jax, jax.numpy as jnp
from jax import lax
from jax.experimental import pallas as pl
from jax.experimental.pallas import tpu as pltpu
from jax.sharding import PartitionSpec as P

BF, F32 = jnp.bfloat16, jnp.float32
IMAGES, SEQ, WIDTH, FFN, HEADS, HEAD = 8, 257, 1280, 5120, 16, 80
MAIN = SEQ - 1
TOKENS = IMAGES * SEQ
TAIL = IMAGES * MAIN
LN_EPS = 1e-5
VMEM_MAX = 67043328
LANE, SUBLANE, QUAD, QKV = 128, 8, 4, 3 * WIDTH
ALL = ...
LANES = WIDTH // LANE
ROWS = 32


def dot(a, b):
    return jnp.dot(a, b, preferred_element_type=F32)


def dot_nt(a, b):
    return lax.dot_general(a, b, (((1,), (1,)), ((), ())), preferred_element_type=F32)


def dot_tn(a, b):
    return lax.dot_general(a, b, (((0,), (0,)), ((), ())), preferred_element_type=F32)


def col_sum(v):
    return jnp.sum(v, axis=0, keepdims=True)


def col_max(v):
    return jnp.max(v, axis=0, keepdims=True)


def row_sum(v):
    return jnp.sum(v, axis=-1, keepdims=True)


def row_mean(v):
    return row_sum(v) * (1.0 / WIDTH)


def clear(*refs):
    for ref in refs:
        ref[ALL] = jnp.zeros_like(ref)


def step_id():
    return pl.program_id(0)


def cost(flops, bytes_accessed, transcendentals=0):
    return pl.CostEstimate(flops=flops, bytes_accessed=bytes_accessed, transcendentals=transcendentals)


def eights(v):
    return jnp.sum(v.reshape(v.shape[0] // SUBLANE, SUBLANE, v.shape[1]), axis=0)


def whole(*shape, **kw):
    return pl.BlockSpec(shape, lambda *i: (0,) * len(shape), **kw)


def by_cols(rows, cols, at=lambda i: i):
    return pl.BlockSpec((rows, cols), lambda i: (0, at(i)))


def by_rows(rows, cols, at=lambda i: i):
    return pl.BlockSpec((rows, cols), lambda i: (at(i), 0))


def steps(first, wide):
    return slice(first * wide, (first + 1) * wide)


def regroup(rows, source, load, store):
    groups = LANE // UNITS
    lane = lax.broadcasted_iota(jnp.int32, (rows, LANE), 1) // UNITS
    for tile in range(FFN // LANE):
        out = None
        for i in range(groups):
            n = source(tile * groups + i)
            piece = load(n // groups)
            shift = (i - n) % groups
            if shift:
                piece = pltpu.roll(piece, shift * UNITS, 1)
            out = piece if out is None else jnp.where(lane == i, piece, out)
        store(tile, out)


def norm_stats(values):
    mean = row_mean(values)
    centered = values - mean
    inv = lax.rsqrt(row_mean(centered * centered) + LN_EPS)
    return centered * inv, inv


BLOCKS = [slice(a, b) for a, b in ((0, 512), (512, 1024), (1024, 1536), (1536, TOKENS))]


def row_tiles(body, step=LANE):
    def loop(i, carry):
        body(pl.multiple_of(i * step, step), step)
        return carry
    lax.fori_loop(0, TAIL // step, loop, 0)
    body(TAIL, IMAGES)


def back_part(body, part):
    tiles = -(-TAIL // ROWS // 3)

    def loop(i, carry):
        tile = part * tiles + i

        @pl.when(tile < TAIL // ROWS)
        def _():
            body(pl.multiple_of(tile * ROWS, ROWS), ROWS)
        return carry
    lax.fori_loop(0, tiles, loop, 0)


def to_image_order(wide, place, step=LANE):
    per = MAIN // step
    def loop(i, carry):
        first = (i % per) * (step * IMAGES) + i // per
        rows = [wide[c, pl.ds(first, step, stride=IMAGES), :] for c in range(LANES)]
        place(pl.multiple_of(i * step, step), step, jnp.concatenate(rows, axis=1))
        return carry
    lax.fori_loop(0, IMAGES * per, loop, 0)
    place(TAIL, IMAGES, joined(wide, TAIL, IMAGES))


def from_image_order(values, wide):
    def loop(i, carry):
        rows = values[pl.ds(pl.multiple_of(i * LANE, LANE), LANE), :]
        for c in range(LANES):
            wide[c, pl.ds((i % 2) * (LANE * IMAGES) + i // 2, LANE, stride=IMAGES), :] = rows[:, steps(c, LANE)]
        return carry
    lax.fori_loop(0, 2 * IMAGES, loop, 0)
    put(wide, TAIL, IMAGES, values[pl.ds(TAIL, IMAGES), :])


def joined(wide, r, n):
    return jnp.concatenate([wide[c, pl.ds(r, n), :] for c in range(LANES)], axis=1)


def put(wide, r, n, values):
    for c in range(LANES):
        wide[c, pl.ds(r, n), :] = values[:, steps(c, LANE)]


def norm_back(dn, hat, inv, gain):
    dhat = dn * gain
    m1 = row_mean(dhat)
    m2 = row_mean(dhat * hat)
    return inv * (dhat - m1 - hat * m2)


ORDERS = ((2, 1, 0), (1, 0, 2), (0, 2, 1))


class Links:
    def find(self, send, recv):
        self.send, self.recv = send, recv
        me = lax.axis_index("fsdp")
        self.core = me % 2
        self.at = (me // SUBLANE, (me // QUAD) % 2, (me // 2) % 2)
        self.other_core = me + 1 - 2 * self.core
        self.other = [me + step - 2 * step * place for step, place in zip((SUBLANE, QUAD, 2), self.at)]
        return self

    def meet(self):
        barrier = pltpu.get_barrier_semaphore()
        devices = (self.other_core, *self.other)
        for device in devices:
            pl.semaphore_signal(barrier, inc=1, device_id=(device,), device_id_type=pl.DeviceIdType.MESH)
        pl.semaphore_wait(barrier, len(devices))

    def remote(self, src, dst, sem, device):
        return pltpu.make_async_remote_copy(src_ref=src, dst_ref=dst, send_sem=self.send.at[sem], recv_sem=self.recv.at[sem],
                                            device_id=(device,), device_id_type=pl.DeviceIdType.MESH)


class Gather(Links):
    COUNT = 2

    def __init__(self, rows, cols, cuts):
        self.rows, self.cols, self.cuts = rows, cols, cuts
        self.parts = range(len(cuts) - 1)
        self.full_shape = jax.ShapeDtypeStruct((2, 2, 2, 2, rows, cols), BF)

    def scratch(self):
        return [pltpu.SemaphoreType.DMA((SEMS,))] * self.COUNT

    def bind(self, own, full, sems):
        self.own, self.full = own, full
        return self.find(*sems)

    def region(self, part, known, arrived=False):
        done = ORDERS[part][:known]
        place = [slice(None) if a in done else self.at[a] for a in range(3)]
        if arrived:
            place[done[-1]] = 1 - self.at[done[-1]]
        return (*place, self.core, pl.ds(self.cuts[part], self.cuts[part + 1] - self.cuts[part]))

    def hop(self, stage, part):
        where = self.full.at[self.region(part, stage - 1)]
        source = self.own.at[self.region(part, 0)[-1]] if stage == 1 else where
        return self.remote(source, where, QUAD * stage + part, self.other[ORDERS[part][stage - 1]])

    def forward(self, stage, part):
        if stage == 0:
            return self.remote(self.own, self.full.at[(*self.at, self.core)], 0, self.other_core)
        where = self.full.at[self.region(part, stage, True)]
        return self.remote(where, where, QUAD * (stage + 3) + part, self.other_core)

    def keep(self):
        return pltpu.make_async_copy(self.own, self.full.at[(*self.at, self.core)], self.send.at[1])

    def begin(self):
        for part in self.parts:
            self.hop(1, part).start()
        self.forward(0, 0).start()
        self.keep().start()

    def turn(self, stage):
        if stage == 1:
            self.keep().wait()
        for part in self.parts:
            self.hop(stage, part).wait()
            if stage < 3:
                self.hop(stage + 1, part).start()
        for part in self.parts:
            self.forward(stage, part).start()

    def end(self):
        self.forward(0, 0).wait()
        for stage in range(1, QUAD):
            for part in self.parts:
                self.forward(stage, part).wait()


SEMS = 28


class Exchange(Links):
    def __init__(self, rows, cols, cuts, along, stride=1, spare=0):
        self.rows, self.cols, self.stride = rows, cols, stride
        self.slots, self.locals = 3 * stride + spare, 1 + stride
        self.blocks = (2, 2, 2, 2, rows, cols)
        self.parts = [((slice(a, b), slice(None)) if along == 0 else (slice(None), slice(a, b))) for a, b in zip(cuts, cuts[1:])]
        self.shapes = [((b - a, cols) if along == 0 else (rows, b - a)) for a, b in zip(cuts, cuts[1:])]

    def scratch(self):
        two = (2, 2, 2)
        out = [pltpu.VMEM((self.locals, *self.blocks), F32), pltpu.VMEM((self.slots, *two, self.rows, self.cols), F32)]
        for axes in (2, 1, 0):
            out += [pltpu.VMEM((self.slots, *two[:axes], *shape), F32) for shape in self.shapes]
        return out + [pltpu.SemaphoreType.DMA((10, self.slots))] * 2

    COUNT = 13

    def bind(self, refs):
        self.local, self.pair = refs[0], refs[1]
        self.held = [None, refs[2:5], refs[5:SUBLANE], refs[SUBLANE:11]]
        return self.find(*refs[11:])

    def index(self, stage, part, side):
        order = ORDERS[part]
        left = [a for a in range(3) if a not in order[:stage - 1]]
        axis = order[stage - 1]
        where = self.at[axis] if side else 1 - self.at[axis]
        return tuple(where if a == axis else slice(None) for a in left)

    def copy(self, stage, part, c):
        slot = c % self.slots
        if stage == 0:
            return self.remote(self.local.at[c % self.locals, :, :, :, 1 - self.core], self.pair.at[slot], (0, slot), self.other_core)
        source = self.pair if stage == 1 else self.held[stage - 1][part]
        tail = self.parts[part] if stage == 1 else ()
        return self.remote(source.at[(slot, *self.index(stage, part, False), *tail)], self.held[stage][part].at[slot],
                           (3 * stage - 2 + part, slot), self.other[ORDERS[part][stage - 1]])

    def start(self, stage, c):
        for part in range(1 if stage == 0 else 3):
            self.copy(stage, part, c).start()

    def wait(self, stage, c):
        for part in range(1 if stage == 0 else 3):
            self.copy(stage, part, c).wait()

    def add(self, stage, c):
        slot = c % self.slots
        if stage == 0:
            for chip in itertools.product(range(2), repeat=3):
                self.pair[(slot, *chip)] += self.local[(c % self.locals, *chip, self.core)]
            return
        for part in range(3):
            source = self.pair if stage == 1 else self.held[stage - 1][part]
            tail = self.parts[part] if stage == 1 else ()
            for place in itertools.product(range(2), repeat=3 - stage):
                free = iter(place)
                kept = tuple(next(free) if isinstance(i, slice) else i for i in self.index(stage, part, True))
                self.held[stage][part][(slot, *place)] += source[(slot, *kept, *tail)]

    def result(self, c, out_ref):
        for part in range(3):
            out_ref[self.parts[part]] = self.held[3][part][c % self.slots]

    def put_local(self, c, values):
        self.local[c % self.locals] = values.reshape(self.blocks)


def comm_params(n):
    return pltpu.CompilerParams(dimension_semantics=("arbitrary",), vmem_limit_bytes=VMEM_MAX, collective_id=n, has_side_effects=True)


def advance(exchanges, t, exists, emit):
    for stage in (3, 2, 1, 0):
        c = t - 1 - (stage + 1) * exchanges[0].stride

        @pl.when(exists(c))
        def _():
            for n, exchange in enumerate(exchanges):
                exchange.wait(stage, c)
                exchange.add(stage, c)
                if stage < 3:
                    exchange.start(stage + 1, c)
                else:
                    emit(n, exchange, c)

    @pl.when(exists(t - 1))
    def _():
        for exchange in exchanges:
            exchange.start(0, t - 1)


def first_chunks(n):
    return lambda c: (c >= 0) & (c < n)


DRAIN = 5


PARTS = 16
SHARD = WIDTH // PARTS
VECTOR_ROWS = PARTS
MLP_F = MAIN
UNITS = MLP_F // PARTS
MLP_STEPS = FFN // MLP_F
WIDTH_CUTS = (0, 384, 896, WIDTH)
GATHER_CUTS = (0, 32, 64, SHARD)
QKV_ALL = Gather(SHARD, QKV, GATHER_CUTS)
OUT_ALL = Gather(SHARD, WIDTH, GATHER_CUTS)
FC_ALL = Gather(SHARD, FFN, GATHER_CUTS)
PROJ_ALL = Gather(FFN // PARTS, WIDTH, (0, 112, 208, FFN // PARTS))
VECTOR_ALL = Gather(SHARD, LANE, (0, SHARD))


def open_kernel(x_hbm, dy_hbm, rows_ref, fc_ref, wq_ref, wo_ref, xim_hbm, dyim_hbm, h_hbm, ht_hbm, vec_ref, fc_own, wq_full, wo_full,
                x, dy, wide, h, ht, rows, vec_own, vec_full, wq_own, wo_own, sems, *comm):
    loads = [pltpu.make_async_copy(src, dst, sems.at[i]) for i, (src, dst) in enumerate(((x_hbm, x), (dy_hbm, dy)))]
    for cp in loads:
        cp.start()
    clear(rows)
    rows[:VECTOR_ROWS, :] = rows_ref[ALL]
    vec_own[ALL] = rows[ALL].T[:SHARD, :].astype(BF)
    wq_own[ALL] = wq_ref[ALL].astype(BF)
    wo_own[ALL] = wo_ref[ALL].astype(BF)
    pairs = [comm[2 * i:2 * i + 2] for i in range(3)]
    vectors = VECTOR_ALL.bind(vec_own, vec_full, pairs[0])
    weights = QKV_ALL.bind(wq_own, wq_full, pairs[1]), OUT_ALL.bind(wo_own, wo_full, pairs[2])
    gathers = (vectors, *weights)
    vectors.meet()
    for gather in gathers:
        gather.begin()
    for cp in loads:
        cp.wait()

    def reorder(tokens):
        def widen(r, n):
            put(wide, r, n, tokens[pl.ds(r, n), :].astype(F32))
        row_tiles(widen)

        def place(r, n, values):
            tokens[pl.ds(r, n), :] = values.astype(BF)
        to_image_order(wide, place)
    reorder(x)
    for gather in gathers:
        gather.turn(1)
    reorder(dy)

    def store_fc(tile, values):
        fc_own[:, steps(tile, LANE)] = values.astype(BF)
    regroup(SHARD, lambda n: n % PARTS * MLP_STEPS + n // PARTS, lambda tile: fc_ref[:, steps(tile, LANE)], store_fc)
    for gather in gathers:
        gather.turn(2)
    vectors.turn(3)
    vectors.end()
    vec_ref[ALL] = vec_full[ALL].reshape(WIDTH, LANE).astype(F32).T[:VECTOR_ROWS, :]
    gain, bias = vec_ref[0:1, :], vec_ref[1:2, :]

    def norm(r, n):
        hat, _ = norm_stats(x[pl.ds(r, n), :].astype(F32))
        h[pl.ds(r, n), :] = (hat * gain + bias).astype(BF)
    row_tiles(norm, ROWS)
    for b in range(IMAGES):
        ht[:, steps(b, MAIN)] = h[steps(b, MAIN), :].T
    ht[:, TAIL:] = h[TAIL:, :].T
    stores = [pltpu.make_async_copy(src, dst, sems.at[i]) for i, (src, dst) in enumerate(((x, xim_hbm), (dy, dyim_hbm), (h, h_hbm), (ht, ht_hbm)))]
    for cp in stores:
        cp.start()
    for gather in weights:
        gather.turn(3)
    for gather in weights:
        gather.end()
    for cp in stores:
        cp.wait()


def open_call(x, dy, rows, fc, wq, wo):
    hbm, vmem = pl.BlockSpec(memory_space=pl.ANY), pl.BlockSpec(memory_space=pltpu.VMEM)
    return pl.pallas_call(
        open_kernel,
        in_specs=[hbm, hbm, vmem, vmem, vmem, vmem],
        out_specs=[hbm, hbm, hbm, hbm, vmem, vmem, hbm, hbm],
        out_shape=[*[jax.ShapeDtypeStruct((TOKENS, WIDTH), BF)] * 3,
                   jax.ShapeDtypeStruct((WIDTH, TOKENS), BF), jax.ShapeDtypeStruct((VECTOR_ROWS, WIDTH), F32),
                   jax.ShapeDtypeStruct(fc.shape, BF), QKV_ALL.full_shape, OUT_ALL.full_shape],
        scratch_shapes=[pltpu.VMEM((TOKENS, WIDTH), BF), pltpu.VMEM((TOKENS, WIDTH), BF), pltpu.VMEM((LANES, TOKENS, LANE), F32),
                        pltpu.VMEM((TOKENS, WIDTH), BF), pltpu.VMEM((WIDTH, TOKENS), BF), pltpu.VMEM((LANE, LANE), F32), pltpu.VMEM((SHARD, LANE), BF),
                        pltpu.VMEM(VECTOR_ALL.full_shape.shape, BF), pltpu.VMEM((SHARD, QKV), BF), pltpu.VMEM((SHARD, WIDTH), BF),
                        pltpu.SemaphoreType.DMA((QUAD,))] + VECTOR_ALL.scratch() + QKV_ALL.scratch() + OUT_ALL.scratch(),
        compiler_params=pltpu.CompilerParams(vmem_limit_bytes=VMEM_MAX, collective_id=3, has_side_effects=True),
        cost_estimate=cost(1_000_000_000, 60_000_000),
        name="open",
    )(x, dy, rows, fc, wq, wo)


QKV_N = 768


def qkv_kernel(h_ref, w_ref, wb_ref, own_ref, qkv_ref, full, *sems):
    t, last = step_id(), pl.num_programs(0) - 1
    gather = FC_ALL.bind(own_ref, full, sems)

    @pl.when(t == 0)
    def _():
        gather.meet()
        gather.begin()

    @pl.when(t == 1)
    def _():
        gather.turn(1)

    @pl.when(t == 3)
    def _():
        gather.turn(2)
    for rows in BLOCKS:
        qkv_ref[rows, :] = (dot(h_ref[rows, :], w_ref[ALL]) + wb_ref[ALL]).astype(BF)

    @pl.when(t == last)
    def _():
        gather.turn(3)
        gather.end()


def qkv_call(h, w, wb, own):
    hbm = pl.BlockSpec(memory_space=pl.ANY)
    return pl.pallas_call(
        qkv_kernel,
        grid=(QKV // QKV_N,),
        in_specs=[whole(TOKENS, WIDTH, pipeline_mode=pl.Buffered(1)), by_cols(WIDTH, QKV_N), by_cols(1, QKV_N), whole(SHARD, FFN)],
        out_specs=[by_cols(TOKENS, QKV_N), hbm],
        out_shape=[jax.ShapeDtypeStruct((TOKENS, QKV), BF), FC_ALL.full_shape],
        scratch_shapes=FC_ALL.scratch(),
        compiler_params=comm_params(QUAD),
        cost_estimate=cost(2 * TOKENS * WIDTH * QKV, 60_000_000),
        name="qkv",
    )(h, w, wb, own)


ROW_CUTS = (0, 24, 48, 80)
FC_SUM = Exchange(SHARD, MLP_F, ROW_CUTS, 0)
PROJ_SUM = Exchange(UNITS, WIDTH, WIDTH_CUTS, 1)
CDF_P = 0.33
CDF_C = (0.1326322871417956, 0.11939570820799192, 0.18103829560051796, -0.08904113226212501,
         0.33075919469138065, -0.22023738432274684, 0.0454530347223348)


def gelu_pair(u):
    bell = jnp.exp(u * u * -0.5)
    t = 1.0 / (1.0 + CDF_P * jnp.abs(u))
    poly = CDF_C[6]
    for c in CDF_C[5::-1]:
        poly = poly * t + c
    tail = poly * t * bell
    cdf = jnp.where(u < 0.0, tail, 1.0 - tail)
    return u * cdf, cdf + u * bell * ((2.0 * math.pi) ** -0.5)


def mlp_kernel(r_hbm, n_hbm, dy_hbm, gain_ref, pb_ref, fc_ref, proj_ref, fcb_ref,
               y_hbm, dr_hbm, dr16_hbm, dfc_ref, dproj_ref, dfcb_ref, small_ref,
               n2, dy, y_acc, dn_acc, g, du, ua, ub, da, db, sem, *comm):
    step = step_id()
    by_row, by_col = FC_SUM.bind(comm[:Exchange.COUNT]), PROJ_SUM.bind(comm[Exchange.COUNT:])

    @pl.when(step == 0)
    def _():
        loads = [pltpu.make_async_copy(n_hbm, n2, sem), pltpu.make_async_copy(dy_hbm, dy, sem)]
        for cp in loads:
            cp.start()
        by_row.meet()
        clear(small_ref, y_acc, dn_acc)
        for cp in loads:
            cp.wait()

    outs = (dfc_ref, dproj_ref)
    advance((by_row, by_col), step, first_chunks(MLP_STEPS), lambda n, exchange, c: exchange.result(c, outs[n]))

    @pl.when(step < MLP_STEPS)
    def _():
        fcb = fcb_ref[ALL]
        fc, proj = fc_ref[ALL], proj_ref[ALL].reshape(MLP_F, WIDTH)
        bias_sum = jnp.zeros((SUBLANE, MLP_F), F32)
        tiles = [(b * MAIN, MAIN) for b in range(IMAGES - 1)] + [((IMAGES - 1) * MAIN, MAIN + IMAGES)]
        pairs = ((ua, da), (ub, db))

        def products(k):
            r, n = tiles[k]
            u_s, d_s = pairs[k % 2]
            u_s[0:n, :] = dot(n2[r:r + n, :], fc)
            d_s[0:n, :] = dot_nt(dy[r:r + n, :], proj)

        def pointwise(k, total):
            r, n = tiles[k]
            u_s, d_s = pairs[k % 2]
            value, slope = gelu_pair(u_s[0:n, :] + fcb)
            g[r:r + n, :] = value.astype(BF)
            grad = d_s[0:n, :] * slope
            du[r:r + n, :] = grad.astype(BF)
            return total + eights(grad)

        products(0)
        for k in range(1, IMAGES):
            products(k)
            bias_sum = pointwise(k - 1, bias_sum)
        bias_sum = pointwise(IMAGES - 1, bias_sum)
        dfcb_ref[ALL] = col_sum(bias_sum)
        y_acc[ALL] += dot(g[ALL], proj)
        for c in range(LANES // 2):
            part = dot_nt(du[ALL], fc_ref[steps(c, MAIN), :])
            dn_acc[2 * c] += part[:, :LANE]
            dn_acc[2 * c + 1] += part[:, LANE:]
        by_col.put_local(step, dot_tn(g[ALL], dy[ALL]))
        by_row.put_local(step, dot_tn(n2[ALL], du[ALL]))

    after = step - MLP_STEPS
    r_copy = pltpu.make_async_copy(r_hbm, n2, sem)
    out_copies = [pltpu.make_async_copy(dn_acc, dr_hbm, sem), pltpu.make_async_copy(n2, dr16_hbm, sem)]
    y_copy = pltpu.make_async_copy(dy, y_hbm, sem)

    def back(r, n):
        wide_r = n2[pl.ds(r, n), :].astype(F32)
        hat, inv = norm_stats(wide_r)
        dn = joined(dn_acc, r, n)
        wide_dy = dy[pl.ds(r, n), :].astype(F32)
        dr = wide_dy + norm_back(dn, hat, inv, gain_ref[ALL])
        put(dn_acc, r, n, dr)
        n2[pl.ds(r, n), :] = dr.astype(BF)
        y_acc[pl.ds(r, n), :] += wide_r + pb_ref[ALL]
        for i, v in enumerate((dn * hat, dn, wide_dy, dr)):
            small_ref[steps(i, SUBLANE), :] += eights(v)

    @pl.when(after == 0)
    def _():
        r_copy.start()
        r_copy.wait()
        back(TAIL, IMAGES)

    @pl.when((after >= 0) & (after < 3))
    def _():
        back_part(back, after)

    @pl.when(after == 2)
    def _():
        for cp in out_copies:
            cp.start()

    @pl.when(after == 3)
    def _():
        for cp in out_copies:
            cp.wait()
        from_image_order(y_acc, dn_acc)

        def narrow(r, n):
            dy[pl.ds(r, n), :] = joined(dn_acc, r, n).astype(BF)
        row_tiles(narrow)
        y_copy.start()

    @pl.when(after == QUAD)
    def _():
        y_copy.wait()


def mlp_call(r, n2, dy, gain, pb, fc, proj, fcb):
    hbm = pl.BlockSpec(memory_space=pl.ANY)
    vec = whole(1, WIDTH)
    now = lambda i: jnp.minimum(i, MLP_STEPS - 1)
    done = lambda i: jnp.maximum(i - DRAIN, 0)
    return pl.pallas_call(
        mlp_kernel,
        grid=(MLP_STEPS + DRAIN,),
        in_specs=[hbm, hbm, hbm, vec, vec, by_cols(WIDTH, MLP_F, now),
                  pl.BlockSpec((PARTS, None, UNITS, WIDTH), lambda i: (0, now(i), 0, 0)),
                  by_cols(1, MLP_F, now)],
        out_specs=[hbm, hbm, hbm, by_cols(SHARD, MLP_F, done),
                   by_rows(UNITS, WIDTH, done),
                   by_cols(1, MLP_F, now), whole(32, WIDTH)],
        out_shape=[jax.ShapeDtypeStruct((TOKENS, WIDTH), BF), jax.ShapeDtypeStruct((LANES, TOKENS, LANE), F32),
                   jax.ShapeDtypeStruct((TOKENS, WIDTH), BF), jax.ShapeDtypeStruct((SHARD, FFN), F32),
                   jax.ShapeDtypeStruct((FFN // PARTS, WIDTH), F32),
                   jax.ShapeDtypeStruct((1, FFN), F32), jax.ShapeDtypeStruct((32, WIDTH), F32)],
        scratch_shapes=[pltpu.VMEM((TOKENS, WIDTH), BF), pltpu.VMEM((TOKENS, WIDTH), BF),
                        pltpu.VMEM((TOKENS, WIDTH), F32), pltpu.VMEM((LANES, TOKENS, LANE), F32),
                        pltpu.VMEM((TOKENS, MLP_F), BF), pltpu.VMEM((TOKENS, MLP_F), BF)]
                       + [pltpu.VMEM((MAIN + IMAGES, MLP_F), F32)] * QUAD + [pltpu.SemaphoreType.DMA]
                       + FC_SUM.scratch() + PROJ_SUM.scratch(),
        compiler_params=comm_params(0),
        cost_estimate=cost(12 * TOKENS * WIDTH * FFN, 150_000_000, TOKENS * FFN),
        name="mlp",
    )(r, n2, dy, gain, pb, fc, proj.reshape(PARTS, MLP_STEPS, UNITS, WIDTH), fcb)


SCALE = HEAD ** -0.5
ATTN_COST = cost(40_000_000_000, 50_000_000, 8_400_000)


def window(h):
    first = min(HEAD * h // LANE * LANE, WIDTH - MAIN)
    wide = LANE if HEAD * h + HEAD <= first + LANE else MAIN
    return first, wide, HEAD * h - first


def lane_mask(h):
    first, wide, off = window(h)
    lane = lax.broadcasted_iota(jnp.int32, (MAIN, wide), 1)
    return (lane >= off) & (lane < off + HEAD)


def thirds(ref, rows=slice(None)):
    return [ref[rows, steps(i, WIDTH)] for i in range(3)]


def head_rows():
    lane = lax.broadcasted_iota(jnp.int32, (HEADS, WIDTH), 1)
    row = lax.broadcasted_iota(jnp.int32, (HEADS, WIDTH), 0)
    return (lane // HEAD == row).astype(F32)


def tail_softmax(s, s_self):
    m = jnp.maximum(jnp.max(s, axis=1, keepdims=True), s_self)
    e = jnp.exp((s - m) * SCALE)
    e_self = jnp.exp((s_self - m) * SCALE)
    inv = 1.0 / (row_sum(e) + e_self)
    return e * inv, e_self * inv


def attn_kernel(qkv_ref, qkvt_ref, x_ref, xt_ref, w_ref, wb_ref, gain_ref, bias_ref, proj_ref, o_hbm, r_hbm, n_hbm,
                max_ref, inv_ref, full,
                tails, o_tail, o_t, ptail, o_buf, r_buf, n_buf, sa, sb, sems, own, *comm):
    b, last = step_id(), pl.num_programs(0) - 1
    slot = b % 2
    gather = PROJ_ALL.bind(own, full, comm)

    @pl.when(b == 0)
    def _():
        tails[ALL] = qkvt_ref[ALL].astype(F32)
        own[ALL] = proj_ref[ALL].astype(BF)
        gather.meet()
        gather.begin()

    @pl.when(b == 1)
    def _():
        gather.turn(1)

    @pl.when(b == 3)
    def _():
        gather.turn(2)

    @pl.when(b == last)
    def _():
        gather.turn(3)

    heads = head_rows()
    q_t, k_t, v_t = (heads * z for z in thirds(tails, pl.ds(b, 1)))
    q, k, v = thirds(qkv_ref)

    p, p_self = tail_softmax(dot_nt(q_t.astype(BF), k), row_sum(q_t * k_t))
    mixed = dot(p.astype(BF), v) * heads + p_self.astype(BF).astype(F32) * v_t
    o_tail[pl.ds(b, 1), :] = col_sum(mixed)

    s_tail = dot_nt(k_t.astype(BF), q)
    v_turned = v.T
    scores = sa, sb

    def next_scores(h):
        first, wide, _ = window(h)
        q_h = jnp.where(lane_mask(h), qkv_ref[:, pl.ds(first, wide)], jnp.zeros((), BF))
        scores[h % 2][ALL] = dot_nt(qkv_ref[:, pl.ds(WIDTH + first, wide)], q_h)
    next_scores(0)
    for h in range(HEADS):
        if h + 1 < HEADS:
            next_scores(h + 1)
        s, mine = scores[h % 2], steps(h, 1)
        top = jnp.maximum(col_max(s[ALL]), s_tail[mine, :])
        e = jnp.exp((s[ALL] - top) * SCALE)
        e_tail = jnp.exp((s_tail[mine, :] - top) * SCALE)
        inv = 1.0 / (col_sum(e) + e_tail)
        max_ref[0, mine, :] = top
        inv_ref[0, mine, :] = inv
        ptail[mine, :] = e_tail * inv
        o_t[steps(h, HEAD), :] = dot(v_turned[steps(h, HEAD), :], (e * inv).astype(BF))

    outs = (o_buf, o_hbm), (r_buf, r_hbm), (n_buf, n_hbm)

    def write(slot, rows, o, x):
        o_buf[slot, rows, :] = o
        r = (x.astype(F32) + dot(o, w_ref[ALL]) + wb_ref[ALL]).astype(BF)
        r_buf[slot, rows, :] = r
        hat, _ = norm_stats(r.astype(F32))
        n_buf[slot, rows, :] = (hat * gain_ref[ALL] + bias_ref[ALL]).astype(BF)

    @pl.when(b >= 2)
    def _():
        for n, (buf, hbm) in enumerate(outs):
            out_copy(buf, hbm, slot, b - 2, sems, n).wait()

    o = (o_t[ALL].T + dot_tn(ptail[ALL].astype(BF), v_t.astype(BF))).astype(BF)
    write(slot, slice(None), o, x_ref[ALL])
    for n, (buf, hbm) in enumerate(outs):
        out_copy(buf, hbm, slot, b, sems, n).start()

    @pl.when(b == last)
    def _():
        for n, (buf, hbm) in enumerate(outs):
            out_copy(buf, hbm, 1 - slot, b - 1, sems, n).wait()
        write(1 - slot, slice(IMAGES), o_tail[ALL].astype(BF), xt_ref[ALL])
        copies = [pltpu.make_async_copy(buf.at[1 - slot, pl.ds(0, IMAGES)], hbm.at[pl.ds(TAIL, IMAGES)], sems.at[n, 1 - slot])
                  for n, (buf, hbm) in enumerate(outs)]
        for cp in copies:
            cp.start()
        for cp in copies:
            cp.wait()
        for n, (buf, hbm) in enumerate(outs):
            out_copy(buf, hbm, slot, b, sems, n).wait()
        gather.end()


def out_copy(buf, hbm, slot, b, sems, n):
    return pltpu.make_async_copy(buf.at[slot], hbm.at[pl.ds(pl.multiple_of(b * MAIN, MAIN), MAIN)], sems.at[n, slot])


def attn_call(qkv, xim, w, wb, gain, bias, proj):
    hbm = pl.BlockSpec(memory_space=pl.ANY)
    main = lambda n: by_rows(MAIN, n)
    tail = lambda n: by_rows(IMAGES, n, lambda i: TAIL // IMAGES)
    stat = pl.BlockSpec((1, HEADS, MAIN), lambda i: (i, 0, 0))
    return pl.pallas_call(
        attn_kernel,
        grid=(IMAGES,),
        in_specs=[main(QKV), tail(QKV), main(WIDTH), tail(WIDTH),
                  whole(WIDTH, WIDTH), *[whole(1, WIDTH)] * 3, whole(*proj.shape)],
        out_specs=[hbm, hbm, hbm, stat, stat, hbm],
        out_shape=[*[jax.ShapeDtypeStruct((TOKENS, WIDTH), BF)] * 3,
                   jax.ShapeDtypeStruct((IMAGES, HEADS, MAIN), F32), jax.ShapeDtypeStruct((IMAGES, HEADS, MAIN), F32),
                   PROJ_ALL.full_shape],
        scratch_shapes=[pltpu.VMEM((IMAGES, QKV), F32), pltpu.VMEM((IMAGES, WIDTH), F32),
                        pltpu.VMEM((WIDTH, MAIN), F32), pltpu.VMEM((HEADS, MAIN), F32),
                        *[pltpu.VMEM((2, MAIN, WIDTH), BF)] * 3, *[pltpu.VMEM((MAIN, MAIN), F32)] * 2, pltpu.SemaphoreType.DMA((3, 2)),
                        pltpu.VMEM(proj.shape, BF)] + PROJ_ALL.scratch(),
        compiler_params=comm_params(5),
        cost_estimate=ATTN_COST,
        name="attn",
    )(qkv, qkv, xim, xim, w, wb, gain, bias, proj)


def outb_kernel(dr_ref, o_ref, w_ref, dfc_ref, y_in, dproj_in, do_ref, dw_ref, dfc_out, y_out, dproj_out, y, dproj, sems):
    c, last = step_id(), pl.num_programs(0) - 1
    loads = [pltpu.make_async_copy(src, dst, sems.at[i]) for i, (src, dst) in enumerate(((y_in, y), (dproj_in, dproj)))]
    stores = [pltpu.make_async_copy(src, dst, sems.at[i]) for i, (src, dst) in enumerate(((y, y_out), (dproj, dproj_out)))]

    @pl.when(c == 0)
    def _():
        for cp in loads:
            cp.start()

    @pl.when(c == 1)
    def _():
        for cp in loads:
            cp.wait()
        for cp in stores:
            cp.start()

        def store_fc(tile, values):
            dfc_out[:, steps(tile, LANE)] = values
        regroup(SHARD, lambda n: n % MLP_STEPS * PARTS + n // MLP_STEPS, lambda tile: dfc_ref[:, steps(tile, LANE)], store_fc)
    do_ref[ALL] = dot_nt(dr_ref[ALL], w_ref[ALL]).astype(BF)
    dw_ref[ALL] = dot_tn(o_ref[ALL], dr_ref[:, pl.ds(pl.multiple_of(c * MAIN, MAIN), MAIN)])

    @pl.when(c == last)
    def _():
        for cp in stores:
            cp.wait()


def outb_call(dr, o, w, dfc, y, dproj):
    full, hbm = whole(TOKENS, WIDTH), pl.BlockSpec(memory_space=pl.ANY)
    like = lambda v: jax.ShapeDtypeStruct(v.shape, v.dtype)
    return pl.pallas_call(
        outb_kernel,
        grid=(WIDTH // MAIN,),
        in_specs=[full, full, by_rows(MAIN, WIDTH), whole(*dfc.shape), hbm, hbm],
        out_specs=[by_cols(TOKENS, MAIN), by_cols(WIDTH, MAIN), whole(*dfc.shape), hbm, hbm],
        out_shape=[like(dr), jax.ShapeDtypeStruct((WIDTH, WIDTH), F32), like(dfc), like(y), like(dproj)],
        scratch_shapes=[pltpu.VMEM(y.shape, BF), pltpu.VMEM(dproj.shape, F32), pltpu.SemaphoreType.DMA((2,))],
        compiler_params=pltpu.CompilerParams(dimension_semantics=("arbitrary",), vmem_limit_bytes=VMEM_MAX),
        cost_estimate=cost(QUAD * TOKENS * WIDTH * WIDTH, 50_000_000),
        name="outb",
    )(dr, o, w, dfc, y, dproj)


def attn_back_kernel(qkv_ref, qkvt_ref, do_ref, dot_ref, max_ref, inv_ref, dw_ref, dqkv_hbm, dwb_ref, dwout_ref,
                     tails, do_tails, grad_tails, dq_t, dk, dv, ds_tail, sa, da, sb, db, buf, sems, *comm):
    b = step_id()
    by_row = FC_SUM.bind(comm)

    @pl.when(b == 0)
    def _():
        by_row.meet()
    advance((by_row,), b, first_chunks(OUT_STEPS), lambda n, exchange, c: exchange.result(c, dwout_ref))

    @pl.when(b < OUT_STEPS)
    def _():
        by_row.put_local(b, dw_ref[ALL])

    @pl.when(b < IMAGES)
    def _():
        image_back(b, qkv_ref, qkvt_ref, do_ref, dot_ref, max_ref, inv_ref, dqkv_hbm, dwb_ref,
                   tails, do_tails, grad_tails, dq_t, dk, dv, ds_tail, ((sa, da), (sb, db)), buf, sems)


OUT_STEPS = WIDTH // MAIN


def image_back(b, qkv_ref, qkvt_ref, do_ref, dot_ref, max_ref, inv_ref, dqkv_hbm, dwb_ref,
               tails, do_tails, grad_tails, dq_t, dk, dv, ds_tail, ahead, buf, sems):
    last = IMAGES - 1
    slot = b % 2

    @pl.when(b == 0)
    def _():
        tails[ALL] = qkvt_ref[ALL].astype(F32)
        do_tails[ALL] = dot_ref[ALL].astype(F32)
        clear(dwb_ref)

    heads = head_rows()
    q_t, k_t, v_t = (heads * z for z in thirds(tails, pl.ds(b, 1)))
    do_t = heads * do_tails[pl.ds(b, 1), :]
    q, k, v = thirds(qkv_ref)
    do = do_ref[ALL]
    q_t16, k_t16, v_t16, do_t16 = (z.astype(BF) for z in (q_t, k_t, v_t, do_t))

    p, p_self = tail_softmax(dot_nt(q_t16, k), row_sum(q_t * k_t))
    dp, dp_self = dot_nt(do_t16, v), row_sum(do_t * v_t)
    inner = row_sum(p * dp) + p_self * dp_self
    ds16 = (p * (dp - inner) * SCALE).astype(BF)
    ds_self = (p_self * (dp_self - inner) * SCALE).astype(BF).astype(F32)
    grad_q = col_sum(dot(ds16, k) * heads + ds_self * k_t)
    grad_k = ds_self * q_t
    grad_v = p_self.astype(BF).astype(F32) * do_t
    dk[ALL] = dot_tn(ds16, q_t16)
    dv[ALL] = dot_tn(p.astype(BF), do_t16)

    p_tail = jnp.exp((dot_nt(k_t16, q) - max_ref[0]) * SCALE) * inv_ref[0]
    dp_tail = dot_nt(v_t16, do)
    inner_tail = p_tail * dp_tail

    k_turned = k.T

    def masked(h):
        first, wide, _ = window(h)
        here, mask = pl.ds(first, wide), lane_mask(h)
        return here, jnp.where(mask, qkv_ref[:, here], jnp.zeros((), BF)), jnp.where(mask, do_ref[:, here], jnp.zeros((), BF))

    def next_products(h):
        first, wide, _ = window(h)
        _, q_h, do_h = masked(h)
        ahead[h % 2][0][ALL] = dot_nt(qkv_ref[:, pl.ds(WIDTH + first, wide)], q_h)
        ahead[h % 2][1][ALL] = dot_nt(qkv_ref[:, pl.ds(2 * WIDTH + first, wide)], do_h)
    next_products(0)
    for h in range(HEADS):
        if h + 1 < HEADS:
            next_products(h + 1)
        here, q_h, do_h = masked(h)
        mine = steps(h, 1)
        s, dp = (ref[ALL] for ref in ahead[h % 2])
        p = jnp.exp((s - max_ref[0, mine, :]) * SCALE) * inv_ref[0, mine, :]
        inner = col_sum(p * dp) + inner_tail[mine, :]
        ds = (p * (dp - inner) * SCALE).astype(BF)
        dv[:, here] += dot(p.astype(BF), do_h)
        dk[:, here] += dot(ds, q_h)
        dq_t[steps(h, HEAD), :] = dot(k_turned[steps(h, HEAD), :], ds)
        ds_tail[mine, :] = p_tail[mine, :] * (dp_tail[mine, :] - inner) * SCALE

    ds_tail16 = ds_tail[ALL].astype(BF)
    grad_k = col_sum(grad_k + dot(ds_tail16, q) * heads)
    grad_v = col_sum(grad_v + dot(p_tail.astype(BF), do) * heads)

    @pl.when(b >= 2)
    def _():
        out_copy(buf, dqkv_hbm, slot, b - 2, sems, 0).wait()

    grad = dq_t[ALL].T + dot_tn(ds_tail16, k_t16)
    for n, (main, tail) in enumerate(((grad, grad_q), (dk[ALL], grad_k), (dv[ALL], grad_v))):
        here = steps(n, WIDTH)
        buf[slot, :, here] = main.astype(BF)
        grad_tails[pl.ds(b, 1), here] = tail
        dwb_ref[:, here] += col_sum(main) + tail
    out_copy(buf, dqkv_hbm, slot, b, sems, 0).start()

    @pl.when(b == last)
    def _():
        out_copy(buf, dqkv_hbm, 1 - slot, b - 1, sems, 0).wait()
        buf[1 - slot, 0:IMAGES, :] = grad_tails[ALL].astype(BF)
        cp = pltpu.make_async_copy(buf.at[1 - slot, pl.ds(0, IMAGES)], dqkv_hbm.at[pl.ds(TAIL, IMAGES)], sems.at[0, 1 - slot])
        cp.start()
        cp.wait()
        out_copy(buf, dqkv_hbm, slot, b, sems, 0).wait()


def attn_back_call(qkv, do, top, inv, dw):
    hbm = pl.BlockSpec(memory_space=pl.ANY)
    image = lambda i: jnp.minimum(i, IMAGES - 1)
    main = lambda n: by_rows(MAIN, n, image)
    tail = lambda n: by_rows(IMAGES, n, lambda i: TAIL // IMAGES)
    stat = pl.BlockSpec((1, HEADS, MAIN), lambda i: (image(i), 0, 0))
    return pl.pallas_call(
        attn_back_kernel,
        grid=(OUT_STEPS + DRAIN,),
        in_specs=[main(QKV), tail(QKV), main(WIDTH), tail(WIDTH), stat, stat,
                  by_cols(WIDTH, MAIN, lambda i: jnp.minimum(i, OUT_STEPS - 1))],
        out_specs=[hbm, whole(1, QKV), by_cols(SHARD, MAIN, lambda i: jnp.maximum(i - DRAIN, 0))],
        out_shape=[jax.ShapeDtypeStruct((TOKENS, QKV), BF), jax.ShapeDtypeStruct((1, QKV), F32),
                   jax.ShapeDtypeStruct((SHARD, WIDTH), F32)],
        scratch_shapes=[pltpu.VMEM((IMAGES, QKV), F32), pltpu.VMEM((IMAGES, WIDTH), F32),
                        pltpu.VMEM((IMAGES, QKV), F32), pltpu.VMEM((WIDTH, MAIN), F32),
                        pltpu.VMEM((MAIN, WIDTH), F32), pltpu.VMEM((MAIN, WIDTH), F32), pltpu.VMEM((HEADS, MAIN), F32),
                        *[pltpu.VMEM((MAIN, MAIN), F32)] * QUAD, pltpu.VMEM((2, MAIN, QKV), BF), pltpu.SemaphoreType.DMA((1, 2))] + FC_SUM.scratch(),
        compiler_params=comm_params(1),
        cost_estimate=ATTN_COST,
        name="attn_back",
    )(qkv, qkv, do, do, top, inv, dw)


QB_N = MAIN
QB_STEPS = QKV // QB_N
QKV_SUM = Exchange(SHARD, QB_N, ROW_CUTS, 0, 2)
VECTOR_SUM = Exchange(3 * SUBLANE, LANE, (0, SUBLANE, 2 * SUBLANE, 3 * SUBLANE), 0)
VECTOR_STEP = QB_STEPS + 2
QB_GRID = QB_STEPS + 1 + QUAD * QKV_SUM.stride


def qkvb_kernel(xim_hbm, dr_hbm, gain_ref, vec_ref, ht_ref, dqkv_ref, w_ref, dx_hbm, dw_ref, out_vec_ref,
                acc, dr, xd, vec, sums, sems, *comm):
    t = step_id()
    by_row, by_vector = QKV_SUM.bind(comm[:Exchange.COUNT]), VECTOR_SUM.bind(comm[Exchange.COUNT:])
    loads = [pltpu.make_async_copy(dr_hbm, dr, sems.at[0]), pltpu.make_async_copy(xim_hbm, xd, sems.at[1])]
    store = pltpu.make_async_copy(xd, dx_hbm, sems.at[1])

    @pl.when(t == 0)
    def _():
        by_row.meet()
        for cp in loads:
            cp.start()
        clear(acc, sums)
        by_vector.local[0] = jnp.zeros(by_vector.blocks, F32)
        vec[ALL] = vec_ref[ALL]

    def emit_vectors(n, exchange, c):
        for part, (rows, _) in enumerate(exchange.parts[:2]):
            out_vec_ref[rows, :] = exchange.held[3][part][0, :, :SHARD]
    advance((by_row,), t, first_chunks(QB_STEPS), lambda n, exchange, c: exchange.result(c, dw_ref))
    advance((by_vector,), t - VECTOR_STEP, first_chunks(1), emit_vectors)

    @pl.when(t < QB_STEPS)
    def _():
        by_row.put_local(t, dot(ht_ref[ALL], dqkv_ref[ALL]))
        acc[ALL] += dot_nt(dqkv_ref[ALL], w_ref[ALL])

    @pl.when(t == QB_STEPS)
    def _():
        for cp in loads:
            cp.wait()

    def back(r, n):
        hat, inv = norm_stats(xd[pl.ds(r, n), :].astype(F32))
        dn = acc[pl.ds(r, n), :]
        for i, v in enumerate((dn * hat, dn)):
            sums[steps(i, SUBLANE), :] += eights(v)
        acc[pl.ds(r, n), :] = joined(dr, r, n) + norm_back(dn, hat, inv, gain_ref[ALL])

    @pl.when((t >= QB_STEPS) & (t <= VECTOR_STEP))
    def _():
        back_part(back, t - QB_STEPS)

    @pl.when(t == VECTOR_STEP)
    def _():
        back(TAIL, IMAGES)
        for i in range(2):
            vec[steps(VECTOR_ROWS - 2 + i, 1), :] = col_sum(sums[steps(i, SUBLANE), :])
        for d, place in enumerate(itertools.product(range(2), repeat=QUAD)):
            by_vector.local[(0, *place, pl.ds(0, VECTOR_ROWS), pl.ds(0, SHARD))] = vec[:, steps(d, SHARD)]

    @pl.when(t == VECTOR_STEP + 1)
    def _():
        from_image_order(acc, dr)

    @pl.when(t == VECTOR_STEP + 2)
    def _():
        def narrow(r, n):
            xd[pl.ds(r, n), :] = joined(dr, r, n).astype(BF)
        row_tiles(narrow)
        store.start()

    @pl.when(t == QB_GRID - 1)
    def _():
        store.wait()


def qkvb_call(xim, dr, gain, vec, ht, dqkv, w):
    hbm = pl.BlockSpec(memory_space=pl.ANY)
    now = lambda i: jnp.minimum(i, QB_STEPS - 1)
    return pl.pallas_call(
        qkvb_kernel,
        grid=(QB_GRID,),
        in_specs=[hbm, hbm, whole(1, WIDTH), whole(VECTOR_ROWS, WIDTH),
                  whole(WIDTH, TOKENS, pipeline_mode=pl.Buffered(1)), by_cols(TOKENS, QB_N, now), by_cols(WIDTH, QB_N, now)],
        out_specs=[hbm, by_cols(SHARD, QB_N, lambda i: jnp.clip(i - 1 - QUAD * QKV_SUM.stride, 0, QB_STEPS - 1)),
                   whole(VECTOR_ROWS, SHARD)],
        out_shape=[jax.ShapeDtypeStruct((TOKENS, WIDTH), BF), jax.ShapeDtypeStruct((SHARD, QKV), F32),
                   jax.ShapeDtypeStruct((VECTOR_ROWS, SHARD), F32)],
        scratch_shapes=[pltpu.VMEM((TOKENS, WIDTH), F32), pltpu.VMEM((LANES, TOKENS, LANE), F32), pltpu.VMEM((TOKENS, WIDTH), BF),
                        pltpu.VMEM((VECTOR_ROWS, WIDTH), F32), pltpu.VMEM((2 * SUBLANE, WIDTH), F32), pltpu.SemaphoreType.DMA((2,))]
                       + QKV_SUM.scratch() + VECTOR_SUM.scratch(),
        compiler_params=comm_params(2),
        cost_estimate=cost(QUAD * TOKENS * WIDTH * QKV, 80_000_000),
        name="qkvb",
    )(xim, dr, gain, vec, ht, dqkv, w)


def to_steps(v):
    rows = v.shape[0]
    return v.reshape(rows, PARTS, MLP_STEPS, UNITS).swapaxes(1, 2).reshape(rows, FFN)


def from_steps(v):
    rows = v.shape[0]
    return v.reshape(rows, MLP_STEPS, PARTS, UNITS).swapaxes(1, 2).reshape(rows, FFN)


def solution(mesh):
    specs = (P("fsdp"),) * 14

    def device_step(resid_in, grad_out, ln1_gain, ln1_bias, qkv_weight, qkv_bias, out_weight, out_bias,
                    ln2_gain, ln2_bias, fc_weight, fc_bias, proj_weight, proj_bias):
        rows = jnp.concatenate([ln1_gain, ln1_bias, qkv_bias, out_bias, ln2_gain, ln2_bias, fc_bias, proj_bias]).reshape(-1, SHARD)
        rows = jnp.pad(rows, ((0, VECTOR_ROWS - len(rows)), (0, LANE - SHARD)))
        x = resid_in.swapaxes(0, 1).reshape(TOKENS, WIDTH)
        dy = grad_out.swapaxes(0, 1).reshape(TOKENS, WIDTH)
        xim, dyim, h, ht, rows, fc, wq, wo = open_call(x, dy, rows, fc_weight, qkv_weight, out_weight)
        wq, wo = wq.reshape(WIDTH, QKV), wo.reshape(WIDTH, WIDTH)
        bo, g2, b2 = rows[5:6], rows[6:7], rows[7:8]
        joint = lambda v: v.reshape(-1, PARTS, SHARD).swapaxes(0, 1).reshape(1, -1)
        qkv, wf = qkv_call(h, wq, joint(rows[2:5]), fc)
        o, r, n2, top, inv, wp = attn_call(qkv, xim, wo, bo, g2, b2, proj_weight)
        y, dr, dr16, dwf, dwp, dbf, small = mlp_call(r, n2, dyim, g2, rows[12:13], wf.reshape(WIDTH, FFN), wp, to_steps(joint(rows[8:12])))
        do, dwo, dwf, y, dwp = outb_call(dr16, o, wo, dwf, y, dwp)
        dqkv, dbq, dwo = attn_back_call(qkv, do, top, inv, dwo)
        owned = lambda v: v.reshape(PARTS, -1, WIDTH // PARTS).swapaxes(0, 1).reshape(-1, WIDTH)
        vec = jnp.concatenate([jnp.sum(small.reshape(4, 8, WIDTH), axis=1), owned(dbq), owned(from_steps(dbf))])
        vec = jnp.pad(vec, ((0, VECTOR_ROWS - len(vec)), (0, 0)))
        dx, dwq, vec = qkvb_call(xim, dr, rows[:1], vec, ht, dqkv, wq)
        dg2, db2, dbp, dbo = vec[:4]
        dbq, dbf = vec[4:7].reshape(-1), vec[7:11].reshape(-1)
        dg1, db1 = vec[VECTOR_ROWS - 2:]
        unturn = lambda t: t.reshape(SEQ, IMAGES, WIDTH).swapaxes(0, 1)
        return (unturn(y), unturn(dx), dg1, db1, dwq, dbq, dwo, dbo, dg2, db2, dwf, dbf, dwp, dbp)

    return jax.shard_map(device_step, mesh=mesh, in_specs=specs, out_specs=specs, check_vma=False)
```

```python
import itertools
import math
import jax, jax.numpy as jnp
from jax import lax
from jax.experimental import pallas as pl
from jax.experimental.pallas import tpu as pltpu
from jax.sharding import PartitionSpec as P

BF, F32 = jnp.bfloat16, jnp.float32
IMAGES, SEQ, WIDTH, FFN, HEADS, HEAD = 8, 257, 1280, 5120, 16, 80
MAIN = SEQ - 1
TOKENS = IMAGES * SEQ
TAIL = IMAGES * MAIN
LN_EPS = 1e-5
VMEM_MAX = 67043328
LANE, SUBLANE, QUAD, QKV = 128, 8, 4, 3 * WIDTH
ALL = ...
LANES = WIDTH // LANE
ROWS = 32


def dot(a, b):
    return jnp.dot(a, b, preferred_element_type=F32)


def dot_nt(a, b):
    return lax.dot_general(a, b, (((1,), (1,)), ((), ())), preferred_element_type=F32)


def dot_tn(a, b):
    return lax.dot_general(a, b, (((0,), (0,)), ((), ())), preferred_element_type=F32)


def col_sum(v):
    return jnp.sum(v, axis=0, keepdims=True)


def col_max(v):
    return jnp.max(v, axis=0, keepdims=True)


def row_sum(v):
    return jnp.sum(v, axis=-1, keepdims=True)


def row_mean(v):
    return row_sum(v) * (1.0 / WIDTH)


def clear(*refs):
    for ref in refs:
        ref[ALL] = jnp.zeros_like(ref)


def step_id():
    return pl.program_id(0)


def cost(flops, bytes_accessed, transcendentals=0):
    return pl.CostEstimate(flops=flops, bytes_accessed=bytes_accessed, transcendentals=transcendentals)


def eights(v):
    return jnp.sum(v.reshape(v.shape[0] // SUBLANE, SUBLANE, v.shape[1]), axis=0)


def whole(*shape, **kw):
    return pl.BlockSpec(shape, lambda *i: (0,) * len(shape), **kw)


def by_cols(rows, cols, at=lambda i: i):
    return pl.BlockSpec((rows, cols), lambda i: (0, at(i)))


def by_rows(rows, cols, at=lambda i: i):
    return pl.BlockSpec((rows, cols), lambda i: (at(i), 0))


def steps(first, wide):
    return slice(first * wide, (first + 1) * wide)


def regroup(rows, source, load, store):
    groups = LANE // UNITS
    lane = lax.broadcasted_iota(jnp.int32, (rows, LANE), 1) // UNITS
    for tile in range(FFN // LANE):
        out = None
        for i in range(groups):
            n = source(tile * groups + i)
            piece = load(n // groups)
            shift = (i - n) % groups
            if shift:
                piece = pltpu.roll(piece, shift * UNITS, 1)
            out = piece if out is None else jnp.where(lane == i, piece, out)
        store(tile, out)


def norm_stats(values):
    mean = row_mean(values)
    centered = values - mean
    inv = lax.rsqrt(row_mean(centered * centered) + LN_EPS)
    return centered * inv, inv


BLOCKS = [slice(a, b) for a, b in ((0, 512), (512, 1024), (1024, 1536), (1536, TOKENS))]


def row_tiles(body, step=LANE):
    def loop(i, carry):
        body(pl.multiple_of(i * step, step), step)
        return carry
    lax.fori_loop(0, TAIL // step, loop, 0)
    body(TAIL, IMAGES)


def back_part(body, part):
    tiles = -(-TAIL // ROWS // 3)

    def loop(i, carry):
        tile = part * tiles + i

        @pl.when(tile < TAIL // ROWS)
        def _():
            body(pl.multiple_of(tile * ROWS, ROWS), ROWS)
        return carry
    lax.fori_loop(0, tiles, loop, 0)


def to_image_order(wide, place, step=LANE):
    per = MAIN // step
    def loop(i, carry):
        first = (i % per) * (step * IMAGES) + i // per
        rows = [wide[c, pl.ds(first, step, stride=IMAGES), :] for c in range(LANES)]
        place(pl.multiple_of(i * step, step), step, jnp.concatenate(rows, axis=1))
        return carry
    lax.fori_loop(0, IMAGES * per, loop, 0)
    place(TAIL, IMAGES, joined(wide, TAIL, IMAGES))


def from_image_order(values, wide):
    def loop(i, carry):
        rows = values[pl.ds(pl.multiple_of(i * LANE, LANE), LANE), :]
        for c in range(LANES):
            wide[c, pl.ds((i % 2) * (LANE * IMAGES) + i // 2, LANE, stride=IMAGES), :] = rows[:, steps(c, LANE)]
        return carry
    lax.fori_loop(0, 2 * IMAGES, loop, 0)
    put(wide, TAIL, IMAGES, values[pl.ds(TAIL, IMAGES), :])


def joined(wide, r, n):
    return jnp.concatenate([wide[c, pl.ds(r, n), :] for c in range(LANES)], axis=1)


def put(wide, r, n, values):
    for c in range(LANES):
        wide[c, pl.ds(r, n), :] = values[:, steps(c, LANE)]


def norm_back(dn, hat, inv, gain):
    dhat = dn * gain
    m1 = row_mean(dhat)
    m2 = row_mean(dhat * hat)
    return inv * (dhat - m1 - hat * m2)


ORDERS = ((2, 1, 0), (1, 0, 2), (0, 2, 1))


class Links:
    def find(self, send, recv):
        self.send, self.recv = send, recv
        me = lax.axis_index("fsdp")
        self.core = me % 2
        self.at = (me // SUBLANE, (me // QUAD) % 2, (me // 2) % 2)
        self.other_core = me + 1 - 2 * self.core
        self.other = [me + step - 2 * step * place for step, place in zip((SUBLANE, QUAD, 2), self.at)]
        return self

    def meet(self):
        barrier = pltpu.get_barrier_semaphore()
        devices = (self.other_core, *self.other)
        for device in devices:
            pl.semaphore_signal(barrier, inc=1, device_id=(device,), device_id_type=pl.DeviceIdType.MESH)
        pl.semaphore_wait(barrier, len(devices))

    def remote(self, src, dst, sem, device):
        return pltpu.make_async_remote_copy(src_ref=src, dst_ref=dst, send_sem=self.send.at[sem], recv_sem=self.recv.at[sem],
                                            device_id=(device,), device_id_type=pl.DeviceIdType.MESH)


class Gather(Links):
    COUNT = 2

    def __init__(self, rows, cols, cuts, by_rows):
        self.rows, self.cols, self.cuts, self.by_rows = rows, cols, cuts, by_rows
        self.parts = range(len(cuts) - 1)
        self.full_shape = jax.ShapeDtypeStruct((2, 2, 2, 2, rows, cols), BF)

    def scratch(self):
        return [pltpu.SemaphoreType.DMA((SEMS,))] * self.COUNT

    def bind(self, own, full, sems):
        self.own, self.full = own, full
        return self.find(*sems)

    def region(self, part, known, arrived=False, half=None):
        done = ORDERS[part][:known]
        place = [slice(None) if a in done else self.at[a] for a in range(3)]
        if half is not None:
            place[done[0]] = half
        if arrived:
            place[done[-1]] = 1 - self.at[done[-1]]
        cut = pl.ds(self.cuts[part], self.cuts[part + 1] - self.cuts[part])
        return (*place, self.core, cut, slice(None)) if self.by_rows else (*place, self.core, slice(None), cut)

    def hop(self, stage, part, half):
        where = self.full.at[self.region(part, stage - 1, half=half)]
        source = self.own.at[self.region(part, 0)[-2:]] if stage == 1 else where
        return self.remote(source, where, self.sem(stage, part, half), self.other[ORDERS[part][stage - 1]])

    def forward(self, stage, part, half=None):
        if stage == 0:
            return self.remote(self.own, self.full.at[(*self.at, self.core)], 0, self.other_core)
        where = self.full.at[self.region(part, stage, True, half)]
        return self.remote(where, where, self.sem(stage + QUAD, part, half), self.other_core)

    def sem(self, row, part, half):
        return QUAD * (row + (half or 0)) + part

    def halves(self, stage):
        return (None,) if stage < 3 else range(2)

    def keep(self):
        return pltpu.make_async_copy(self.own, self.full.at[(*self.at, self.core)], self.send.at[1])

    def begin(self):
        for part in self.parts:
            self.hop(1, part, None).start()
        self.forward(0, 0).start()
        self.keep().start()

    def turn(self, stage):
        if stage == 1:
            self.keep().wait()
        for half in self.halves(stage):
            for part in self.parts:
                self.hop(stage, part, half).wait()
                if stage < 3:
                    for onward in self.halves(stage + 1):
                        self.hop(stage + 1, part, onward).start()
            for part in self.parts:
                self.forward(stage, part, half).start()

    def end(self):
        self.forward(0, 0).wait()
        for stage in range(1, QUAD):
            for half in self.halves(stage):
                for part in self.parts:
                    self.forward(stage, part, half).wait()


SEMS = 36


class Exchange(Links):
    def __init__(self, rows, cols, cuts, along, stride=1, spare=0):
        self.rows, self.cols, self.stride = rows, cols, stride
        self.slots, self.locals = 3 * stride + spare, 1 + stride
        self.blocks = (2, 2, 2, 2, rows, cols)
        self.parts = [((slice(a, b), slice(None)) if along == 0 else (slice(None), slice(a, b))) for a, b in zip(cuts, cuts[1:])]
        self.shapes = [((b - a, cols) if along == 0 else (rows, b - a)) for a, b in zip(cuts, cuts[1:])]

    def scratch(self):
        two = (2, 2, 2)
        out = [pltpu.VMEM((self.locals, *self.blocks), F32), pltpu.VMEM((self.slots, *two, self.rows, self.cols), F32)]
        for axes in (2, 1, 0):
            out += [pltpu.VMEM((self.slots, *two[:axes], *shape), F32) for shape in self.shapes]
        return out + [pltpu.SemaphoreType.DMA((10, self.slots))] * 2

    COUNT = 13

    def bind(self, refs):
        self.local, self.pair = refs[0], refs[1]
        self.held = [None, refs[2:5], refs[5:SUBLANE], refs[SUBLANE:11]]
        return self.find(*refs[11:])

    def index(self, stage, part, side):
        order = ORDERS[part]
        left = [a for a in range(3) if a not in order[:stage - 1]]
        axis = order[stage - 1]
        where = self.at[axis] if side else 1 - self.at[axis]
        return tuple(where if a == axis else slice(None) for a in left)

    def copy(self, stage, part, c):
        slot = c % self.slots
        if stage == 0:
            return self.remote(self.local.at[c % self.locals, :, :, :, 1 - self.core], self.pair.at[slot], (0, slot), self.other_core)
        source = self.pair if stage == 1 else self.held[stage - 1][part]
        tail = self.parts[part] if stage == 1 else ()
        return self.remote(source.at[(slot, *self.index(stage, part, False), *tail)], self.held[stage][part].at[slot],
                           (3 * stage - 2 + part, slot), self.other[ORDERS[part][stage - 1]])

    def start(self, stage, c):
        for part in range(1 if stage == 0 else 3):
            self.copy(stage, part, c).start()

    def wait(self, stage, c):
        for part in range(1 if stage == 0 else 3):
            self.copy(stage, part, c).wait()

    def add(self, stage, c):
        slot = c % self.slots
        if stage == 0:
            for chip in itertools.product(range(2), repeat=3):
                self.pair[(slot, *chip)] += self.local[(c % self.locals, *chip, self.core)]
            return
        for part in range(3):
            source = self.pair if stage == 1 else self.held[stage - 1][part]
            tail = self.parts[part] if stage == 1 else ()
            for place in itertools.product(range(2), repeat=3 - stage):
                free = iter(place)
                kept = tuple(next(free) if isinstance(i, slice) else i for i in self.index(stage, part, True))
                self.held[stage][part][(slot, *place)] += source[(slot, *kept, *tail)]

    def result(self, c, out_ref):
        for part in range(3):
            out_ref[self.parts[part]] = self.held[3][part][c % self.slots]

    def put_local(self, c, values):
        self.local[c % self.locals] = values.reshape(self.blocks)


def comm_params(n):
    return pltpu.CompilerParams(dimension_semantics=("arbitrary",), vmem_limit_bytes=VMEM_MAX, collective_id=n, has_side_effects=True)


def advance(exchanges, t, exists, emit):
    for stage in (3, 2, 1, 0):
        c = t - 1 - (stage + 1) * exchanges[0].stride

        @pl.when(exists(c))
        def _():
            for n, exchange in enumerate(exchanges):
                exchange.wait(stage, c)
                exchange.add(stage, c)
                if stage < 3:
                    exchange.start(stage + 1, c)
                else:
                    emit(n, exchange, c)

    @pl.when(exists(t - 1))
    def _():
        for exchange in exchanges:
            exchange.start(0, t - 1)


def first_chunks(n):
    return lambda c: (c >= 0) & (c < n)


DRAIN = 5


PARTS = 16
SHARD = WIDTH // PARTS
VECTOR_ROWS = PARTS
MLP_F = MAIN
UNITS = MLP_F // PARTS
MLP_STEPS = FFN // MLP_F
WIDTH_CUTS = (0, 384, 896, WIDTH)
QKV_ALL = Gather(SHARD, QKV, (0, WIDTH, 2 * WIDTH, QKV), False)
OUT_ALL = Gather(SHARD, WIDTH, (0, 384, 768, WIDTH), False)
FC_ALL = Gather(SHARD, FFN, (0, 1664, 3328, FFN), False)
PROJ_ALL = Gather(FFN // PARTS, WIDTH, (0, 112, 208, FFN // PARTS), True)
VECTOR_ALL = Gather(SHARD, LANE, (0, SHARD), True)


def open_kernel(x_hbm, dy_hbm, rows_ref, fc_ref, wq_ref, wo_ref, xim_hbm, dyim_hbm, h_hbm, ht_hbm, vec_ref, fc_own, wq_full, wo_full,
                x, dy, wide, h, ht, rows, vec_own, vec_full, wq_own, wo_own, sems, *comm):
    loads = [pltpu.make_async_copy(src, dst, sems.at[i]) for i, (src, dst) in enumerate(((x_hbm, x), (dy_hbm, dy)))]
    for cp in loads:
        cp.start()
    clear(rows)
    rows[:VECTOR_ROWS, :] = rows_ref[ALL]
    vec_own[ALL] = rows[ALL].T[:SHARD, :].astype(BF)
    wq_own[ALL] = wq_ref[ALL].astype(BF)
    wo_own[ALL] = wo_ref[ALL].astype(BF)
    pairs = [comm[2 * i:2 * i + 2] for i in range(3)]
    vectors = VECTOR_ALL.bind(vec_own, vec_full, pairs[0])
    weights = QKV_ALL.bind(wq_own, wq_full, pairs[1]), OUT_ALL.bind(wo_own, wo_full, pairs[2])
    gathers = (vectors, *weights)
    vectors.meet()
    for gather in gathers:
        gather.begin()
    for cp in loads:
        cp.wait()

    def reorder(tokens):
        def widen(r, n):
            put(wide, r, n, tokens[pl.ds(r, n), :].astype(F32))
        row_tiles(widen)

        def place(r, n, values):
            tokens[pl.ds(r, n), :] = values.astype(BF)
        to_image_order(wide, place)
    reorder(x)
    for gather in gathers:
        gather.turn(1)
    reorder(dy)
    for gather in gathers:
        gather.turn(2)
    vectors.turn(3)
    vectors.end()
    vec_ref[ALL] = vec_full[ALL].reshape(WIDTH, LANE).astype(F32).T[:VECTOR_ROWS, :]
    gain, bias = vec_ref[0:1, :], vec_ref[1:2, :]

    def norm(r, n):
        hat, _ = norm_stats(x[pl.ds(r, n), :].astype(F32))
        h[pl.ds(r, n), :] = (hat * gain + bias).astype(BF)
    row_tiles(norm, ROWS)
    for b in range(IMAGES):
        ht[:, steps(b, MAIN)] = h[steps(b, MAIN), :].T
    ht[:, TAIL:] = h[TAIL:, :].T
    stores = [pltpu.make_async_copy(src, dst, sems.at[i]) for i, (src, dst) in enumerate(((x, xim_hbm), (dy, dyim_hbm), (h, h_hbm), (ht, ht_hbm)))]
    for cp in stores:
        cp.start()
    def store_fc(tile, values):
        fc_own[:, steps(tile, LANE)] = values.astype(BF)
    regroup(SHARD, lambda n: n % PARTS * MLP_STEPS + n // PARTS, lambda tile: fc_ref[:, steps(tile, LANE)], store_fc)
    for gather in weights:
        gather.turn(3)
    for gather in weights:
        gather.end()
    for cp in stores:
        cp.wait()


def open_call(x, dy, rows, fc, wq, wo):
    hbm, vmem = pl.BlockSpec(memory_space=pl.ANY), pl.BlockSpec(memory_space=pltpu.VMEM)
    return pl.pallas_call(
        open_kernel,
        in_specs=[hbm, hbm, vmem, vmem, vmem, vmem],
        out_specs=[hbm, hbm, hbm, hbm, vmem, vmem, hbm, hbm],
        out_shape=[*[jax.ShapeDtypeStruct((TOKENS, WIDTH), BF)] * 3,
                   jax.ShapeDtypeStruct((WIDTH, TOKENS), BF), jax.ShapeDtypeStruct((VECTOR_ROWS, WIDTH), F32),
                   jax.ShapeDtypeStruct(fc.shape, BF), QKV_ALL.full_shape, OUT_ALL.full_shape],
        scratch_shapes=[pltpu.VMEM((TOKENS, WIDTH), BF), pltpu.VMEM((TOKENS, WIDTH), BF), pltpu.VMEM((LANES, TOKENS, LANE), F32),
                        pltpu.VMEM((TOKENS, WIDTH), BF), pltpu.VMEM((WIDTH, TOKENS), BF), pltpu.VMEM((LANE, LANE), F32), pltpu.VMEM((SHARD, LANE), BF),
                        pltpu.VMEM(VECTOR_ALL.full_shape.shape, BF), pltpu.VMEM((SHARD, QKV), BF), pltpu.VMEM((SHARD, WIDTH), BF),
                        pltpu.SemaphoreType.DMA((QUAD,))] + VECTOR_ALL.scratch() + QKV_ALL.scratch() + OUT_ALL.scratch(),
        compiler_params=pltpu.CompilerParams(vmem_limit_bytes=VMEM_MAX, collective_id=3, has_side_effects=True),
        cost_estimate=cost(1_000_000_000, 60_000_000),
        name="open",
    )(x, dy, rows, fc, wq, wo)


QKV_N = 768


def qkv_kernel(h_ref, w_ref, wb_ref, own_ref, qkv_ref, full, *sems):
    t, last = step_id(), pl.num_programs(0) - 1
    gather = FC_ALL.bind(own_ref, full, sems)

    @pl.when(t == 0)
    def _():
        gather.meet()
        gather.begin()

    @pl.when(t == 1)
    def _():
        gather.turn(1)

    @pl.when(t == 3)
    def _():
        gather.turn(2)
    for rows in BLOCKS:
        qkv_ref[rows, :] = (dot(h_ref[rows, :], w_ref[ALL]) + wb_ref[ALL]).astype(BF)

    @pl.when(t == last)
    def _():
        gather.turn(3)
        gather.end()


def qkv_call(h, w, wb, own):
    hbm = pl.BlockSpec(memory_space=pl.ANY)
    return pl.pallas_call(
        qkv_kernel,
        grid=(QKV // QKV_N,),
        in_specs=[whole(TOKENS, WIDTH, pipeline_mode=pl.Buffered(1)), by_cols(WIDTH, QKV_N), by_cols(1, QKV_N), whole(SHARD, FFN)],
        out_specs=[by_cols(TOKENS, QKV_N), hbm],
        out_shape=[jax.ShapeDtypeStruct((TOKENS, QKV), BF), FC_ALL.full_shape],
        scratch_shapes=FC_ALL.scratch(),
        compiler_params=comm_params(QUAD),
        cost_estimate=cost(2 * TOKENS * WIDTH * QKV, 60_000_000),
        name="qkv",
    )(h, w, wb, own)


ROW_CUTS = (0, 24, 48, 80)
FC_SUM = Exchange(SHARD, MLP_F, ROW_CUTS, 0)
PROJ_SUM = Exchange(UNITS, WIDTH, WIDTH_CUTS, 1)
CDF_P = 0.33
CDF_C = (0.1326322871417956, 0.11939570820799192, 0.18103829560051796, -0.08904113226212501,
         0.33075919469138065, -0.22023738432274684, 0.0454530347223348)


def gelu_pair(u):
    bell = jnp.exp(u * u * -0.5)
    t = 1.0 / (1.0 + CDF_P * jnp.abs(u))
    poly = CDF_C[6]
    for c in CDF_C[5::-1]:
        poly = poly * t + c
    tail = poly * t * bell
    cdf = jnp.where(u < 0.0, tail, 1.0 - tail)
    return u * cdf, cdf + u * bell * ((2.0 * math.pi) ** -0.5)


def mlp_kernel(r_hbm, n_hbm, dy_hbm, gain_ref, pb_ref, fc_ref, proj_ref, fcb_ref,
               y_hbm, dr_hbm, dr16_hbm, dfc_ref, dproj_ref, dfcb_ref, small_ref,
               n2, dy, y_acc, dn_acc, g, du, ua, ub, da, db, sem, *comm):
    step = step_id()
    by_row, by_col = FC_SUM.bind(comm[:Exchange.COUNT]), PROJ_SUM.bind(comm[Exchange.COUNT:])

    @pl.when(step == 0)
    def _():
        loads = [pltpu.make_async_copy(n_hbm, n2, sem), pltpu.make_async_copy(dy_hbm, dy, sem)]
        for cp in loads:
            cp.start()
        by_row.meet()
        clear(small_ref, y_acc, dn_acc)
        for cp in loads:
            cp.wait()

    outs = (dfc_ref, dproj_ref)
    advance((by_row, by_col), step, first_chunks(MLP_STEPS), lambda n, exchange, c: exchange.result(c, outs[n]))

    @pl.when(step < MLP_STEPS)
    def _():
        fcb = fcb_ref[ALL]
        fc, proj = fc_ref[ALL], proj_ref[ALL].reshape(MLP_F, WIDTH)
        bias_sum = jnp.zeros((SUBLANE, MLP_F), F32)
        tiles = [(b * MAIN, MAIN) for b in range(IMAGES - 1)] + [((IMAGES - 1) * MAIN, MAIN + IMAGES)]
        pairs = ((ua, da), (ub, db))

        def products(k):
            r, n = tiles[k]
            u_s, d_s = pairs[k % 2]
            u_s[0:n, :] = dot(n2[r:r + n, :], fc)
            d_s[0:n, :] = dot_nt(dy[r:r + n, :], proj)

        def pointwise(k, total):
            r, n = tiles[k]
            u_s, d_s = pairs[k % 2]
            value, slope = gelu_pair(u_s[0:n, :] + fcb)
            g[r:r + n, :] = value.astype(BF)
            grad = d_s[0:n, :] * slope
            du[r:r + n, :] = grad.astype(BF)
            return total + eights(grad)

        products(0)
        for k in range(1, IMAGES):
            products(k)
            bias_sum = pointwise(k - 1, bias_sum)
        bias_sum = pointwise(IMAGES - 1, bias_sum)
        dfcb_ref[ALL] = col_sum(bias_sum)
        y_acc[ALL] += dot(g[ALL], proj)
        for c in range(LANES // 2):
            part = dot_nt(du[ALL], fc_ref[steps(c, MAIN), :])
            dn_acc[2 * c] += part[:, :LANE]
            dn_acc[2 * c + 1] += part[:, LANE:]
        by_col.put_local(step, dot_tn(g[ALL], dy[ALL]))
        by_row.put_local(step, dot_tn(n2[ALL], du[ALL]))

    after = step - MLP_STEPS
    r_copy = pltpu.make_async_copy(r_hbm, n2, sem)
    out_copies = [pltpu.make_async_copy(dn_acc, dr_hbm, sem), pltpu.make_async_copy(n2, dr16_hbm, sem)]
    y_copy = pltpu.make_async_copy(dy, y_hbm, sem)

    def back(r, n):
        wide_r = n2[pl.ds(r, n), :].astype(F32)
        hat, inv = norm_stats(wide_r)
        dn = joined(dn_acc, r, n)
        wide_dy = dy[pl.ds(r, n), :].astype(F32)
        dr = wide_dy + norm_back(dn, hat, inv, gain_ref[ALL])
        put(dn_acc, r, n, dr)
        n2[pl.ds(r, n), :] = dr.astype(BF)
        y_acc[pl.ds(r, n), :] += wide_r + pb_ref[ALL]
        for i, v in enumerate((dn * hat, dn, wide_dy, dr)):
            small_ref[steps(i, SUBLANE), :] += eights(v)

    @pl.when(after == 0)
    def _():
        r_copy.start()
        r_copy.wait()
        back(TAIL, IMAGES)

    @pl.when((after >= 0) & (after < 3))
    def _():
        back_part(back, after)

    @pl.when(after == 2)
    def _():
        for cp in out_copies:
            cp.start()

    @pl.when(after == 3)
    def _():
        for cp in out_copies:
            cp.wait()
        from_image_order(y_acc, dn_acc)

        def narrow(r, n):
            dy[pl.ds(r, n), :] = joined(dn_acc, r, n).astype(BF)
        row_tiles(narrow)
        y_copy.start()

    @pl.when(after == QUAD)
    def _():
        y_copy.wait()


def mlp_call(r, n2, dy, gain, pb, fc, proj, fcb):
    hbm = pl.BlockSpec(memory_space=pl.ANY)
    vec = whole(1, WIDTH)
    now = lambda i: jnp.minimum(i, MLP_STEPS - 1)
    done = lambda i: jnp.maximum(i - DRAIN, 0)
    return pl.pallas_call(
        mlp_kernel,
        grid=(MLP_STEPS + DRAIN,),
        in_specs=[hbm, hbm, hbm, vec, vec, by_cols(WIDTH, MLP_F, now),
                  pl.BlockSpec((PARTS, None, UNITS, WIDTH), lambda i: (0, now(i), 0, 0)),
                  by_cols(1, MLP_F, now)],
        out_specs=[hbm, hbm, hbm, by_cols(SHARD, MLP_F, done),
                   by_rows(UNITS, WIDTH, done),
                   by_cols(1, MLP_F, now), whole(32, WIDTH)],
        out_shape=[jax.ShapeDtypeStruct((TOKENS, WIDTH), BF), jax.ShapeDtypeStruct((LANES, TOKENS, LANE), F32),
                   jax.ShapeDtypeStruct((TOKENS, WIDTH), BF), jax.ShapeDtypeStruct((SHARD, FFN), F32),
                   jax.ShapeDtypeStruct((FFN // PARTS, WIDTH), F32),
                   jax.ShapeDtypeStruct((1, FFN), F32), jax.ShapeDtypeStruct((32, WIDTH), F32)],
        scratch_shapes=[pltpu.VMEM((TOKENS, WIDTH), BF), pltpu.VMEM((TOKENS, WIDTH), BF),
                        pltpu.VMEM((TOKENS, WIDTH), F32), pltpu.VMEM((LANES, TOKENS, LANE), F32),
                        pltpu.VMEM((TOKENS, MLP_F), BF), pltpu.VMEM((TOKENS, MLP_F), BF)]
                       + [pltpu.VMEM((MAIN + IMAGES, MLP_F), F32)] * QUAD + [pltpu.SemaphoreType.DMA]
                       + FC_SUM.scratch() + PROJ_SUM.scratch(),
        compiler_params=comm_params(0),
        cost_estimate=cost(12 * TOKENS * WIDTH * FFN, 150_000_000, TOKENS * FFN),
        name="mlp",
    )(r, n2, dy, gain, pb, fc, proj.reshape(PARTS, MLP_STEPS, UNITS, WIDTH), fcb)


SCALE = HEAD ** -0.5
ATTN_COST = cost(40_000_000_000, 50_000_000, 8_400_000)


def window(h):
    first = min(HEAD * h // LANE * LANE, WIDTH - MAIN)
    wide = LANE if HEAD * h + HEAD <= first + LANE else MAIN
    return first, wide, HEAD * h - first


def lane_mask(h):
    first, wide, off = window(h)
    lane = lax.broadcasted_iota(jnp.int32, (MAIN, wide), 1)
    return (lane >= off) & (lane < off + HEAD)


def thirds(ref, rows=slice(None)):
    return [ref[rows, steps(i, WIDTH)] for i in range(3)]


def head_rows():
    lane = lax.broadcasted_iota(jnp.int32, (HEADS, WIDTH), 1)
    row = lax.broadcasted_iota(jnp.int32, (HEADS, WIDTH), 0)
    return (lane // HEAD == row).astype(F32)


def tail_softmax(s, s_self):
    m = jnp.maximum(jnp.max(s, axis=1, keepdims=True), s_self)
    e = jnp.exp((s - m) * SCALE)
    e_self = jnp.exp((s_self - m) * SCALE)
    inv = 1.0 / (row_sum(e) + e_self)
    return e * inv, e_self * inv


def attn_kernel(qkv_ref, qkvt_ref, x_ref, xt_ref, w_ref, wb_ref, gain_ref, bias_ref, proj_ref, o_hbm, r_hbm, n_hbm,
                max_ref, inv_ref, full,
                tails, o_tail, o_t, ptail, o_buf, r_buf, n_buf, sa, sb, sems, own, *comm):
    b, last = step_id(), pl.num_programs(0) - 1
    slot = b % 2
    gather = PROJ_ALL.bind(own, full, comm)

    @pl.when(b == 0)
    def _():
        tails[ALL] = qkvt_ref[ALL].astype(F32)
        own[ALL] = proj_ref[ALL].astype(BF)
        gather.meet()
        gather.begin()

    @pl.when(b == 1)
    def _():
        gather.turn(1)

    @pl.when(b == 3)
    def _():
        gather.turn(2)

    @pl.when(b == last)
    def _():
        gather.turn(3)

    heads = head_rows()
    q_t, k_t, v_t = (heads * z for z in thirds(tails, pl.ds(b, 1)))
    q, k, v = thirds(qkv_ref)

    p, p_self = tail_softmax(dot_nt(q_t.astype(BF), k), row_sum(q_t * k_t))
    mixed = dot(p.astype(BF), v) * heads + p_self.astype(BF).astype(F32) * v_t
    o_tail[pl.ds(b, 1), :] = col_sum(mixed)

    s_tail = dot_nt(k_t.astype(BF), q)
    v_turned = v.T
    scores = sa, sb

    def next_scores(h):
        first, wide, _ = window(h)
        q_h = jnp.where(lane_mask(h), qkv_ref[:, pl.ds(first, wide)], jnp.zeros((), BF))
        scores[h % 2][ALL] = dot_nt(qkv_ref[:, pl.ds(WIDTH + first, wide)], q_h)
    next_scores(0)
    for h in range(HEADS):
        if h + 1 < HEADS:
            next_scores(h + 1)
        s, mine = scores[h % 2], steps(h, 1)
        top = jnp.maximum(col_max(s[ALL]), s_tail[mine, :])
        e = jnp.exp((s[ALL] - top) * SCALE)
        e_tail = jnp.exp((s_tail[mine, :] - top) * SCALE)
        inv = 1.0 / (col_sum(e) + e_tail)
        max_ref[0, mine, :] = top
        inv_ref[0, mine, :] = inv
        ptail[mine, :] = e_tail * inv
        o_t[steps(h, HEAD), :] = dot(v_turned[steps(h, HEAD), :], (e * inv).astype(BF))

    outs = (o_buf, o_hbm), (r_buf, r_hbm), (n_buf, n_hbm)

    def write(slot, rows, o, x):
        o_buf[slot, rows, :] = o
        r = (x.astype(F32) + dot(o, w_ref[ALL]) + wb_ref[ALL]).astype(BF)
        r_buf[slot, rows, :] = r
        hat, _ = norm_stats(r.astype(F32))
        n_buf[slot, rows, :] = (hat * gain_ref[ALL] + bias_ref[ALL]).astype(BF)

    @pl.when(b >= 2)
    def _():
        for n, (buf, hbm) in enumerate(outs):
            out_copy(buf, hbm, slot, b - 2, sems, n).wait()

    o = (o_t[ALL].T + dot_tn(ptail[ALL].astype(BF), v_t.astype(BF))).astype(BF)
    write(slot, slice(None), o, x_ref[ALL])
    for n, (buf, hbm) in enumerate(outs):
        out_copy(buf, hbm, slot, b, sems, n).start()

    @pl.when(b == last)
    def _():
        for n, (buf, hbm) in enumerate(outs):
            out_copy(buf, hbm, 1 - slot, b - 1, sems, n).wait()
        write(1 - slot, slice(IMAGES), o_tail[ALL].astype(BF), xt_ref[ALL])
        copies = [pltpu.make_async_copy(buf.at[1 - slot, pl.ds(0, IMAGES)], hbm.at[pl.ds(TAIL, IMAGES)], sems.at[n, 1 - slot])
                  for n, (buf, hbm) in enumerate(outs)]
        for cp in copies:
            cp.start()
        for cp in copies:
            cp.wait()
        for n, (buf, hbm) in enumerate(outs):
            out_copy(buf, hbm, slot, b, sems, n).wait()
        gather.end()


def out_copy(buf, hbm, slot, b, sems, n):
    return pltpu.make_async_copy(buf.at[slot], hbm.at[pl.ds(pl.multiple_of(b * MAIN, MAIN), MAIN)], sems.at[n, slot])


def attn_call(qkv, xim, w, wb, gain, bias, proj):
    hbm = pl.BlockSpec(memory_space=pl.ANY)
    main = lambda n: by_rows(MAIN, n)
    tail = lambda n: by_rows(IMAGES, n, lambda i: TAIL // IMAGES)
    stat = pl.BlockSpec((1, HEADS, MAIN), lambda i: (i, 0, 0))
    return pl.pallas_call(
        attn_kernel,
        grid=(IMAGES,),
        in_specs=[main(QKV), tail(QKV), main(WIDTH), tail(WIDTH),
                  whole(WIDTH, WIDTH), *[whole(1, WIDTH)] * 3, whole(*proj.shape)],
        out_specs=[hbm, hbm, hbm, stat, stat, hbm],
        out_shape=[*[jax.ShapeDtypeStruct((TOKENS, WIDTH), BF)] * 3,
                   jax.ShapeDtypeStruct((IMAGES, HEADS, MAIN), F32), jax.ShapeDtypeStruct((IMAGES, HEADS, MAIN), F32),
                   PROJ_ALL.full_shape],
        scratch_shapes=[pltpu.VMEM((IMAGES, QKV), F32), pltpu.VMEM((IMAGES, WIDTH), F32),
                        pltpu.VMEM((WIDTH, MAIN), F32), pltpu.VMEM((HEADS, MAIN), F32),
                        *[pltpu.VMEM((2, MAIN, WIDTH), BF)] * 3, *[pltpu.VMEM((MAIN, MAIN), F32)] * 2, pltpu.SemaphoreType.DMA((3, 2)),
                        pltpu.VMEM(proj.shape, BF)] + PROJ_ALL.scratch(),
        compiler_params=comm_params(5),
        cost_estimate=ATTN_COST,
        name="attn",
    )(qkv, qkv, xim, xim, w, wb, gain, bias, proj)


def outb_kernel(dr_ref, o_ref, w_ref, dfc_ref, y_in, dproj_in, do_ref, dw_ref, dfc_out, y_out, dproj_out, y, dproj, sems):
    c, last = step_id(), pl.num_programs(0) - 1
    loads = [pltpu.make_async_copy(src, dst, sems.at[i]) for i, (src, dst) in enumerate(((y_in, y), (dproj_in, dproj)))]
    stores = [pltpu.make_async_copy(src, dst, sems.at[i]) for i, (src, dst) in enumerate(((y, y_out), (dproj, dproj_out)))]

    @pl.when(c == 0)
    def _():
        for cp in loads:
            cp.start()

    @pl.when(c == 1)
    def _():
        for cp in loads:
            cp.wait()
        for cp in stores:
            cp.start()

        def store_fc(tile, values):
            dfc_out[:, steps(tile, LANE)] = values
        regroup(SHARD, lambda n: n % MLP_STEPS * PARTS + n // MLP_STEPS, lambda tile: dfc_ref[:, steps(tile, LANE)], store_fc)
    do_ref[ALL] = dot_nt(dr_ref[ALL], w_ref[ALL]).astype(BF)
    dw_ref[ALL] = dot_tn(o_ref[ALL], dr_ref[:, pl.ds(pl.multiple_of(c * MAIN, MAIN), MAIN)])

    @pl.when(c == last)
    def _():
        for cp in stores:
            cp.wait()


def outb_call(dr, o, w, dfc, y, dproj):
    full, hbm = whole(TOKENS, WIDTH), pl.BlockSpec(memory_space=pl.ANY)
    like = lambda v: jax.ShapeDtypeStruct(v.shape, v.dtype)
    return pl.pallas_call(
        outb_kernel,
        grid=(WIDTH // MAIN,),
        in_specs=[full, full, by_rows(MAIN, WIDTH), whole(*dfc.shape), hbm, hbm],
        out_specs=[by_cols(TOKENS, MAIN), by_cols(WIDTH, MAIN), whole(*dfc.shape), hbm, hbm],
        out_shape=[like(dr), jax.ShapeDtypeStruct((WIDTH, WIDTH), F32), like(dfc), like(y), like(dproj)],
        scratch_shapes=[pltpu.VMEM(y.shape, BF), pltpu.VMEM(dproj.shape, F32), pltpu.SemaphoreType.DMA((2,))],
        compiler_params=pltpu.CompilerParams(dimension_semantics=("arbitrary",), vmem_limit_bytes=VMEM_MAX),
        cost_estimate=cost(QUAD * TOKENS * WIDTH * WIDTH, 50_000_000),
        name="outb",
    )(dr, o, w, dfc, y, dproj)


def attn_back_kernel(qkv_ref, qkvt_ref, do_ref, dot_ref, max_ref, inv_ref, dw_ref, dqkv_hbm, dwb_ref, dwout_ref,
                     tails, do_tails, grad_tails, dq_t, dk, dv, ds_tail, sa, da, sb, db, buf, sems, *comm):
    b = step_id()
    by_row = OUT_SUM.bind(comm)

    @pl.when(b == 0)
    def _():
        by_row.meet()
    advance((by_row,), b, first_chunks(OUT_STEPS), lambda n, exchange, c: exchange.result(c, dwout_ref))

    @pl.when(b < OUT_STEPS)
    def _():
        by_row.put_local(b, dw_ref[ALL])

    @pl.when(b < IMAGES)
    def _():
        image_back(b, qkv_ref, qkvt_ref, do_ref, dot_ref, max_ref, inv_ref, dqkv_hbm, dwb_ref,
                   tails, do_tails, grad_tails, dq_t, dk, dv, ds_tail, ((sa, da), (sb, db)), buf, sems)


OUT_N = WIDTH // 2
OUT_STEPS = WIDTH // OUT_N
OUT_SUM = Exchange(SHARD, OUT_N, ROW_CUTS, 0)


def image_back(b, qkv_ref, qkvt_ref, do_ref, dot_ref, max_ref, inv_ref, dqkv_hbm, dwb_ref,
               tails, do_tails, grad_tails, dq_t, dk, dv, ds_tail, ahead, buf, sems):
    last = IMAGES - 1
    slot = b % 2

    @pl.when(b == 0)
    def _():
        tails[ALL] = qkvt_ref[ALL].astype(F32)
        do_tails[ALL] = dot_ref[ALL].astype(F32)
        clear(dwb_ref)

    heads = head_rows()
    q_t, k_t, v_t = (heads * z for z in thirds(tails, pl.ds(b, 1)))
    do_t = heads * do_tails[pl.ds(b, 1), :]
    q, k, v = thirds(qkv_ref)
    do = do_ref[ALL]
    q_t16, k_t16, v_t16, do_t16 = (z.astype(BF) for z in (q_t, k_t, v_t, do_t))

    p, p_self = tail_softmax(dot_nt(q_t16, k), row_sum(q_t * k_t))
    dp, dp_self = dot_nt(do_t16, v), row_sum(do_t * v_t)
    inner = row_sum(p * dp) + p_self * dp_self
    ds16 = (p * (dp - inner) * SCALE).astype(BF)
    ds_self = (p_self * (dp_self - inner) * SCALE).astype(BF).astype(F32)
    grad_q = col_sum(dot(ds16, k) * heads + ds_self * k_t)
    grad_k = ds_self * q_t
    grad_v = p_self.astype(BF).astype(F32) * do_t
    dk[ALL] = dot_tn(ds16, q_t16)
    dv[ALL] = dot_tn(p.astype(BF), do_t16)

    p_tail = jnp.exp((dot_nt(k_t16, q) - max_ref[0]) * SCALE) * inv_ref[0]
    dp_tail = dot_nt(v_t16, do)
    inner_tail = p_tail * dp_tail

    k_turned = k.T

    def masked(h):
        first, wide, _ = window(h)
        here, mask = pl.ds(first, wide), lane_mask(h)
        return here, jnp.where(mask, qkv_ref[:, here], jnp.zeros((), BF)), jnp.where(mask, do_ref[:, here], jnp.zeros((), BF))

    def next_products(h):
        first, wide, _ = window(h)
        _, q_h, do_h = masked(h)
        ahead[h % 2][0][ALL] = dot_nt(qkv_ref[:, pl.ds(WIDTH + first, wide)], q_h)
        ahead[h % 2][1][ALL] = dot_nt(qkv_ref[:, pl.ds(2 * WIDTH + first, wide)], do_h)
    next_products(0)
    for h in range(HEADS):
        if h + 1 < HEADS:
            next_products(h + 1)
        here, q_h, do_h = masked(h)
        mine = steps(h, 1)
        s, dp = (ref[ALL] for ref in ahead[h % 2])
        p = jnp.exp((s - max_ref[0, mine, :]) * SCALE) * inv_ref[0, mine, :]
        inner = col_sum(p * dp) + inner_tail[mine, :]
        ds = (p * (dp - inner) * SCALE).astype(BF)
        dv[:, here] += dot(p.astype(BF), do_h)
        dk[:, here] += dot(ds, q_h)
        dq_t[steps(h, HEAD), :] = dot(k_turned[steps(h, HEAD), :], ds)
        ds_tail[mine, :] = p_tail[mine, :] * (dp_tail[mine, :] - inner) * SCALE

    ds_tail16 = ds_tail[ALL].astype(BF)
    grad_k = col_sum(grad_k + dot(ds_tail16, q) * heads)
    grad_v = col_sum(grad_v + dot(p_tail.astype(BF), do) * heads)

    @pl.when(b >= 2)
    def _():
        out_copy(buf, dqkv_hbm, slot, b - 2, sems, 0).wait()

    grad = dq_t[ALL].T + dot_tn(ds_tail16, k_t16)
    for n, (main, tail) in enumerate(((grad, grad_q), (dk[ALL], grad_k), (dv[ALL], grad_v))):
        here = steps(n, WIDTH)
        buf[slot, :, here] = main.astype(BF)
        grad_tails[pl.ds(b, 1), here] = tail
        dwb_ref[:, here] += col_sum(main) + tail
    out_copy(buf, dqkv_hbm, slot, b, sems, 0).start()

    @pl.when(b == last)
    def _():
        out_copy(buf, dqkv_hbm, 1 - slot, b - 1, sems, 0).wait()
        buf[1 - slot, 0:IMAGES, :] = grad_tails[ALL].astype(BF)
        cp = pltpu.make_async_copy(buf.at[1 - slot, pl.ds(0, IMAGES)], dqkv_hbm.at[pl.ds(TAIL, IMAGES)], sems.at[0, 1 - slot])
        cp.start()
        cp.wait()
        out_copy(buf, dqkv_hbm, slot, b, sems, 0).wait()


def attn_back_call(qkv, do, top, inv, dw):
    hbm = pl.BlockSpec(memory_space=pl.ANY)
    image = lambda i: jnp.minimum(i, IMAGES - 1)
    main = lambda n: by_rows(MAIN, n, image)
    tail = lambda n: by_rows(IMAGES, n, lambda i: TAIL // IMAGES)
    stat = pl.BlockSpec((1, HEADS, MAIN), lambda i: (image(i), 0, 0))
    return pl.pallas_call(
        attn_back_kernel,
        grid=(max(IMAGES, OUT_STEPS + DRAIN),),
        in_specs=[main(QKV), tail(QKV), main(WIDTH), tail(WIDTH), stat, stat,
                  by_cols(WIDTH, OUT_N, lambda i: jnp.minimum(i, OUT_STEPS - 1))],
        out_specs=[hbm, whole(1, QKV), by_cols(SHARD, OUT_N, lambda i: jnp.clip(i - DRAIN, 0, OUT_STEPS - 1))],
        out_shape=[jax.ShapeDtypeStruct((TOKENS, QKV), BF), jax.ShapeDtypeStruct((1, QKV), F32),
                   jax.ShapeDtypeStruct((SHARD, WIDTH), F32)],
        scratch_shapes=[pltpu.VMEM((IMAGES, QKV), F32), pltpu.VMEM((IMAGES, WIDTH), F32),
                        pltpu.VMEM((IMAGES, QKV), F32), pltpu.VMEM((WIDTH, MAIN), F32),
                        pltpu.VMEM((MAIN, WIDTH), F32), pltpu.VMEM((MAIN, WIDTH), F32), pltpu.VMEM((HEADS, MAIN), F32),
                        *[pltpu.VMEM((MAIN, MAIN), F32)] * QUAD, pltpu.VMEM((2, MAIN, QKV), BF), pltpu.SemaphoreType.DMA((1, 2))] + OUT_SUM.scratch(),
        compiler_params=comm_params(1),
        cost_estimate=ATTN_COST,
        name="attn_back",
    )(qkv, qkv, do, do, top, inv, dw)


QB_N = MAIN
QB_STEPS = QKV // QB_N
QKV_SUM = Exchange(SHARD, QB_N, ROW_CUTS, 0, 2)
VECTOR_SUM = Exchange(3 * SUBLANE, LANE, (0, SUBLANE, 2 * SUBLANE, 3 * SUBLANE), 0)
VECTOR_STEP = QB_STEPS + 2
QB_GRID = QB_STEPS + 1 + QUAD * QKV_SUM.stride


def qkvb_kernel(xim_hbm, dr_hbm, gain_ref, sums_ref, qb_ref, fb_ref, ht_ref, dqkv_ref, w_ref, dx_hbm, dw_ref, out_vec_ref,
                acc, dr, xd, sums, sems, *comm):
    t = step_id()
    by_row, by_vector = QKV_SUM.bind(comm[:Exchange.COUNT]), VECTOR_SUM.bind(comm[Exchange.COUNT:])
    loads = [pltpu.make_async_copy(dr_hbm, dr, sems.at[0]), pltpu.make_async_copy(xim_hbm, xd, sems.at[1])]
    store = pltpu.make_async_copy(xd, dx_hbm, sems.at[1])

    def put_row(place, row, lane, values):
        by_vector.local[(0, *place, pl.ds(row, len(values)), pl.ds(lane, values.shape[1]))] = values

    def share(row, values):
        for d, place in enumerate(DEVICES):
            put_row(place, row, 0, values[:, steps(d, SHARD)])

    @pl.when(t == 0)
    def _():
        by_row.meet()
        for cp in loads:
            cp.start()
        clear(acc, sums)
        by_vector.local[0] = jnp.zeros(by_vector.blocks, F32)
        share(0, jnp.concatenate([col_sum(sums_ref[steps(i, SUBLANE), :]) for i in range(QUAD)], axis=0))
        for d, place in enumerate(DEVICES):
            for i in range(3):
                put_row(place, QUAD + i, 0, qb_ref[:, pl.ds((3 * d + i) * SHARD, SHARD)])
            for n in range(MLP_STEPS):
                put_row(place, QUAD + 3 + n * UNITS // SHARD, n * UNITS % SHARD, fb_ref[:, pl.ds(n * MLP_F + d * UNITS, UNITS)])

    def emit_vectors(n, exchange, c):
        for part, (rows, _) in enumerate(exchange.parts[:2]):
            out_vec_ref[rows, :] = exchange.held[3][part][0, :, :SHARD]
    advance((by_row,), t, first_chunks(QB_STEPS), lambda n, exchange, c: exchange.result(c, dw_ref))
    advance((by_vector,), t - VECTOR_STEP, first_chunks(1), emit_vectors)

    @pl.when(t < QB_STEPS)
    def _():
        by_row.put_local(t, dot(ht_ref[ALL], dqkv_ref[ALL]))
        acc[ALL] += dot_nt(dqkv_ref[ALL], w_ref[ALL])

    @pl.when(t == QB_STEPS)
    def _():
        for cp in loads:
            cp.wait()

    def back(r, n):
        hat, inv = norm_stats(xd[pl.ds(r, n), :].astype(F32))
        dn = acc[pl.ds(r, n), :]
        for i, v in enumerate((dn * hat, dn)):
            sums[steps(i, SUBLANE), :] += eights(v)
        acc[pl.ds(r, n), :] = joined(dr, r, n) + norm_back(dn, hat, inv, gain_ref[ALL])

    @pl.when((t >= QB_STEPS) & (t <= VECTOR_STEP))
    def _():
        back_part(back, t - QB_STEPS)

    @pl.when(t == VECTOR_STEP)
    def _():
        back(TAIL, IMAGES)
        share(VECTOR_ROWS - 2, jnp.concatenate([col_sum(sums[steps(i, SUBLANE), :]) for i in range(2)], axis=0))

    @pl.when(t == VECTOR_STEP + 1)
    def _():
        from_image_order(acc, dr)

    @pl.when(t == VECTOR_STEP + 2)
    def _():
        def narrow(r, n):
            xd[pl.ds(r, n), :] = joined(dr, r, n).astype(BF)
        row_tiles(narrow)
        store.start()

    @pl.when(t == QB_GRID - 1)
    def _():
        store.wait()


DEVICES = list(itertools.product(range(2), repeat=QUAD))


def qkvb_call(xim, dr, gain, sums, qb, fb, ht, dqkv, w):
    hbm = pl.BlockSpec(memory_space=pl.ANY)
    now = lambda i: jnp.minimum(i, QB_STEPS - 1)
    return pl.pallas_call(
        qkvb_kernel,
        grid=(QB_GRID,),
        in_specs=[hbm, hbm, whole(1, WIDTH), *(whole(*v.shape) for v in (sums, qb, fb)),
                  whole(WIDTH, TOKENS, pipeline_mode=pl.Buffered(1)), by_cols(TOKENS, QB_N, now), by_cols(WIDTH, QB_N, now)],
        out_specs=[hbm, by_cols(SHARD, QB_N, lambda i: jnp.clip(i - 1 - QUAD * QKV_SUM.stride, 0, QB_STEPS - 1)),
                   whole(VECTOR_ROWS, SHARD)],
        out_shape=[jax.ShapeDtypeStruct((TOKENS, WIDTH), BF), jax.ShapeDtypeStruct((SHARD, QKV), F32),
                   jax.ShapeDtypeStruct((VECTOR_ROWS, SHARD), F32)],
        scratch_shapes=[pltpu.VMEM((TOKENS, WIDTH), F32), pltpu.VMEM((LANES, TOKENS, LANE), F32), pltpu.VMEM((TOKENS, WIDTH), BF),
                        pltpu.VMEM((2 * SUBLANE, WIDTH), F32), pltpu.SemaphoreType.DMA((2,))]
                       + QKV_SUM.scratch() + VECTOR_SUM.scratch(),
        compiler_params=comm_params(2),
        cost_estimate=cost(QUAD * TOKENS * WIDTH * QKV, 80_000_000),
        name="qkvb",
    )(xim, dr, gain, sums, qb, fb, ht, dqkv, w)


def to_steps(v):
    rows = v.shape[0]
    return v.reshape(rows, PARTS, MLP_STEPS, UNITS).swapaxes(1, 2).reshape(rows, FFN)


def solution(mesh):
    specs = (P("fsdp"),) * 14

    def device_step(resid_in, grad_out, ln1_gain, ln1_bias, qkv_weight, qkv_bias, out_weight, out_bias,
                    ln2_gain, ln2_bias, fc_weight, fc_bias, proj_weight, proj_bias):
        rows = jnp.concatenate([ln1_gain, ln1_bias, qkv_bias, out_bias, ln2_gain, ln2_bias, fc_bias, proj_bias]).reshape(-1, SHARD)
        rows = jnp.pad(rows, ((0, VECTOR_ROWS - len(rows)), (0, LANE - SHARD)))
        x = resid_in.swapaxes(0, 1).reshape(TOKENS, WIDTH)
        dy = grad_out.swapaxes(0, 1).reshape(TOKENS, WIDTH)
        xim, dyim, h, ht, rows, fc, wq, wo = open_call(x, dy, rows, fc_weight, qkv_weight, out_weight)
        wq, wo = wq.reshape(WIDTH, QKV), wo.reshape(WIDTH, WIDTH)
        bo, g2, b2 = rows[5:6], rows[6:7], rows[7:8]
        joint = lambda v: v.reshape(-1, PARTS, SHARD).swapaxes(0, 1).reshape(1, -1)
        qkv, wf = qkv_call(h, wq, joint(rows[2:5]), fc)
        o, r, n2, top, inv, wp = attn_call(qkv, xim, wo, bo, g2, b2, proj_weight)
        y, dr, dr16, dwf, dwp, dbf, small = mlp_call(r, n2, dyim, g2, rows[12:13], wf.reshape(WIDTH, FFN), wp, to_steps(joint(rows[8:12])))
        do, dwo, dwf, y, dwp = outb_call(dr16, o, wo, dwf, y, dwp)
        dqkv, dbq, dwo = attn_back_call(qkv, do, top, inv, dwo)
        dx, dwq, vec = qkvb_call(xim, dr, rows[:1], small, dbq, dbf, ht, dqkv, wq)
        dg2, db2, dbp, dbo = vec[:4]
        dbq, dbf = vec[4:7].reshape(-1), vec[7:11].reshape(-1)
        dg1, db1 = vec[VECTOR_ROWS - 2:]
        unturn = lambda t: t.reshape(SEQ, IMAGES, WIDTH).swapaxes(0, 1)
        return (unturn(y), unturn(dx), dg1, db1, dwq, dbq, dwo, dbo, dg2, db2, dwf, dbf, dwp, dbp)

    return jax.shard_map(device_step, mesh=mesh, in_specs=specs, out_specs=specs, check_vma=False)
```

```python
import itertools
import math
import jax, jax.numpy as jnp
from jax import lax
from jax.experimental import pallas as pl
from jax.experimental.pallas import tpu as pltpu
from jax.sharding import PartitionSpec as P

BF, F32 = jnp.bfloat16, jnp.float32
IMAGES, SEQ, WIDTH, FFN, HEADS, HEAD = 8, 257, 1280, 5120, 16, 80
MAIN = SEQ - 1
TOKENS = IMAGES * SEQ
TAIL = IMAGES * MAIN
LN_EPS = 1e-5
VMEM_MAX = 67043328
LANE, SUBLANE, QUAD, QKV = 128, 8, 4, 3 * WIDTH
ALL = ...
LANES = WIDTH // LANE
ROWS = 32


def dot(a, b):
    return jnp.dot(a, b, preferred_element_type=F32)


def dot_nt(a, b):
    return lax.dot_general(a, b, (((1,), (1,)), ((), ())), preferred_element_type=F32)


def dot_tn(a, b):
    return lax.dot_general(a, b, (((0,), (0,)), ((), ())), preferred_element_type=F32)


def col_sum(v):
    return jnp.sum(v, axis=0, keepdims=True)


def col_max(v):
    return jnp.max(v, axis=0, keepdims=True)


def row_sum(v):
    return jnp.sum(v, axis=-1, keepdims=True)


def row_mean(v):
    return row_sum(v) * (1.0 / WIDTH)


def clear(*refs):
    for ref in refs:
        ref[ALL] = jnp.zeros_like(ref)


def step_id():
    return pl.program_id(0)


def cost(flops, bytes_accessed, transcendentals=0):
    return pl.CostEstimate(flops=flops, bytes_accessed=bytes_accessed, transcendentals=transcendentals)


def eights(v):
    return jnp.sum(v.reshape(v.shape[0] // SUBLANE, SUBLANE, v.shape[1]), axis=0)


def whole(*shape, **kw):
    return pl.BlockSpec(shape, lambda *i: (0,) * len(shape), **kw)


def by_cols(rows, cols, at=lambda i: i):
    return pl.BlockSpec((rows, cols), lambda i: (0, at(i)))


def by_rows(rows, cols, at=lambda i: i):
    return pl.BlockSpec((rows, cols), lambda i: (at(i), 0))


def steps(first, wide):
    return slice(first * wide, (first + 1) * wide)


def regroup(rows, source, load, store):
    groups = LANE // UNITS
    lane = lax.broadcasted_iota(jnp.int32, (rows, LANE), 1) // UNITS
    for tile in range(FFN // LANE):
        out = None
        for i in range(groups):
            n = source(tile * groups + i)
            piece = load(n // groups)
            shift = (i - n) % groups
            if shift:
                piece = pltpu.roll(piece, shift * UNITS, 1)
            out = piece if out is None else jnp.where(lane == i, piece, out)
        store(tile, out)


def norm_stats(values):
    mean = row_mean(values)
    centered = values - mean
    inv = lax.rsqrt(row_mean(centered * centered) + LN_EPS)
    return centered * inv, inv


BLOCKS = [slice(a, b) for a, b in ((0, 512), (512, 1024), (1024, 1536), (1536, TOKENS))]


def row_tiles(body, step=LANE):
    def loop(i, carry):
        body(pl.multiple_of(i * step, step), step)
        return carry
    lax.fori_loop(0, TAIL // step, loop, 0)
    body(TAIL, IMAGES)


def back_part(body, part, parts):
    tiles = -(-TAIL // ROWS // parts)

    def loop(i, carry):
        tile = part * tiles + i

        @pl.when(tile < TAIL // ROWS)
        def _():
            body(pl.multiple_of(tile * ROWS, ROWS), ROWS)
        return carry
    lax.fori_loop(0, tiles, loop, 0)


def to_image_order(wide, place, step=LANE):
    per = MAIN // step
    def loop(i, carry):
        first = (i % per) * (step * IMAGES) + i // per
        rows = [wide[c, pl.ds(first, step, stride=IMAGES), :] for c in range(LANES)]
        place(pl.multiple_of(i * step, step), step, jnp.concatenate(rows, axis=1))
        return carry
    lax.fori_loop(0, IMAGES * per, loop, 0)
    place(TAIL, IMAGES, joined(wide, TAIL, IMAGES))


def from_image_order(values, wide):
    def loop(i, carry):
        rows = values[pl.ds(pl.multiple_of(i * LANE, LANE), LANE), :]
        for c in range(LANES):
            wide[c, pl.ds((i % 2) * (LANE * IMAGES) + i // 2, LANE, stride=IMAGES), :] = rows[:, steps(c, LANE)]
        return carry
    lax.fori_loop(0, 2 * IMAGES, loop, 0)
    put(wide, TAIL, IMAGES, values[pl.ds(TAIL, IMAGES), :])


def joined(wide, r, n):
    return jnp.concatenate([wide[c, pl.ds(r, n), :] for c in range(LANES)], axis=1)


def put(wide, r, n, values):
    for c in range(LANES):
        wide[c, pl.ds(r, n), :] = values[:, steps(c, LANE)]


def norm_back(dn, hat, inv, gain):
    dhat = dn * gain
    m1 = row_mean(dhat)
    m2 = row_mean(dhat * hat)
    return inv * (dhat - m1 - hat * m2)


ORDERS = ((2, 1, 0), (1, 0, 2), (0, 2, 1))


class Links:
    def find(self, send, recv):
        self.send, self.recv = send, recv
        me = lax.axis_index("fsdp")
        self.core = me % 2
        self.at = (me // SUBLANE, (me // QUAD) % 2, (me // 2) % 2)
        self.other_core = me + 1 - 2 * self.core
        self.other = [me + step - 2 * step * place for step, place in zip((SUBLANE, QUAD, 2), self.at)]
        return self

    def meet(self):
        barrier = pltpu.get_barrier_semaphore()
        devices = (self.other_core, *self.other)
        for device in devices:
            pl.semaphore_signal(barrier, inc=1, device_id=(device,), device_id_type=pl.DeviceIdType.MESH)
        pl.semaphore_wait(barrier, len(devices))

    def remote(self, src, dst, sem, device):
        return pltpu.make_async_remote_copy(src_ref=src, dst_ref=dst, send_sem=self.send.at[sem], recv_sem=self.recv.at[sem],
                                            device_id=(device,), device_id_type=pl.DeviceIdType.MESH)


class Gather(Links):
    COUNT = 2

    def __init__(self, rows, cols, cuts, by_rows):
        self.rows, self.cols, self.cuts, self.by_rows = rows, cols, cuts, by_rows
        self.parts = range(len(cuts) - 1)
        self.full_shape = jax.ShapeDtypeStruct((2, 2, 2, 2, rows, cols), BF)

    def scratch(self):
        return [pltpu.SemaphoreType.DMA((SEMS,))] * self.COUNT

    def bind(self, own, full, sems):
        self.own, self.full = own, full
        return self.find(*sems)

    def region(self, part, known, arrived=False, half=None):
        done = ORDERS[part][:known]
        place = [slice(None) if a in done else self.at[a] for a in range(3)]
        if half is not None:
            place[done[0]] = half
        if arrived:
            place[done[-1]] = 1 - self.at[done[-1]]
        cut = pl.ds(self.cuts[part], self.cuts[part + 1] - self.cuts[part])
        return (*place, self.core, cut, slice(None)) if self.by_rows else (*place, self.core, slice(None), cut)

    def hop(self, stage, part, half):
        where = self.full.at[self.region(part, stage - 1, half=half)]
        source = self.own.at[self.region(part, 0)[-2:]] if stage == 1 else where
        return self.remote(source, where, self.sem(stage, part, half), self.other[ORDERS[part][stage - 1]])

    def forward(self, stage, part, half=None):
        if stage == 0:
            return self.remote(self.own, self.full.at[(*self.at, self.core)], 0, self.other_core)
        where = self.full.at[self.region(part, stage, True, half)]
        return self.remote(where, where, self.sem(stage + QUAD, part, half), self.other_core)

    def sem(self, row, part, half):
        return QUAD * (row + (half or 0)) + part

    def halves(self, stage):
        return (None,) if stage < 3 else range(2)

    def keep(self):
        return pltpu.make_async_copy(self.own, self.full.at[(*self.at, self.core)], self.send.at[1])

    def begin(self):
        for part in self.parts:
            self.hop(1, part, None).start()
        self.forward(0, 0).start()
        self.keep().start()

    def turn(self, stage):
        if stage == 1:
            self.keep().wait()
        for half in self.halves(stage):
            for part in self.parts:
                self.hop(stage, part, half).wait()
                if stage < 3:
                    for onward in self.halves(stage + 1):
                        self.hop(stage + 1, part, onward).start()
            for part in self.parts:
                self.forward(stage, part, half).start()

    def end(self):
        self.forward(0, 0).wait()
        for stage in range(1, QUAD):
            for half in self.halves(stage):
                for part in self.parts:
                    self.forward(stage, part, half).wait()


SEMS = 36


class Exchange(Links):
    def __init__(self, rows, cols, cuts, along, stride=1, spare=0):
        self.rows, self.cols, self.stride = rows, cols, stride
        self.slots, self.locals = 3 * stride + spare, 1 + stride
        self.blocks = (2, 2, 2, 2, rows, cols)
        self.parts = [((slice(a, b), slice(None)) if along == 0 else (slice(None), slice(a, b))) for a, b in zip(cuts, cuts[1:])]
        self.shapes = [((b - a, cols) if along == 0 else (rows, b - a)) for a, b in zip(cuts, cuts[1:])]

    def scratch(self):
        two = (2, 2, 2)
        out = [pltpu.VMEM((self.locals, *self.blocks), F32), pltpu.VMEM((self.slots, *two, self.rows, self.cols), F32)]
        for axes in (2, 1, 0):
            out += [pltpu.VMEM((self.slots, *two[:axes], *shape), F32) for shape in self.shapes]
        return out + [pltpu.SemaphoreType.DMA((10, self.slots))] * 2

    COUNT = 13

    def bind(self, refs):
        self.local, self.pair = refs[0], refs[1]
        self.held = [None, refs[2:5], refs[5:SUBLANE], refs[SUBLANE:11]]
        return self.find(*refs[11:])

    def index(self, stage, part, side):
        order = ORDERS[part]
        left = [a for a in range(3) if a not in order[:stage - 1]]
        axis = order[stage - 1]
        where = self.at[axis] if side else 1 - self.at[axis]
        return tuple(where if a == axis else slice(None) for a in left)

    def copy(self, stage, part, c):
        slot = c % self.slots
        if stage == 0:
            return self.remote(self.local.at[c % self.locals, :, :, :, 1 - self.core], self.pair.at[slot], (0, slot), self.other_core)
        source = self.pair if stage == 1 else self.held[stage - 1][part]
        tail = self.parts[part] if stage == 1 else ()
        return self.remote(source.at[(slot, *self.index(stage, part, False), *tail)], self.held[stage][part].at[slot],
                           (3 * stage - 2 + part, slot), self.other[ORDERS[part][stage - 1]])

    def start(self, stage, c):
        for part in range(1 if stage == 0 else 3):
            self.copy(stage, part, c).start()

    def wait(self, stage, c):
        for part in range(1 if stage == 0 else 3):
            self.copy(stage, part, c).wait()

    def add(self, stage, c):
        slot = c % self.slots
        if stage == 0:
            for chip in itertools.product(range(2), repeat=3):
                self.pair[(slot, *chip)] += self.local[(c % self.locals, *chip, self.core)]
            return
        for part in range(3):
            source = self.pair if stage == 1 else self.held[stage - 1][part]
            tail = self.parts[part] if stage == 1 else ()
            for place in itertools.product(range(2), repeat=3 - stage):
                free = iter(place)
                kept = tuple(next(free) if isinstance(i, slice) else i for i in self.index(stage, part, True))
                self.held[stage][part][(slot, *place)] += source[(slot, *kept, *tail)]

    def result(self, c, out_ref):
        for part in range(3):
            out_ref[self.parts[part]] = self.held[3][part][c % self.slots]

    def put_local(self, c, values):
        self.local[c % self.locals] = values.reshape(self.blocks)


def comm_params(n):
    return pltpu.CompilerParams(dimension_semantics=("arbitrary",), vmem_limit_bytes=VMEM_MAX, collective_id=n, has_side_effects=True)


def advance(exchanges, t, exists, emit):
    for stage in (3, 2, 1, 0):
        c = t - 1 - (stage + 1) * exchanges[0].stride

        @pl.when(exists(c))
        def _():
            for n, exchange in enumerate(exchanges):
                exchange.wait(stage, c)
                exchange.add(stage, c)
                if stage < 3:
                    exchange.start(stage + 1, c)
                else:
                    emit(n, exchange, c)

    @pl.when(exists(t - 1))
    def _():
        for exchange in exchanges:
            exchange.start(0, t - 1)


def first_chunks(n):
    return lambda c: (c >= 0) & (c < n)


DRAIN = 5


PARTS = 16
SHARD = WIDTH // PARTS
VECTOR_ROWS = PARTS
LN1_GAIN, LN1_BIAS, QKV_BIAS, OUT_BIAS, LN2_GAIN, LN2_BIAS, FC_BIAS, PROJ_BIAS = 0, 1, 2, 5, 6, 7, 8, 12
MLP_F = MAIN
UNITS = MLP_F // PARTS
MLP_STEPS = FFN // MLP_F
WIDTH_CUTS = (0, 384, 896, WIDTH)
QKV_ALL = Gather(SHARD, QKV, (0, WIDTH, 2 * WIDTH, QKV), False)
OUT_ALL = Gather(SHARD, WIDTH, (0, 384, 768, WIDTH), False)
FC_ALL = Gather(SHARD, FFN, (0, 1664, 3328, FFN), False)
PROJ_ALL = Gather(FFN // PARTS, WIDTH, (0, 112, 208, FFN // PARTS), True)
VECTOR_ALL = Gather(SHARD, LANE, (0, SHARD), True)


def open_kernel(x_hbm, dy_hbm, rows_ref, fc_ref, wq_ref, wo_ref, xim_hbm, dyim_hbm, h_hbm, ht_hbm, vec_ref, qb_ref, fb_ref, fc_own, wq_full, wo_full,
                x, dy, wide, h, ht, rows, vec_own, vec_full, wq_own, wo_own, sems, *comm):
    loads = [pltpu.make_async_copy(src, dst, sems.at[i]) for i, (src, dst) in enumerate(((x_hbm, x), (dy_hbm, dy)))]
    for cp in loads:
        cp.start()
    clear(rows)
    rows[:VECTOR_ROWS, :] = rows_ref[ALL]
    vec_own[ALL] = rows[ALL].T[:SHARD, :].astype(BF)
    wq_own[ALL] = wq_ref[ALL].astype(BF)
    wo_own[ALL] = wo_ref[ALL].astype(BF)
    pairs = [comm[2 * i:2 * i + 2] for i in range(3)]
    vectors = VECTOR_ALL.bind(vec_own, vec_full, pairs[0])
    weights = QKV_ALL.bind(wq_own, wq_full, pairs[1]), OUT_ALL.bind(wo_own, wo_full, pairs[2])
    gathers = (vectors, *weights)
    vectors.meet()
    for gather in gathers:
        gather.begin()
    for cp in loads:
        cp.wait()

    def reorder(tokens):
        def widen(r, n):
            put(wide, r, n, tokens[pl.ds(r, n), :].astype(F32))
        row_tiles(widen)

        def place(r, n, values):
            tokens[pl.ds(r, n), :] = values.astype(BF)
        to_image_order(wide, place)
    reorder(x)
    for gather in gathers:
        gather.turn(1)
    reorder(dy)
    for gather in gathers:
        gather.turn(2)
    vectors.turn(3)
    vectors.end()
    vec_ref[ALL] = vec_full[ALL].reshape(WIDTH, LANE).astype(F32).T[:VECTOR_ROWS, :]
    gain, bias = vec_ref[steps(LN1_GAIN, 1), :], vec_ref[steps(LN1_BIAS, 1), :]
    for d in range(PARTS):
        for i in range(3):
            qb_ref[:, steps(3 * d + i, SHARD)] = vec_ref[steps(QKV_BIAS + i, 1), steps(d, SHARD)]
        for n in range(MLP_STEPS):
            place = pl.ds(d * SHARD + n * UNITS % SHARD, UNITS)
            fb_ref[:, pl.ds(n * MLP_F + d * UNITS, UNITS)] = vec_ref[steps(FC_BIAS + n * UNITS // SHARD, 1), place]

    def norm(r, n):
        hat, _ = norm_stats(x[pl.ds(r, n), :].astype(F32))
        h[pl.ds(r, n), :] = (hat * gain + bias).astype(BF)
    row_tiles(norm, ROWS)
    for b in range(IMAGES):
        ht[:, steps(b, MAIN)] = h[steps(b, MAIN), :].T
    ht[:, TAIL:] = h[TAIL:, :].T
    stores = [pltpu.make_async_copy(src, dst, sems.at[i]) for i, (src, dst) in enumerate(((x, xim_hbm), (dy, dyim_hbm), (h, h_hbm), (ht, ht_hbm)))]
    for cp in stores:
        cp.start()
    def store_fc(tile, values):
        fc_own[:, steps(tile, LANE)] = values.astype(BF)
    regroup(SHARD, lambda n: n % PARTS * MLP_STEPS + n // PARTS, lambda tile: fc_ref[:, steps(tile, LANE)], store_fc)
    for gather in weights:
        gather.turn(3)
    for gather in weights:
        gather.end()
    for cp in stores:
        cp.wait()


def open_call(x, dy, rows, fc, wq, wo):
    hbm, vmem = pl.BlockSpec(memory_space=pl.ANY), pl.BlockSpec(memory_space=pltpu.VMEM)
    return pl.pallas_call(
        open_kernel,
        in_specs=[hbm, hbm, vmem, vmem, vmem, vmem],
        out_specs=[hbm, hbm, hbm, hbm, vmem, vmem, vmem, vmem, hbm, hbm],
        out_shape=[*[jax.ShapeDtypeStruct((TOKENS, WIDTH), BF)] * 3,
                   jax.ShapeDtypeStruct((WIDTH, TOKENS), BF), jax.ShapeDtypeStruct((VECTOR_ROWS, WIDTH), F32),
                   *(jax.ShapeDtypeStruct((1, n), F32) for n in (QKV, FFN)), jax.ShapeDtypeStruct(fc.shape, BF), QKV_ALL.full_shape, OUT_ALL.full_shape],
        scratch_shapes=[pltpu.VMEM((TOKENS, WIDTH), BF), pltpu.VMEM((TOKENS, WIDTH), BF), pltpu.VMEM((LANES, TOKENS, LANE), F32),
                        pltpu.VMEM((TOKENS, WIDTH), BF), pltpu.VMEM((WIDTH, TOKENS), BF), pltpu.VMEM((LANE, LANE), F32), pltpu.VMEM((SHARD, LANE), BF),
                        pltpu.VMEM(VECTOR_ALL.full_shape.shape, BF), pltpu.VMEM((SHARD, QKV), BF), pltpu.VMEM((SHARD, WIDTH), BF),
                        pltpu.SemaphoreType.DMA((QUAD,))] + VECTOR_ALL.scratch() + QKV_ALL.scratch() + OUT_ALL.scratch(),
        compiler_params=pltpu.CompilerParams(vmem_limit_bytes=VMEM_MAX, collective_id=3, has_side_effects=True),
        cost_estimate=cost(1_000_000_000, 60_000_000),
        name="open",
    )(x, dy, rows, fc, wq, wo)


QKV_N = 768


def qkv_kernel(h_ref, w_ref, wb_ref, own_ref, qkv_ref, full, *sems):
    t, last = step_id(), pl.num_programs(0) - 1
    gather = FC_ALL.bind(own_ref, full, sems)

    @pl.when(t == 0)
    def _():
        gather.meet()
        gather.begin()

    @pl.when(t == 1)
    def _():
        gather.turn(1)

    @pl.when(t == 3)
    def _():
        gather.turn(2)
    for rows in BLOCKS:
        qkv_ref[rows, :] = (dot(h_ref[rows, :], w_ref[ALL]) + wb_ref[ALL]).astype(BF)

    @pl.when(t == last)
    def _():
        gather.turn(3)
        gather.end()


def qkv_call(h, w, wb, own):
    hbm = pl.BlockSpec(memory_space=pl.ANY)
    return pl.pallas_call(
        qkv_kernel,
        grid=(QKV // QKV_N,),
        in_specs=[whole(TOKENS, WIDTH, pipeline_mode=pl.Buffered(1)), by_cols(WIDTH, QKV_N), by_cols(1, QKV_N), whole(SHARD, FFN)],
        out_specs=[by_cols(TOKENS, QKV_N), hbm],
        out_shape=[jax.ShapeDtypeStruct((TOKENS, QKV), BF), FC_ALL.full_shape],
        scratch_shapes=FC_ALL.scratch(),
        compiler_params=comm_params(QUAD),
        cost_estimate=cost(2 * TOKENS * WIDTH * QKV, 60_000_000),
        name="qkv",
    )(h, w, wb, own)


ROW_CUTS = (0, 24, 48, 80)
FC_SUM = Exchange(SHARD, MLP_F, ROW_CUTS, 0)
PROJ_SUM = Exchange(UNITS, WIDTH, WIDTH_CUTS, 1)
CDF_P = 0.33
CDF_C = (0.1326322871417956, 0.11939570820799192, 0.18103829560051796, -0.08904113226212501,
         0.33075919469138065, -0.22023738432274684, 0.0454530347223348)


def gelu_pair(u):
    bell = jnp.exp(u * u * -0.5)
    t = 1.0 / (1.0 + CDF_P * jnp.abs(u))
    poly = CDF_C[6]
    for c in CDF_C[5::-1]:
        poly = poly * t + c
    tail = poly * t * bell
    cdf = jnp.where(u < 0.0, tail, 1.0 - tail)
    return u * cdf, cdf + u * bell * ((2.0 * math.pi) ** -0.5)


def mlp_kernel(r_hbm, n_hbm, dy_hbm, vec_ref, fc_ref, proj_ref, fcb_ref,
               y_hbm, dr_hbm, dr16_hbm, dfc_ref, dproj_ref, dfcb_ref, small_ref,
               n2, dy, y_acc, dn_acc, g, du, ua, ub, da, db, sem, *comm):
    step = step_id()
    by_row, by_col = FC_SUM.bind(comm[:Exchange.COUNT]), PROJ_SUM.bind(comm[Exchange.COUNT:])

    @pl.when(step == 0)
    def _():
        loads = [pltpu.make_async_copy(n_hbm, n2, sem), pltpu.make_async_copy(dy_hbm, dy, sem)]
        for cp in loads:
            cp.start()
        by_row.meet()
        clear(small_ref, y_acc, dn_acc)
        for cp in loads:
            cp.wait()

    outs = (dfc_ref, dproj_ref)
    advance((by_row, by_col), step, first_chunks(MLP_STEPS), lambda n, exchange, c: exchange.result(c, outs[n]))

    @pl.when(step < MLP_STEPS)
    def _():
        fcb = fcb_ref[ALL]
        fc, proj = fc_ref[ALL], proj_ref[ALL].reshape(MLP_F, WIDTH)
        bias_sum = jnp.zeros((SUBLANE, MLP_F), F32)
        tiles = [(b * MAIN, MAIN) for b in range(IMAGES - 1)] + [((IMAGES - 1) * MAIN, MAIN + IMAGES)]
        pairs = ((ua, da), (ub, db))

        def products(k):
            r, n = tiles[k]
            u_s, d_s = pairs[k % 2]
            u_s[0:n, :] = dot(n2[r:r + n, :], fc)
            d_s[0:n, :] = dot_nt(dy[r:r + n, :], proj)

        def pointwise(k, total):
            r, n = tiles[k]
            u_s, d_s = pairs[k % 2]
            value, slope = gelu_pair(u_s[0:n, :] + fcb)
            g[r:r + n, :] = value.astype(BF)
            grad = d_s[0:n, :] * slope
            du[r:r + n, :] = grad.astype(BF)
            return total + eights(grad)

        products(0)
        for k in range(1, IMAGES):
            products(k)
            bias_sum = pointwise(k - 1, bias_sum)
        bias_sum = pointwise(IMAGES - 1, bias_sum)
        dfcb_ref[ALL] = col_sum(bias_sum)
        y_acc[ALL] += dot(g[ALL], proj)
        for c in range(LANES // 2):
            part = dot_nt(du[ALL], fc_ref[steps(c, MAIN), :])
            dn_acc[2 * c] += part[:, :LANE]
            dn_acc[2 * c + 1] += part[:, LANE:]
        by_col.put_local(step, dot_tn(g[ALL], dy[ALL]))
        by_row.put_local(step, dot_tn(n2[ALL], du[ALL]))

    after = step - MLP_STEPS
    r_copy = pltpu.make_async_copy(r_hbm, n2, sem)
    out_copies = [pltpu.make_async_copy(dn_acc, dr_hbm, sem), pltpu.make_async_copy(n2, dr16_hbm, sem)]
    y_copy = pltpu.make_async_copy(dy, y_hbm, sem)

    def back(r, n):
        wide_r = n2[pl.ds(r, n), :].astype(F32)
        hat, inv = norm_stats(wide_r)
        dn = joined(dn_acc, r, n)
        wide_dy = dy[pl.ds(r, n), :].astype(F32)
        dr = wide_dy + norm_back(dn, hat, inv, vec_ref[steps(LN2_GAIN, 1), :])
        put(dn_acc, r, n, dr)
        n2[pl.ds(r, n), :] = dr.astype(BF)
        y_acc[pl.ds(r, n), :] += wide_r + vec_ref[steps(PROJ_BIAS, 1), :]
        for i, v in enumerate((dn * hat, dn, wide_dy, dr)):
            small_ref[steps(i, SUBLANE), :] += eights(v)

    @pl.when(after == 0)
    def _():
        r_copy.start()
        r_copy.wait()
        back(TAIL, IMAGES)

    @pl.when((after >= 0) & (after < 3))
    def _():
        back_part(back, after, 3)

    @pl.when(after == 2)
    def _():
        for cp in out_copies:
            cp.start()

    @pl.when(after == 3)
    def _():
        for cp in out_copies:
            cp.wait()
        from_image_order(y_acc, dn_acc)

        def narrow(r, n):
            dy[pl.ds(r, n), :] = joined(dn_acc, r, n).astype(BF)
        row_tiles(narrow)
        y_copy.start()

    @pl.when(after == QUAD)
    def _():
        y_copy.wait()


def mlp_call(r, n2, dy, vec, fc, proj, fcb):
    hbm = pl.BlockSpec(memory_space=pl.ANY)
    now = lambda i: jnp.minimum(i, MLP_STEPS - 1)
    done = lambda i: jnp.maximum(i - DRAIN, 0)
    return pl.pallas_call(
        mlp_kernel,
        grid=(MLP_STEPS + DRAIN,),
        in_specs=[hbm, hbm, hbm, whole(*vec.shape), by_cols(WIDTH, MLP_F, now),
                  pl.BlockSpec((PARTS, None, UNITS, WIDTH), lambda i: (0, now(i), 0, 0)),
                  by_cols(1, MLP_F, now)],
        out_specs=[hbm, hbm, hbm, by_cols(SHARD, MLP_F, done),
                   by_rows(UNITS, WIDTH, done),
                   by_cols(1, MLP_F, now), whole(32, WIDTH)],
        out_shape=[jax.ShapeDtypeStruct((TOKENS, WIDTH), BF), jax.ShapeDtypeStruct((LANES, TOKENS, LANE), F32),
                   jax.ShapeDtypeStruct((TOKENS, WIDTH), BF), jax.ShapeDtypeStruct((SHARD, FFN), F32),
                   jax.ShapeDtypeStruct((FFN // PARTS, WIDTH), F32),
                   jax.ShapeDtypeStruct((1, FFN), F32), jax.ShapeDtypeStruct((32, WIDTH), F32)],
        scratch_shapes=[pltpu.VMEM((TOKENS, WIDTH), BF), pltpu.VMEM((TOKENS, WIDTH), BF),
                        pltpu.VMEM((TOKENS, WIDTH), F32), pltpu.VMEM((LANES, TOKENS, LANE), F32),
                        pltpu.VMEM((TOKENS, MLP_F), BF), pltpu.VMEM((TOKENS, MLP_F), BF)]
                       + [pltpu.VMEM((MAIN + IMAGES, MLP_F), F32)] * QUAD + [pltpu.SemaphoreType.DMA]
                       + FC_SUM.scratch() + PROJ_SUM.scratch(),
        compiler_params=comm_params(0),
        cost_estimate=cost(12 * TOKENS * WIDTH * FFN, 150_000_000, TOKENS * FFN),
        name="mlp",
    )(r, n2, dy, vec, fc, proj.reshape(PARTS, MLP_STEPS, UNITS, WIDTH), fcb)


SCALE = HEAD ** -0.5
ATTN_COST = cost(40_000_000_000, 50_000_000, 8_400_000)


def window(h):
    first = min(HEAD * h // LANE * LANE, WIDTH - MAIN)
    wide = LANE if HEAD * h + HEAD <= first + LANE else MAIN
    return first, wide, HEAD * h - first


def lane_mask(h):
    first, wide, off = window(h)
    lane = lax.broadcasted_iota(jnp.int32, (MAIN, wide), 1)
    return (lane >= off) & (lane < off + HEAD)


def thirds(ref, rows=slice(None)):
    return [ref[rows, steps(i, WIDTH)] for i in range(3)]


def head_rows():
    lane = lax.broadcasted_iota(jnp.int32, (HEADS, WIDTH), 1)
    row = lax.broadcasted_iota(jnp.int32, (HEADS, WIDTH), 0)
    return (lane // HEAD == row).astype(F32)


def tail_softmax(s, s_self):
    m = jnp.maximum(jnp.max(s, axis=1, keepdims=True), s_self)
    e = jnp.exp((s - m) * SCALE)
    e_self = jnp.exp((s_self - m) * SCALE)
    inv = 1.0 / (row_sum(e) + e_self)
    return e * inv, e_self * inv


def attn_kernel(qkv_ref, qkvt_ref, x_ref, xt_ref, w_ref, vec_ref, proj_ref, o_hbm, r_hbm, n_hbm,
                max_ref, inv_ref, full,
                tails, o_tail, o_t, ptail, o_buf, r_buf, n_buf, sa, sb, sems, own, *comm):
    b, last = step_id(), pl.num_programs(0) - 1
    slot = b % 2
    gather = PROJ_ALL.bind(own, full, comm)

    @pl.when(b == 0)
    def _():
        tails[ALL] = qkvt_ref[ALL].astype(F32)
        own[ALL] = proj_ref[ALL].astype(BF)
        gather.meet()
        gather.begin()

    @pl.when(b == 1)
    def _():
        gather.turn(1)

    @pl.when(b == 3)
    def _():
        gather.turn(2)

    @pl.when(b == last)
    def _():
        gather.turn(3)

    heads = head_rows()
    q_t, k_t, v_t = (heads * z for z in thirds(tails, pl.ds(b, 1)))
    q, k, v = thirds(qkv_ref)

    p, p_self = tail_softmax(dot_nt(q_t.astype(BF), k), row_sum(q_t * k_t))
    mixed = dot(p.astype(BF), v) * heads + p_self.astype(BF).astype(F32) * v_t
    o_tail[pl.ds(b, 1), :] = col_sum(mixed)

    s_tail = dot_nt(k_t.astype(BF), q)
    v_turned = v.T
    scores = sa, sb

    def next_scores(h):
        first, wide, _ = window(h)
        q_h = jnp.where(lane_mask(h), qkv_ref[:, pl.ds(first, wide)], jnp.zeros((), BF))
        scores[h % 2][ALL] = dot_nt(qkv_ref[:, pl.ds(WIDTH + first, wide)], q_h)
    next_scores(0)
    for h in range(HEADS):
        if h + 1 < HEADS:
            next_scores(h + 1)
        s, mine = scores[h % 2], steps(h, 1)
        top = jnp.maximum(col_max(s[ALL]), s_tail[mine, :])
        e = jnp.exp((s[ALL] - top) * SCALE)
        e_tail = jnp.exp((s_tail[mine, :] - top) * SCALE)
        inv = 1.0 / (col_sum(e) + e_tail)
        max_ref[0, mine, :] = top
        inv_ref[0, mine, :] = inv
        ptail[mine, :] = e_tail * inv
        o_t[steps(h, HEAD), :] = dot(v_turned[steps(h, HEAD), :], (e * inv).astype(BF))

    outs = (o_buf, o_hbm), (r_buf, r_hbm), (n_buf, n_hbm)
    out_bias, gain, bias = (vec_ref[steps(i, 1), :] for i in (OUT_BIAS, LN2_GAIN, LN2_BIAS))

    def write(slot, rows, o, x):
        o_buf[slot, rows, :] = o
        r = (x.astype(F32) + dot(o, w_ref[ALL]) + out_bias).astype(BF)
        r_buf[slot, rows, :] = r
        hat, _ = norm_stats(r.astype(F32))
        n_buf[slot, rows, :] = (hat * gain + bias).astype(BF)

    @pl.when(b >= 2)
    def _():
        for n, (buf, hbm) in enumerate(outs):
            out_copy(buf, hbm, slot, b - 2, sems, n).wait()

    o = (o_t[ALL].T + dot_tn(ptail[ALL].astype(BF), v_t.astype(BF))).astype(BF)
    write(slot, slice(None), o, x_ref[ALL])
    for n, (buf, hbm) in enumerate(outs):
        out_copy(buf, hbm, slot, b, sems, n).start()

    @pl.when(b == last)
    def _():
        for n, (buf, hbm) in enumerate(outs):
            out_copy(buf, hbm, 1 - slot, b - 1, sems, n).wait()
        write(1 - slot, slice(IMAGES), o_tail[ALL].astype(BF), xt_ref[ALL])
        copies = [pltpu.make_async_copy(buf.at[1 - slot, pl.ds(0, IMAGES)], hbm.at[pl.ds(TAIL, IMAGES)], sems.at[n, 1 - slot])
                  for n, (buf, hbm) in enumerate(outs)]
        for cp in copies:
            cp.start()
        for cp in copies:
            cp.wait()
        for n, (buf, hbm) in enumerate(outs):
            out_copy(buf, hbm, slot, b, sems, n).wait()
        gather.end()


def out_copy(buf, hbm, slot, b, sems, n):
    return pltpu.make_async_copy(buf.at[slot], hbm.at[pl.ds(pl.multiple_of(b * MAIN, MAIN), MAIN)], sems.at[n, slot])


def attn_call(qkv, xim, w, vec, proj):
    hbm = pl.BlockSpec(memory_space=pl.ANY)
    main = lambda n: by_rows(MAIN, n)
    tail = lambda n: by_rows(IMAGES, n, lambda i: TAIL // IMAGES)
    stat = pl.BlockSpec((1, HEADS, MAIN), lambda i: (i, 0, 0))
    return pl.pallas_call(
        attn_kernel,
        grid=(IMAGES,),
        in_specs=[main(QKV), tail(QKV), main(WIDTH), tail(WIDTH),
                  whole(WIDTH, WIDTH), whole(*vec.shape), whole(*proj.shape)],
        out_specs=[hbm, hbm, hbm, stat, stat, hbm],
        out_shape=[*[jax.ShapeDtypeStruct((TOKENS, WIDTH), BF)] * 3,
                   jax.ShapeDtypeStruct((IMAGES, HEADS, MAIN), F32), jax.ShapeDtypeStruct((IMAGES, HEADS, MAIN), F32),
                   PROJ_ALL.full_shape],
        scratch_shapes=[pltpu.VMEM((IMAGES, QKV), F32), pltpu.VMEM((IMAGES, WIDTH), F32),
                        pltpu.VMEM((WIDTH, MAIN), F32), pltpu.VMEM((HEADS, MAIN), F32),
                        *[pltpu.VMEM((2, MAIN, WIDTH), BF)] * 3, *[pltpu.VMEM((MAIN, MAIN), F32)] * 2, pltpu.SemaphoreType.DMA((3, 2)),
                        pltpu.VMEM(proj.shape, BF)] + PROJ_ALL.scratch(),
        compiler_params=comm_params(5),
        cost_estimate=ATTN_COST,
        name="attn",
    )(qkv, qkv, xim, xim, w, vec, proj)


def outb_kernel(dr_ref, o_ref, w_ref, dfc_ref, y_in, dproj_in, do_ref, dw_ref, dfc_out, y_out, dproj_out, y, dproj, sems):
    c, last = step_id(), pl.num_programs(0) - 1
    loads = [pltpu.make_async_copy(src, dst, sems.at[i]) for i, (src, dst) in enumerate(((y_in, y), (dproj_in, dproj)))]
    stores = [pltpu.make_async_copy(src, dst, sems.at[i]) for i, (src, dst) in enumerate(((y, y_out), (dproj, dproj_out)))]

    @pl.when(c == 0)
    def _():
        for cp in loads:
            cp.start()

    @pl.when(c == 1)
    def _():
        for cp in loads:
            cp.wait()
        for cp in stores:
            cp.start()

        def store_fc(tile, values):
            dfc_out[:, steps(tile, LANE)] = values
        regroup(SHARD, lambda n: n % MLP_STEPS * PARTS + n // MLP_STEPS, lambda tile: dfc_ref[:, steps(tile, LANE)], store_fc)
    do_ref[ALL] = dot_nt(dr_ref[ALL], w_ref[ALL]).astype(BF)
    dw_ref[ALL] = dot_tn(o_ref[ALL], dr_ref[:, pl.ds(pl.multiple_of(c * MAIN, MAIN), MAIN)])

    @pl.when(c == last)
    def _():
        for cp in stores:
            cp.wait()


def outb_call(dr, o, w, dfc, y, dproj):
    full, hbm = whole(TOKENS, WIDTH), pl.BlockSpec(memory_space=pl.ANY)
    like = lambda v: jax.ShapeDtypeStruct(v.shape, v.dtype)
    return pl.pallas_call(
        outb_kernel,
        grid=(WIDTH // MAIN,),
        in_specs=[full, full, by_rows(MAIN, WIDTH), whole(*dfc.shape), hbm, hbm],
        out_specs=[by_cols(TOKENS, MAIN), by_cols(WIDTH, MAIN), whole(*dfc.shape), hbm, hbm],
        out_shape=[like(dr), jax.ShapeDtypeStruct((WIDTH, WIDTH), F32), like(dfc), like(y), like(dproj)],
        scratch_shapes=[pltpu.VMEM(y.shape, BF), pltpu.VMEM(dproj.shape, F32), pltpu.SemaphoreType.DMA((2,))],
        compiler_params=pltpu.CompilerParams(dimension_semantics=("arbitrary",), vmem_limit_bytes=VMEM_MAX),
        cost_estimate=cost(QUAD * TOKENS * WIDTH * WIDTH, 50_000_000),
        name="outb",
    )(dr, o, w, dfc, y, dproj)


def attn_back_kernel(qkv_ref, qkvt_ref, do_ref, dot_ref, max_ref, inv_ref, dw_ref, dqkv_hbm, dwb_ref, dwout_ref,
                     tails, do_tails, grad_tails, dq_t, dk, dv, ds_tail, sa, da, sb, db, buf, sems, *comm):
    b = step_id()
    by_row = OUT_SUM.bind(comm)

    @pl.when(b == 0)
    def _():
        by_row.meet()

    @pl.when(b < OUT_STEPS)
    def _():
        by_row.put_local(b, dw_ref[ALL])
    advance((by_row,), b + 1, first_chunks(OUT_STEPS), lambda n, exchange, c: exchange.result(c, dwout_ref))

    @pl.when(b < IMAGES)
    def _():
        image_back(b, qkv_ref, qkvt_ref, do_ref, dot_ref, max_ref, inv_ref, dqkv_hbm, dwb_ref,
                   tails, do_tails, grad_tails, dq_t, dk, dv, ds_tail, ((sa, da), (sb, db)), buf, sems)


OUT_N = MAIN
OUT_STEPS = WIDTH // OUT_N
OUT_SUM = Exchange(SHARD, OUT_N, ROW_CUTS, 0)


def image_back(b, qkv_ref, qkvt_ref, do_ref, dot_ref, max_ref, inv_ref, dqkv_hbm, dwb_ref,
               tails, do_tails, grad_tails, dq_t, dk, dv, ds_tail, ahead, buf, sems):
    last = IMAGES - 1
    slot = b % 2

    @pl.when(b == 0)
    def _():
        tails[ALL] = qkvt_ref[ALL].astype(F32)
        do_tails[ALL] = dot_ref[ALL].astype(F32)
        clear(dwb_ref)

    heads = head_rows()
    q_t, k_t, v_t = (heads * z for z in thirds(tails, pl.ds(b, 1)))
    do_t = heads * do_tails[pl.ds(b, 1), :]
    q, k, v = thirds(qkv_ref)
    do = do_ref[ALL]
    q_t16, k_t16, v_t16, do_t16 = (z.astype(BF) for z in (q_t, k_t, v_t, do_t))

    p, p_self = tail_softmax(dot_nt(q_t16, k), row_sum(q_t * k_t))
    dp, dp_self = dot_nt(do_t16, v), row_sum(do_t * v_t)
    inner = row_sum(p * dp) + p_self * dp_self
    ds16 = (p * (dp - inner) * SCALE).astype(BF)
    ds_self = (p_self * (dp_self - inner) * SCALE).astype(BF).astype(F32)
    grad_q = col_sum(dot(ds16, k) * heads + ds_self * k_t)
    grad_k = ds_self * q_t
    grad_v = p_self.astype(BF).astype(F32) * do_t
    dk[ALL] = dot_tn(ds16, q_t16)
    dv[ALL] = dot_tn(p.astype(BF), do_t16)

    p_tail = jnp.exp((dot_nt(k_t16, q) - max_ref[0]) * SCALE) * inv_ref[0]
    dp_tail = dot_nt(v_t16, do)
    inner_tail = p_tail * dp_tail

    k_turned = k.T

    def masked(h):
        first, wide, _ = window(h)
        here, mask = pl.ds(first, wide), lane_mask(h)
        return here, jnp.where(mask, qkv_ref[:, here], jnp.zeros((), BF)), jnp.where(mask, do_ref[:, here], jnp.zeros((), BF))

    def next_products(h):
        first, wide, _ = window(h)
        _, q_h, do_h = masked(h)
        ahead[h % 2][0][ALL] = dot_nt(qkv_ref[:, pl.ds(WIDTH + first, wide)], q_h)
        ahead[h % 2][1][ALL] = dot_nt(qkv_ref[:, pl.ds(2 * WIDTH + first, wide)], do_h)
    next_products(0)
    for h in range(HEADS):
        if h + 1 < HEADS:
            next_products(h + 1)
        here, q_h, do_h = masked(h)
        mine = steps(h, 1)
        s, dp = (ref[ALL] for ref in ahead[h % 2])
        p = jnp.exp((s - max_ref[0, mine, :]) * SCALE) * inv_ref[0, mine, :]
        inner = col_sum(p * dp) + inner_tail[mine, :]
        ds = (p * (dp - inner) * SCALE).astype(BF)
        dv[:, here] += dot(p.astype(BF), do_h)
        dk[:, here] += dot(ds, q_h)
        dq_t[steps(h, HEAD), :] = dot(k_turned[steps(h, HEAD), :], ds)
        ds_tail[mine, :] = p_tail[mine, :] * (dp_tail[mine, :] - inner) * SCALE

    ds_tail16 = ds_tail[ALL].astype(BF)
    grad_k = col_sum(grad_k + dot(ds_tail16, q) * heads)
    grad_v = col_sum(grad_v + dot(p_tail.astype(BF), do) * heads)

    @pl.when(b >= 2)
    def _():
        out_copy(buf, dqkv_hbm, slot, b - 2, sems, 0).wait()

    grad = dq_t[ALL].T + dot_tn(ds_tail16, k_t16)
    for n, (main, tail) in enumerate(((grad, grad_q), (dk[ALL], grad_k), (dv[ALL], grad_v))):
        here = steps(n, WIDTH)
        buf[slot, :, here] = main.astype(BF)
        grad_tails[pl.ds(b, 1), here] = tail
        dwb_ref[:, here] += col_sum(main) + tail
    out_copy(buf, dqkv_hbm, slot, b, sems, 0).start()

    @pl.when(b == last)
    def _():
        out_copy(buf, dqkv_hbm, 1 - slot, b - 1, sems, 0).wait()
        buf[1 - slot, 0:IMAGES, :] = grad_tails[ALL].astype(BF)
        cp = pltpu.make_async_copy(buf.at[1 - slot, pl.ds(0, IMAGES)], dqkv_hbm.at[pl.ds(TAIL, IMAGES)], sems.at[0, 1 - slot])
        cp.start()
        cp.wait()
        out_copy(buf, dqkv_hbm, slot, b, sems, 0).wait()


def attn_back_call(qkv, do, top, inv, dw):
    hbm = pl.BlockSpec(memory_space=pl.ANY)
    image = lambda i: jnp.minimum(i, IMAGES - 1)
    main = lambda n: by_rows(MAIN, n, image)
    tail = lambda n: by_rows(IMAGES, n, lambda i: TAIL // IMAGES)
    stat = pl.BlockSpec((1, HEADS, MAIN), lambda i: (image(i), 0, 0))
    return pl.pallas_call(
        attn_back_kernel,
        grid=(OUT_STEPS + DRAIN - 1,),
        in_specs=[main(QKV), tail(QKV), main(WIDTH), tail(WIDTH), stat, stat,
                  by_cols(WIDTH, OUT_N, lambda i: jnp.minimum(i, OUT_STEPS - 1))],
        out_specs=[hbm, whole(1, QKV), by_cols(SHARD, OUT_N, lambda i: jnp.clip(i + 1 - DRAIN, 0, OUT_STEPS - 1))],
        out_shape=[jax.ShapeDtypeStruct((TOKENS, QKV), BF), jax.ShapeDtypeStruct((1, QKV), F32),
                   jax.ShapeDtypeStruct((SHARD, WIDTH), F32)],
        scratch_shapes=[pltpu.VMEM((IMAGES, QKV), F32), pltpu.VMEM((IMAGES, WIDTH), F32),
                        pltpu.VMEM((IMAGES, QKV), F32), pltpu.VMEM((WIDTH, MAIN), F32),
                        pltpu.VMEM((MAIN, WIDTH), F32), pltpu.VMEM((MAIN, WIDTH), F32), pltpu.VMEM((HEADS, MAIN), F32),
                        *[pltpu.VMEM((MAIN, MAIN), F32)] * QUAD, pltpu.VMEM((2, MAIN, QKV), BF), pltpu.SemaphoreType.DMA((1, 2))] + OUT_SUM.scratch(),
        compiler_params=comm_params(1),
        cost_estimate=ATTN_COST,
        name="attn_back",
    )(qkv, qkv, do, do, top, inv, dw)


QB_N = MAIN
QB_STEPS = QKV // QB_N
QKV_SUM = Exchange(SHARD, QB_N, ROW_CUTS, 0, 2)
VECTOR_SUM = Exchange(3 * SUBLANE, LANE, (0, SUBLANE, 2 * SUBLANE, 3 * SUBLANE), 0)
VECTOR_STEP = QB_STEPS - 1
BACK_STEP = VECTOR_STEP - 4
QB_GRID = QB_STEPS + 1 + QUAD * QKV_SUM.stride


def qkvb_kernel(xim_hbm, dr_hbm, vec_ref, sums_ref, qb_ref, fb_ref, ht_ref, dqkv_ref, wide_ref, w_ref, dx_hbm, dw_ref, out_vec_ref,
                acc, dr, xd, sums, sems, *comm):
    t = step_id()
    by_row, by_vector = QKV_SUM.bind(comm[:Exchange.COUNT]), VECTOR_SUM.bind(comm[Exchange.COUNT:])
    loads = [pltpu.make_async_copy(dr_hbm, dr, sems.at[0]), pltpu.make_async_copy(xim_hbm, xd, sems.at[1])]
    store = pltpu.make_async_copy(xd, dx_hbm, sems.at[1])

    def put_row(place, row, lane, values):
        by_vector.local[(0, *place, pl.ds(row, len(values)), pl.ds(lane, values.shape[1]))] = values

    def share(row, values):
        for d, place in enumerate(DEVICES):
            put_row(place, row, 0, values[:, steps(d, SHARD)])

    @pl.when(t == 0)
    def _():
        by_row.meet()
        for cp in loads:
            cp.start()
        clear(acc, sums)
        by_vector.local[0] = jnp.zeros(by_vector.blocks, F32)
        share(0, jnp.concatenate([col_sum(sums_ref[steps(i, SUBLANE), :]) for i in range(QUAD)], axis=0))
        for d, place in enumerate(DEVICES):
            for i in range(3):
                put_row(place, QUAD + i, 0, qb_ref[:, pl.ds((3 * d + i) * SHARD, SHARD)])
            for n in range(MLP_STEPS):
                put_row(place, QUAD + 3 + n * UNITS // SHARD, n * UNITS % SHARD, fb_ref[:, pl.ds(n * MLP_F + d * UNITS, UNITS)])

    def emit_vectors(n, exchange, c):
        for part, (rows, _) in enumerate(exchange.parts[:2]):
            out_vec_ref[rows, :] = exchange.held[3][part][0, :, :SHARD]
    advance((by_row,), t, first_chunks(QB_STEPS), lambda n, exchange, c: exchange.result(c, dw_ref))
    advance((by_vector,), t - VECTOR_STEP, first_chunks(1), emit_vectors)

    @pl.when(t < QB_STEPS)
    def _():
        by_row.put_local(t, dot(ht_ref[ALL], dqkv_ref[ALL]))

    @pl.when((t < BACK_STEP) & (t % 2 == 0))
    def _():
        acc[ALL] += dot_nt(wide_ref[ALL], w_ref[ALL])

    @pl.when(t == BACK_STEP)
    def _():
        for cp in loads:
            cp.wait()

    def back(r, n):
        hat, inv = norm_stats(xd[pl.ds(r, n), :].astype(F32))
        dn = acc[pl.ds(r, n), :]
        for i, v in enumerate((dn * hat, dn)):
            sums[steps(i, SUBLANE), :] += eights(v)
        acc[pl.ds(r, n), :] = joined(dr, r, n) + norm_back(dn, hat, inv, vec_ref[steps(LN1_GAIN, 1), :])

    @pl.when((t >= BACK_STEP) & (t <= VECTOR_STEP))
    def _():
        back_part(back, t - BACK_STEP, 5)

    @pl.when(t == VECTOR_STEP)
    def _():
        back(TAIL, IMAGES)
        share(VECTOR_ROWS - 2, jnp.concatenate([col_sum(sums[steps(i, SUBLANE), :]) for i in range(2)], axis=0))

    @pl.when(t == VECTOR_STEP + 1)
    def _():
        from_image_order(acc, dr)

    @pl.when(t == VECTOR_STEP + 2)
    def _():
        def narrow(r, n):
            xd[pl.ds(r, n), :] = joined(dr, r, n).astype(BF)
        row_tiles(narrow)
        store.start()

    @pl.when(t == QB_GRID - 1)
    def _():
        store.wait()


DEVICES = list(itertools.product(range(2), repeat=QUAD))


def qkvb_call(xim, dr, vec, sums, qb, fb, ht, dqkv, w):
    hbm = pl.BlockSpec(memory_space=pl.ANY)
    now = lambda i: jnp.minimum(i, QB_STEPS - 1)
    wide = lambda i: jnp.minimum(i // 2, QKV // QKV_N - 1)
    return pl.pallas_call(
        qkvb_kernel,
        grid=(QB_GRID,),
        in_specs=[hbm, hbm, *(whole(*v.shape) for v in (vec, sums, qb, fb)),
                  whole(WIDTH, TOKENS, pipeline_mode=pl.Buffered(1)), by_cols(TOKENS, QB_N, now), by_cols(TOKENS, QKV_N, wide), by_cols(WIDTH, QKV_N, wide)],
        out_specs=[hbm, by_cols(SHARD, QB_N, lambda i: jnp.clip(i - 1 - QUAD * QKV_SUM.stride, 0, QB_STEPS - 1)),
                   whole(VECTOR_ROWS, SHARD)],
        out_shape=[jax.ShapeDtypeStruct((TOKENS, WIDTH), BF), jax.ShapeDtypeStruct((SHARD, QKV), F32),
                   jax.ShapeDtypeStruct((VECTOR_ROWS, SHARD), F32)],
        scratch_shapes=[pltpu.VMEM((TOKENS, WIDTH), F32), pltpu.VMEM((LANES, TOKENS, LANE), F32), pltpu.VMEM((TOKENS, WIDTH), BF),
                        pltpu.VMEM((2 * SUBLANE, WIDTH), F32), pltpu.SemaphoreType.DMA((2,))]
                       + QKV_SUM.scratch() + VECTOR_SUM.scratch(),
        compiler_params=comm_params(2),
        cost_estimate=cost(QUAD * TOKENS * WIDTH * QKV, 80_000_000),
        name="qkvb",
    )(xim, dr, vec, sums, qb, fb, ht, dqkv, dqkv, w)


def solution(mesh):
    specs = (P("fsdp"),) * 14

    def device_step(resid_in, grad_out, ln1_gain, ln1_bias, qkv_weight, qkv_bias, out_weight, out_bias,
                    ln2_gain, ln2_bias, fc_weight, fc_bias, proj_weight, proj_bias):
        rows = jnp.concatenate([ln1_gain, ln1_bias, qkv_bias, out_bias, ln2_gain, ln2_bias, fc_bias, proj_bias]).reshape(-1, SHARD)
        rows = jnp.pad(rows, ((0, VECTOR_ROWS - len(rows)), (0, LANE - SHARD)))
        x = resid_in.swapaxes(0, 1).reshape(TOKENS, WIDTH)
        dy = grad_out.swapaxes(0, 1).reshape(TOKENS, WIDTH)
        xim, dyim, h, ht, rows, bq, bf, fc, wq, wo = open_call(x, dy, rows, fc_weight, qkv_weight, out_weight)
        wq, wo = wq.reshape(WIDTH, QKV), wo.reshape(WIDTH, WIDTH)
        qkv, wf = qkv_call(h, wq, bq, fc)
        o, r, n2, top, inv, wp = attn_call(qkv, xim, wo, rows, proj_weight)
        y, dr, dr16, dwf, dwp, dbf, small = mlp_call(r, n2, dyim, rows, wf.reshape(WIDTH, FFN), wp, bf)
        do, dwo, dwf, y, dwp = outb_call(dr16, o, wo, dwf, y, dwp)
        dqkv, dbq, dwo = attn_back_call(qkv, do, top, inv, dwo)
        dx, dwq, vec = qkvb_call(xim, dr, rows, small, dbq, dbf, ht, dqkv, wq)
        dg2, db2, dbp, dbo = vec[:4]
        dbq, dbf = vec[4:7].reshape(-1), vec[7:11].reshape(-1)
        dg1, db1 = vec[VECTOR_ROWS - 2:]
        unturn = lambda t: t.reshape(SEQ, IMAGES, WIDTH).swapaxes(0, 1)
        return (unturn(y), unturn(dx), dg1, db1, dwq, dbq, dwo, dbo, dg2, db2, dwf, dbf, dwp, dbp)

    return jax.shard_map(device_step, mesh=mesh, in_specs=specs, out_specs=specs, check_vma=False)
```

```python
import itertools
import math
import jax, jax.numpy as jnp
from jax import lax
from jax.experimental import pallas as pl
from jax.experimental.pallas import tpu as pltpu
from jax.sharding import PartitionSpec as P

BF, F32 = jnp.bfloat16, jnp.float32
IMAGES, SEQ, WIDTH, FFN, HEADS, HEAD = 8, 257, 1280, 5120, 16, 80
MAIN = SEQ - 1
TOKENS = IMAGES * SEQ
TAIL = IMAGES * MAIN
LN_EPS = 1e-5
VMEM_MAX = 67043328
LANE, SUBLANE, QUAD, QKV = 128, 8, 4, 3 * WIDTH
ALL = ...
TORUS = (2,) * QUAD
LANES = WIDTH // LANE
ROWS = 32


def dot(a, b):
    return jnp.dot(a, b, preferred_element_type=F32)


def dot_nt(a, b):
    return lax.dot_general(a, b, (((1,), (1,)), ((), ())), preferred_element_type=F32)


def dot_tn(a, b):
    return lax.dot_general(a, b, (((0,), (0,)), ((), ())), preferred_element_type=F32)


def col_sum(v):
    return jnp.sum(v, axis=0, keepdims=True)


def col_max(v):
    return jnp.max(v, axis=0, keepdims=True)


def row_sum(v):
    return jnp.sum(v, axis=-1, keepdims=True)


def row_mean(v):
    return row_sum(v) * (1.0 / WIDTH)


def clear(*refs):
    for ref in refs:
        ref[ALL] = jnp.zeros_like(ref)


def step_id():
    return pl.program_id(0)


def cost(flops, bytes_accessed, transcendentals=0):
    return pl.CostEstimate(flops=flops, bytes_accessed=bytes_accessed, transcendentals=transcendentals)


def eights(v):
    return jnp.sum(v.reshape(v.shape[0] // SUBLANE, SUBLANE, v.shape[1]), axis=0)


def whole(*shape, **kw):
    return pl.BlockSpec(shape, lambda *i: (0,) * len(shape), **kw)


def by_cols(rows, cols, at=lambda i: i):
    return pl.BlockSpec((rows, cols), lambda i: (0, at(i)))


def by_rows(rows, cols, at=lambda i: i):
    return pl.BlockSpec((rows, cols), lambda i: (at(i), 0))


def steps(first, wide):
    return slice(first * wide, (first + 1) * wide)


def regroup(rows, source, load, store):
    groups = LANE // UNITS
    lane = lax.broadcasted_iota(jnp.int32, (rows, LANE), 1) // UNITS
    for tile in range(FFN // LANE):
        out = None
        for i in range(groups):
            n = source(tile * groups + i)
            piece = load(n // groups)
            shift = (i - n) % groups
            if shift:
                piece = pltpu.roll(piece, shift * UNITS, 1)
            out = piece if out is None else jnp.where(lane == i, piece, out)
        store(tile, out)


def norm_stats(values):
    mean = row_mean(values)
    centered = values - mean
    inv = lax.rsqrt(row_mean(centered * centered) + LN_EPS)
    return centered * inv, inv


BLOCKS = [slice(i * 512, i * 512 + 512) for i in range(3)] + [slice(1536, TOKENS)]


def row_tiles(body, step=LANE):
    def loop(i, carry):
        body(pl.multiple_of(i * step, step), step)
        return carry
    lax.fori_loop(0, TAIL // step, loop, 0)
    body(TAIL, IMAGES)


def back_part(body, part, parts):
    tiles = -(-TAIL // ROWS // parts)

    def loop(i, carry):
        tile = part * tiles + i

        @pl.when(tile < TAIL // ROWS)
        def _():
            body(pl.multiple_of(tile * ROWS, ROWS), ROWS)
        return carry
    lax.fori_loop(0, tiles, loop, 0)


def to_image_order(wide, place, step=LANE):
    per = MAIN // step
    def loop(i, carry):
        first = (i % per) * (step * IMAGES) + i // per
        rows = [wide[c, pl.ds(first, step, stride=IMAGES), :] for c in range(LANES)]
        place(pl.multiple_of(i * step, step), step, jnp.concatenate(rows, axis=1))
        return carry
    lax.fori_loop(0, IMAGES * per, loop, 0)
    place(TAIL, IMAGES, joined(wide, TAIL, IMAGES))


def from_image_order(values, wide):
    def loop(i, carry):
        rows = values[pl.ds(pl.multiple_of(i * LANE, LANE), LANE), :]
        for c in range(LANES):
            wide[c, pl.ds((i % 2) * (LANE * IMAGES) + i // 2, LANE, stride=IMAGES), :] = rows[:, steps(c, LANE)]
        return carry
    lax.fori_loop(0, 2 * IMAGES, loop, 0)
    put(wide, TAIL, IMAGES, values[pl.ds(TAIL, IMAGES), :])


def joined(wide, r, n):
    return jnp.concatenate([wide[c, pl.ds(r, n), :] for c in range(LANES)], axis=1)


def put(wide, r, n, values):
    for c in range(LANES):
        wide[c, pl.ds(r, n), :] = values[:, steps(c, LANE)]


def norm_back(dn, hat, inv, gain):
    dhat = dn * gain
    m1 = row_mean(dhat)
    m2 = row_mean(dhat * hat)
    return inv * (dhat - m1 - hat * m2)


ORDERS = ((2, 1, 0), (1, 0, 2), (0, 2, 1))


def all_blocks(rows, cols):
    return jax.ShapeDtypeStruct((*TORUS, rows, cols), BF)


class Links:
    def find(self, send, recv):
        self.send, self.recv = send, recv
        me = lax.axis_index("fsdp")
        self.core = me % 2
        self.at = (me // SUBLANE, (me // QUAD) % 2, (me // 2) % 2)
        self.other_core = me + 1 - 2 * self.core
        self.other = [me + step - 2 * step * place for step, place in zip((SUBLANE, QUAD, 2), self.at)]
        return self

    def meet(self):
        barrier = pltpu.get_barrier_semaphore()
        devices = (self.other_core, *self.other)
        for device in devices:
            pl.semaphore_signal(barrier, inc=1, device_id=(device,), device_id_type=pl.DeviceIdType.MESH)
        pl.semaphore_wait(barrier, len(devices))

    def remote(self, src, dst, sem, device):
        return pltpu.make_async_remote_copy(src_ref=src, dst_ref=dst, send_sem=self.send.at[sem], recv_sem=self.recv.at[sem],
                                            device_id=(device,), device_id_type=pl.DeviceIdType.MESH)


class Gather(Links):
    COUNT = 2

    def __init__(self, rows, cols, cuts, by_rows):
        self.rows, self.cols, self.cuts, self.by_rows = rows, cols, cuts, by_rows
        self.parts = range(len(cuts) - 1)
        self.full_shape = all_blocks(rows, cols)

    def scratch(self):
        return [pltpu.SemaphoreType.DMA((SEMS,))] * self.COUNT

    def bind(self, own, full, sems):
        self.own, self.full = own, full
        return self.find(*sems)

    def region(self, part, known, arrived=False, half=None):
        done = ORDERS[part][:known]
        place = [slice(None) if a in done else self.at[a] for a in range(3)]
        if half is not None:
            place[done[0]] = half
        if arrived:
            place[done[-1]] = 1 - self.at[done[-1]]
        cut = pl.ds(self.cuts[part], self.cuts[part + 1] - self.cuts[part])
        return (*place, self.core, cut, slice(None)) if self.by_rows else (*place, self.core, slice(None), cut)

    def hop(self, stage, part, half):
        where = self.full.at[self.region(part, stage - 1, half=half)]
        source = self.own.at[self.region(part, 0)[-2:]] if stage == 1 else where
        return self.remote(source, where, self.sem(stage, part, half), self.other[ORDERS[part][stage - 1]])

    def forward(self, stage, part, half=None):
        if stage == 0:
            return self.remote(self.own, self.full.at[(*self.at, self.core)], 0, self.other_core)
        where = self.full.at[self.region(part, stage, True, half)]
        return self.remote(where, where, self.sem(stage + QUAD, part, half), self.other_core)

    def sem(self, row, part, half):
        return QUAD * (row + (half or 0)) + part

    def halves(self, stage):
        return (None,) if stage < 3 else range(2)

    def keep(self):
        return pltpu.make_async_copy(self.own, self.full.at[(*self.at, self.core)], self.send.at[1])

    def begin(self):
        for part in self.parts:
            self.hop(1, part, None).start()
        self.forward(0, 0).start()
        self.keep().start()

    def turn(self, stage):
        if stage == 1:
            self.keep().wait()
        for half in self.halves(stage):
            for part in self.parts:
                self.hop(stage, part, half).wait()
                if stage < 3:
                    for onward in self.halves(stage + 1):
                        self.hop(stage + 1, part, onward).start()
            for part in self.parts:
                self.forward(stage, part, half).start()

    def end(self):
        self.forward(0, 0).wait()
        for stage in range(1, QUAD):
            for half in self.halves(stage):
                for part in self.parts:
                    self.forward(stage, part, half).wait()


SEMS = 36


class Exchange(Links):
    def __init__(self, rows, cols, cuts, along, stride=1, spare=0):
        self.rows, self.cols, self.stride = rows, cols, stride
        self.slots, self.locals = 3 * stride + spare, 1 + stride
        self.blocks = (*TORUS, rows, cols)
        self.parts = [((slice(a, b), slice(None)) if along == 0 else (slice(None), slice(a, b))) for a, b in zip(cuts, cuts[1:])]
        self.shapes = [((b - a, cols) if along == 0 else (rows, b - a)) for a, b in zip(cuts, cuts[1:])]

    def scratch(self):
        out = [pltpu.VMEM((self.locals, *self.blocks), F32), pltpu.VMEM((self.slots, *TORUS[1:], self.rows, self.cols), F32)]
        for axes in (2, 1, 0):
            out += [pltpu.VMEM((self.slots, *TORUS[:axes], *shape), F32) for shape in self.shapes]
        return out + [pltpu.SemaphoreType.DMA((10, self.slots))] * 2

    COUNT = 13

    def bind(self, refs):
        self.local, self.pair, *rest = refs
        self.held = [None, *(rest[steps(i, 3)] for i in range(3))]
        return self.find(*rest[9:])

    def index(self, stage, part, side):
        order = ORDERS[part]
        left = [a for a in range(3) if a not in order[:stage - 1]]
        axis = order[stage - 1]
        where = self.at[axis] if side else 1 - self.at[axis]
        return tuple(where if a == axis else slice(None) for a in left)

    def copy(self, stage, part, c):
        slot = c % self.slots
        if stage == 0:
            return self.remote(self.local.at[c % self.locals, :, :, :, 1 - self.core], self.pair.at[slot], (0, slot), self.other_core)
        source = self.pair if stage == 1 else self.held[stage - 1][part]
        tail = self.parts[part] if stage == 1 else ()
        return self.remote(source.at[(slot, *self.index(stage, part, False), *tail)], self.held[stage][part].at[slot],
                           (3 * stage - 2 + part, slot), self.other[ORDERS[part][stage - 1]])

    def start(self, stage, c):
        for part in range(1 if stage == 0 else 3):
            self.copy(stage, part, c).start()

    def wait(self, stage, c):
        for part in range(1 if stage == 0 else 3):
            self.copy(stage, part, c).wait()

    def add(self, stage, c):
        slot = c % self.slots
        if stage == 0:
            for chip in itertools.product(range(2), repeat=3):
                self.pair[(slot, *chip)] += self.local[(c % self.locals, *chip, self.core)]
            return
        for part in range(3):
            source = self.pair if stage == 1 else self.held[stage - 1][part]
            tail = self.parts[part] if stage == 1 else ()
            for place in itertools.product(range(2), repeat=3 - stage):
                free = iter(place)
                kept = tuple(next(free) if isinstance(i, slice) else i for i in self.index(stage, part, True))
                self.held[stage][part][(slot, *place)] += source[(slot, *kept, *tail)]

    def result(self, c, out_ref):
        for part in range(3):
            out_ref[self.parts[part]] = self.held[3][part][c % self.slots]

    def put_local(self, c, values):
        self.local[c % self.locals] = values.reshape(self.blocks)


def comm_params(n):
    return pltpu.CompilerParams(dimension_semantics=("arbitrary",), vmem_limit_bytes=VMEM_MAX, collective_id=n, has_side_effects=True)


def advance(exchanges, t, exists, emit):
    for stage in (3, 2, 1, 0):
        c = t - 1 - (stage + 1) * exchanges[0].stride

        @pl.when(exists(c))
        def _():
            for n, exchange in enumerate(exchanges):
                exchange.wait(stage, c)
                exchange.add(stage, c)
                if stage < 3:
                    exchange.start(stage + 1, c)
                else:
                    emit(n, exchange, c)

    @pl.when(exists(t - 1))
    def _():
        for exchange in exchanges:
            exchange.start(0, t - 1)


def first_chunks(n):
    return lambda c: (c >= 0) & (c < n)


DRAIN = 5


PARTS = 16
SHARD = WIDTH // PARTS
VECTOR_ROWS = PARTS
LN1_GAIN, LN1_BIAS, QKV_BIAS, OUT_BIAS, LN2_GAIN, LN2_BIAS, FC_BIAS, PROJ_BIAS = 0, 1, 2, 5, 6, 7, 8, 12
MLP_F = MAIN
UNITS = MLP_F // PARTS
MLP_STEPS = FFN // MLP_F
WIDTH_CUTS = (0, 384, 896, WIDTH)
QKV_ALL = Gather(SHARD, QKV, (0, WIDTH, 2 * WIDTH, QKV), False)
OUT_ALL = Gather(SHARD, WIDTH, (0, 384, 768, WIDTH), False)
FC_HALF = FFN // 2
FC_ALL = [Gather(SHARD, FC_HALF, (0, 896, 1792, FC_HALF), False) for _ in range(2)]
PROJ_FIRST = 144
PROJ_ALL = [Gather(PROJ_FIRST, WIDTH, (0, 48, 96, PROJ_FIRST), True), Gather(FFN // PARTS - PROJ_FIRST, WIDTH, (0, 64, 128, 176), True)]
VECTOR_ALL = Gather(SHARD, LANE, (0, SHARD), True)


def open_kernel(x_hbm, dy_hbm, rows_ref, fc_ref, wq_ref, wo_ref, xim_hbm, dyim_hbm, h_hbm, ht_hbm, vec_ref, qb_ref, fb_ref, fc_own, wq_full, wo_full,
                x, dy, wide, h, ht, rows, vec_own, vec_full, wq_own, wo_own, sems, *comm):
    loads = [pltpu.make_async_copy(src, dst, sems.at[i]) for i, (src, dst) in enumerate(((x_hbm, x), (dy_hbm, dy)))]
    for cp in loads:
        cp.start()
    clear(rows)
    rows[:VECTOR_ROWS, :] = rows_ref[ALL]
    vec_own[ALL] = rows[ALL].T[:SHARD, :].astype(BF)
    wq_own[ALL] = wq_ref[ALL].astype(BF)
    wo_own[ALL] = wo_ref[ALL].astype(BF)
    pairs = [comm[steps(i, 2)] for i in range(3)]
    vectors = VECTOR_ALL.bind(vec_own, vec_full, pairs[0])
    weights = QKV_ALL.bind(wq_own, wq_full, pairs[1]), OUT_ALL.bind(wo_own, wo_full, pairs[2])
    gathers = (vectors, *weights)
    vectors.meet()
    for gather in gathers:
        gather.begin()
    for cp in loads:
        cp.wait()

    def reorder(tokens):
        def widen(r, n):
            put(wide, r, n, tokens[pl.ds(r, n), :].astype(F32))
        row_tiles(widen)

        def place(r, n, values):
            tokens[pl.ds(r, n), :] = values.astype(BF)
        to_image_order(wide, place)
    reorder(x)
    for gather in gathers:
        gather.turn(1)
    reorder(dy)
    for gather in gathers:
        gather.turn(2)
    vectors.turn(3)
    vectors.end()
    vec_ref[ALL] = vec_full[ALL].reshape(WIDTH, LANE).astype(F32).T[:VECTOR_ROWS, :]
    gain, bias = vec_ref[steps(LN1_GAIN, 1), :], vec_ref[steps(LN1_BIAS, 1), :]
    for d in range(PARTS):
        for i in range(3):
            qb_ref[:, steps(3 * d + i, SHARD)] = vec_ref[steps(QKV_BIAS + i, 1), steps(d, SHARD)]
        for n in range(MLP_STEPS):
            place = pl.ds(d * SHARD + n * UNITS % SHARD, UNITS)
            fb_ref[:, pl.ds(n * MLP_F + d * UNITS, UNITS)] = vec_ref[steps(FC_BIAS + n * UNITS // SHARD, 1), place]

    def norm(r, n):
        hat, _ = norm_stats(x[pl.ds(r, n), :].astype(F32))
        h[pl.ds(r, n), :] = (hat * gain + bias).astype(BF)
    row_tiles(norm, ROWS)
    for b in range(IMAGES):
        ht[:, steps(b, MAIN)] = h[steps(b, MAIN), :].T
    ht[:, TAIL:] = h[TAIL:, :].T
    stores = [pltpu.make_async_copy(src, dst, sems.at[i]) for i, (src, dst) in enumerate(((x, xim_hbm), (dy, dyim_hbm), (h, h_hbm), (ht, ht_hbm)))]
    for cp in stores:
        cp.start()
    def store_fc(tile, values):
        fc_own[:, steps(tile, LANE)] = values.astype(BF)
    regroup(SHARD, lambda n: n % PARTS * MLP_STEPS + n // PARTS, lambda tile: fc_ref[:, steps(tile, LANE)], store_fc)
    for gather in weights:
        gather.turn(3)
    for gather in weights:
        gather.end()
    for cp in stores:
        cp.wait()


def open_call(x, dy, rows, fc, wq, wo):
    hbm, vmem = pl.BlockSpec(memory_space=pl.ANY), pl.BlockSpec(memory_space=pltpu.VMEM)
    return pl.pallas_call(
        open_kernel,
        in_specs=[hbm, hbm, vmem, vmem, vmem, vmem],
        out_specs=[hbm, hbm, hbm, hbm, vmem, vmem, vmem, vmem, hbm, hbm],
        out_shape=[*[jax.ShapeDtypeStruct((TOKENS, WIDTH), BF)] * 3,
                   jax.ShapeDtypeStruct((WIDTH, TOKENS), BF), jax.ShapeDtypeStruct((VECTOR_ROWS, WIDTH), F32),
                   *(jax.ShapeDtypeStruct((1, n), F32) for n in (QKV, FFN)), jax.ShapeDtypeStruct(fc.shape, BF), QKV_ALL.full_shape, OUT_ALL.full_shape],
        scratch_shapes=[pltpu.VMEM((TOKENS, WIDTH), BF), pltpu.VMEM((TOKENS, WIDTH), BF), pltpu.VMEM((LANES, TOKENS, LANE), F32),
                        pltpu.VMEM((TOKENS, WIDTH), BF), pltpu.VMEM((WIDTH, TOKENS), BF), pltpu.VMEM((LANE, LANE), F32), pltpu.VMEM((SHARD, LANE), BF),
                        pltpu.VMEM(VECTOR_ALL.full_shape.shape, BF), pltpu.VMEM((SHARD, QKV), BF), pltpu.VMEM((SHARD, WIDTH), BF),
                        pltpu.SemaphoreType.DMA((QUAD,))] + VECTOR_ALL.scratch() + QKV_ALL.scratch() + OUT_ALL.scratch(),
        compiler_params=pltpu.CompilerParams(vmem_limit_bytes=VMEM_MAX, collective_id=3, has_side_effects=True),
        cost_estimate=cost(1_000_000_000, 60_000_000),
        name="open",
    )(x, dy, rows, fc, wq, wo)


QKV_N = 768


def qkv_kernel(h_ref, w_ref, wb_ref, own_ref, qkv_ref, full, *sems):
    t, last = step_id(), pl.num_programs(0) - 1
    gathers = []
    for i, kind in enumerate(FC_ALL):
        part = pl.ds(i * FC_HALF, FC_HALF)
        gathers.append(kind.bind(own_ref.at[:, part], full.at[(*EVERY, part)], sems[steps(i, 2)]))

    @pl.when(t == 0)
    def _():
        gathers[0].meet()
        for gather in gathers:
            gather.begin()

    @pl.when(t == 1)
    def _():
        for gather in gathers:
            gather.turn(1)
    for i in range(2):
        @pl.when(t == i + 2)
        def _():
            gathers[i].turn(2)
    for rows in BLOCKS:
        qkv_ref[rows, :] = (dot(h_ref[rows, :], w_ref[ALL]) + wb_ref[ALL]).astype(BF)

    @pl.when(t == last)
    def _():
        for gather in gathers:
            gather.turn(3)
        for gather in gathers:
            gather.end()


EVERY = [slice(None)] * 5


def qkv_call(h, w, wb, own):
    hbm = pl.BlockSpec(memory_space=pl.ANY)
    return pl.pallas_call(
        qkv_kernel,
        grid=(QKV // QKV_N,),
        in_specs=[whole(TOKENS, WIDTH, pipeline_mode=pl.Buffered(1)), by_cols(WIDTH, QKV_N), by_cols(1, QKV_N), whole(SHARD, FFN)],
        out_specs=[by_cols(TOKENS, QKV_N), hbm],
        out_shape=[jax.ShapeDtypeStruct((TOKENS, QKV), BF), all_blocks(SHARD, FFN)],
        scratch_shapes=FC_ALL[0].scratch() * 2,
        compiler_params=comm_params(QUAD),
        cost_estimate=cost(2 * TOKENS * WIDTH * QKV, 60_000_000),
        name="qkv",
    )(h, w, wb, own)


ROW_CUTS = (0, 24, 48, 80)
FC_SUM = Exchange(SHARD, MLP_F, ROW_CUTS, 0)
PROJ_SUM = Exchange(UNITS, WIDTH, WIDTH_CUTS, 1)
CDF_P = 0.33
CDF_C = (0.1326322871417956, 0.11939570820799192, 0.18103829560051796, -0.08904113226212501,
         0.33075919469138065, -0.22023738432274684, 0.0454530347223348)


def gelu_pair(u):
    bell = jnp.exp(u * u * -0.5)
    t = 1.0 / (1.0 + CDF_P * jnp.abs(u))
    poly = CDF_C[6]
    for c in CDF_C[5::-1]:
        poly = poly * t + c
    tail = poly * t * bell
    cdf = jnp.where(u < 0.0, tail, 1.0 - tail)
    return u * cdf, cdf + u * bell * ((2.0 * math.pi) ** -0.5)


def mlp_kernel(r_hbm, n_hbm, dy_hbm, vec_ref, fc_ref, proj_ref, fcb_ref,
               y_hbm, dr_hbm, dr16_hbm, dfc_ref, dproj_ref, dfcb_ref, small_ref,
               n2, dy, y_acc, dn_acc, g, du, ua, ub, da, db, sem, *comm):
    step = step_id()
    by_row, by_col = FC_SUM.bind(comm[:Exchange.COUNT]), PROJ_SUM.bind(comm[Exchange.COUNT:])

    @pl.when(step == 0)
    def _():
        loads = [pltpu.make_async_copy(n_hbm, n2, sem), pltpu.make_async_copy(dy_hbm, dy, sem)]
        for cp in loads:
            cp.start()
        by_row.meet()
        clear(small_ref, y_acc, dn_acc)
        for cp in loads:
            cp.wait()

    outs = (dfc_ref, dproj_ref)
    advance((by_row, by_col), step, first_chunks(MLP_STEPS), lambda n, exchange, c: exchange.result(c, outs[n]))

    @pl.when(step < MLP_STEPS)
    def _():
        fcb = fcb_ref[ALL]
        fc, proj = fc_ref[ALL], proj_ref[ALL].reshape(MLP_F, WIDTH)
        bias_sum = jnp.zeros((SUBLANE, MLP_F), F32)
        tiles = [(b * MAIN, MAIN) for b in range(IMAGES - 1)] + [((IMAGES - 1) * MAIN, MAIN + IMAGES)]
        pairs = ((ua, da), (ub, db))

        def products(k):
            r, n = tiles[k]
            u_s, d_s = pairs[k % 2]
            u_s[0:n, :] = dot(n2[r:r + n, :], fc)
            d_s[0:n, :] = dot_nt(dy[r:r + n, :], proj)

        def pointwise(k, total):
            r, n = tiles[k]
            u_s, d_s = pairs[k % 2]
            value, slope = gelu_pair(u_s[0:n, :] + fcb)
            g[r:r + n, :] = value.astype(BF)
            grad = d_s[0:n, :] * slope
            du[r:r + n, :] = grad.astype(BF)
            return total + eights(grad)

        products(0)
        for k in range(1, IMAGES):
            products(k)
            bias_sum = pointwise(k - 1, bias_sum)
        bias_sum = pointwise(IMAGES - 1, bias_sum)
        dfcb_ref[ALL] = col_sum(bias_sum)
        y_acc[ALL] += dot(g[ALL], proj)
        for c in range(LANES // 2):
            part = dot_nt(du[ALL], fc_ref[steps(c, MAIN), :])
            dn_acc[2 * c] += part[:, :LANE]
            dn_acc[2 * c + 1] += part[:, LANE:]
        by_col.put_local(step, dot_tn(g[ALL], dy[ALL]))
        by_row.put_local(step, dot_tn(n2[ALL], du[ALL]))

    after = step - MLP_STEPS
    r_copy = pltpu.make_async_copy(r_hbm, n2, sem)
    out_copies = [pltpu.make_async_copy(dn_acc, dr_hbm, sem), pltpu.make_async_copy(n2, dr16_hbm, sem)]
    y_copy = pltpu.make_async_copy(dy, y_hbm, sem)

    def back(r, n):
        wide_r = n2[pl.ds(r, n), :].astype(F32)
        hat, inv = norm_stats(wide_r)
        dn = joined(dn_acc, r, n)
        wide_dy = dy[pl.ds(r, n), :].astype(F32)
        dr = wide_dy + norm_back(dn, hat, inv, vec_ref[steps(LN2_GAIN, 1), :])
        put(dn_acc, r, n, dr)
        n2[pl.ds(r, n), :] = dr.astype(BF)
        y_acc[pl.ds(r, n), :] += wide_r + vec_ref[steps(PROJ_BIAS, 1), :]
        for i, v in enumerate((dn * hat, dn, wide_dy, dr)):
            small_ref[steps(i, SUBLANE), :] += eights(v)

    @pl.when(after == 0)
    def _():
        r_copy.start()
        r_copy.wait()
        back(TAIL, IMAGES)

    @pl.when((after >= 0) & (after < 3))
    def _():
        back_part(back, after, 3)

    @pl.when(after == 2)
    def _():
        for cp in out_copies:
            cp.start()

    @pl.when(after == 3)
    def _():
        for cp in out_copies:
            cp.wait()
        from_image_order(y_acc, dn_acc)

        def narrow(r, n):
            dy[pl.ds(r, n), :] = joined(dn_acc, r, n).astype(BF)
        row_tiles(narrow)
        y_copy.start()

    @pl.when(after == QUAD)
    def _():
        y_copy.wait()


def mlp_call(r, n2, dy, vec, fc, proj, fcb):
    hbm = pl.BlockSpec(memory_space=pl.ANY)
    now = lambda i: jnp.minimum(i, MLP_STEPS - 1)
    done = lambda i: jnp.maximum(i - DRAIN, 0)
    return pl.pallas_call(
        mlp_kernel,
        grid=(MLP_STEPS + DRAIN,),
        in_specs=[hbm, hbm, hbm, whole(*vec.shape), by_cols(WIDTH, MLP_F, now),
                  pl.BlockSpec((PARTS, None, UNITS, WIDTH), lambda i: (0, now(i), 0, 0)),
                  by_cols(1, MLP_F, now)],
        out_specs=[hbm, hbm, hbm, by_cols(SHARD, MLP_F, done),
                   by_rows(UNITS, WIDTH, done),
                   by_cols(1, MLP_F, now), whole(32, WIDTH)],
        out_shape=[jax.ShapeDtypeStruct((TOKENS, WIDTH), BF), jax.ShapeDtypeStruct((LANES, TOKENS, LANE), F32),
                   jax.ShapeDtypeStruct((TOKENS, WIDTH), BF), jax.ShapeDtypeStruct((SHARD, FFN), F32),
                   jax.ShapeDtypeStruct((FFN // PARTS, WIDTH), F32),
                   jax.ShapeDtypeStruct((1, FFN), F32), jax.ShapeDtypeStruct((32, WIDTH), F32)],
        scratch_shapes=[pltpu.VMEM((TOKENS, WIDTH), BF), pltpu.VMEM((TOKENS, WIDTH), BF),
                        pltpu.VMEM((TOKENS, WIDTH), F32), pltpu.VMEM((LANES, TOKENS, LANE), F32),
                        pltpu.VMEM((TOKENS, MLP_F), BF), pltpu.VMEM((TOKENS, MLP_F), BF)]
                       + [pltpu.VMEM((MAIN + IMAGES, MLP_F), F32)] * QUAD + [pltpu.SemaphoreType.DMA]
                       + FC_SUM.scratch() + PROJ_SUM.scratch(),
        compiler_params=comm_params(0),
        cost_estimate=cost(12 * TOKENS * WIDTH * FFN, 150_000_000, TOKENS * FFN),
        name="mlp",
    )(r, n2, dy, vec, fc, proj.reshape(PARTS, MLP_STEPS, UNITS, WIDTH), fcb)


SCALE = HEAD ** -0.5
ATTN_COST = cost(40_000_000_000, 50_000_000, 8_400_000)


def window(h):
    first = min(HEAD * h // LANE * LANE, WIDTH - MAIN)
    wide = LANE if HEAD * h + HEAD <= first + LANE else MAIN
    return first, wide, HEAD * h - first


def lane_mask(h):
    first, wide, off = window(h)
    lane = lax.broadcasted_iota(jnp.int32, (MAIN, wide), 1)
    return (lane >= off) & (lane < off + HEAD)


def thirds(ref, rows=slice(None)):
    return [ref[rows, steps(i, WIDTH)] for i in range(3)]


def head_rows():
    lane = lax.broadcasted_iota(jnp.int32, (HEADS, WIDTH), 1)
    row = lax.broadcasted_iota(jnp.int32, (HEADS, WIDTH), 0)
    return (lane // HEAD == row).astype(F32)


def tail_softmax(s, s_self):
    m = jnp.maximum(jnp.max(s, axis=1, keepdims=True), s_self)
    e = jnp.exp((s - m) * SCALE)
    e_self = jnp.exp((s_self - m) * SCALE)
    inv = 1.0 / (row_sum(e) + e_self)
    return e * inv, e_self * inv


def attn_kernel(qkv_ref, qkvt_ref, x_ref, xt_ref, w_ref, vec_ref, proj_ref, o_hbm, r_hbm, n_hbm,
                max_ref, inv_ref, full,
                tails, o_tail, o_t, ptail, o_buf, r_buf, n_buf, sa, sb, sems, own, *comm):
    b, last = step_id(), pl.num_programs(0) - 1
    slot = b % 2
    gathers = []
    for i, kind in enumerate(PROJ_ALL):
        part = pl.ds(i * PROJ_FIRST, kind.rows)
        gathers.append(kind.bind(own.at[part], full.at[(*EVERY[1:], part)], comm[steps(i, 2)]))

    @pl.when(b == 0)
    def _():
        tails[ALL] = qkvt_ref[ALL].astype(F32)
        own[ALL] = proj_ref[ALL].astype(BF)
        gathers[0].meet()
        for gather in gathers:
            gather.begin()

    for turn, (stage, i) in enumerate(itertools.product((1, 2, 3), range(2))):
        @pl.when(b == turn + 1 + stage // 3)
        def _():
            gathers[i].turn(stage)

    heads = head_rows()
    q_t, k_t, v_t = (heads * z for z in thirds(tails, pl.ds(b, 1)))
    q, k, v = thirds(qkv_ref)

    p, p_self = tail_softmax(dot_nt(q_t.astype(BF), k), row_sum(q_t * k_t))
    mixed = dot(p.astype(BF), v) * heads + p_self.astype(BF).astype(F32) * v_t
    o_tail[pl.ds(b, 1), :] = col_sum(mixed)

    s_tail = dot_nt(k_t.astype(BF), q)
    v_turned = v.T
    scores = sa, sb

    def next_scores(h):
        first, wide, _ = window(h)
        q_h = jnp.where(lane_mask(h), qkv_ref[:, pl.ds(first, wide)], jnp.zeros((), BF))
        scores[h % 2][ALL] = dot_nt(qkv_ref[:, pl.ds(WIDTH + first, wide)], q_h)
    next_scores(0)
    for h in range(HEADS):
        if h + 1 < HEADS:
            next_scores(h + 1)
        s, mine = scores[h % 2], steps(h, 1)
        top = jnp.maximum(col_max(s[ALL]), s_tail[mine, :])
        e = jnp.exp((s[ALL] - top) * SCALE)
        e_tail = jnp.exp((s_tail[mine, :] - top) * SCALE)
        inv = 1.0 / (col_sum(e) + e_tail)
        max_ref[0, mine, :] = top
        inv_ref[0, mine, :] = inv
        ptail[mine, :] = e_tail * inv
        o_t[steps(h, HEAD), :] = dot(v_turned[steps(h, HEAD), :], (e * inv).astype(BF))

    outs = (o_buf, o_hbm), (r_buf, r_hbm), (n_buf, n_hbm)
    out_bias, gain, bias = (vec_ref[steps(i, 1), :] for i in (OUT_BIAS, LN2_GAIN, LN2_BIAS))

    def write(slot, rows, o, x):
        o_buf[slot, rows, :] = o
        r = (x.astype(F32) + dot(o, w_ref[ALL]) + out_bias).astype(BF)
        r_buf[slot, rows, :] = r
        hat, _ = norm_stats(r.astype(F32))
        n_buf[slot, rows, :] = (hat * gain + bias).astype(BF)

    @pl.when(b >= 2)
    def _():
        for n, (buf, hbm) in enumerate(outs):
            out_copy(buf, hbm, slot, b - 2, sems, n).wait()

    o = (o_t[ALL].T + dot_tn(ptail[ALL].astype(BF), v_t.astype(BF))).astype(BF)
    write(slot, slice(None), o, x_ref[ALL])
    for n, (buf, hbm) in enumerate(outs):
        out_copy(buf, hbm, slot, b, sems, n).start()

    @pl.when(b == last)
    def _():
        for n, (buf, hbm) in enumerate(outs):
            out_copy(buf, hbm, 1 - slot, b - 1, sems, n).wait()
        write(1 - slot, slice(IMAGES), o_tail[ALL].astype(BF), xt_ref[ALL])
        copies = [pltpu.make_async_copy(buf.at[1 - slot, pl.ds(0, IMAGES)], hbm.at[pl.ds(TAIL, IMAGES)], sems.at[n, 1 - slot])
                  for n, (buf, hbm) in enumerate(outs)]
        for cp in copies:
            cp.start()
        for cp in copies:
            cp.wait()
        for n, (buf, hbm) in enumerate(outs):
            out_copy(buf, hbm, slot, b, sems, n).wait()
        for gather in gathers:
            gather.end()


def out_copy(buf, hbm, slot, b, sems, n):
    return pltpu.make_async_copy(buf.at[slot], hbm.at[pl.ds(pl.multiple_of(b * MAIN, MAIN), MAIN)], sems.at[n, slot])


def attn_call(qkv, xim, w, vec, proj):
    hbm = pl.BlockSpec(memory_space=pl.ANY)
    main = lambda n: by_rows(MAIN, n)
    tail = lambda n: by_rows(IMAGES, n, lambda i: TAIL // IMAGES)
    stat = pl.BlockSpec((1, HEADS, MAIN), lambda i: (i, 0, 0))
    return pl.pallas_call(
        attn_kernel,
        grid=(IMAGES,),
        in_specs=[main(QKV), tail(QKV), main(WIDTH), tail(WIDTH),
                  whole(WIDTH, WIDTH), whole(*vec.shape), whole(*proj.shape)],
        out_specs=[hbm, hbm, hbm, stat, stat, hbm],
        out_shape=[*[jax.ShapeDtypeStruct((TOKENS, WIDTH), BF)] * 3,
                   jax.ShapeDtypeStruct((IMAGES, HEADS, MAIN), F32), jax.ShapeDtypeStruct((IMAGES, HEADS, MAIN), F32),
                   all_blocks(*proj.shape)],
        scratch_shapes=[pltpu.VMEM((IMAGES, QKV), F32), pltpu.VMEM((IMAGES, WIDTH), F32),
                        pltpu.VMEM((WIDTH, MAIN), F32), pltpu.VMEM((HEADS, MAIN), F32),
                        *[pltpu.VMEM((2, MAIN, WIDTH), BF)] * 3, *[pltpu.VMEM((MAIN, MAIN), F32)] * 2, pltpu.SemaphoreType.DMA((3, 2)),
                        pltpu.VMEM(proj.shape, BF)] + PROJ_ALL[0].scratch() * 2,
        compiler_params=comm_params(5),
        cost_estimate=ATTN_COST,
        name="attn",
    )(qkv, qkv, xim, xim, w, vec, proj)


def outb_kernel(dr_ref, o_ref, w_ref, dfc_ref, y_in, dproj_in, do_ref, dw_ref, dfc_out, y_out, dproj_out, y, dproj, sems):
    c, last = step_id(), pl.num_programs(0) - 1
    loads = [pltpu.make_async_copy(src, dst, sems.at[i]) for i, (src, dst) in enumerate(((y_in, y), (dproj_in, dproj)))]
    stores = [pltpu.make_async_copy(src, dst, sems.at[i]) for i, (src, dst) in enumerate(((y, y_out), (dproj, dproj_out)))]

    @pl.when(c == 0)
    def _():
        for cp in loads:
            cp.start()

    @pl.when(c == 1)
    def _():
        for cp in loads:
            cp.wait()
        for cp in stores:
            cp.start()

        def store_fc(tile, values):
            dfc_out[:, steps(tile, LANE)] = values
        regroup(SHARD, lambda n: n % MLP_STEPS * PARTS + n // MLP_STEPS, lambda tile: dfc_ref[:, steps(tile, LANE)], store_fc)
    do_ref[ALL] = dot_nt(dr_ref[ALL], w_ref[ALL]).astype(BF)
    dw_ref[ALL] = dot_tn(o_ref[ALL], dr_ref[:, pl.ds(pl.multiple_of(c * MAIN, MAIN), MAIN)])

    @pl.when(c == last)
    def _():
        for cp in stores:
            cp.wait()


def outb_call(dr, o, w, dfc, y, dproj):
    full, hbm = whole(TOKENS, WIDTH), pl.BlockSpec(memory_space=pl.ANY)
    like = lambda v: jax.ShapeDtypeStruct(v.shape, v.dtype)
    return pl.pallas_call(
        outb_kernel,
        grid=(WIDTH // MAIN,),
        in_specs=[full, full, by_rows(MAIN, WIDTH), whole(*dfc.shape), hbm, hbm],
        out_specs=[by_cols(TOKENS, MAIN), by_cols(WIDTH, MAIN), whole(*dfc.shape), hbm, hbm],
        out_shape=[like(dr), jax.ShapeDtypeStruct((WIDTH, WIDTH), F32), like(dfc), like(y), like(dproj)],
        scratch_shapes=[pltpu.VMEM(y.shape, BF), pltpu.VMEM(dproj.shape, F32), pltpu.SemaphoreType.DMA((2,))],
        compiler_params=pltpu.CompilerParams(dimension_semantics=("arbitrary",), vmem_limit_bytes=VMEM_MAX),
        cost_estimate=cost(QUAD * TOKENS * WIDTH * WIDTH, 50_000_000),
        name="outb",
    )(dr, o, w, dfc, y, dproj)


def attn_back_kernel(qkv_ref, qkvt_ref, do_ref, dot_ref, max_ref, inv_ref, dw_ref, dqkv_hbm, dwb_ref, dwout_ref,
                     tails, do_tails, grad_tails, dq_t, dk, dv, ds_tail, sa, da, sb, db, buf, sems, *comm):
    b = step_id()
    by_row = OUT_SUM.bind(comm)

    @pl.when(b == 0)
    def _():
        by_row.meet()

    @pl.when(b < OUT_STEPS)
    def _():
        by_row.put_local(b, dw_ref[ALL])
    advance((by_row,), b + 1, first_chunks(OUT_STEPS), lambda n, exchange, c: exchange.result(c, dwout_ref))

    @pl.when(b < IMAGES)
    def _():
        image_back(b, qkv_ref, qkvt_ref, do_ref, dot_ref, max_ref, inv_ref, dqkv_hbm, dwb_ref,
                   tails, do_tails, grad_tails, dq_t, dk, dv, ds_tail, ((sa, da), (sb, db)), buf, sems)


OUT_N = MAIN
OUT_STEPS = WIDTH // OUT_N
OUT_SUM = Exchange(SHARD, OUT_N, ROW_CUTS, 0)


def image_back(b, qkv_ref, qkvt_ref, do_ref, dot_ref, max_ref, inv_ref, dqkv_hbm, dwb_ref,
               tails, do_tails, grad_tails, dq_t, dk, dv, ds_tail, ahead, buf, sems):
    last = IMAGES - 1
    slot = b % 2

    @pl.when(b == 0)
    def _():
        tails[ALL] = qkvt_ref[ALL].astype(F32)
        do_tails[ALL] = dot_ref[ALL].astype(F32)
        clear(dwb_ref)

    heads = head_rows()
    q_t, k_t, v_t = (heads * z for z in thirds(tails, pl.ds(b, 1)))
    do_t = heads * do_tails[pl.ds(b, 1), :]
    q, k, v = thirds(qkv_ref)
    do = do_ref[ALL]
    q_t16, k_t16, v_t16, do_t16 = (z.astype(BF) for z in (q_t, k_t, v_t, do_t))

    p, p_self = tail_softmax(dot_nt(q_t16, k), row_sum(q_t * k_t))
    dp, dp_self = dot_nt(do_t16, v), row_sum(do_t * v_t)
    inner = row_sum(p * dp) + p_self * dp_self
    ds16 = (p * (dp - inner) * SCALE).astype(BF)
    ds_self = (p_self * (dp_self - inner) * SCALE).astype(BF).astype(F32)
    grad_q = col_sum(dot(ds16, k) * heads + ds_self * k_t)
    grad_k = ds_self * q_t
    grad_v = p_self.astype(BF).astype(F32) * do_t
    dk[ALL] = dot_tn(ds16, q_t16)
    dv[ALL] = dot_tn(p.astype(BF), do_t16)

    p_tail = jnp.exp((dot_nt(k_t16, q) - max_ref[0]) * SCALE) * inv_ref[0]
    dp_tail = dot_nt(v_t16, do)
    inner_tail = p_tail * dp_tail

    k_turned = k.T

    def masked(h):
        first, wide, _ = window(h)
        here, mask = pl.ds(first, wide), lane_mask(h)
        return here, jnp.where(mask, qkv_ref[:, here], jnp.zeros((), BF)), jnp.where(mask, do_ref[:, here], jnp.zeros((), BF))

    def next_products(h):
        first, wide, _ = window(h)
        _, q_h, do_h = masked(h)
        ahead[h % 2][0][ALL] = dot_nt(qkv_ref[:, pl.ds(WIDTH + first, wide)], q_h)
        ahead[h % 2][1][ALL] = dot_nt(qkv_ref[:, pl.ds(2 * WIDTH + first, wide)], do_h)
    next_products(0)
    for h in range(HEADS):
        if h + 1 < HEADS:
            next_products(h + 1)
        here, q_h, do_h = masked(h)
        mine = steps(h, 1)
        s, dp = (ref[ALL] for ref in ahead[h % 2])
        p = jnp.exp((s - max_ref[0, mine, :]) * SCALE) * inv_ref[0, mine, :]
        inner = col_sum(p * dp) + inner_tail[mine, :]
        ds = (p * (dp - inner) * SCALE).astype(BF)
        dv[:, here] += dot(p.astype(BF), do_h)
        dk[:, here] += dot(ds, q_h)
        dq_t[steps(h, HEAD), :] = dot(k_turned[steps(h, HEAD), :], ds)
        ds_tail[mine, :] = p_tail[mine, :] * (dp_tail[mine, :] - inner) * SCALE

    ds_tail16 = ds_tail[ALL].astype(BF)
    grad_k = col_sum(grad_k + dot(ds_tail16, q) * heads)
    grad_v = col_sum(grad_v + dot(p_tail.astype(BF), do) * heads)

    @pl.when(b >= 2)
    def _():
        out_copy(buf, dqkv_hbm, slot, b - 2, sems, 0).wait()

    grad = dq_t[ALL].T + dot_tn(ds_tail16, k_t16)
    for n, (main, tail) in enumerate(((grad, grad_q), (dk[ALL], grad_k), (dv[ALL], grad_v))):
        here = steps(n, WIDTH)
        buf[slot, :, here] = main.astype(BF)
        grad_tails[pl.ds(b, 1), here] = tail
        dwb_ref[:, here] += col_sum(main) + tail
    out_copy(buf, dqkv_hbm, slot, b, sems, 0).start()

    @pl.when(b == last)
    def _():
        out_copy(buf, dqkv_hbm, 1 - slot, b - 1, sems, 0).wait()
        buf[1 - slot, 0:IMAGES, :] = grad_tails[ALL].astype(BF)
        cp = pltpu.make_async_copy(buf.at[1 - slot, pl.ds(0, IMAGES)], dqkv_hbm.at[pl.ds(TAIL, IMAGES)], sems.at[0, 1 - slot])
        cp.start()
        cp.wait()
        out_copy(buf, dqkv_hbm, slot, b, sems, 0).wait()


def attn_back_call(qkv, do, top, inv, dw):
    hbm = pl.BlockSpec(memory_space=pl.ANY)
    image = lambda i: jnp.minimum(i, IMAGES - 1)
    main = lambda n: by_rows(MAIN, n, image)
    tail = lambda n: by_rows(IMAGES, n, lambda i: TAIL // IMAGES)
    stat = pl.BlockSpec((1, HEADS, MAIN), lambda i: (image(i), 0, 0))
    return pl.pallas_call(
        attn_back_kernel,
        grid=(OUT_STEPS + DRAIN - 1,),
        in_specs=[main(QKV), tail(QKV), main(WIDTH), tail(WIDTH), stat, stat,
                  by_cols(WIDTH, OUT_N, lambda i: jnp.minimum(i, OUT_STEPS - 1))],
        out_specs=[hbm, whole(1, QKV), by_cols(SHARD, OUT_N, lambda i: jnp.clip(i + 1 - DRAIN, 0, OUT_STEPS - 1))],
        out_shape=[jax.ShapeDtypeStruct((TOKENS, QKV), BF), jax.ShapeDtypeStruct((1, QKV), F32),
                   jax.ShapeDtypeStruct((SHARD, WIDTH), F32)],
        scratch_shapes=[pltpu.VMEM((IMAGES, QKV), F32), pltpu.VMEM((IMAGES, WIDTH), F32),
                        pltpu.VMEM((IMAGES, QKV), F32), pltpu.VMEM((WIDTH, MAIN), F32),
                        pltpu.VMEM((MAIN, WIDTH), F32), pltpu.VMEM((MAIN, WIDTH), F32), pltpu.VMEM((HEADS, MAIN), F32),
                        *[pltpu.VMEM((MAIN, MAIN), F32)] * QUAD, pltpu.VMEM((2, MAIN, QKV), BF), pltpu.SemaphoreType.DMA((1, 2))] + OUT_SUM.scratch(),
        compiler_params=comm_params(1),
        cost_estimate=ATTN_COST,
        name="attn_back",
    )(qkv, qkv, do, do, top, inv, dw)


QB_N = MAIN
QB_STEPS = QKV // QB_N
QKV_SUM = Exchange(SHARD, QB_N, ROW_CUTS, 0, 2)
VECTOR_SUM = Exchange(3 * SUBLANE, LANE, (0, SUBLANE, 2 * SUBLANE, 3 * SUBLANE), 0)
VECTOR_STEP = QB_STEPS + 2
QB_GRID = QB_STEPS + 1 + QUAD * QKV_SUM.stride


def qkvb_kernel(xim_hbm, dr_hbm, vec_ref, sums_ref, qb_ref, fb_ref, ht_ref, dqkv_ref, w_ref, dx_hbm, dw_ref, out_vec_ref,
                acc, dr, xd, sums, sems, *comm):
    t = step_id()
    by_row, by_vector = QKV_SUM.bind(comm[:Exchange.COUNT]), VECTOR_SUM.bind(comm[Exchange.COUNT:])
    loads = [pltpu.make_async_copy(dr_hbm, dr, sems.at[0]), pltpu.make_async_copy(xim_hbm, xd, sems.at[1])]
    store = pltpu.make_async_copy(xd, dx_hbm, sems.at[1])

    def put_row(place, row, lane, values):
        by_vector.local[(0, *place, pl.ds(row, len(values)), pl.ds(lane, values.shape[1]))] = values

    def share(row, values):
        for d, place in enumerate(DEVICES):
            put_row(place, row, 0, values[:, steps(d, SHARD)])

    @pl.when(t == 0)
    def _():
        by_row.meet()
        for cp in loads:
            cp.start()
        clear(acc, sums)
        by_vector.local[0] = jnp.zeros(by_vector.blocks, F32)
        share(0, jnp.concatenate([col_sum(sums_ref[steps(i, SUBLANE), :]) for i in range(QUAD)], axis=0))
        for d, place in enumerate(DEVICES):
            for i in range(3):
                put_row(place, QUAD + i, 0, qb_ref[:, pl.ds((3 * d + i) * SHARD, SHARD)])
            for n in range(MLP_STEPS):
                put_row(place, QUAD + 3 + n * UNITS // SHARD, n * UNITS % SHARD, fb_ref[:, pl.ds(n * MLP_F + d * UNITS, UNITS)])

    def emit_vectors(n, exchange, c):
        for part, (rows, _) in enumerate(exchange.parts[:2]):
            out_vec_ref[rows, :] = exchange.held[3][part][0, :, :SHARD]
    advance((by_row,), t, first_chunks(QB_STEPS), lambda n, exchange, c: exchange.result(c, dw_ref))
    advance((by_vector,), t - VECTOR_STEP, first_chunks(1), emit_vectors)

    @pl.when(t < QB_STEPS)
    def _():
        by_row.put_local(t, dot(ht_ref[ALL], dqkv_ref[ALL]))
        acc[ALL] += dot_nt(dqkv_ref[ALL], w_ref[ALL])

    @pl.when(t == QB_STEPS)
    def _():
        for cp in loads:
            cp.wait()

    def back(r, n):
        hat, inv = norm_stats(xd[pl.ds(r, n), :].astype(F32))
        dn = acc[pl.ds(r, n), :]
        for i, v in enumerate((dn * hat, dn)):
            sums[steps(i, SUBLANE), :] += eights(v)
        acc[pl.ds(r, n), :] = joined(dr, r, n) + norm_back(dn, hat, inv, vec_ref[steps(LN1_GAIN, 1), :])

    @pl.when((t >= QB_STEPS) & (t <= VECTOR_STEP))
    def _():
        back_part(back, t - QB_STEPS, 3)

    @pl.when(t == VECTOR_STEP)
    def _():
        back(TAIL, IMAGES)
        share(VECTOR_ROWS - 2, jnp.concatenate([col_sum(sums[steps(i, SUBLANE), :]) for i in range(2)], axis=0))

    @pl.when(t == VECTOR_STEP + 1)
    def _():
        from_image_order(acc, dr)

    @pl.when(t == VECTOR_STEP + 2)
    def _():
        def narrow(r, n):
            xd[pl.ds(r, n), :] = joined(dr, r, n).astype(BF)
        row_tiles(narrow)
        store.start()

    @pl.when(t == QB_GRID - 1)
    def _():
        store.wait()


DEVICES = list(itertools.product(range(2), repeat=QUAD))


def qkvb_call(xim, dr, vec, sums, qb, fb, ht, dqkv, w):
    hbm = pl.BlockSpec(memory_space=pl.ANY)
    now = lambda i: jnp.minimum(i, QB_STEPS - 1)
    return pl.pallas_call(
        qkvb_kernel,
        grid=(QB_GRID,),
        in_specs=[hbm, hbm, *(whole(*v.shape) for v in (vec, sums, qb, fb)),
                  whole(WIDTH, TOKENS, pipeline_mode=pl.Buffered(1)), by_cols(TOKENS, QB_N, now), by_cols(WIDTH, QB_N, now)],
        out_specs=[hbm, by_cols(SHARD, QB_N, lambda i: jnp.clip(i - 1 - QUAD * QKV_SUM.stride, 0, QB_STEPS - 1)),
                   whole(VECTOR_ROWS, SHARD)],
        out_shape=[jax.ShapeDtypeStruct((TOKENS, WIDTH), BF), jax.ShapeDtypeStruct((SHARD, QKV), F32),
                   jax.ShapeDtypeStruct((VECTOR_ROWS, SHARD), F32)],
        scratch_shapes=[pltpu.VMEM((TOKENS, WIDTH), F32), pltpu.VMEM((LANES, TOKENS, LANE), F32), pltpu.VMEM((TOKENS, WIDTH), BF),
                        pltpu.VMEM((2 * SUBLANE, WIDTH), F32), pltpu.SemaphoreType.DMA((2,))]
                       + QKV_SUM.scratch() + VECTOR_SUM.scratch(),
        compiler_params=comm_params(2),
        cost_estimate=cost(QUAD * TOKENS * WIDTH * QKV, 80_000_000),
        name="qkvb",
    )(xim, dr, vec, sums, qb, fb, ht, dqkv, w)


def solution(mesh):
    specs = (P("fsdp"),) * 14

    def device_step(resid_in, grad_out, ln1_gain, ln1_bias, qkv_weight, qkv_bias, out_weight, out_bias,
                    ln2_gain, ln2_bias, fc_weight, fc_bias, proj_weight, proj_bias):
        rows = jnp.concatenate([ln1_gain, ln1_bias, qkv_bias, out_bias, ln2_gain, ln2_bias, fc_bias, proj_bias]).reshape(-1, SHARD)
        rows = jnp.pad(rows, ((0, VECTOR_ROWS - len(rows)), (0, LANE - SHARD)))
        x = resid_in.swapaxes(0, 1).reshape(TOKENS, WIDTH)
        dy = grad_out.swapaxes(0, 1).reshape(TOKENS, WIDTH)
        xim, dyim, h, ht, rows, bq, bf, fc, wq, wo = open_call(x, dy, rows, fc_weight, qkv_weight, out_weight)
        wq, wo = wq.reshape(WIDTH, QKV), wo.reshape(WIDTH, WIDTH)
        qkv, wf = qkv_call(h, wq, bq, fc)
        o, r, n2, top, inv, wp = attn_call(qkv, xim, wo, rows, proj_weight)
        y, dr, dr16, dwf, dwp, dbf, small = mlp_call(r, n2, dyim, rows, wf.reshape(WIDTH, FFN), wp, bf)
        do, dwo, dwf, y, dwp = outb_call(dr16, o, wo, dwf, y, dwp)
        dqkv, dbq, dwo = attn_back_call(qkv, do, top, inv, dwo)
        dx, dwq, vec = qkvb_call(xim, dr, rows, small, dbq, dbf, ht, dqkv, wq)
        dg2, db2, dbp, dbo = vec[:4]
        dbq, dbf = vec[4:7].reshape(-1), vec[7:11].reshape(-1)
        dg1, db1 = vec[VECTOR_ROWS - 2:]
        unturn = lambda t: t.reshape(SEQ, IMAGES, WIDTH).swapaxes(0, 1)
        return (unturn(y), unturn(dx), dg1, db1, dwq, dbq, dwo, dbo, dg2, db2, dwf, dbf, dwp, dbp)

    return jax.shard_map(device_step, mesh=mesh, in_specs=specs, out_specs=specs, check_vma=False)
```

```python
import itertools
import math
import jax, jax.numpy as jnp
from jax import lax
from jax.experimental import pallas as pl
from jax.experimental.pallas import tpu as pltpu
from jax.sharding import PartitionSpec as P

BF, F32 = jnp.bfloat16, jnp.float32
IMAGES, SEQ, WIDTH, FFN, HEADS, HEAD = 8, 257, 1280, 5120, 16, 80
MAIN = SEQ - 1
TOKENS = IMAGES * SEQ
TAIL = IMAGES * MAIN
LN_EPS = 1e-5
LOG2E = math.log2(math.e)
VMEM_MAX = 67043328
LANE, SUBLANE, QUAD, QKV = 128, 8, 4, 3 * WIDTH
ALL = ...
TORUS = (2,) * QUAD
LANES = WIDTH // LANE
ROWS = 32


def dot(a, b):
    return jnp.dot(a, b, preferred_element_type=F32)


def dot_nt(a, b):
    return lax.dot_general(a, b, (((1,), (1,)), ((), ())), preferred_element_type=F32)


def dot_tn(a, b):
    return lax.dot_general(a, b, (((0,), (0,)), ((), ())), preferred_element_type=F32)


def col_sum(v):
    return jnp.sum(v, axis=0, keepdims=True)


def col_max(v):
    return jnp.max(v, axis=0, keepdims=True)


def row_sum(v):
    return jnp.sum(v, axis=-1, keepdims=True)


def row_mean(v):
    return row_sum(v) * (1.0 / WIDTH)


def clear(*refs):
    for ref in refs:
        ref[ALL] = jnp.zeros_like(ref)


def step_id():
    return pl.program_id(0)


def cost(flops, bytes_accessed, transcendentals=0):
    return pl.CostEstimate(flops=flops, bytes_accessed=bytes_accessed, transcendentals=transcendentals)


def eights(v):
    return jnp.sum(v.reshape(v.shape[0] // SUBLANE, SUBLANE, v.shape[1]), axis=0)


def whole(*shape, **kw):
    return pl.BlockSpec(shape, lambda *i: (0,) * len(shape), **kw)


def by_cols(rows, cols, at=lambda i: i):
    return pl.BlockSpec((rows, cols), lambda i: (0, at(i)))


def by_rows(rows, cols, at=lambda i: i):
    return pl.BlockSpec((rows, cols), lambda i: (at(i), 0))


def steps(first, wide):
    return slice(first * wide, (first + 1) * wide)


def regroup(rows, source, load, store):
    groups = LANE // UNITS
    lane = lax.broadcasted_iota(jnp.int32, (rows, LANE), 1) // UNITS
    for tile in range(FFN // LANE):
        out = None
        for i in range(groups):
            n = source(tile * groups + i)
            piece = load(n // groups)
            shift = (i - n) % groups
            if shift:
                piece = pltpu.roll(piece, shift * UNITS, 1)
            out = piece if out is None else jnp.where(lane == i, piece, out)
        store(tile, out)


def norm_stats(values):
    mean = row_mean(values)
    centered = values - mean
    inv = lax.rsqrt(row_mean(centered * centered) + LN_EPS)
    return centered * inv, inv


BLOCKS = [slice(i * 512, i * 512 + 512) for i in range(3)] + [slice(1536, TOKENS)]


def row_tiles(body, step=LANE):
    def loop(i, carry):
        body(pl.multiple_of(i * step, step), step)
        return carry
    lax.fori_loop(0, TAIL // step, loop, 0)
    body(TAIL, IMAGES)


def back_part(body, part, parts):
    tiles = -(-TAIL // ROWS // parts)

    def loop(i, carry):
        tile = part * tiles + i

        @pl.when(tile < TAIL // ROWS)
        def _():
            body(pl.multiple_of(tile * ROWS, ROWS), ROWS)
        return carry
    lax.fori_loop(0, tiles, loop, 0)


def to_image_order(wide, place, step=LANE):
    per = MAIN // step
    def loop(i, carry):
        first = (i % per) * (step * IMAGES) + i // per
        rows = [wide[c, pl.ds(first, step, stride=IMAGES), :] for c in range(LANES)]
        place(pl.multiple_of(i * step, step), step, jnp.concatenate(rows, axis=1))
        return carry
    lax.fori_loop(0, IMAGES * per, loop, 0)
    place(TAIL, IMAGES, joined(wide, TAIL, IMAGES))


def from_image_order(values, wide):
    def loop(i, carry):
        rows = values[pl.ds(pl.multiple_of(i * LANE, LANE), LANE), :]
        for c in range(LANES):
            wide[c, pl.ds((i % 2) * (LANE * IMAGES) + i // 2, LANE, stride=IMAGES), :] = rows[:, steps(c, LANE)]
        return carry
    lax.fori_loop(0, 2 * IMAGES, loop, 0)
    put(wide, TAIL, IMAGES, values[pl.ds(TAIL, IMAGES), :])


def joined(wide, r, n):
    return jnp.concatenate([wide[c, pl.ds(r, n), :] for c in range(LANES)], axis=1)


def put(wide, r, n, values):
    for c in range(LANES):
        wide[c, pl.ds(r, n), :] = values[:, steps(c, LANE)]


def norm_back(dn, hat, inv, gain):
    dhat = dn * gain
    m1 = row_mean(dhat)
    m2 = row_mean(dhat * hat)
    return inv * (dhat - m1 - hat * m2)


ORDERS = ((2, 1, 0), (1, 0, 2), (0, 2, 1))


def all_blocks(rows, cols):
    return jax.ShapeDtypeStruct((*TORUS, rows, cols), BF)


class Links:
    def find(self, send, recv):
        self.send, self.recv = send, recv
        me = lax.axis_index("fsdp")
        self.core = me % 2
        self.at = (me // SUBLANE, (me // QUAD) % 2, (me // 2) % 2)
        self.other_core = me + 1 - 2 * self.core
        self.other = [me + step - 2 * step * place for step, place in zip((SUBLANE, QUAD, 2), self.at)]
        return self

    def meet(self):
        barrier = pltpu.get_barrier_semaphore()
        devices = (self.other_core, *self.other)
        for device in devices:
            pl.semaphore_signal(barrier, inc=1, device_id=(device,), device_id_type=pl.DeviceIdType.MESH)
        pl.semaphore_wait(barrier, len(devices))

    def remote(self, src, dst, sem, device):
        return pltpu.make_async_remote_copy(src_ref=src, dst_ref=dst, send_sem=self.send.at[sem], recv_sem=self.recv.at[sem],
                                            device_id=(device,), device_id_type=pl.DeviceIdType.MESH)


class Gather(Links):
    COUNT = 2

    def __init__(self, rows, cols, cuts, by_rows):
        self.rows, self.cols, self.cuts, self.by_rows = rows, cols, cuts, by_rows
        self.parts = range(len(cuts) - 1)
        self.full_shape = all_blocks(rows, cols)

    def scratch(self):
        return [pltpu.SemaphoreType.DMA((SEMS,))] * self.COUNT

    def bind(self, own, full, sems):
        self.own, self.full = own, full
        return self.find(*sems)

    def region(self, part, known, arrived=False, half=None):
        done = ORDERS[part][:known]
        place = [slice(None) if a in done else self.at[a] for a in range(3)]
        if half is not None:
            place[done[0]] = half
        if arrived:
            place[done[-1]] = 1 - self.at[done[-1]]
        cut = pl.ds(self.cuts[part], self.cuts[part + 1] - self.cuts[part])
        return (*place, self.core, cut, slice(None)) if self.by_rows else (*place, self.core, slice(None), cut)

    def hop(self, stage, part, half):
        where = self.full.at[self.region(part, stage - 1, half=half)]
        source = self.own.at[self.region(part, 0)[-2:]] if stage == 1 else where
        return self.remote(source, where, self.sem(stage, part, half), self.other[ORDERS[part][stage - 1]])

    def forward(self, stage, part, half=None):
        if stage == 0:
            return self.remote(self.own, self.full.at[(*self.at, self.core)], 0, self.other_core)
        where = self.full.at[self.region(part, stage, True, half)]
        return self.remote(where, where, self.sem(stage + QUAD, part, half), self.other_core)

    def sem(self, row, part, half):
        return QUAD * (row + (half or 0)) + part

    def halves(self, stage):
        return (None,) if stage < 3 else range(2)

    def keep(self):
        return pltpu.make_async_copy(self.own, self.full.at[(*self.at, self.core)], self.send.at[1])

    def begin(self):
        for part in self.parts:
            self.hop(1, part, None).start()
        self.forward(0, 0).start()
        self.keep().start()

    def turn(self, stage):
        if stage == 1:
            self.keep().wait()
        for half in self.halves(stage):
            for part in self.parts:
                self.hop(stage, part, half).wait()
                if stage < 3:
                    for onward in self.halves(stage + 1):
                        self.hop(stage + 1, part, onward).start()
            for part in self.parts:
                self.forward(stage, part, half).start()

    def end(self):
        self.forward(0, 0).wait()
        for stage in range(1, QUAD):
            for half in self.halves(stage):
                for part in self.parts:
                    self.forward(stage, part, half).wait()


SEMS = 36


class Exchange(Links):
    def __init__(self, rows, cols, cuts, along, stride=1, spare=0):
        self.rows, self.cols, self.stride = rows, cols, stride
        self.slots, self.locals = 3 * stride + spare, 1 + stride
        self.blocks = (*TORUS, rows, cols)
        self.parts = [((slice(a, b), slice(None)) if along == 0 else (slice(None), slice(a, b))) for a, b in zip(cuts, cuts[1:])]
        self.shapes = [((b - a, cols) if along == 0 else (rows, b - a)) for a, b in zip(cuts, cuts[1:])]

    def scratch(self):
        out = [pltpu.VMEM((self.locals, *self.blocks), F32), pltpu.VMEM((self.slots, *TORUS[1:], self.rows, self.cols), F32)]
        for axes in (2, 1, 0):
            out += [pltpu.VMEM((self.slots, *TORUS[:axes], *shape), F32) for shape in self.shapes]
        return out + [pltpu.SemaphoreType.DMA((10, self.slots))] * 2

    COUNT = 13

    def bind(self, refs):
        self.local, self.pair, *rest = refs
        self.held = [None, *(rest[steps(i, 3)] for i in range(3))]
        return self.find(*rest[9:])

    def index(self, stage, part, side):
        order = ORDERS[part]
        left = [a for a in range(3) if a not in order[:stage - 1]]
        axis = order[stage - 1]
        where = self.at[axis] if side else 1 - self.at[axis]
        return tuple(where if a == axis else slice(None) for a in left)

    def copy(self, stage, part, c):
        slot = c % self.slots
        if stage == 0:
            return self.remote(self.local.at[c % self.locals, :, :, :, 1 - self.core], self.pair.at[slot], (0, slot), self.other_core)
        source = self.pair if stage == 1 else self.held[stage - 1][part]
        tail = self.parts[part] if stage == 1 else ()
        return self.remote(source.at[(slot, *self.index(stage, part, False), *tail)], self.held[stage][part].at[slot],
                           (3 * stage - 2 + part, slot), self.other[ORDERS[part][stage - 1]])

    def start(self, stage, c):
        for part in range(1 if stage == 0 else 3):
            self.copy(stage, part, c).start()

    def wait(self, stage, c):
        for part in range(1 if stage == 0 else 3):
            self.copy(stage, part, c).wait()

    def add(self, stage, c):
        slot = c % self.slots
        if stage == 0:
            for chip in itertools.product(range(2), repeat=3):
                self.pair[(slot, *chip)] += self.local[(c % self.locals, *chip, self.core)]
            return
        for part in range(3):
            source = self.pair if stage == 1 else self.held[stage - 1][part]
            tail = self.parts[part] if stage == 1 else ()
            for place in itertools.product(range(2), repeat=3 - stage):
                free = iter(place)
                kept = tuple(next(free) if isinstance(i, slice) else i for i in self.index(stage, part, True))
                self.held[stage][part][(slot, *place)] += source[(slot, *kept, *tail)]

    def result(self, c, out_ref):
        for part in range(3):
            out_ref[self.parts[part]] = self.held[3][part][c % self.slots]

    def put_local(self, c, values):
        self.local[c % self.locals] = values.reshape(self.blocks)


def comm_params(n):
    return pltpu.CompilerParams(dimension_semantics=("arbitrary",), vmem_limit_bytes=VMEM_MAX, collective_id=n, has_side_effects=True)


def advance(exchanges, t, exists, emit):
    for stage in (3, 2, 1, 0):
        c = t - 1 - (stage + 1) * exchanges[0].stride

        @pl.when(exists(c))
        def _():
            for n, exchange in enumerate(exchanges):
                exchange.wait(stage, c)
                exchange.add(stage, c)
                if stage < 3:
                    exchange.start(stage + 1, c)
                else:
                    emit(n, exchange, c)

    @pl.when(exists(t - 1))
    def _():
        for exchange in exchanges:
            exchange.start(0, t - 1)


def first_chunks(n):
    return lambda c: (c >= 0) & (c < n)


DRAIN = 5


PARTS = 16
SHARD = WIDTH // PARTS
VECTOR_ROWS = PARTS
LN1_GAIN, LN1_BIAS, QKV_BIAS, OUT_BIAS, LN2_GAIN, LN2_BIAS, FC_BIAS, PROJ_BIAS = 0, 1, 2, 5, 6, 7, 8, 12
MLP_F = MAIN
UNITS = MLP_F // PARTS
MLP_STEPS = FFN // MLP_F
WIDTH_CUTS = (0, 384, 896, WIDTH)
QKV_HALF = QKV // 2
QKV_ALL = [Gather(SHARD, QKV_HALF, (0, MLP_F * 5 // 2, WIDTH, QKV_HALF), False) for _ in range(2)]
OUT_ALL = Gather(SHARD, WIDTH, (0, 384, 768, WIDTH), False)
FC_HALF = FFN // 2
FC_ALL = [Gather(SHARD, FC_HALF, (0, 896, 1792, FC_HALF), False) for _ in range(2)]
PROJ_FIRST = 144
PROJ_ALL = [Gather(PROJ_FIRST, WIDTH, (0, 48, 96, PROJ_FIRST), True), Gather(FFN // PARTS - PROJ_FIRST, WIDTH, (0, 64, 128, 176), True)]
VECTOR_ALL = Gather(SHARD, LANE, (0, SHARD), True)


def open_kernel(x_hbm, dy_hbm, lg_ref, lb_ref, qv_ref, ov_ref, mg_ref, mb_ref, fv_ref, pv_ref, fc_ref, wq_ref, wo_ref, xim_hbm, dyim_hbm, h_hbm, ht_hbm, vec_ref, qb_ref, fb_ref, fc_own, wq_full, wo_full,
                x, dy, wide, h, ht, rows, vec_own, vec_full, wq_own, wo_own, sems, *comm):
    loads = [pltpu.make_async_copy(src, dst, sems.at[i]) for i, (src, dst) in enumerate(((x_hbm, x), (dy_hbm, dy)))]
    for cp in loads:
        cp.start()
    clear(rows)
    row = 0
    for ref in (lg_ref, lb_ref, qv_ref, ov_ref, mg_ref, mb_ref, fv_ref, pv_ref):
        for i in range(ref.shape[1] // SHARD):
            rows[steps(row, 1), :SHARD] = ref[:, steps(i, SHARD)]
            row += 1
    vec_own[ALL] = rows[ALL].T[:SHARD, :].astype(BF)
    wq_own[ALL] = wq_ref[ALL].astype(BF)
    wo_own[ALL] = wo_ref[ALL].astype(BF)
    pairs = [comm[steps(i, 2)] for i in range(QUAD)]
    vectors = VECTOR_ALL.bind(vec_own, vec_full, pairs[0])
    weights = [OUT_ALL.bind(wo_own, wo_full, pairs[1])]
    for i, kind in enumerate(QKV_ALL):
        part = pl.ds(i * QKV_HALF, QKV_HALF)
        weights.append(kind.bind(wq_own.at[:, part], wq_full.at[(*EVERY, part)], pairs[2 + i]))
    gathers = (vectors, *weights)
    vectors.meet()
    for gather in gathers:
        gather.begin()
    for cp in loads:
        cp.wait()

    def reorder(tokens):
        def widen(r, n):
            put(wide, r, n, tokens[pl.ds(r, n), :].astype(F32))
        row_tiles(widen)

        def place(r, n, values):
            tokens[pl.ds(r, n), :] = values.astype(BF)
        to_image_order(wide, place)
    reorder(x)
    for gather in gathers:
        gather.turn(1)
    reorder(dy)
    for gather in gathers:
        gather.turn(2)
    vectors.turn(3)
    vectors.end()
    vec_ref[ALL] = vec_full[ALL].reshape(WIDTH, LANE).astype(F32).T[:VECTOR_ROWS, :]
    gain, bias = vec_ref[steps(LN1_GAIN, 1), :], vec_ref[steps(LN1_BIAS, 1), :]
    for d in range(PARTS):
        for i in range(3):
            qb_ref[:, steps(3 * d + i, SHARD)] = vec_ref[steps(QKV_BIAS + i, 1), steps(d, SHARD)]
        for n in range(MLP_STEPS):
            place = pl.ds(d * SHARD + n * UNITS % SHARD, UNITS)
            fb_ref[:, pl.ds(n * MLP_F + d * UNITS, UNITS)] = vec_ref[steps(FC_BIAS + n * UNITS // SHARD, 1), place]

    def norm(r, n):
        hat, _ = norm_stats(x[pl.ds(r, n), :].astype(F32))
        h[pl.ds(r, n), :] = (hat * gain + bias).astype(BF)
    row_tiles(norm, ROWS)
    for b in range(IMAGES):
        ht[:, steps(b, MAIN)] = h[steps(b, MAIN), :].T
    ht[:, TAIL:] = h[TAIL:, :].T
    stores = [pltpu.make_async_copy(src, dst, sems.at[i]) for i, (src, dst) in enumerate(((x, xim_hbm), (dy, dyim_hbm), (h, h_hbm), (ht, ht_hbm)))]
    for cp in stores:
        cp.start()
    def store_fc(tile, values):
        fc_own[:, steps(tile, LANE)] = values.astype(BF)
    regroup(SHARD, lambda n: n % PARTS * MLP_STEPS + n // PARTS, lambda tile: fc_ref[:, steps(tile, LANE)], store_fc)
    for gather in weights:
        gather.turn(3)
    for gather in weights:
        gather.end()
    for cp in stores:
        cp.wait()


def open_call(x, dy, vectors, fc, wq, wo):
    hbm, vmem = pl.BlockSpec(memory_space=pl.ANY), pl.BlockSpec(memory_space=pltpu.VMEM)
    return pl.pallas_call(
        open_kernel,
        in_specs=[hbm, hbm] + [vmem] * (len(vectors) + 3),
        out_specs=[hbm, hbm, hbm, hbm, vmem, vmem, vmem, vmem, hbm, hbm],
        out_shape=[*[jax.ShapeDtypeStruct((TOKENS, WIDTH), BF)] * 3,
                   jax.ShapeDtypeStruct((WIDTH, TOKENS), BF), jax.ShapeDtypeStruct((VECTOR_ROWS, WIDTH), F32),
                   *(jax.ShapeDtypeStruct((1, n), F32) for n in (QKV, FFN)), jax.ShapeDtypeStruct(fc.shape, BF), all_blocks(SHARD, QKV), OUT_ALL.full_shape],
        scratch_shapes=[pltpu.VMEM((TOKENS, WIDTH), BF), pltpu.VMEM((TOKENS, WIDTH), BF), pltpu.VMEM((LANES, TOKENS, LANE), F32),
                        pltpu.VMEM((TOKENS, WIDTH), BF), pltpu.VMEM((WIDTH, TOKENS), BF), pltpu.VMEM((LANE, LANE), F32), pltpu.VMEM((SHARD, LANE), BF),
                        pltpu.VMEM(VECTOR_ALL.full_shape.shape, BF), pltpu.VMEM((SHARD, QKV), BF), pltpu.VMEM((SHARD, WIDTH), BF),
                        pltpu.SemaphoreType.DMA((QUAD,))] + VECTOR_ALL.scratch() * QUAD,
        compiler_params=pltpu.CompilerParams(vmem_limit_bytes=VMEM_MAX, collective_id=3, has_side_effects=True),
        cost_estimate=cost(1_000_000_000, 60_000_000),
        name="open",
    )(x, dy, *vectors, fc, wq, wo)


QKV_N = 768


def qkv_kernel(h_ref, w_ref, wb_ref, own_ref, qkv_ref, full, *sems):
    t, last = step_id(), pl.num_programs(0) - 1
    gathers = []
    for i, kind in enumerate(FC_ALL):
        part = pl.ds(i * FC_HALF, FC_HALF)
        gathers.append(kind.bind(own_ref.at[:, part], full.at[(*EVERY, part)], sems[steps(i, 2)]))

    @pl.when(t == 0)
    def _():
        gathers[0].meet()
        for gather in gathers:
            gather.begin()

    @pl.when(t == 1)
    def _():
        for gather in gathers:
            gather.turn(1)
    for i in range(2):
        @pl.when(t == i + 2)
        def _():
            gathers[i].turn(2)
    for rows in BLOCKS:
        qkv_ref[rows, :] = (dot(h_ref[rows, :], w_ref[ALL]) + wb_ref[ALL]).astype(BF)

    @pl.when(t == last)
    def _():
        for gather in gathers:
            gather.turn(3)
        for gather in gathers:
            gather.end()


EVERY = [slice(None)] * 5


def qkv_call(h, w, wb, own):
    hbm = pl.BlockSpec(memory_space=pl.ANY)
    return pl.pallas_call(
        qkv_kernel,
        grid=(QKV // QKV_N,),
        in_specs=[whole(TOKENS, WIDTH, pipeline_mode=pl.Buffered(1)), by_cols(WIDTH, QKV_N), by_cols(1, QKV_N), whole(SHARD, FFN)],
        out_specs=[by_cols(TOKENS, QKV_N), hbm],
        out_shape=[jax.ShapeDtypeStruct((TOKENS, QKV), BF), all_blocks(SHARD, FFN)],
        scratch_shapes=FC_ALL[0].scratch() * 2,
        compiler_params=comm_params(QUAD),
        cost_estimate=cost(2 * TOKENS * WIDTH * QKV, 60_000_000),
        name="qkv",
    )(h, w, wb, own)


ROW_CUTS = (0, 24, 48, 80)
FC_SUM = Exchange(SHARD, MLP_F, ROW_CUTS, 0)
PROJ_SUM = Exchange(UNITS, WIDTH, WIDTH_CUTS, 1)
CDF_P = 0.33
CDF_C = (0.1326322871417956, 0.11939570820799192, 0.18103829560051796, -0.08904113226212501,
         0.33075919469138065, -0.22023738432274684, 0.0454530347223348)


def gelu_pair(u):
    bell = jnp.exp2(u * u * (-0.5 * LOG2E))
    t = 1.0 / (1.0 + CDF_P * jnp.abs(u))
    poly = CDF_C[6]
    for c in CDF_C[5::-1]:
        poly = poly * t + c
    tail = poly * t * bell
    cdf = jnp.where(u < 0.0, tail, 1.0 - tail)
    return u * cdf, cdf + u * bell * ((2.0 * math.pi) ** -0.5)


def mlp_kernel(r_hbm, n_hbm, dy_hbm, vec_ref, fc_ref, proj_ref, fcb_ref,
               y_hbm, dr_hbm, dr16_hbm, dfc_ref, dproj_ref, dfcb_ref, small_ref,
               n2, dy, y_acc, dn_acc, g, du, ua, ub, da, db, sem, *comm):
    step = step_id()
    by_row, by_col = FC_SUM.bind(comm[:Exchange.COUNT]), PROJ_SUM.bind(comm[Exchange.COUNT:])

    @pl.when(step == 0)
    def _():
        loads = [pltpu.make_async_copy(n_hbm, n2, sem), pltpu.make_async_copy(dy_hbm, dy, sem)]
        for cp in loads:
            cp.start()
        by_row.meet()
        clear(small_ref, y_acc, dn_acc)
        for cp in loads:
            cp.wait()

    outs = (dfc_ref, dproj_ref)
    advance((by_row, by_col), step, first_chunks(MLP_STEPS), lambda n, exchange, c: exchange.result(c, outs[n]))

    @pl.when(step < MLP_STEPS)
    def _():
        fcb = fcb_ref[ALL]
        fc, proj = fc_ref[ALL], proj_ref[ALL].reshape(MLP_F, WIDTH)
        bias_sum = jnp.zeros((SUBLANE, MLP_F), F32)
        tiles = [(b * MAIN, MAIN) for b in range(IMAGES - 1)] + [((IMAGES - 1) * MAIN, MAIN + IMAGES)]
        pairs = ((ua, da), (ub, db))

        def products(k):
            r, n = tiles[k]
            u_s, d_s = pairs[k % 2]
            u_s[0:n, :] = dot(n2[r:r + n, :], fc)
            d_s[0:n, :] = dot_nt(dy[r:r + n, :], proj)

        def pointwise(k, total):
            r, n = tiles[k]
            u_s, d_s = pairs[k % 2]
            value, slope = gelu_pair(u_s[0:n, :] + fcb)
            g[r:r + n, :] = value.astype(BF)
            grad = d_s[0:n, :] * slope
            du[r:r + n, :] = grad.astype(BF)
            return total + eights(grad)

        products(0)
        for k in range(1, IMAGES):
            products(k)
            bias_sum = pointwise(k - 1, bias_sum)
        bias_sum = pointwise(IMAGES - 1, bias_sum)
        dfcb_ref[ALL] = col_sum(bias_sum)
        y_acc[ALL] += dot(g[ALL], proj)
        for c in range(LANES // 2):
            part = dot_nt(du[ALL], fc_ref[steps(c, MAIN), :])
            dn_acc[2 * c] += part[:, :LANE]
            dn_acc[2 * c + 1] += part[:, LANE:]
        by_col.put_local(step, dot_tn(g[ALL], dy[ALL]))
        by_row.put_local(step, dot_tn(n2[ALL], du[ALL]))

    after = step - MLP_STEPS
    r_copy = pltpu.make_async_copy(r_hbm, n2, sem)
    out_copies = [pltpu.make_async_copy(dn_acc, dr_hbm, sem), pltpu.make_async_copy(n2, dr16_hbm, sem)]
    y_copy = pltpu.make_async_copy(dy, y_hbm, sem)

    def back(r, n):
        wide_r = n2[pl.ds(r, n), :].astype(F32)
        hat, inv = norm_stats(wide_r)
        dn = joined(dn_acc, r, n)
        wide_dy = dy[pl.ds(r, n), :].astype(F32)
        dr = wide_dy + norm_back(dn, hat, inv, vec_ref[steps(LN2_GAIN, 1), :])
        put(dn_acc, r, n, dr)
        n2[pl.ds(r, n), :] = dr.astype(BF)
        y_acc[pl.ds(r, n), :] += wide_r + vec_ref[steps(PROJ_BIAS, 1), :]
        for i, v in enumerate((dn * hat, dn, wide_dy, dr)):
            small_ref[steps(i, SUBLANE), :] += eights(v)

    @pl.when(after == 0)
    def _():
        r_copy.start()
        r_copy.wait()
        back(TAIL, IMAGES)

    @pl.when((after >= 0) & (after < 3))
    def _():
        back_part(back, after, 3)

    @pl.when(after == 2)
    def _():
        for cp in out_copies:
            cp.start()

    @pl.when(after == 3)
    def _():
        for cp in out_copies:
            cp.wait()
        from_image_order(y_acc, dn_acc)

        def narrow(r, n):
            dy[pl.ds(r, n), :] = joined(dn_acc, r, n).astype(BF)
        row_tiles(narrow)
        y_copy.start()

    @pl.when(after == QUAD)
    def _():
        y_copy.wait()


def mlp_call(r, n2, dy, vec, fc, proj, fcb):
    hbm = pl.BlockSpec(memory_space=pl.ANY)
    now = lambda i: jnp.minimum(i, MLP_STEPS - 1)
    done = lambda i: jnp.maximum(i - DRAIN, 0)
    return pl.pallas_call(
        mlp_kernel,
        grid=(MLP_STEPS + DRAIN,),
        in_specs=[hbm, hbm, hbm, whole(*vec.shape), by_cols(WIDTH, MLP_F, now),
                  pl.BlockSpec((PARTS, None, UNITS, WIDTH), lambda i: (0, now(i), 0, 0)),
                  by_cols(1, MLP_F, now)],
        out_specs=[hbm, hbm, hbm, by_cols(SHARD, MLP_F, done),
                   by_rows(UNITS, WIDTH, done),
                   by_cols(1, MLP_F, now), whole(32, WIDTH)],
        out_shape=[jax.ShapeDtypeStruct((TOKENS, WIDTH), BF), jax.ShapeDtypeStruct((LANES, TOKENS, LANE), F32),
                   jax.ShapeDtypeStruct((TOKENS, WIDTH), BF), jax.ShapeDtypeStruct((SHARD, FFN), F32),
                   jax.ShapeDtypeStruct((FFN // PARTS, WIDTH), F32),
                   jax.ShapeDtypeStruct((1, FFN), F32), jax.ShapeDtypeStruct((32, WIDTH), F32)],
        scratch_shapes=[pltpu.VMEM((TOKENS, WIDTH), BF), pltpu.VMEM((TOKENS, WIDTH), BF),
                        pltpu.VMEM((TOKENS, WIDTH), F32), pltpu.VMEM((LANES, TOKENS, LANE), F32),
                        pltpu.VMEM((TOKENS, MLP_F), BF), pltpu.VMEM((TOKENS, MLP_F), BF)]
                       + [pltpu.VMEM((MAIN + IMAGES, MLP_F), F32)] * QUAD + [pltpu.SemaphoreType.DMA]
                       + FC_SUM.scratch() + PROJ_SUM.scratch(),
        compiler_params=comm_params(0),
        cost_estimate=cost(12 * TOKENS * WIDTH * FFN, 150_000_000, TOKENS * FFN),
        name="mlp",
    )(r, n2, dy, vec, fc, proj.reshape(PARTS, MLP_STEPS, UNITS, WIDTH), fcb)


SCALE = HEAD ** -0.5
SCALE2 = SCALE * LOG2E
ATTN_COST = cost(40_000_000_000, 50_000_000, 8_400_000)


def window(h):
    first = min(HEAD * h // LANE * LANE, WIDTH - MAIN)
    wide = LANE if HEAD * h + HEAD <= first + LANE else MAIN
    return first, wide, HEAD * h - first


def lane_mask(h):
    first, wide, off = window(h)
    lane = lax.broadcasted_iota(jnp.int32, (MAIN, wide), 1)
    return (lane >= off) & (lane < off + HEAD)


def thirds(ref, rows=slice(None)):
    return [ref[rows, steps(i, WIDTH)] for i in range(3)]


def head_rows():
    lane = lax.broadcasted_iota(jnp.int32, (HEADS, WIDTH), 1)
    row = lax.broadcasted_iota(jnp.int32, (HEADS, WIDTH), 0)
    return (lane // HEAD == row).astype(F32)


def tail_softmax(s, s_self):
    m = jnp.maximum(jnp.max(s, axis=1, keepdims=True), s_self)
    e = jnp.exp2((s - m) * SCALE2)
    e_self = jnp.exp2((s_self - m) * SCALE2)
    inv = 1.0 / (row_sum(e) + e_self)
    return e * inv, e_self * inv


def attn_kernel(qkv_ref, qkvt_ref, x_ref, xt_ref, w_ref, vec_ref, proj_ref, o_hbm, r_hbm, n_hbm,
                max_ref, inv_ref, full,
                tails, o_tail, o_t, ptail, o_buf, r_buf, n_buf, sa, sb, sems, own, *comm):
    b, last = step_id(), pl.num_programs(0) - 1
    slot = b % 2
    gathers = []
    for i, kind in enumerate(PROJ_ALL):
        part = pl.ds(i * PROJ_FIRST, kind.rows)
        gathers.append(kind.bind(own.at[part], full.at[(*EVERY[1:], part)], comm[steps(i, 2)]))

    @pl.when(b == 0)
    def _():
        tails[ALL] = qkvt_ref[ALL].astype(F32)
        own[ALL] = proj_ref[ALL].astype(BF)
        gathers[0].meet()
        for gather in gathers:
            gather.begin()

    for turn, (stage, i) in enumerate(itertools.product((1, 2, 3), range(2))):
        @pl.when(b == turn + 1 + stage // 3)
        def _():
            gathers[i].turn(stage)

    heads = head_rows()
    q_t, k_t, v_t = (heads * z for z in thirds(tails, pl.ds(b, 1)))
    q, k, v = thirds(qkv_ref)

    p, p_self = tail_softmax(dot_nt(q_t.astype(BF), k), row_sum(q_t * k_t))
    mixed = dot(p.astype(BF), v) * heads + p_self.astype(BF).astype(F32) * v_t
    o_tail[pl.ds(b, 1), :] = col_sum(mixed)

    s_tail = dot_nt(k_t.astype(BF), q)
    v_turned = v.T
    scores = sa, sb

    def next_scores(h):
        first, wide, _ = window(h)
        q_h = jnp.where(lane_mask(h), qkv_ref[:, pl.ds(first, wide)], jnp.zeros((), BF))
        scores[h % 2][ALL] = dot_nt(qkv_ref[:, pl.ds(WIDTH + first, wide)], q_h)
    next_scores(0)
    for h in range(HEADS):
        if h + 1 < HEADS:
            next_scores(h + 1)
        s, mine = scores[h % 2], steps(h, 1)
        top = jnp.maximum(col_max(s[ALL]), s_tail[mine, :])
        e = jnp.exp2((s[ALL] - top) * SCALE2)
        e_tail = jnp.exp2((s_tail[mine, :] - top) * SCALE2)
        inv = 1.0 / (col_sum(e) + e_tail)
        max_ref[0, mine, :] = top
        inv_ref[0, mine, :] = inv
        ptail[mine, :] = e_tail * inv
        o_t[steps(h, HEAD), :] = dot(v_turned[steps(h, HEAD), :], (e * inv).astype(BF))

    outs = (o_buf, o_hbm), (r_buf, r_hbm), (n_buf, n_hbm)
    out_bias, gain, bias = (vec_ref[steps(i, 1), :] for i in (OUT_BIAS, LN2_GAIN, LN2_BIAS))

    def write(slot, rows, o, x):
        o_buf[slot, rows, :] = o
        r = (x.astype(F32) + dot(o, w_ref[ALL]) + out_bias).astype(BF)
        r_buf[slot, rows, :] = r
        hat, _ = norm_stats(r.astype(F32))
        n_buf[slot, rows, :] = (hat * gain + bias).astype(BF)

    @pl.when(b >= 2)
    def _():
        for n, (buf, hbm) in enumerate(outs):
            out_copy(buf, hbm, slot, b - 2, sems, n).wait()

    o = (o_t[ALL].T + dot_tn(ptail[ALL].astype(BF), v_t.astype(BF))).astype(BF)
    write(slot, slice(None), o, x_ref[ALL])
    for n, (buf, hbm) in enumerate(outs):
        out_copy(buf, hbm, slot, b, sems, n).start()

    @pl.when(b == last)
    def _():
        for n, (buf, hbm) in enumerate(outs):
            out_copy(buf, hbm, 1 - slot, b - 1, sems, n).wait()
        write(1 - slot, slice(IMAGES), o_tail[ALL].astype(BF), xt_ref[ALL])
        copies = [pltpu.make_async_copy(buf.at[1 - slot, pl.ds(0, IMAGES)], hbm.at[pl.ds(TAIL, IMAGES)], sems.at[n, 1 - slot])
                  for n, (buf, hbm) in enumerate(outs)]
        for cp in copies:
            cp.start()
        for cp in copies:
            cp.wait()
        for n, (buf, hbm) in enumerate(outs):
            out_copy(buf, hbm, slot, b, sems, n).wait()
        for gather in gathers:
            gather.end()


def out_copy(buf, hbm, slot, b, sems, n):
    return pltpu.make_async_copy(buf.at[slot], hbm.at[pl.ds(pl.multiple_of(b * MAIN, MAIN), MAIN)], sems.at[n, slot])


def attn_call(qkv, xim, w, vec, proj):
    hbm = pl.BlockSpec(memory_space=pl.ANY)
    main = lambda n: by_rows(MAIN, n)
    tail = lambda n: by_rows(IMAGES, n, lambda i: TAIL // IMAGES)
    stat = pl.BlockSpec((1, HEADS, MAIN), lambda i: (i, 0, 0))
    return pl.pallas_call(
        attn_kernel,
        grid=(IMAGES,),
        in_specs=[main(QKV), tail(QKV), main(WIDTH), tail(WIDTH),
                  whole(WIDTH, WIDTH), whole(*vec.shape), whole(*proj.shape)],
        out_specs=[hbm, hbm, hbm, stat, stat, hbm],
        out_shape=[*[jax.ShapeDtypeStruct((TOKENS, WIDTH), BF)] * 3,
                   jax.ShapeDtypeStruct((IMAGES, HEADS, MAIN), F32), jax.ShapeDtypeStruct((IMAGES, HEADS, MAIN), F32),
                   all_blocks(*proj.shape)],
        scratch_shapes=[pltpu.VMEM((IMAGES, QKV), F32), pltpu.VMEM((IMAGES, WIDTH), F32),
                        pltpu.VMEM((WIDTH, MAIN), F32), pltpu.VMEM((HEADS, MAIN), F32),
                        *[pltpu.VMEM((2, MAIN, WIDTH), BF)] * 3, *[pltpu.VMEM((MAIN, MAIN), F32)] * 2, pltpu.SemaphoreType.DMA((3, 2)),
                        pltpu.VMEM(proj.shape, BF)] + PROJ_ALL[0].scratch() * 2,
        compiler_params=comm_params(5),
        cost_estimate=ATTN_COST,
        name="attn",
    )(qkv, qkv, xim, xim, w, vec, proj)


def outb_kernel(dr_ref, o_ref, w_ref, dfc_ref, y_in, dproj_in, do_ref, dw_ref, dfc_out, y_out, dproj_out, y, dproj, sems):
    c, last = step_id(), pl.num_programs(0) - 1
    loads = [pltpu.make_async_copy(src, dst, sems.at[i]) for i, (src, dst) in enumerate(((y_in, y), (dproj_in, dproj)))]
    stores = [pltpu.make_async_copy(src, dst, sems.at[i]) for i, (src, dst) in enumerate(((y, y_out), (dproj, dproj_out)))]

    @pl.when(c == 0)
    def _():
        for cp in loads:
            cp.start()

    @pl.when(c == 1)
    def _():
        for cp in loads:
            cp.wait()
        for cp in stores:
            cp.start()

        def store_fc(tile, values):
            dfc_out[:, steps(tile, LANE)] = values
        regroup(SHARD, lambda n: n % MLP_STEPS * PARTS + n // MLP_STEPS, lambda tile: dfc_ref[:, steps(tile, LANE)], store_fc)
    do_ref[ALL] = dot_nt(dr_ref[ALL], w_ref[ALL]).astype(BF)
    dw_ref[ALL] = dot_tn(o_ref[ALL], dr_ref[:, pl.ds(pl.multiple_of(c * MAIN, MAIN), MAIN)])

    @pl.when(c == last)
    def _():
        for cp in stores:
            cp.wait()


def outb_call(dr, o, w, dfc, y, dproj):
    full, hbm = whole(TOKENS, WIDTH), pl.BlockSpec(memory_space=pl.ANY)
    like = lambda v: jax.ShapeDtypeStruct(v.shape, v.dtype)
    return pl.pallas_call(
        outb_kernel,
        grid=(WIDTH // MAIN,),
        in_specs=[full, full, by_rows(MAIN, WIDTH), whole(*dfc.shape), hbm, hbm],
        out_specs=[by_cols(TOKENS, MAIN), by_cols(WIDTH, MAIN), whole(*dfc.shape), hbm, hbm],
        out_shape=[like(dr), jax.ShapeDtypeStruct((WIDTH, WIDTH), F32), like(dfc), like(y), like(dproj)],
        scratch_shapes=[pltpu.VMEM(y.shape, BF), pltpu.VMEM(dproj.shape, F32), pltpu.SemaphoreType.DMA((2,))],
        compiler_params=pltpu.CompilerParams(dimension_semantics=("arbitrary",), vmem_limit_bytes=VMEM_MAX),
        cost_estimate=cost(QUAD * TOKENS * WIDTH * WIDTH, 50_000_000),
        name="outb",
    )(dr, o, w, dfc, y, dproj)


def attn_back_kernel(qkv_ref, qkvt_ref, do_ref, dot_ref, max_ref, inv_ref, dw_ref, dqkv_hbm, dwb_ref, dwout_ref,
                     tails, do_tails, grad_tails, dq_t, dk, dv, ds_tail, sa, da, sb, db, buf, sems, *comm):
    b = step_id()
    by_row = OUT_SUM.bind(comm)

    @pl.when(b == 0)
    def _():
        by_row.meet()

    @pl.when(b < OUT_STEPS)
    def _():
        by_row.put_local(b, dw_ref[ALL])
    advance((by_row,), b + 1, first_chunks(OUT_STEPS), lambda n, exchange, c: exchange.result(c, dwout_ref))

    @pl.when(b < IMAGES)
    def _():
        image_back(b, qkv_ref, qkvt_ref, do_ref, dot_ref, max_ref, inv_ref, dqkv_hbm, dwb_ref,
                   tails, do_tails, grad_tails, dq_t, dk, dv, ds_tail, ((sa, da), (sb, db)), buf, sems)


OUT_N = MAIN
OUT_STEPS = WIDTH // OUT_N
OUT_SUM = Exchange(SHARD, OUT_N, ROW_CUTS, 0)


def image_back(b, qkv_ref, qkvt_ref, do_ref, dot_ref, max_ref, inv_ref, dqkv_hbm, dwb_ref,
               tails, do_tails, grad_tails, dq_t, dk, dv, ds_tail, ahead, buf, sems):
    last = IMAGES - 1
    slot = b % 2

    @pl.when(b == 0)
    def _():
        tails[ALL] = qkvt_ref[ALL].astype(F32)
        do_tails[ALL] = dot_ref[ALL].astype(F32)
        clear(dwb_ref)

    heads = head_rows()
    q_t, k_t, v_t = (heads * z for z in thirds(tails, pl.ds(b, 1)))
    do_t = heads * do_tails[pl.ds(b, 1), :]
    q, k, v = thirds(qkv_ref)
    do = do_ref[ALL]
    q_t16, k_t16, v_t16, do_t16 = (z.astype(BF) for z in (q_t, k_t, v_t, do_t))

    p, p_self = tail_softmax(dot_nt(q_t16, k), row_sum(q_t * k_t))
    dp, dp_self = dot_nt(do_t16, v), row_sum(do_t * v_t)
    inner = row_sum(p * dp) + p_self * dp_self
    ds16 = (p * (dp - inner) * SCALE).astype(BF)
    ds_self = (p_self * (dp_self - inner) * SCALE).astype(BF).astype(F32)
    grad_q = col_sum(dot(ds16, k) * heads + ds_self * k_t)
    grad_k = ds_self * q_t
    grad_v = p_self.astype(BF).astype(F32) * do_t
    dk[ALL] = dot_tn(ds16, q_t16)
    dv[ALL] = dot_tn(p.astype(BF), do_t16)

    p_tail = jnp.exp2((dot_nt(k_t16, q) - max_ref[0]) * SCALE2) * inv_ref[0]
    dp_tail = dot_nt(v_t16, do)
    inner_tail = p_tail * dp_tail

    k_turned = k.T

    def masked(h):
        first, wide, _ = window(h)
        here, mask = pl.ds(first, wide), lane_mask(h)
        return here, jnp.where(mask, qkv_ref[:, here], jnp.zeros((), BF)), jnp.where(mask, do_ref[:, here], jnp.zeros((), BF))

    def next_products(h):
        first, wide, _ = window(h)
        _, q_h, do_h = masked(h)
        ahead[h % 2][0][ALL] = dot_nt(qkv_ref[:, pl.ds(WIDTH + first, wide)], q_h)
        ahead[h % 2][1][ALL] = dot_nt(qkv_ref[:, pl.ds(2 * WIDTH + first, wide)], do_h)
    next_products(0)
    for h in range(HEADS):
        if h + 1 < HEADS:
            next_products(h + 1)
        here, q_h, do_h = masked(h)
        mine = steps(h, 1)
        s, dp = (ref[ALL] for ref in ahead[h % 2])
        p = jnp.exp2((s - max_ref[0, mine, :]) * SCALE2) * inv_ref[0, mine, :]
        inner = col_sum(p * dp) + inner_tail[mine, :]
        ds = (p * (dp - inner) * SCALE).astype(BF)
        dv[:, here] += dot(p.astype(BF), do_h)
        dk[:, here] += dot(ds, q_h)
        dq_t[steps(h, HEAD), :] = dot(k_turned[steps(h, HEAD), :], ds)
        ds_tail[mine, :] = p_tail[mine, :] * (dp_tail[mine, :] - inner) * SCALE

    ds_tail16 = ds_tail[ALL].astype(BF)
    grad_k = col_sum(grad_k + dot(ds_tail16, q) * heads)
    grad_v = col_sum(grad_v + dot(p_tail.astype(BF), do) * heads)

    @pl.when(b >= 2)
    def _():
        out_copy(buf, dqkv_hbm, slot, b - 2, sems, 0).wait()

    grad = dq_t[ALL].T + dot_tn(ds_tail16, k_t16)
    for n, (main, tail) in enumerate(((grad, grad_q), (dk[ALL], grad_k), (dv[ALL], grad_v))):
        here = steps(n, WIDTH)
        buf[slot, :, here] = main.astype(BF)
        grad_tails[pl.ds(b, 1), here] = tail
        dwb_ref[:, here] += col_sum(main) + tail
    out_copy(buf, dqkv_hbm, slot, b, sems, 0).start()

    @pl.when(b == last)
    def _():
        out_copy(buf, dqkv_hbm, 1 - slot, b - 1, sems, 0).wait()
        buf[1 - slot, 0:IMAGES, :] = grad_tails[ALL].astype(BF)
        cp = pltpu.make_async_copy(buf.at[1 - slot, pl.ds(0, IMAGES)], dqkv_hbm.at[pl.ds(TAIL, IMAGES)], sems.at[0, 1 - slot])
        cp.start()
        cp.wait()
        out_copy(buf, dqkv_hbm, slot, b, sems, 0).wait()


def attn_back_call(qkv, do, top, inv, dw):
    hbm = pl.BlockSpec(memory_space=pl.ANY)
    image = lambda i: jnp.minimum(i, IMAGES - 1)
    main = lambda n: by_rows(MAIN, n, image)
    tail = lambda n: by_rows(IMAGES, n, lambda i: TAIL // IMAGES)
    stat = pl.BlockSpec((1, HEADS, MAIN), lambda i: (image(i), 0, 0))
    return pl.pallas_call(
        attn_back_kernel,
        grid=(OUT_STEPS + DRAIN - 1,),
        in_specs=[main(QKV), tail(QKV), main(WIDTH), tail(WIDTH), stat, stat,
                  by_cols(WIDTH, OUT_N, lambda i: jnp.minimum(i, OUT_STEPS - 1))],
        out_specs=[hbm, whole(1, QKV), by_cols(SHARD, OUT_N, lambda i: jnp.clip(i + 1 - DRAIN, 0, OUT_STEPS - 1))],
        out_shape=[jax.ShapeDtypeStruct((TOKENS, QKV), BF), jax.ShapeDtypeStruct((1, QKV), F32),
                   jax.ShapeDtypeStruct((SHARD, WIDTH), F32)],
        scratch_shapes=[pltpu.VMEM((IMAGES, QKV), F32), pltpu.VMEM((IMAGES, WIDTH), F32),
                        pltpu.VMEM((IMAGES, QKV), F32), pltpu.VMEM((WIDTH, MAIN), F32),
                        pltpu.VMEM((MAIN, WIDTH), F32), pltpu.VMEM((MAIN, WIDTH), F32), pltpu.VMEM((HEADS, MAIN), F32),
                        *[pltpu.VMEM((MAIN, MAIN), F32)] * QUAD, pltpu.VMEM((2, MAIN, QKV), BF), pltpu.SemaphoreType.DMA((1, 2))] + OUT_SUM.scratch(),
        compiler_params=comm_params(1),
        cost_estimate=ATTN_COST,
        name="attn_back",
    )(qkv, qkv, do, do, top, inv, dw)


QB_N = MAIN
QB_STEPS = QKV // QB_N
QKV_SUM = Exchange(SHARD, QB_N, ROW_CUTS, 0, 2)
VECTOR_SUM = Exchange(3 * SUBLANE, LANE, (0, SUBLANE, 2 * SUBLANE, 3 * SUBLANE), 0)
VECTOR_STEP = QB_STEPS + 2
QB_GRID = QB_STEPS + 1 + QUAD * QKV_SUM.stride


def qkvb_kernel(xim_hbm, dr_hbm, vec_ref, sums_ref, qb_ref, fb_ref, ht_ref, dqkv_ref, w_ref, dx_hbm, dw_ref, out_vec_ref,
                acc, dr, xd, sums, sems, *comm):
    t = step_id()
    by_row, by_vector = QKV_SUM.bind(comm[:Exchange.COUNT]), VECTOR_SUM.bind(comm[Exchange.COUNT:])
    loads = [pltpu.make_async_copy(dr_hbm, dr, sems.at[0]), pltpu.make_async_copy(xim_hbm, xd, sems.at[1])]
    store = pltpu.make_async_copy(xd, dx_hbm, sems.at[1])

    def put_row(place, row, lane, values):
        by_vector.local[(0, *place, pl.ds(row, len(values)), pl.ds(lane, values.shape[1]))] = values

    def share(row, values):
        for d, place in enumerate(DEVICES):
            put_row(place, row, 0, values[:, steps(d, SHARD)])

    @pl.when(t == 0)
    def _():
        by_row.meet()
        for cp in loads:
            cp.start()
        clear(acc, sums)
        by_vector.local[0] = jnp.zeros(by_vector.blocks, F32)
        share(0, jnp.concatenate([col_sum(sums_ref[steps(i, SUBLANE), :]) for i in range(QUAD)], axis=0))
        for d, place in enumerate(DEVICES):
            for i in range(3):
                put_row(place, QUAD + i, 0, qb_ref[:, pl.ds((3 * d + i) * SHARD, SHARD)])
            for n in range(MLP_STEPS):
                put_row(place, QUAD + 3 + n * UNITS // SHARD, n * UNITS % SHARD, fb_ref[:, pl.ds(n * MLP_F + d * UNITS, UNITS)])

    def emit_vectors(n, exchange, c):
        for part, (rows, _) in enumerate(exchange.parts[:2]):
            out_vec_ref[rows, :] = exchange.held[3][part][0, :, :SHARD]
    advance((by_row,), t, first_chunks(QB_STEPS), lambda n, exchange, c: exchange.result(c, dw_ref))
    advance((by_vector,), t - VECTOR_STEP, first_chunks(1), emit_vectors)

    @pl.when(t < QB_STEPS)
    def _():
        by_row.put_local(t, dot(ht_ref[ALL], dqkv_ref[ALL]))
        acc[ALL] += dot_nt(dqkv_ref[ALL], w_ref[ALL])

    @pl.when(t == QB_STEPS)
    def _():
        for cp in loads:
            cp.wait()

    def back(r, n):
        hat, inv = norm_stats(xd[pl.ds(r, n), :].astype(F32))
        dn = acc[pl.ds(r, n), :]
        for i, v in enumerate((dn * hat, dn)):
            sums[steps(i, SUBLANE), :] += eights(v)
        acc[pl.ds(r, n), :] = joined(dr, r, n) + norm_back(dn, hat, inv, vec_ref[steps(LN1_GAIN, 1), :])

    @pl.when((t >= QB_STEPS) & (t <= VECTOR_STEP))
    def _():
        back_part(back, t - QB_STEPS, 3)

    @pl.when(t == VECTOR_STEP)
    def _():
        back(TAIL, IMAGES)
        share(VECTOR_ROWS - 2, jnp.concatenate([col_sum(sums[steps(i, SUBLANE), :]) for i in range(2)], axis=0))

    @pl.when(t == VECTOR_STEP + 1)
    def _():
        from_image_order(acc, dr)

    @pl.when(t == VECTOR_STEP + 2)
    def _():
        def narrow(r, n):
            xd[pl.ds(r, n), :] = joined(dr, r, n).astype(BF)
        row_tiles(narrow)
        store.start()

    @pl.when(t == QB_GRID - 1)
    def _():
        store.wait()


DEVICES = list(itertools.product(range(2), repeat=QUAD))


def qkvb_call(xim, dr, vec, sums, qb, fb, ht, dqkv, w):
    hbm = pl.BlockSpec(memory_space=pl.ANY)
    now = lambda i: jnp.minimum(i, QB_STEPS - 1)
    return pl.pallas_call(
        qkvb_kernel,
        grid=(QB_GRID,),
        in_specs=[hbm, hbm, *(whole(*v.shape) for v in (vec, sums, qb, fb)),
                  whole(WIDTH, TOKENS, pipeline_mode=pl.Buffered(1)), by_cols(TOKENS, QB_N, now), by_cols(WIDTH, QB_N, now)],
        out_specs=[hbm, by_cols(SHARD, QB_N, lambda i: jnp.clip(i - 1 - QUAD * QKV_SUM.stride, 0, QB_STEPS - 1)),
                   whole(VECTOR_ROWS, SHARD)],
        out_shape=[jax.ShapeDtypeStruct((TOKENS, WIDTH), BF), jax.ShapeDtypeStruct((SHARD, QKV), F32),
                   jax.ShapeDtypeStruct((VECTOR_ROWS, SHARD), F32)],
        scratch_shapes=[pltpu.VMEM((TOKENS, WIDTH), F32), pltpu.VMEM((LANES, TOKENS, LANE), F32), pltpu.VMEM((TOKENS, WIDTH), BF),
                        pltpu.VMEM((2 * SUBLANE, WIDTH), F32), pltpu.SemaphoreType.DMA((2,))]
                       + QKV_SUM.scratch() + VECTOR_SUM.scratch(),
        compiler_params=comm_params(2),
        cost_estimate=cost(QUAD * TOKENS * WIDTH * QKV, 80_000_000),
        name="qkvb",
    )(xim, dr, vec, sums, qb, fb, ht, dqkv, w)


def solution(mesh):
    specs = (P("fsdp"),) * 14

    def device_step(resid_in, grad_out, ln1_gain, ln1_bias, qkv_weight, qkv_bias, out_weight, out_bias,
                    ln2_gain, ln2_bias, fc_weight, fc_bias, proj_weight, proj_bias):
        vectors = [v.reshape(1, -1) for v in (ln1_gain, ln1_bias, qkv_bias, out_bias, ln2_gain, ln2_bias, fc_bias, proj_bias)]
        x = resid_in.swapaxes(0, 1).reshape(TOKENS, WIDTH)
        dy = grad_out.swapaxes(0, 1).reshape(TOKENS, WIDTH)
        xim, dyim, h, ht, rows, bq, bf, fc, wq, wo = open_call(x, dy, vectors, fc_weight, qkv_weight, out_weight)
        wq, wo = wq.reshape(WIDTH, QKV), wo.reshape(WIDTH, WIDTH)
        qkv, wf = qkv_call(h, wq, bq, fc)
        o, r, n2, top, inv, wp = attn_call(qkv, xim, wo, rows, proj_weight)
        y, dr, dr16, dwf, dwp, dbf, small = mlp_call(r, n2, dyim, rows, wf.reshape(WIDTH, FFN), wp, bf)
        do, dwo, dwf, y, dwp = outb_call(dr16, o, wo, dwf, y, dwp)
        dqkv, dbq, dwo = attn_back_call(qkv, do, top, inv, dwo)
        dx, dwq, vec = qkvb_call(xim, dr, rows, small, dbq, dbf, ht, dqkv, wq)
        dg2, db2, dbp, dbo = vec[:4]
        dbq, dbf = vec[4:7].reshape(-1), vec[7:11].reshape(-1)
        dg1, db1 = vec[VECTOR_ROWS - 2:]
        unturn = lambda t: t.reshape(SEQ, IMAGES, WIDTH).swapaxes(0, 1)
        return (unturn(y), unturn(dx), dg1, db1, dwq, dbq, dwo, dbo, dg2, db2, dwf, dbf, dwp, dbp)

    return jax.shard_map(device_step, mesh=mesh, in_specs=specs, out_specs=specs, check_vma=False)
```

```python
import itertools
import math
import jax, jax.numpy as jnp
from jax import lax
from jax.experimental import pallas as pl
from jax.experimental.pallas import tpu as pltpu
from jax.sharding import PartitionSpec as P

BF, F32 = jnp.bfloat16, jnp.float32
IMAGES, SEQ, WIDTH, FFN, HEADS, HEAD = 8, 257, 1280, 5120, 16, 80
MAIN = SEQ - 1
TOKENS = IMAGES * SEQ
TAIL = IMAGES * MAIN
LN_EPS = 1e-5
LOG2E = math.log2(math.e)
VMEM_MAX = 67043328
LANE, SUBLANE, QUAD, QKV = 128, 8, 4, 3 * WIDTH
ALL = ...
TORUS = (2,) * QUAD
LANES = WIDTH // LANE
ROWS = 32


def dot(a, b):
    return jnp.dot(a, b, preferred_element_type=F32)


def dot_nt(a, b):
    return lax.dot_general(a, b, (((1,), (1,)), ((), ())), preferred_element_type=F32)


def dot_tn(a, b):
    return lax.dot_general(a, b, (((0,), (0,)), ((), ())), preferred_element_type=F32)


def col_sum(v):
    return jnp.sum(v, axis=0, keepdims=True)


def col_max(v):
    return jnp.max(v, axis=0, keepdims=True)


def row_sum(v):
    return jnp.sum(v, axis=-1, keepdims=True)


def row_mean(v):
    return row_sum(v) * (1.0 / WIDTH)


def clear(*refs):
    for ref in refs:
        ref[ALL] = jnp.zeros_like(ref)


def step_id():
    return pl.program_id(0)


def cost(flops, bytes_accessed, transcendentals=0):
    return pl.CostEstimate(flops=flops, bytes_accessed=bytes_accessed, transcendentals=transcendentals)


def eights(v):
    return jnp.sum(v.reshape(v.shape[0] // SUBLANE, SUBLANE, v.shape[1]), axis=0)


def whole(*shape, **kw):
    return pl.BlockSpec(shape, lambda *i: (0,) * len(shape), **kw)


def by_cols(rows, cols, at=lambda i: i):
    return pl.BlockSpec((rows, cols), lambda i: (0, at(i)))


def by_rows(rows, cols, at=lambda i: i):
    return pl.BlockSpec((rows, cols), lambda i: (at(i), 0))


def steps(first, wide):
    return slice(first * wide, (first + 1) * wide)


def regroup(rows, source, load, store):
    groups = LANE // UNITS
    lane = lax.broadcasted_iota(jnp.int32, (rows, LANE), 1) // UNITS
    for tile in range(FFN // LANE):
        out = None
        for i in range(groups):
            n = source(tile * groups + i)
            piece = load(n // groups)
            shift = (i - n) % groups
            if shift:
                piece = pltpu.roll(piece, shift * UNITS, 1)
            out = piece if out is None else jnp.where(lane == i, piece, out)
        store(tile, out)


def norm_stats(values):
    mean = row_mean(values)
    centered = values - mean
    inv = lax.rsqrt(row_mean(centered * centered) + LN_EPS)
    return centered * inv, inv


BLOCKS = [slice(i * 512, i * 512 + 512) for i in range(3)] + [slice(1536, TOKENS)]


def row_tiles(body, step=LANE):
    def loop(i, carry):
        body(pl.multiple_of(i * step, step), step)
        return carry
    lax.fori_loop(0, TAIL // step, loop, 0)
    body(TAIL, IMAGES)


def back_part(body, part, parts):
    tiles = -(-TAIL // ROWS // parts)

    def loop(i, carry):
        tile = part * tiles + i

        @pl.when(tile < TAIL // ROWS)
        def _():
            body(pl.multiple_of(tile * ROWS, ROWS), ROWS)
        return carry
    lax.fori_loop(0, tiles, loop, 0)


def to_image_order(wide, place, step=LANE):
    per = MAIN // step
    def loop(i, carry):
        first = (i % per) * (step * IMAGES) + i // per
        rows = [wide[c, pl.ds(first, step, stride=IMAGES), :] for c in range(LANES)]
        place(pl.multiple_of(i * step, step), step, jnp.concatenate(rows, axis=1))
        return carry
    lax.fori_loop(0, IMAGES * per, loop, 0)
    place(TAIL, IMAGES, joined(wide, TAIL, IMAGES))


def from_image_order(values, wide):
    def loop(i, carry):
        rows = values[pl.ds(pl.multiple_of(i * LANE, LANE), LANE), :]
        for c in range(LANES):
            wide[c, pl.ds((i % 2) * (LANE * IMAGES) + i // 2, LANE, stride=IMAGES), :] = rows[:, steps(c, LANE)]
        return carry
    lax.fori_loop(0, 2 * IMAGES, loop, 0)
    put(wide, TAIL, IMAGES, values[pl.ds(TAIL, IMAGES), :])


def joined(wide, r, n):
    return jnp.concatenate([wide[c, pl.ds(r, n), :] for c in range(LANES)], axis=1)


def put(wide, r, n, values):
    for c in range(LANES):
        wide[c, pl.ds(r, n), :] = values[:, steps(c, LANE)]


def norm_back(dn, hat, inv, gain):
    dhat = dn * gain
    m1 = row_mean(dhat)
    m2 = row_mean(dhat * hat)
    return inv * (dhat - m1 - hat * m2)


ORDERS = ((2, 1, 0), (1, 0, 2), (0, 2, 1))


def all_blocks(rows, cols):
    return jax.ShapeDtypeStruct((*TORUS, rows, cols), BF)


class Links:
    def find(self, send, recv):
        self.send, self.recv = send, recv
        me = lax.axis_index("fsdp")
        self.core = me % 2
        self.at = (me // SUBLANE, (me // QUAD) % 2, (me // 2) % 2)
        self.other_core = me + 1 - 2 * self.core
        self.other = [me + step - 2 * step * place for step, place in zip((SUBLANE, QUAD, 2), self.at)]
        return self

    def meet(self):
        barrier = pltpu.get_barrier_semaphore()
        devices = (self.other_core, *self.other)
        for device in devices:
            pl.semaphore_signal(barrier, inc=1, device_id=(device,), device_id_type=pl.DeviceIdType.MESH)
        pl.semaphore_wait(barrier, len(devices))

    def remote(self, src, dst, sem, device):
        return pltpu.make_async_remote_copy(src_ref=src, dst_ref=dst, send_sem=self.send.at[sem], recv_sem=self.recv.at[sem],
                                            device_id=(device,), device_id_type=pl.DeviceIdType.MESH)


class Gather(Links):
    COUNT = 2

    def __init__(self, rows, cols, cuts, by_rows):
        self.rows, self.cols, self.cuts, self.by_rows = rows, cols, cuts, by_rows
        self.parts = range(len(cuts) - 1)
        self.full_shape = all_blocks(rows, cols)

    def scratch(self):
        return [pltpu.SemaphoreType.DMA((SEMS,))] * self.COUNT

    def bind(self, own, full, sems):
        self.own, self.full = own, full
        return self.find(*sems)

    def region(self, part, known, arrived=False, half=None):
        done = ORDERS[part][:known]
        place = [slice(None) if a in done else self.at[a] for a in range(3)]
        if half is not None:
            place[done[0]] = half
        if arrived:
            place[done[-1]] = 1 - self.at[done[-1]]
        cut = pl.ds(self.cuts[part], self.cuts[part + 1] - self.cuts[part])
        return (*place, self.core, cut, slice(None)) if self.by_rows else (*place, self.core, slice(None), cut)

    def hop(self, stage, part, half):
        where = self.full.at[self.region(part, stage - 1, half=half)]
        source = self.own.at[self.region(part, 0)[-2:]] if stage == 1 else where
        return self.remote(source, where, self.sem(stage, part, half), self.other[ORDERS[part][stage - 1]])

    def forward(self, stage, part, half=None):
        if stage == 0:
            return self.remote(self.own, self.full.at[(*self.at, self.core)], 0, self.other_core)
        where = self.full.at[self.region(part, stage, True, half)]
        return self.remote(where, where, self.sem(stage + QUAD, part, half), self.other_core)

    def sem(self, row, part, half):
        return QUAD * (row + (half or 0)) + part

    def halves(self, stage):
        return (None,) if stage < 3 else range(2)

    def keep(self):
        return pltpu.make_async_copy(self.own, self.full.at[(*self.at, self.core)], self.send.at[1])

    def begin(self):
        for part in self.parts:
            self.hop(1, part, None).start()
        self.forward(0, 0).start()
        self.keep().start()

    def turn(self, stage):
        if stage == 1:
            self.keep().wait()
        for half in self.halves(stage):
            for part in self.parts:
                self.hop(stage, part, half).wait()
                if stage < 3:
                    for onward in self.halves(stage + 1):
                        self.hop(stage + 1, part, onward).start()
            for part in self.parts:
                self.forward(stage, part, half).start()

    def end(self):
        self.forward(0, 0).wait()
        for stage in range(1, QUAD):
            for half in self.halves(stage):
                for part in self.parts:
                    self.forward(stage, part, half).wait()


SEMS = 36


class Exchange(Links):
    def __init__(self, rows, cols, cuts, along, stride=1, spare=0):
        self.rows, self.cols, self.stride = rows, cols, stride
        self.slots, self.locals = 3 * stride + spare, 1 + stride
        self.blocks = (*TORUS, rows, cols)
        self.parts = [((slice(a, b), slice(None)) if along == 0 else (slice(None), slice(a, b))) for a, b in zip(cuts, cuts[1:])]
        self.shapes = [((b - a, cols) if along == 0 else (rows, b - a)) for a, b in zip(cuts, cuts[1:])]

    def scratch(self):
        out = [pltpu.VMEM((self.locals, *self.blocks), F32), pltpu.VMEM((self.slots, *TORUS[1:], self.rows, self.cols), F32)]
        for axes in (2, 1, 0):
            out += [pltpu.VMEM((self.slots, *TORUS[:axes], *shape), F32) for shape in self.shapes]
        return out + [pltpu.SemaphoreType.DMA((10, self.slots))] * 2

    COUNT = 13

    def bind(self, refs):
        self.local, self.pair, *rest = refs
        self.held = [None, *(rest[steps(i, 3)] for i in range(3))]
        return self.find(*rest[9:])

    def index(self, stage, part, side):
        order = ORDERS[part]
        left = [a for a in range(3) if a not in order[:stage - 1]]
        axis = order[stage - 1]
        where = self.at[axis] if side else 1 - self.at[axis]
        return tuple(where if a == axis else slice(None) for a in left)

    def copy(self, stage, part, c):
        slot = c % self.slots
        if stage == 0:
            return self.remote(self.local.at[c % self.locals, :, :, :, 1 - self.core], self.pair.at[slot], (0, slot), self.other_core)
        source = self.pair if stage == 1 else self.held[stage - 1][part]
        tail = self.parts[part] if stage == 1 else ()
        return self.remote(source.at[(slot, *self.index(stage, part, False), *tail)], self.held[stage][part].at[slot],
                           (3 * stage - 2 + part, slot), self.other[ORDERS[part][stage - 1]])

    def start(self, stage, c):
        for part in range(1 if stage == 0 else 3):
            self.copy(stage, part, c).start()

    def wait(self, stage, c):
        for part in range(1 if stage == 0 else 3):
            self.copy(stage, part, c).wait()

    def add(self, stage, c):
        slot = c % self.slots
        if stage == 0:
            for chip in itertools.product(range(2), repeat=3):
                self.pair[(slot, *chip)] += self.local[(c % self.locals, *chip, self.core)]
            return
        for part in range(3):
            source = self.pair if stage == 1 else self.held[stage - 1][part]
            tail = self.parts[part] if stage == 1 else ()
            for place in itertools.product(range(2), repeat=3 - stage):
                free = iter(place)
                kept = tuple(next(free) if isinstance(i, slice) else i for i in self.index(stage, part, True))
                self.held[stage][part][(slot, *place)] += source[(slot, *kept, *tail)]

    def result(self, c, out_ref):
        for part in range(3):
            out_ref[self.parts[part]] = self.held[3][part][c % self.slots]

    def put_local(self, c, values):
        self.local[c % self.locals] = values.reshape(self.blocks)


def comm_params(n):
    return pltpu.CompilerParams(dimension_semantics=("arbitrary",), vmem_limit_bytes=VMEM_MAX, collective_id=n, has_side_effects=True)


def advance(exchanges, t, exists, emit):
    for stage in (3, 2, 1, 0):
        c = t - 1 - (stage + 1) * exchanges[0].stride

        @pl.when(exists(c))
        def _():
            for n, exchange in enumerate(exchanges):
                exchange.wait(stage, c)
                exchange.add(stage, c)
                if stage < 3:
                    exchange.start(stage + 1, c)
                else:
                    emit(n, exchange, c)

    @pl.when(exists(t - 1))
    def _():
        for exchange in exchanges:
            exchange.start(0, t - 1)


def first_chunks(n):
    return lambda c: (c >= 0) & (c < n)


DRAIN = 5


PARTS = 16
SHARD = WIDTH // PARTS
VECTOR_ROWS = PARTS
LN1_GAIN, LN1_BIAS, QKV_BIAS, OUT_BIAS, LN2_GAIN, LN2_BIAS, FC_BIAS, PROJ_BIAS = 0, 1, 2, 5, 6, 7, 8, 12
MLP_F = MAIN
UNITS = MLP_F // PARTS
MLP_STEPS = FFN // MLP_F
WIDTH_CUTS = (0, 384, 896, WIDTH)
QKV_ALL = Gather(SHARD, QKV, (0, WIDTH, 2 * WIDTH, QKV), False)
OUT_ALL = Gather(SHARD, WIDTH, (0, 384, 768, WIDTH), False)
FC_HALF = FFN // 2
FC_ALL = [Gather(SHARD, FC_HALF, (0, 896, 1792, FC_HALF), False) for _ in range(2)]
PROJ_FIRST = 144
PROJ_ALL = [Gather(PROJ_FIRST, WIDTH, (0, 48, 96, PROJ_FIRST), True), Gather(FFN // PARTS - PROJ_FIRST, WIDTH, (0, 64, 128, 176), True)]
VECTOR_ALL = Gather(SHARD, LANE, (0, SHARD), True)


def open_kernel(x_hbm, dy_hbm, rows_ref, fc_ref, wq_ref, wo_ref, xim_hbm, dyim_hbm, h_hbm, ht_hbm, vec_ref, qb_ref, fb_ref, fc_own, wq_full, wo_full,
                x, dy, wide, h, ht, rows, vec_own, vec_full, wq_own, wo_own, sems, *comm):
    loads = [pltpu.make_async_copy(src, dst, sems.at[i]) for i, (src, dst) in enumerate(((x_hbm, x), (dy_hbm, dy)))]
    for cp in loads:
        cp.start()
    clear(rows)
    rows[:VECTOR_ROWS, :] = rows_ref[ALL]
    vec_own[ALL] = rows[ALL].T[:SHARD, :].astype(BF)
    wq_own[ALL] = wq_ref[ALL].astype(BF)
    wo_own[ALL] = wo_ref[ALL].astype(BF)
    pairs = [comm[steps(i, 2)] for i in range(3)]
    vectors = VECTOR_ALL.bind(vec_own, vec_full, pairs[0])
    weights = QKV_ALL.bind(wq_own, wq_full, pairs[1]), OUT_ALL.bind(wo_own, wo_full, pairs[2])
    gathers = (vectors, *weights)
    vectors.meet()
    for gather in gathers:
        gather.begin()
    for cp in loads:
        cp.wait()

    def reorder(tokens):
        def widen(r, n):
            put(wide, r, n, tokens[pl.ds(r, n), :].astype(F32))
        row_tiles(widen)

        def place(r, n, values):
            tokens[pl.ds(r, n), :] = values.astype(BF)
        to_image_order(wide, place)
    reorder(x)
    for gather in gathers:
        gather.turn(1)
    reorder(dy)
    for gather in gathers:
        gather.turn(2)
    vectors.turn(3)
    vectors.end()
    vec_ref[ALL] = vec_full[ALL].reshape(WIDTH, LANE).astype(F32).T[:VECTOR_ROWS, :]
    gain, bias = vec_ref[steps(LN1_GAIN, 1), :], vec_ref[steps(LN1_BIAS, 1), :]
    for d in range(PARTS):
        for i in range(3):
            qb_ref[:, steps(3 * d + i, SHARD)] = vec_ref[steps(QKV_BIAS + i, 1), steps(d, SHARD)]
        for n in range(MLP_STEPS):
            place = pl.ds(d * SHARD + n * UNITS % SHARD, UNITS)
            fb_ref[:, pl.ds(n * MLP_F + d * UNITS, UNITS)] = vec_ref[steps(FC_BIAS + n * UNITS // SHARD, 1), place]

    def norm(r, n):
        hat, _ = norm_stats(x[pl.ds(r, n), :].astype(F32))
        h[pl.ds(r, n), :] = (hat * gain + bias).astype(BF)
    row_tiles(norm, ROWS)
    for b in range(IMAGES):
        ht[:, steps(b, MAIN)] = h[steps(b, MAIN), :].T
    ht[:, TAIL:] = h[TAIL:, :].T
    stores = [pltpu.make_async_copy(src, dst, sems.at[i]) for i, (src, dst) in enumerate(((x, xim_hbm), (dy, dyim_hbm), (h, h_hbm), (ht, ht_hbm)))]
    for cp in stores:
        cp.start()
    def store_fc(tile, values):
        fc_own[:, steps(tile, LANE)] = values.astype(BF)
    regroup(SHARD, lambda n: n % PARTS * MLP_STEPS + n // PARTS, lambda tile: fc_ref[:, steps(tile, LANE)], store_fc)
    for gather in weights:
        gather.turn(3)
    for gather in weights:
        gather.end()
    for cp in stores:
        cp.wait()


def open_call(x, dy, rows, fc, wq, wo):
    hbm, vmem = pl.BlockSpec(memory_space=pl.ANY), pl.BlockSpec(memory_space=pltpu.VMEM)
    return pl.pallas_call(
        open_kernel,
        in_specs=[hbm, hbm, vmem, vmem, vmem, vmem],
        out_specs=[hbm, hbm, hbm, hbm, vmem, vmem, vmem, vmem, hbm, hbm],
        out_shape=[*[jax.ShapeDtypeStruct((TOKENS, WIDTH), BF)] * 3,
                   jax.ShapeDtypeStruct((WIDTH, TOKENS), BF), jax.ShapeDtypeStruct((VECTOR_ROWS, WIDTH), F32),
                   *(jax.ShapeDtypeStruct((1, n), F32) for n in (QKV, FFN)), jax.ShapeDtypeStruct(fc.shape, BF), QKV_ALL.full_shape, OUT_ALL.full_shape],
        scratch_shapes=[pltpu.VMEM((TOKENS, WIDTH), BF), pltpu.VMEM((TOKENS, WIDTH), BF), pltpu.VMEM((LANES, TOKENS, LANE), F32),
                        pltpu.VMEM((TOKENS, WIDTH), BF), pltpu.VMEM((WIDTH, TOKENS), BF), pltpu.VMEM((LANE, LANE), F32), pltpu.VMEM((SHARD, LANE), BF),
                        pltpu.VMEM(VECTOR_ALL.full_shape.shape, BF), pltpu.VMEM((SHARD, QKV), BF), pltpu.VMEM((SHARD, WIDTH), BF),
                        pltpu.SemaphoreType.DMA((QUAD,))] + VECTOR_ALL.scratch() + QKV_ALL.scratch() + OUT_ALL.scratch(),
        compiler_params=pltpu.CompilerParams(vmem_limit_bytes=VMEM_MAX, collective_id=3, has_side_effects=True),
        cost_estimate=cost(1_000_000_000, 60_000_000),
        name="open",
    )(x, dy, rows, fc, wq, wo)


QKV_N = 768


def qkv_kernel(h_ref, w_ref, wb_ref, own_ref, qkv_ref, full, *sems):
    t, last = step_id(), pl.num_programs(0) - 1
    gathers = []
    for i, kind in enumerate(FC_ALL):
        part = pl.ds(i * FC_HALF, FC_HALF)
        gathers.append(kind.bind(own_ref.at[:, part], full.at[(*EVERY, part)], sems[steps(i, 2)]))

    @pl.when(t == 0)
    def _():
        gathers[0].meet()
        for gather in gathers:
            gather.begin()

    @pl.when(t == 1)
    def _():
        for gather in gathers:
            gather.turn(1)
    for i in range(2):
        @pl.when(t == i + 2)
        def _():
            gathers[i].turn(2)
    for rows in BLOCKS:
        qkv_ref[rows, :] = (dot(h_ref[rows, :], w_ref[ALL]) + wb_ref[ALL]).astype(BF)

    @pl.when(t == last)
    def _():
        for gather in gathers:
            gather.turn(3)
        for gather in gathers:
            gather.end()


EVERY = [slice(None)] * 5


def qkv_call(h, w, wb, own):
    hbm = pl.BlockSpec(memory_space=pl.ANY)
    return pl.pallas_call(
        qkv_kernel,
        grid=(QKV // QKV_N,),
        in_specs=[whole(TOKENS, WIDTH, pipeline_mode=pl.Buffered(1)), by_cols(WIDTH, QKV_N), by_cols(1, QKV_N), whole(SHARD, FFN)],
        out_specs=[by_cols(TOKENS, QKV_N), hbm],
        out_shape=[jax.ShapeDtypeStruct((TOKENS, QKV), BF), all_blocks(SHARD, FFN)],
        scratch_shapes=FC_ALL[0].scratch() * 2,
        compiler_params=comm_params(QUAD),
        cost_estimate=cost(2 * TOKENS * WIDTH * QKV, 60_000_000),
        name="qkv",
    )(h, w, wb, own)


ROW_CUTS = (0, 24, 48, 80)
FC_SUM = Exchange(SHARD, MLP_F, ROW_CUTS, 0)
PROJ_SUM = Exchange(UNITS, WIDTH, WIDTH_CUTS, 1)
CDF_P = 0.33
CDF_C = (0.1326322871417956, 0.11939570820799192, 0.18103829560051796, -0.08904113226212501,
         0.33075919469138065, -0.22023738432274684, 0.0454530347223348)


def gelu_pair(u):
    bell = jnp.exp2(u * u * (-0.5 * LOG2E))
    t = 1.0 / (1.0 + CDF_P * jnp.abs(u))
    poly = CDF_C[6]
    for c in CDF_C[5::-1]:
        poly = poly * t + c
    tail = poly * t * bell
    cdf = jnp.where(u < 0.0, tail, 1.0 - tail)
    return u * cdf, cdf + u * bell * ((2.0 * math.pi) ** -0.5)


def mlp_kernel(r_hbm, n_hbm, dy_hbm, vec_ref, fc_ref, proj_ref, fcb_ref,
               y_hbm, dr_hbm, dr16_hbm, dfc_ref, dproj_ref, dfcb_ref, small_ref,
               n2, dy, y_acc, dn_acc, g, du, ua, ub, da, db, sem, *comm):
    step = step_id()
    by_row, by_col = FC_SUM.bind(comm[:Exchange.COUNT]), PROJ_SUM.bind(comm[Exchange.COUNT:])

    @pl.when(step == 0)
    def _():
        loads = [pltpu.make_async_copy(n_hbm, n2, sem), pltpu.make_async_copy(dy_hbm, dy, sem)]
        for cp in loads:
            cp.start()
        by_row.meet()
        clear(small_ref, y_acc, dn_acc)
        for cp in loads:
            cp.wait()

    outs = (dfc_ref, dproj_ref)
    advance((by_row, by_col), step, first_chunks(MLP_STEPS), lambda n, exchange, c: exchange.result(c, outs[n]))

    @pl.when(step < MLP_STEPS)
    def _():
        fcb = fcb_ref[ALL]
        fc, proj = fc_ref[ALL], proj_ref[ALL].reshape(MLP_F, WIDTH)
        bias_sum = jnp.zeros((SUBLANE, MLP_F), F32)
        tiles = [(b * MAIN, MAIN) for b in range(IMAGES - 1)] + [((IMAGES - 1) * MAIN, MAIN + IMAGES)]
        pairs = ((ua, da), (ub, db))

        def products(k):
            r, n = tiles[k]
            u_s, d_s = pairs[k % 2]
            u_s[0:n, :] = dot(n2[r:r + n, :], fc)
            d_s[0:n, :] = dot_nt(dy[r:r + n, :], proj)

        def pointwise(k, total):
            r, n = tiles[k]
            u_s, d_s = pairs[k % 2]
            value, slope = gelu_pair(u_s[0:n, :] + fcb)
            g[r:r + n, :] = value.astype(BF)
            grad = d_s[0:n, :] * slope
            du[r:r + n, :] = grad.astype(BF)
            return total + eights(grad)

        products(0)
        for k in range(1, IMAGES):
            products(k)
            bias_sum = pointwise(k - 1, bias_sum)
        bias_sum = pointwise(IMAGES - 1, bias_sum)
        dfcb_ref[ALL] = col_sum(bias_sum)
        y_acc[ALL] += dot(g[ALL], proj)
        for c in range(LANES // 2):
            part = dot_nt(du[ALL], fc_ref[steps(c, MAIN), :])
            dn_acc[2 * c] += part[:, :LANE]
            dn_acc[2 * c + 1] += part[:, LANE:]
        by_col.put_local(step, dot_tn(g[ALL], dy[ALL]))
        by_row.put_local(step, dot_tn(n2[ALL], du[ALL]))

    after = step - MLP_STEPS
    r_copy = pltpu.make_async_copy(r_hbm, n2, sem)
    out_copies = [pltpu.make_async_copy(dn_acc, dr_hbm, sem), pltpu.make_async_copy(n2, dr16_hbm, sem)]
    y_copy = pltpu.make_async_copy(dy, y_hbm, sem)

    def back(r, n):
        wide_r = n2[pl.ds(r, n), :].astype(F32)
        hat, inv = norm_stats(wide_r)
        dn = joined(dn_acc, r, n)
        wide_dy = dy[pl.ds(r, n), :].astype(F32)
        dr = wide_dy + norm_back(dn, hat, inv, vec_ref[steps(LN2_GAIN, 1), :])
        put(dn_acc, r, n, dr)
        n2[pl.ds(r, n), :] = dr.astype(BF)
        y_acc[pl.ds(r, n), :] += wide_r + vec_ref[steps(PROJ_BIAS, 1), :]
        for i, v in enumerate((dn * hat, dn, wide_dy, dr)):
            small_ref[steps(i, SUBLANE), :] += eights(v)

    @pl.when(after == 0)
    def _():
        r_copy.start()
        r_copy.wait()
        back(TAIL, IMAGES)

    @pl.when((after >= 0) & (after < 3))
    def _():
        back_part(back, after, 3)

    @pl.when(after == 2)
    def _():
        for cp in out_copies:
            cp.start()

    @pl.when(after == 3)
    def _():
        for cp in out_copies:
            cp.wait()
        from_image_order(y_acc, dn_acc)

        def narrow(r, n):
            dy[pl.ds(r, n), :] = joined(dn_acc, r, n).astype(BF)
        row_tiles(narrow)
        y_copy.start()

    @pl.when(after == QUAD)
    def _():
        y_copy.wait()


def mlp_call(r, n2, dy, vec, fc, proj, fcb):
    hbm = pl.BlockSpec(memory_space=pl.ANY)
    now = lambda i: jnp.minimum(i, MLP_STEPS - 1)
    done = lambda i: jnp.maximum(i - DRAIN, 0)
    return pl.pallas_call(
        mlp_kernel,
        grid=(MLP_STEPS + DRAIN,),
        in_specs=[hbm, hbm, hbm, whole(*vec.shape), by_cols(WIDTH, MLP_F, now),
                  pl.BlockSpec((PARTS, None, UNITS, WIDTH), lambda i: (0, now(i), 0, 0)),
                  by_cols(1, MLP_F, now)],
        out_specs=[hbm, hbm, hbm, by_cols(SHARD, MLP_F, done),
                   by_rows(UNITS, WIDTH, done),
                   by_cols(1, MLP_F, now), whole(32, WIDTH)],
        out_shape=[jax.ShapeDtypeStruct((TOKENS, WIDTH), BF), jax.ShapeDtypeStruct((LANES, TOKENS, LANE), F32),
                   jax.ShapeDtypeStruct((TOKENS, WIDTH), BF), jax.ShapeDtypeStruct((SHARD, FFN), F32),
                   jax.ShapeDtypeStruct((FFN // PARTS, WIDTH), F32),
                   jax.ShapeDtypeStruct((1, FFN), F32), jax.ShapeDtypeStruct((32, WIDTH), F32)],
        scratch_shapes=[pltpu.VMEM((TOKENS, WIDTH), BF), pltpu.VMEM((TOKENS, WIDTH), BF),
                        pltpu.VMEM((TOKENS, WIDTH), F32), pltpu.VMEM((LANES, TOKENS, LANE), F32),
                        pltpu.VMEM((TOKENS, MLP_F), BF), pltpu.VMEM((TOKENS, MLP_F), BF)]
                       + [pltpu.VMEM((MAIN + IMAGES, MLP_F), F32)] * QUAD + [pltpu.SemaphoreType.DMA]
                       + FC_SUM.scratch() + PROJ_SUM.scratch(),
        compiler_params=comm_params(0),
        cost_estimate=cost(12 * TOKENS * WIDTH * FFN, 150_000_000, TOKENS * FFN),
        name="mlp",
    )(r, n2, dy, vec, fc, proj.reshape(PARTS, MLP_STEPS, UNITS, WIDTH), fcb)


SCALE = HEAD ** -0.5
SCALE2 = SCALE * LOG2E
ATTN_COST = cost(40_000_000_000, 50_000_000, 8_400_000)


def window(h):
    first = min(HEAD * h // LANE * LANE, WIDTH - MAIN)
    wide = LANE if HEAD * h + HEAD <= first + LANE else MAIN
    return first, wide, HEAD * h - first


def lane_mask(h):
    first, wide, off = window(h)
    lane = lax.broadcasted_iota(jnp.int32, (MAIN, wide), 1)
    return (lane >= off) & (lane < off + HEAD)


def thirds(ref, rows=slice(None)):
    return [ref[rows, steps(i, WIDTH)] for i in range(3)]


def head_rows():
    lane = lax.broadcasted_iota(jnp.int32, (HEADS, WIDTH), 1)
    row = lax.broadcasted_iota(jnp.int32, (HEADS, WIDTH), 0)
    return (lane // HEAD == row).astype(F32)


def tail_softmax(s, s_self):
    m = jnp.maximum(jnp.max(s, axis=1, keepdims=True), s_self)
    e = jnp.exp((s - m) * SCALE)
    e_self = jnp.exp((s_self - m) * SCALE)
    inv = 1.0 / (row_sum(e) + e_self)
    return e * inv, e_self * inv


def attn_kernel(qkv_ref, qkvt_ref, x_ref, xt_ref, w_ref, vec_ref, proj_ref, o_hbm, r_hbm, n_hbm,
                max_ref, inv_ref, full,
                tails, o_tail, o_t, ptail, o_buf, r_buf, n_buf, sa, sb, sems, own, *comm):
    b, last = step_id(), pl.num_programs(0) - 1
    slot = b % 2
    gathers = []
    for i, kind in enumerate(PROJ_ALL):
        part = pl.ds(i * PROJ_FIRST, kind.rows)
        gathers.append(kind.bind(own.at[part], full.at[(*EVERY[1:], part)], comm[steps(i, 2)]))

    @pl.when(b == 0)
    def _():
        tails[ALL] = qkvt_ref[ALL].astype(F32)
        own[ALL] = proj_ref[ALL].astype(BF)
        gathers[0].meet()
        for gather in gathers:
            gather.begin()

    for turn, (stage, i) in enumerate(itertools.product((1, 2, 3), range(2))):
        @pl.when(b == turn + 1 + stage // 3)
        def _():
            gathers[i].turn(stage)

    heads = head_rows()
    q_t, k_t, v_t = (heads * z for z in thirds(tails, pl.ds(b, 1)))
    q, k, v = thirds(qkv_ref)

    p, p_self = tail_softmax(dot_nt(q_t.astype(BF), k), row_sum(q_t * k_t))
    mixed = dot(p.astype(BF), v) * heads + p_self.astype(BF).astype(F32) * v_t
    o_tail[pl.ds(b, 1), :] = col_sum(mixed)

    s_tail = dot_nt(k_t.astype(BF), q)
    v_turned = v.T
    scores = sa, sb

    def next_scores(h):
        first, wide, _ = window(h)
        q_h = jnp.where(lane_mask(h), qkv_ref[:, pl.ds(first, wide)], jnp.zeros((), BF))
        scores[h % 2][ALL] = dot_nt(qkv_ref[:, pl.ds(WIDTH + first, wide)], q_h)
    next_scores(0)
    for h in range(HEADS):
        if h + 1 < HEADS:
            next_scores(h + 1)
        s, mine = scores[h % 2], steps(h, 1)
        top = jnp.maximum(col_max(s[ALL]), s_tail[mine, :])
        e = jnp.exp((s[ALL] - top) * SCALE)
        e_tail = jnp.exp((s_tail[mine, :] - top) * SCALE)
        inv = 1.0 / (col_sum(e) + e_tail)
        max_ref[0, mine, :] = top
        inv_ref[0, mine, :] = inv
        ptail[mine, :] = e_tail * inv
        o_t[steps(h, HEAD), :] = dot(v_turned[steps(h, HEAD), :], (e * inv).astype(BF))

    outs = (o_buf, o_hbm), (r_buf, r_hbm), (n_buf, n_hbm)
    out_bias, gain, bias = (vec_ref[steps(i, 1), :] for i in (OUT_BIAS, LN2_GAIN, LN2_BIAS))

    def write(slot, rows, o, x):
        o_buf[slot, rows, :] = o
        r = (x.astype(F32) + dot(o, w_ref[ALL]) + out_bias).astype(BF)
        r_buf[slot, rows, :] = r
        hat, _ = norm_stats(r.astype(F32))
        n_buf[slot, rows, :] = (hat * gain + bias).astype(BF)

    @pl.when(b >= 2)
    def _():
        for n, (buf, hbm) in enumerate(outs):
            out_copy(buf, hbm, slot, b - 2, sems, n).wait()

    o = (o_t[ALL].T + dot_tn(ptail[ALL].astype(BF), v_t.astype(BF))).astype(BF)
    write(slot, slice(None), o, x_ref[ALL])
    for n, (buf, hbm) in enumerate(outs):
        out_copy(buf, hbm, slot, b, sems, n).start()

    @pl.when(b == last)
    def _():
        for n, (buf, hbm) in enumerate(outs):
            out_copy(buf, hbm, 1 - slot, b - 1, sems, n).wait()
        write(1 - slot, slice(IMAGES), o_tail[ALL].astype(BF), xt_ref[ALL])
        copies = [pltpu.make_async_copy(buf.at[1 - slot, pl.ds(0, IMAGES)], hbm.at[pl.ds(TAIL, IMAGES)], sems.at[n, 1 - slot])
                  for n, (buf, hbm) in enumerate(outs)]
        for cp in copies:
            cp.start()
        for cp in copies:
            cp.wait()
        for n, (buf, hbm) in enumerate(outs):
            out_copy(buf, hbm, slot, b, sems, n).wait()
        for gather in gathers:
            gather.end()


def out_copy(buf, hbm, slot, b, sems, n):
    return pltpu.make_async_copy(buf.at[slot], hbm.at[pl.ds(pl.multiple_of(b * MAIN, MAIN), MAIN)], sems.at[n, slot])


def attn_call(qkv, xim, w, vec, proj):
    hbm = pl.BlockSpec(memory_space=pl.ANY)
    main = lambda n: by_rows(MAIN, n)
    tail = lambda n: by_rows(IMAGES, n, lambda i: TAIL // IMAGES)
    stat = pl.BlockSpec((1, HEADS, MAIN), lambda i: (i, 0, 0))
    return pl.pallas_call(
        attn_kernel,
        grid=(IMAGES,),
        in_specs=[main(QKV), tail(QKV), main(WIDTH), tail(WIDTH),
                  whole(WIDTH, WIDTH), whole(*vec.shape), whole(*proj.shape)],
        out_specs=[hbm, hbm, hbm, stat, stat, hbm],
        out_shape=[*[jax.ShapeDtypeStruct((TOKENS, WIDTH), BF)] * 3,
                   jax.ShapeDtypeStruct((IMAGES, HEADS, MAIN), F32), jax.ShapeDtypeStruct((IMAGES, HEADS, MAIN), F32),
                   all_blocks(*proj.shape)],
        scratch_shapes=[pltpu.VMEM((IMAGES, QKV), F32), pltpu.VMEM((IMAGES, WIDTH), F32),
                        pltpu.VMEM((WIDTH, MAIN), F32), pltpu.VMEM((HEADS, MAIN), F32),
                        *[pltpu.VMEM((2, MAIN, WIDTH), BF)] * 3, *[pltpu.VMEM((MAIN, MAIN), F32)] * 2, pltpu.SemaphoreType.DMA((3, 2)),
                        pltpu.VMEM(proj.shape, BF)] + PROJ_ALL[0].scratch() * 2,
        compiler_params=comm_params(5),
        cost_estimate=ATTN_COST,
        name="attn",
    )(qkv, qkv, xim, xim, w, vec, proj)


def outb_kernel(dr_ref, o_ref, w_ref, dfc_ref, y_in, dproj_in, do_ref, dw_ref, dfc_out, y_out, dproj_out, y, dproj, sems):
    c, last = step_id(), pl.num_programs(0) - 1
    loads = [pltpu.make_async_copy(src, dst, sems.at[i]) for i, (src, dst) in enumerate(((y_in, y), (dproj_in, dproj)))]
    stores = [pltpu.make_async_copy(src, dst, sems.at[i]) for i, (src, dst) in enumerate(((y, y_out), (dproj, dproj_out)))]

    @pl.when(c == 0)
    def _():
        for cp in loads:
            cp.start()

    @pl.when(c == 1)
    def _():
        for cp in loads:
            cp.wait()
        for cp in stores:
            cp.start()

        def store_fc(tile, values):
            dfc_out[:, steps(tile, LANE)] = values
        regroup(SHARD, lambda n: n % MLP_STEPS * PARTS + n // MLP_STEPS, lambda tile: dfc_ref[:, steps(tile, LANE)], store_fc)
    do_ref[ALL] = dot_nt(dr_ref[ALL], w_ref[ALL]).astype(BF)
    dw_ref[ALL] = dot_tn(o_ref[ALL], dr_ref[:, pl.ds(pl.multiple_of(c * MAIN, MAIN), MAIN)])

    @pl.when(c == last)
    def _():
        for cp in stores:
            cp.wait()


def outb_call(dr, o, w, dfc, y, dproj):
    full, hbm = whole(TOKENS, WIDTH), pl.BlockSpec(memory_space=pl.ANY)
    like = lambda v: jax.ShapeDtypeStruct(v.shape, v.dtype)
    return pl.pallas_call(
        outb_kernel,
        grid=(WIDTH // MAIN,),
        in_specs=[full, full, by_rows(MAIN, WIDTH), whole(*dfc.shape), hbm, hbm],
        out_specs=[by_cols(TOKENS, MAIN), by_cols(WIDTH, MAIN), whole(*dfc.shape), hbm, hbm],
        out_shape=[like(dr), jax.ShapeDtypeStruct((WIDTH, WIDTH), F32), like(dfc), like(y), like(dproj)],
        scratch_shapes=[pltpu.VMEM(y.shape, BF), pltpu.VMEM(dproj.shape, F32), pltpu.SemaphoreType.DMA((2,))],
        compiler_params=pltpu.CompilerParams(dimension_semantics=("arbitrary",), vmem_limit_bytes=VMEM_MAX),
        cost_estimate=cost(QUAD * TOKENS * WIDTH * WIDTH, 50_000_000),
        name="outb",
    )(dr, o, w, dfc, y, dproj)


def attn_back_kernel(qkv_ref, qkvt_ref, do_ref, dot_ref, max_ref, inv_ref, dw_ref, dqkv_hbm, dwb_ref, dwout_ref,
                     tails, do_tails, grad_tails, dq_t, dk, dv, ds_tail, sa, da, sb, db, buf, sems, *comm):
    b = step_id()
    by_row = OUT_SUM.bind(comm)

    @pl.when(b == 0)
    def _():
        by_row.meet()

    @pl.when(b < OUT_STEPS)
    def _():
        by_row.put_local(b, dw_ref[ALL])
    advance((by_row,), b + 1, first_chunks(OUT_STEPS), lambda n, exchange, c: exchange.result(c, dwout_ref))

    @pl.when(b < IMAGES)
    def _():
        image_back(b, qkv_ref, qkvt_ref, do_ref, dot_ref, max_ref, inv_ref, dqkv_hbm, dwb_ref,
                   tails, do_tails, grad_tails, dq_t, dk, dv, ds_tail, ((sa, da), (sb, db)), buf, sems)


OUT_N = MAIN
OUT_STEPS = WIDTH // OUT_N
OUT_SUM = Exchange(SHARD, OUT_N, ROW_CUTS, 0)


def image_back(b, qkv_ref, qkvt_ref, do_ref, dot_ref, max_ref, inv_ref, dqkv_hbm, dwb_ref,
               tails, do_tails, grad_tails, dq_t, dk, dv, ds_tail, ahead, buf, sems):
    last = IMAGES - 1
    slot = b % 2

    @pl.when(b == 0)
    def _():
        tails[ALL] = qkvt_ref[ALL].astype(F32)
        do_tails[ALL] = dot_ref[ALL].astype(F32)
        clear(dwb_ref)

    heads = head_rows()
    q_t, k_t, v_t = (heads * z for z in thirds(tails, pl.ds(b, 1)))
    do_t = heads * do_tails[pl.ds(b, 1), :]
    q, k, v = thirds(qkv_ref)
    do = do_ref[ALL]
    q_t16, k_t16, v_t16, do_t16 = (z.astype(BF) for z in (q_t, k_t, v_t, do_t))

    p, p_self = tail_softmax(dot_nt(q_t16, k), row_sum(q_t * k_t))
    dp, dp_self = dot_nt(do_t16, v), row_sum(do_t * v_t)
    inner = row_sum(p * dp) + p_self * dp_self
    ds16 = (p * (dp - inner) * SCALE).astype(BF)
    ds_self = (p_self * (dp_self - inner) * SCALE).astype(BF).astype(F32)
    grad_q = col_sum(dot(ds16, k) * heads + ds_self * k_t)
    grad_k = ds_self * q_t
    grad_v = p_self.astype(BF).astype(F32) * do_t
    dk[ALL] = dot_tn(ds16, q_t16)
    dv[ALL] = dot_tn(p.astype(BF), do_t16)

    p_tail = jnp.exp2((dot_nt(k_t16, q) - max_ref[0]) * SCALE2) * inv_ref[0]
    dp_tail = dot_nt(v_t16, do)
    inner_tail = p_tail * dp_tail

    k_turned = k.T

    def masked(h):
        first, wide, _ = window(h)
        here, mask = pl.ds(first, wide), lane_mask(h)
        return here, jnp.where(mask, qkv_ref[:, here], jnp.zeros((), BF)), jnp.where(mask, do_ref[:, here], jnp.zeros((), BF))

    def next_products(h):
        first, wide, _ = window(h)
        _, q_h, do_h = masked(h)
        ahead[h % 2][0][ALL] = dot_nt(qkv_ref[:, pl.ds(WIDTH + first, wide)], q_h)
        ahead[h % 2][1][ALL] = dot_nt(qkv_ref[:, pl.ds(2 * WIDTH + first, wide)], do_h)
    next_products(0)
    for h in range(HEADS):
        if h + 1 < HEADS:
            next_products(h + 1)
        here, q_h, do_h = masked(h)
        mine = steps(h, 1)
        s, dp = (ref[ALL] for ref in ahead[h % 2])
        p = jnp.exp2((s - max_ref[0, mine, :]) * SCALE2) * inv_ref[0, mine, :]
        inner = col_sum(p * dp) + inner_tail[mine, :]
        ds = (p * (dp - inner) * SCALE).astype(BF)
        dv[:, here] += dot(p.astype(BF), do_h)
        dk[:, here] += dot(ds, q_h)
        dq_t[steps(h, HEAD), :] = dot(k_turned[steps(h, HEAD), :], ds)
        ds_tail[mine, :] = p_tail[mine, :] * (dp_tail[mine, :] - inner) * SCALE

    ds_tail16 = ds_tail[ALL].astype(BF)
    grad_k = col_sum(grad_k + dot(ds_tail16, q) * heads)
    grad_v = col_sum(grad_v + dot(p_tail.astype(BF), do) * heads)

    @pl.when(b >= 2)
    def _():
        out_copy(buf, dqkv_hbm, slot, b - 2, sems, 0).wait()

    grad = dq_t[ALL].T + dot_tn(ds_tail16, k_t16)
    for n, (main, tail) in enumerate(((grad, grad_q), (dk[ALL], grad_k), (dv[ALL], grad_v))):
        here = steps(n, WIDTH)
        buf[slot, :, here] = main.astype(BF)
        grad_tails[pl.ds(b, 1), here] = tail
        dwb_ref[:, here] += col_sum(main) + tail
    out_copy(buf, dqkv_hbm, slot, b, sems, 0).start()

    @pl.when(b == last)
    def _():
        out_copy(buf, dqkv_hbm, 1 - slot, b - 1, sems, 0).wait()
        buf[1 - slot, 0:IMAGES, :] = grad_tails[ALL].astype(BF)
        cp = pltpu.make_async_copy(buf.at[1 - slot, pl.ds(0, IMAGES)], dqkv_hbm.at[pl.ds(TAIL, IMAGES)], sems.at[0, 1 - slot])
        cp.start()
        cp.wait()
        out_copy(buf, dqkv_hbm, slot, b, sems, 0).wait()


def attn_back_call(qkv, do, top, inv, dw):
    hbm = pl.BlockSpec(memory_space=pl.ANY)
    image = lambda i: jnp.minimum(i, IMAGES - 1)
    main = lambda n: by_rows(MAIN, n, image)
    tail = lambda n: by_rows(IMAGES, n, lambda i: TAIL // IMAGES)
    stat = pl.BlockSpec((1, HEADS, MAIN), lambda i: (image(i), 0, 0))
    return pl.pallas_call(
        attn_back_kernel,
        grid=(OUT_STEPS + DRAIN - 1,),
        in_specs=[main(QKV), tail(QKV), main(WIDTH), tail(WIDTH), stat, stat,
                  by_cols(WIDTH, OUT_N, lambda i: jnp.minimum(i, OUT_STEPS - 1))],
        out_specs=[hbm, whole(1, QKV), by_cols(SHARD, OUT_N, lambda i: jnp.clip(i + 1 - DRAIN, 0, OUT_STEPS - 1))],
        out_shape=[jax.ShapeDtypeStruct((TOKENS, QKV), BF), jax.ShapeDtypeStruct((1, QKV), F32),
                   jax.ShapeDtypeStruct((SHARD, WIDTH), F32)],
        scratch_shapes=[pltpu.VMEM((IMAGES, QKV), F32), pltpu.VMEM((IMAGES, WIDTH), F32),
                        pltpu.VMEM((IMAGES, QKV), F32), pltpu.VMEM((WIDTH, MAIN), F32),
                        pltpu.VMEM((MAIN, WIDTH), F32), pltpu.VMEM((MAIN, WIDTH), F32), pltpu.VMEM((HEADS, MAIN), F32),
                        *[pltpu.VMEM((MAIN, MAIN), F32)] * QUAD, pltpu.VMEM((2, MAIN, QKV), BF), pltpu.SemaphoreType.DMA((1, 2))] + OUT_SUM.scratch(),
        compiler_params=comm_params(1),
        cost_estimate=ATTN_COST,
        name="attn_back",
    )(qkv, qkv, do, do, top, inv, dw)


QB_N = MAIN
QB_STEPS = QKV // QB_N
QKV_SUM = Exchange(SHARD, QB_N, ROW_CUTS, 0, 2)
VECTOR_SUM = Exchange(3 * SUBLANE, LANE, (0, SUBLANE, 2 * SUBLANE, 3 * SUBLANE), 0)
VECTOR_STEP = QB_STEPS + 2
QB_GRID = QB_STEPS + 1 + QUAD * QKV_SUM.stride


def qkvb_kernel(xim_hbm, dr_hbm, vec_ref, sums_ref, qb_ref, fb_ref, ht_ref, dqkv_ref, w_ref, dx_hbm, dw_ref, out_vec_ref,
                acc, dr, xd, sums, sems, *comm):
    t = step_id()
    by_row, by_vector = QKV_SUM.bind(comm[:Exchange.COUNT]), VECTOR_SUM.bind(comm[Exchange.COUNT:])
    loads = [pltpu.make_async_copy(dr_hbm, dr, sems.at[0]), pltpu.make_async_copy(xim_hbm, xd, sems.at[1])]
    store = pltpu.make_async_copy(xd, dx_hbm, sems.at[1])

    def put_row(place, row, lane, values):
        by_vector.local[(0, *place, pl.ds(row, len(values)), pl.ds(lane, values.shape[1]))] = values

    def share(row, values):
        for d, place in enumerate(DEVICES):
            put_row(place, row, 0, values[:, steps(d, SHARD)])

    @pl.when(t == 0)
    def _():
        by_row.meet()
        for cp in loads:
            cp.start()
        clear(acc, sums)
        by_vector.local[0] = jnp.zeros(by_vector.blocks, F32)
        share(0, jnp.concatenate([col_sum(sums_ref[steps(i, SUBLANE), :]) for i in range(QUAD)], axis=0))
        for d, place in enumerate(DEVICES):
            for i in range(3):
                put_row(place, QUAD + i, 0, qb_ref[:, pl.ds((3 * d + i) * SHARD, SHARD)])
            for n in range(MLP_STEPS):
                put_row(place, QUAD + 3 + n * UNITS // SHARD, n * UNITS % SHARD, fb_ref[:, pl.ds(n * MLP_F + d * UNITS, UNITS)])

    def emit_vectors(n, exchange, c):
        for part, (rows, _) in enumerate(exchange.parts[:2]):
            out_vec_ref[rows, :] = exchange.held[3][part][0, :, :SHARD]
    advance((by_row,), t, first_chunks(QB_STEPS), lambda n, exchange, c: exchange.result(c, dw_ref))
    advance((by_vector,), t - VECTOR_STEP, first_chunks(1), emit_vectors)

    @pl.when(t < QB_STEPS)
    def _():
        by_row.put_local(t, dot(ht_ref[ALL], dqkv_ref[ALL]))
        acc[ALL] += dot_nt(dqkv_ref[ALL], w_ref[ALL])

    @pl.when(t == QB_STEPS)
    def _():
        for cp in loads:
            cp.wait()

    def back(r, n):
        hat, inv = norm_stats(xd[pl.ds(r, n), :].astype(F32))
        dn = acc[pl.ds(r, n), :]
        for i, v in enumerate((dn * hat, dn)):
            sums[steps(i, SUBLANE), :] += eights(v)
        acc[pl.ds(r, n), :] = joined(dr, r, n) + norm_back(dn, hat, inv, vec_ref[steps(LN1_GAIN, 1), :])

    @pl.when((t >= QB_STEPS) & (t <= VECTOR_STEP))
    def _():
        back_part(back, t - QB_STEPS, 3)

    @pl.when(t == VECTOR_STEP)
    def _():
        back(TAIL, IMAGES)
        share(VECTOR_ROWS - 2, jnp.concatenate([col_sum(sums[steps(i, SUBLANE), :]) for i in range(2)], axis=0))

    @pl.when(t == VECTOR_STEP + 1)
    def _():
        from_image_order(acc, dr)

    @pl.when(t == VECTOR_STEP + 2)
    def _():
        def narrow(r, n):
            xd[pl.ds(r, n), :] = joined(dr, r, n).astype(BF)
        row_tiles(narrow)
        store.start()

    @pl.when(t == QB_GRID - 1)
    def _():
        store.wait()


DEVICES = list(itertools.product(range(2), repeat=QUAD))


def qkvb_call(xim, dr, vec, sums, qb, fb, ht, dqkv, w):
    hbm = pl.BlockSpec(memory_space=pl.ANY)
    now = lambda i: jnp.minimum(i, QB_STEPS - 1)
    return pl.pallas_call(
        qkvb_kernel,
        grid=(QB_GRID,),
        in_specs=[hbm, hbm, *(whole(*v.shape) for v in (vec, sums, qb, fb)),
                  whole(WIDTH, TOKENS, pipeline_mode=pl.Buffered(1)), by_cols(TOKENS, QB_N, now), by_cols(WIDTH, QB_N, now)],
        out_specs=[hbm, by_cols(SHARD, QB_N, lambda i: jnp.clip(i - 1 - QUAD * QKV_SUM.stride, 0, QB_STEPS - 1)),
                   whole(VECTOR_ROWS, SHARD)],
        out_shape=[jax.ShapeDtypeStruct((TOKENS, WIDTH), BF), jax.ShapeDtypeStruct((SHARD, QKV), F32),
                   jax.ShapeDtypeStruct((VECTOR_ROWS, SHARD), F32)],
        scratch_shapes=[pltpu.VMEM((TOKENS, WIDTH), F32), pltpu.VMEM((LANES, TOKENS, LANE), F32), pltpu.VMEM((TOKENS, WIDTH), BF),
                        pltpu.VMEM((2 * SUBLANE, WIDTH), F32), pltpu.SemaphoreType.DMA((2,))]
                       + QKV_SUM.scratch() + VECTOR_SUM.scratch(),
        compiler_params=comm_params(2),
        cost_estimate=cost(QUAD * TOKENS * WIDTH * QKV, 80_000_000),
        name="qkvb",
    )(xim, dr, vec, sums, qb, fb, ht, dqkv, w)


def solution(mesh):
    specs = (P("fsdp"),) * 14

    def device_step(resid_in, grad_out, ln1_gain, ln1_bias, qkv_weight, qkv_bias, out_weight, out_bias,
                    ln2_gain, ln2_bias, fc_weight, fc_bias, proj_weight, proj_bias):
        rows = jnp.concatenate([ln1_gain, ln1_bias, qkv_bias, out_bias, ln2_gain, ln2_bias, fc_bias, proj_bias]).reshape(-1, SHARD)
        rows = jnp.pad(rows, ((0, VECTOR_ROWS - len(rows)), (0, LANE - SHARD)))
        x = resid_in.swapaxes(0, 1).reshape(TOKENS, WIDTH)
        dy = grad_out.swapaxes(0, 1).reshape(TOKENS, WIDTH)
        xim, dyim, h, ht, rows, bq, bf, fc, wq, wo = open_call(x, dy, rows, fc_weight, qkv_weight, out_weight)
        wq, wo = wq.reshape(WIDTH, QKV), wo.reshape(WIDTH, WIDTH)
        qkv, wf = qkv_call(h, wq, bq, fc)
        o, r, n2, top, inv, wp = attn_call(qkv, xim, wo, rows, proj_weight)
        y, dr, dr16, dwf, dwp, dbf, small = mlp_call(r, n2, dyim, rows, wf.reshape(WIDTH, FFN), wp, bf)
        do, dwo, dwf, y, dwp = outb_call(dr16, o, wo, dwf, y, dwp)
        dqkv, dbq, dwo = attn_back_call(qkv, do, top, inv, dwo)
        dx, dwq, vec = qkvb_call(xim, dr, rows, small, dbq, dbf, ht, dqkv, wq)
        dg2, db2, dbp, dbo = vec[:4]
        dbq, dbf = vec[4:7].reshape(-1), vec[7:11].reshape(-1)
        dg1, db1 = vec[VECTOR_ROWS - 2:]
        unturn = lambda t: t.reshape(SEQ, IMAGES, WIDTH).swapaxes(0, 1)
        return (unturn(y), unturn(dx), dg1, db1, dwq, dbq, dwo, dbo, dg2, db2, dwf, dbf, dwp, dbp)

    return jax.shard_map(device_step, mesh=mesh, in_specs=specs, out_specs=specs, check_vma=False)
```

```python
import itertools
import math
import jax, jax.numpy as jnp
from jax import lax
from jax.experimental import pallas as pl
from jax.experimental.pallas import tpu as pltpu
from jax.sharding import PartitionSpec as P

BF, F32 = jnp.bfloat16, jnp.float32
IMAGES, SEQ, WIDTH, FFN, HEADS, HEAD = 8, 257, 1280, 5120, 16, 80
MAIN = SEQ - 1
TOKENS = IMAGES * SEQ
TAIL = IMAGES * MAIN
LN_EPS = 1e-5
LOG2E = math.log2(math.e)
VMEM_MAX = 67043328
LANE, SUBLANE, QUAD, QKV = 128, 8, 4, 3 * WIDTH
ALL = ...
TORUS = (2,) * QUAD
LANES = WIDTH // LANE
ROWS = 32


def dot(a, b):
    return jnp.dot(a, b, preferred_element_type=F32)


def dot_nt(a, b):
    return lax.dot_general(a, b, (((1,), (1,)), ((), ())), preferred_element_type=F32)


def dot_tn(a, b):
    return lax.dot_general(a, b, (((0,), (0,)), ((), ())), preferred_element_type=F32)


def col_sum(v):
    return jnp.sum(v, axis=0, keepdims=True)


def col_max(v):
    return jnp.max(v, axis=0, keepdims=True)


def row_sum(v):
    return jnp.sum(v, axis=-1, keepdims=True)


def row_mean(v):
    return row_sum(v) * (1.0 / WIDTH)


def clear(*refs):
    for ref in refs:
        ref[ALL] = jnp.zeros_like(ref)


def step_id():
    return pl.program_id(0)


def cost(flops, bytes_accessed, transcendentals=0):
    return pl.CostEstimate(flops=flops, bytes_accessed=bytes_accessed, transcendentals=transcendentals)


def eights(v):
    return jnp.sum(v.reshape(v.shape[0] // SUBLANE, SUBLANE, v.shape[1]), axis=0)


def whole(*shape, **kw):
    return pl.BlockSpec(shape, lambda *i: (0,) * len(shape), **kw)


def by_cols(rows, cols, at=lambda i: i):
    return pl.BlockSpec((rows, cols), lambda i: (0, at(i)))


def by_rows(rows, cols, at=lambda i: i):
    return pl.BlockSpec((rows, cols), lambda i: (at(i), 0))


def steps(first, wide):
    return slice(first * wide, (first + 1) * wide)


def regroup(rows, source, load, store):
    groups = LANE // UNITS
    lane = lax.broadcasted_iota(jnp.int32, (rows, LANE), 1) // UNITS
    for tile in range(FFN // LANE):
        out = None
        for i in range(groups):
            n = source(tile * groups + i)
            piece = load(n // groups)
            shift = (i - n) % groups
            if shift:
                piece = pltpu.roll(piece, shift * UNITS, 1)
            out = piece if out is None else jnp.where(lane == i, piece, out)
        store(tile, out)


def norm_stats(values):
    mean = row_mean(values)
    centered = values - mean
    inv = lax.rsqrt(row_mean(centered * centered) + LN_EPS)
    return centered * inv, inv


BLOCKS = [slice(i * 512, i * 512 + 512) for i in range(3)] + [slice(1536, TOKENS)]


def row_tiles(body, step=LANE):
    def loop(i, carry):
        body(pl.multiple_of(i * step, step), step)
        return carry
    lax.fori_loop(0, TAIL // step, loop, 0)
    body(TAIL, IMAGES)


def back_part(body, part, parts):
    tiles = -(-TAIL // ROWS // parts)

    def loop(i, carry):
        tile = part * tiles + i

        @pl.when(tile < TAIL // ROWS)
        def _():
            body(pl.multiple_of(tile * ROWS, ROWS), ROWS)
        return carry
    lax.fori_loop(0, tiles, loop, 0)


def to_image_order(wide, place, step=LANE):
    per = MAIN // step
    def loop(i, carry):
        first = (i % per) * (step * IMAGES) + i // per
        rows = [wide[c, pl.ds(first, step, stride=IMAGES), :] for c in range(LANES)]
        place(pl.multiple_of(i * step, step), step, jnp.concatenate(rows, axis=1))
        return carry
    lax.fori_loop(0, IMAGES * per, loop, 0)
    place(TAIL, IMAGES, joined(wide, TAIL, IMAGES))


def from_image_order(values, wide):
    def loop(i, carry):
        rows = values[pl.ds(pl.multiple_of(i * LANE, LANE), LANE), :]
        for c in range(LANES):
            wide[c, pl.ds((i % 2) * (LANE * IMAGES) + i // 2, LANE, stride=IMAGES), :] = rows[:, steps(c, LANE)]
        return carry
    lax.fori_loop(0, 2 * IMAGES, loop, 0)
    put(wide, TAIL, IMAGES, values[pl.ds(TAIL, IMAGES), :])


def joined(wide, r, n):
    return jnp.concatenate([wide[c, pl.ds(r, n), :] for c in range(LANES)], axis=1)


def put(wide, r, n, values):
    for c in range(LANES):
        wide[c, pl.ds(r, n), :] = values[:, steps(c, LANE)]


def norm_back(dn, hat, inv, gain):
    dhat = dn * gain
    m1 = row_mean(dhat)
    m2 = row_mean(dhat * hat)
    return inv * (dhat - m1 - hat * m2)


ORDERS = ((2, 1, 0), (1, 0, 2), (0, 2, 1))


def all_blocks(rows, cols):
    return jax.ShapeDtypeStruct((*TORUS, rows, cols), BF)


class Links:
    def find(self, send, recv):
        self.send, self.recv = send, recv
        me = lax.axis_index("fsdp")
        self.core = me % 2
        self.at = (me // SUBLANE, (me // QUAD) % 2, (me // 2) % 2)
        self.other_core = me + 1 - 2 * self.core
        self.other = [me + step - 2 * step * place for step, place in zip((SUBLANE, QUAD, 2), self.at)]
        return self

    def meet(self):
        barrier = pltpu.get_barrier_semaphore()
        devices = (self.other_core, *self.other)
        for device in devices:
            pl.semaphore_signal(barrier, inc=1, device_id=(device,), device_id_type=pl.DeviceIdType.MESH)
        pl.semaphore_wait(barrier, len(devices))

    def remote(self, src, dst, sem, device):
        return pltpu.make_async_remote_copy(src_ref=src, dst_ref=dst, send_sem=self.send.at[sem], recv_sem=self.recv.at[sem],
                                            device_id=(device,), device_id_type=pl.DeviceIdType.MESH)


class Gather(Links):
    COUNT = 2

    def __init__(self, rows, cols, cuts, by_rows):
        self.rows, self.cols, self.cuts, self.by_rows = rows, cols, cuts, by_rows
        self.parts = range(len(cuts) - 1)
        self.full_shape = all_blocks(rows, cols)

    def scratch(self):
        return [pltpu.SemaphoreType.DMA((SEMS,))] * self.COUNT

    def bind(self, own, full, sems):
        self.own, self.full = own, full
        return self.find(*sems)

    def region(self, part, known, arrived=False, half=None):
        done = ORDERS[part][:known]
        place = [slice(None) if a in done else self.at[a] for a in range(3)]
        if half is not None:
            place[done[0]] = half
        if arrived:
            place[done[-1]] = 1 - self.at[done[-1]]
        cut = pl.ds(self.cuts[part], self.cuts[part + 1] - self.cuts[part])
        return (*place, self.core, cut, slice(None)) if self.by_rows else (*place, self.core, slice(None), cut)

    def hop(self, stage, part, half):
        where = self.full.at[self.region(part, stage - 1, half=half)]
        source = self.own.at[self.region(part, 0)[-2:]] if stage == 1 else where
        return self.remote(source, where, self.sem(stage, part, half), self.other[ORDERS[part][stage - 1]])

    def forward(self, stage, part, half=None):
        if stage == 0:
            return self.remote(self.own, self.full.at[(*self.at, self.core)], 0, self.other_core)
        where = self.full.at[self.region(part, stage, True, half)]
        return self.remote(where, where, self.sem(stage + QUAD, part, half), self.other_core)

    def sem(self, row, part, half):
        return QUAD * (row + (half or 0)) + part

    def halves(self, stage):
        return (None,) if stage < 3 else range(2)

    def keep(self):
        return pltpu.make_async_copy(self.own, self.full.at[(*self.at, self.core)], self.send.at[1])

    def begin(self):
        for part in self.parts:
            self.hop(1, part, None).start()
        self.forward(0, 0).start()
        self.keep().start()

    def turn(self, stage):
        if stage == 1:
            self.keep().wait()
        for half in self.halves(stage):
            for part in self.parts:
                self.hop(stage, part, half).wait()
                if stage < 3:
                    for onward in self.halves(stage + 1):
                        self.hop(stage + 1, part, onward).start()
            for part in self.parts:
                self.forward(stage, part, half).start()

    def end(self):
        self.forward(0, 0).wait()
        for stage in range(1, QUAD):
            for half in self.halves(stage):
                for part in self.parts:
                    self.forward(stage, part, half).wait()


SEMS = 36


class Exchange(Links):
    def __init__(self, rows, cols, cuts, along, stride=1, spare=0):
        self.rows, self.cols, self.stride = rows, cols, stride
        self.slots, self.locals = 3 * stride + spare, 1 + stride
        self.blocks = (*TORUS, rows, cols)
        self.parts = [((slice(a, b), slice(None)) if along == 0 else (slice(None), slice(a, b))) for a, b in zip(cuts, cuts[1:])]
        self.shapes = [((b - a, cols) if along == 0 else (rows, b - a)) for a, b in zip(cuts, cuts[1:])]

    def scratch(self):
        out = [pltpu.VMEM((self.locals, *self.blocks), F32), pltpu.VMEM((self.slots, *TORUS[1:], self.rows, self.cols), F32)]
        for axes in (2, 1, 0):
            out += [pltpu.VMEM((self.slots, *TORUS[:axes], *shape), F32) for shape in self.shapes]
        return out + [pltpu.SemaphoreType.DMA((10, self.slots))] * 2

    COUNT = 13

    def bind(self, refs):
        self.local, self.pair, *rest = refs
        self.held = [None, *(rest[steps(i, 3)] for i in range(3))]
        return self.find(*rest[9:])

    def index(self, stage, part, side):
        order = ORDERS[part]
        left = [a for a in range(3) if a not in order[:stage - 1]]
        axis = order[stage - 1]
        where = self.at[axis] if side else 1 - self.at[axis]
        return tuple(where if a == axis else slice(None) for a in left)

    def copy(self, stage, part, c):
        slot = c % self.slots
        if stage == 0:
            return self.remote(self.local.at[c % self.locals, :, :, :, 1 - self.core], self.pair.at[slot], (0, slot), self.other_core)
        source = self.pair if stage == 1 else self.held[stage - 1][part]
        tail = self.parts[part] if stage == 1 else ()
        return self.remote(source.at[(slot, *self.index(stage, part, False), *tail)], self.held[stage][part].at[slot],
                           (3 * stage - 2 + part, slot), self.other[ORDERS[part][stage - 1]])

    def start(self, stage, c):
        for part in range(1 if stage == 0 else 3):
            self.copy(stage, part, c).start()

    def wait(self, stage, c):
        for part in range(1 if stage == 0 else 3):
            self.copy(stage, part, c).wait()

    def add(self, stage, c):
        slot = c % self.slots
        if stage == 0:
            for chip in itertools.product(range(2), repeat=3):
                self.pair[(slot, *chip)] += self.local[(c % self.locals, *chip, self.core)]
            return
        for part in range(3):
            source = self.pair if stage == 1 else self.held[stage - 1][part]
            tail = self.parts[part] if stage == 1 else ()
            for place in itertools.product(range(2), repeat=3 - stage):
                free = iter(place)
                kept = tuple(next(free) if isinstance(i, slice) else i for i in self.index(stage, part, True))
                self.held[stage][part][(slot, *place)] += source[(slot, *kept, *tail)]

    def result(self, c, out_ref):
        for part in range(3):
            out_ref[self.parts[part]] = self.held[3][part][c % self.slots]

    def put_local(self, c, values):
        self.local[c % self.locals] = values.reshape(self.blocks)


def comm_params(n):
    return pltpu.CompilerParams(dimension_semantics=("arbitrary",), vmem_limit_bytes=VMEM_MAX, collective_id=n, has_side_effects=True)


def advance(exchanges, t, exists, emit):
    for stage in (3, 2, 1, 0):
        c = t - 1 - (stage + 1) * exchanges[0].stride

        @pl.when(exists(c))
        def _():
            for n, exchange in enumerate(exchanges):
                exchange.wait(stage, c)
                exchange.add(stage, c)
                if stage < 3:
                    exchange.start(stage + 1, c)
                else:
                    emit(n, exchange, c)

    @pl.when(exists(t - 1))
    def _():
        for exchange in exchanges:
            exchange.start(0, t - 1)


def first_chunks(n):
    return lambda c: (c >= 0) & (c < n)


DRAIN = 5


PARTS = 16
SHARD = WIDTH // PARTS
VECTOR_ROWS = PARTS
LN1_GAIN, LN1_BIAS, QKV_BIAS, OUT_BIAS, LN2_GAIN, LN2_BIAS, FC_BIAS, PROJ_BIAS = 0, 1, 2, 5, 6, 7, 8, 12
MLP_F = MAIN
UNITS = MLP_F // PARTS
MLP_STEPS = FFN // MLP_F
WIDTH_CUTS = (0, 384, 896, WIDTH)
QKV_ALL = Gather(SHARD, QKV, (0, WIDTH, 2 * WIDTH, QKV), False)
OUT_ALL = Gather(SHARD, WIDTH, (0, 384, 768, WIDTH), False)
FC_HALF = FFN // 2
FC_ALL = [Gather(SHARD, FC_HALF, (0, 896, 1792, FC_HALF), False) for _ in range(2)]
PROJ_FIRST = 144
PROJ_ALL = [Gather(PROJ_FIRST, WIDTH, (0, 48, 96, PROJ_FIRST), True), Gather(FFN // PARTS - PROJ_FIRST, WIDTH, (0, 64, 128, 176), True)]
VECTOR_ALL = Gather(SHARD, LANE, (0, SHARD), True)


def open_kernel(x_hbm, dy_hbm, rows_ref, fc_ref, wq_ref, wo_ref, xim_hbm, dyim_hbm, h_hbm, ht_hbm, vec_ref, qb_ref, fb_ref, fc_own, wq_full, wo_full,
                x, dy, wide, h, ht, rows, vec_own, vec_full, wq_own, wo_own, sems, *comm):
    loads = [pltpu.make_async_copy(src, dst, sems.at[i]) for i, (src, dst) in enumerate(((x_hbm, x), (dy_hbm, dy)))]
    for cp in loads:
        cp.start()
    clear(rows)
    rows[:VECTOR_ROWS, :] = rows_ref[ALL]
    vec_own[ALL] = rows[ALL].T[:SHARD, :].astype(BF)
    wq_own[ALL] = wq_ref[ALL].astype(BF)
    wo_own[ALL] = wo_ref[ALL].astype(BF)
    pairs = [comm[steps(i, 2)] for i in range(3)]
    vectors = VECTOR_ALL.bind(vec_own, vec_full, pairs[0])
    weights = QKV_ALL.bind(wq_own, wq_full, pairs[1]), OUT_ALL.bind(wo_own, wo_full, pairs[2])
    gathers = (vectors, *weights)
    vectors.meet()
    for gather in gathers:
        gather.begin()
    for cp in loads:
        cp.wait()

    def reorder(tokens):
        def widen(r, n):
            put(wide, r, n, tokens[pl.ds(r, n), :].astype(F32))
        row_tiles(widen)

        def place(r, n, values):
            tokens[pl.ds(r, n), :] = values.astype(BF)
        to_image_order(wide, place)
    reorder(x)
    for gather in gathers:
        gather.turn(1)
    reorder(dy)
    for gather in gathers:
        gather.turn(2)
    vectors.turn(3)
    vectors.end()
    vec_ref[ALL] = vec_full[ALL].reshape(WIDTH, LANE).astype(F32).T[:VECTOR_ROWS, :]
    gain, bias = vec_ref[steps(LN1_GAIN, 1), :], vec_ref[steps(LN1_BIAS, 1), :]
    for d in range(PARTS):
        for i in range(3):
            qb_ref[:, steps(3 * d + i, SHARD)] = vec_ref[steps(QKV_BIAS + i, 1), steps(d, SHARD)]
        for n in range(MLP_STEPS):
            place = pl.ds(d * SHARD + n * UNITS % SHARD, UNITS)
            fb_ref[:, pl.ds(n * MLP_F + d * UNITS, UNITS)] = vec_ref[steps(FC_BIAS + n * UNITS // SHARD, 1), place]

    def norm(r, n):
        hat, _ = norm_stats(x[pl.ds(r, n), :].astype(F32))
        h[pl.ds(r, n), :] = (hat * gain + bias).astype(BF)
    row_tiles(norm, ROWS)

    def turn(b, carry):
        image = pl.ds(pl.multiple_of(b * MAIN, MAIN), MAIN)
        ht[:, image] = h[image, :].T
        return carry
    lax.fori_loop(0, IMAGES, turn, 0)
    ht[:, TAIL:] = h[TAIL:, :].T
    stores = [pltpu.make_async_copy(src, dst, sems.at[i]) for i, (src, dst) in enumerate(((x, xim_hbm), (dy, dyim_hbm), (h, h_hbm), (ht, ht_hbm)))]
    for cp in stores:
        cp.start()
    def store_fc(tile, values):
        fc_own[:, steps(tile, LANE)] = values.astype(BF)
    regroup(SHARD, lambda n: n % PARTS * MLP_STEPS + n // PARTS, lambda tile: fc_ref[:, steps(tile, LANE)], store_fc)
    for gather in weights:
        gather.turn(3)
    for gather in weights:
        gather.end()
    for cp in stores:
        cp.wait()


def open_call(x, dy, rows, fc, wq, wo):
    hbm, vmem = pl.BlockSpec(memory_space=pl.ANY), pl.BlockSpec(memory_space=pltpu.VMEM)
    return pl.pallas_call(
        open_kernel,
        in_specs=[hbm, hbm, vmem, vmem, vmem, vmem],
        out_specs=[hbm, hbm, hbm, hbm, vmem, vmem, vmem, vmem, hbm, hbm],
        out_shape=[*[jax.ShapeDtypeStruct((TOKENS, WIDTH), BF)] * 3,
                   jax.ShapeDtypeStruct((WIDTH, TOKENS), BF), jax.ShapeDtypeStruct((VECTOR_ROWS, WIDTH), F32),
                   *(jax.ShapeDtypeStruct((1, n), F32) for n in (QKV, FFN)), jax.ShapeDtypeStruct(fc.shape, BF), QKV_ALL.full_shape, OUT_ALL.full_shape],
        scratch_shapes=[pltpu.VMEM((TOKENS, WIDTH), BF), pltpu.VMEM((TOKENS, WIDTH), BF), pltpu.VMEM((LANES, TOKENS, LANE), F32),
                        pltpu.VMEM((TOKENS, WIDTH), BF), pltpu.VMEM((WIDTH, TOKENS), BF), pltpu.VMEM((LANE, LANE), F32), pltpu.VMEM((SHARD, LANE), BF),
                        pltpu.VMEM(VECTOR_ALL.full_shape.shape, BF), pltpu.VMEM((SHARD, QKV), BF), pltpu.VMEM((SHARD, WIDTH), BF),
                        pltpu.SemaphoreType.DMA((QUAD,))] + VECTOR_ALL.scratch() + QKV_ALL.scratch() + OUT_ALL.scratch(),
        compiler_params=pltpu.CompilerParams(vmem_limit_bytes=VMEM_MAX, collective_id=3, has_side_effects=True),
        cost_estimate=cost(1_000_000_000, 60_000_000),
        name="open",
    )(x, dy, rows, fc, wq, wo)


QKV_N = 768


def qkv_kernel(h_ref, w_ref, wb_ref, own_ref, qkv_ref, full, *sems):
    t, last = step_id(), pl.num_programs(0) - 1
    gathers = []
    for i, kind in enumerate(FC_ALL):
        part = pl.ds(i * FC_HALF, FC_HALF)
        gathers.append(kind.bind(own_ref.at[:, part], full.at[(*EVERY, part)], sems[steps(i, 2)]))

    @pl.when(t == 0)
    def _():
        gathers[0].meet()
        for gather in gathers:
            gather.begin()

    @pl.when(t == 1)
    def _():
        for gather in gathers:
            gather.turn(1)
    for i in range(2):
        @pl.when(t == i + 2)
        def _():
            gathers[i].turn(2)
    for rows in BLOCKS:
        qkv_ref[rows, :] = (dot(h_ref[rows, :], w_ref[ALL]) + wb_ref[ALL]).astype(BF)

    @pl.when(t == last)
    def _():
        for gather in gathers:
            gather.turn(3)
        for gather in gathers:
            gather.end()


EVERY = [slice(None)] * 5


def qkv_call(h, w, wb, own):
    hbm = pl.BlockSpec(memory_space=pl.ANY)
    return pl.pallas_call(
        qkv_kernel,
        grid=(QKV // QKV_N,),
        in_specs=[whole(TOKENS, WIDTH, pipeline_mode=pl.Buffered(1)), by_cols(WIDTH, QKV_N), by_cols(1, QKV_N), whole(SHARD, FFN)],
        out_specs=[by_cols(TOKENS, QKV_N), hbm],
        out_shape=[jax.ShapeDtypeStruct((TOKENS, QKV), BF), all_blocks(SHARD, FFN)],
        scratch_shapes=FC_ALL[0].scratch() * 2,
        compiler_params=comm_params(QUAD),
        cost_estimate=cost(2 * TOKENS * WIDTH * QKV, 60_000_000),
        name="qkv",
    )(h, w, wb, own)


ROW_CUTS = (0, 24, 48, 80)
FC_SUM = Exchange(SHARD, MLP_F, ROW_CUTS, 0)
PROJ_SUM = Exchange(UNITS, WIDTH, WIDTH_CUTS, 1)
CDF_P = 0.33
CDF_C = (0.1326322871417956, 0.11939570820799192, 0.18103829560051796, -0.08904113226212501,
         0.33075919469138065, -0.22023738432274684, 0.0454530347223348)


def gelu_pair(u):
    bell = jnp.exp2(u * u * (-0.5 * LOG2E))
    t = 1.0 / (1.0 + CDF_P * jnp.abs(u))
    poly = CDF_C[6]
    for c in CDF_C[5::-1]:
        poly = poly * t + c
    tail = poly * t * bell
    cdf = jnp.where(u < 0.0, tail, 1.0 - tail)
    return u * cdf, cdf + u * bell * ((2.0 * math.pi) ** -0.5)


def mlp_kernel(r_hbm, n_hbm, dy_hbm, vec_ref, fc_ref, proj_ref, fcb_ref,
               y_hbm, dr_hbm, dr16_hbm, dfc_ref, dproj_ref, dfcb_ref, small_ref,
               n2, dy, y_acc, dn_acc, g, du, ua, ub, da, db, sem, *comm):
    step = step_id()
    by_row, by_col = FC_SUM.bind(comm[:Exchange.COUNT]), PROJ_SUM.bind(comm[Exchange.COUNT:])

    @pl.when(step == 0)
    def _():
        loads = [pltpu.make_async_copy(n_hbm, n2, sem), pltpu.make_async_copy(dy_hbm, dy, sem)]
        for cp in loads:
            cp.start()
        by_row.meet()
        clear(small_ref, y_acc, dn_acc)
        for cp in loads:
            cp.wait()

    outs = (dfc_ref, dproj_ref)
    advance((by_row, by_col), step, first_chunks(MLP_STEPS), lambda n, exchange, c: exchange.result(c, outs[n]))

    @pl.when(step < MLP_STEPS)
    def _():
        fcb = fcb_ref[ALL]
        fc, proj = fc_ref[ALL], proj_ref[ALL].reshape(MLP_F, WIDTH)
        bias_sum = jnp.zeros((SUBLANE, MLP_F), F32)
        tiles = [(b * MAIN, MAIN) for b in range(IMAGES - 1)] + [((IMAGES - 1) * MAIN, MAIN + IMAGES)]
        pairs = ((ua, da), (ub, db))

        def products(k):
            r, n = tiles[k]
            u_s, d_s = pairs[k % 2]
            u_s[0:n, :] = dot(n2[r:r + n, :], fc)
            d_s[0:n, :] = dot_nt(dy[r:r + n, :], proj)

        def pointwise(k, total):
            r, n = tiles[k]
            u_s, d_s = pairs[k % 2]
            value, slope = gelu_pair(u_s[0:n, :] + fcb)
            g[r:r + n, :] = value.astype(BF)
            grad = d_s[0:n, :] * slope
            du[r:r + n, :] = grad.astype(BF)
            return total + eights(grad)

        products(0)
        for k in range(1, IMAGES):
            products(k)
            bias_sum = pointwise(k - 1, bias_sum)
        bias_sum = pointwise(IMAGES - 1, bias_sum)
        dfcb_ref[ALL] = col_sum(bias_sum)
        y_acc[ALL] += dot(g[ALL], proj)
        for c in range(LANES // 2):
            part = dot_nt(du[ALL], fc_ref[steps(c, MAIN), :])
            dn_acc[2 * c] += part[:, :LANE]
            dn_acc[2 * c + 1] += part[:, LANE:]
        by_col.put_local(step, dot_tn(g[ALL], dy[ALL]))
        by_row.put_local(step, dot_tn(n2[ALL], du[ALL]))

    after = step - MLP_STEPS
    r_copy = pltpu.make_async_copy(r_hbm, n2, sem)
    out_copies = [pltpu.make_async_copy(dn_acc, dr_hbm, sem), pltpu.make_async_copy(n2, dr16_hbm, sem)]
    y_copy = pltpu.make_async_copy(dy, y_hbm, sem)

    def back(r, n):
        wide_r = n2[pl.ds(r, n), :].astype(F32)
        hat, inv = norm_stats(wide_r)
        dn = joined(dn_acc, r, n)
        wide_dy = dy[pl.ds(r, n), :].astype(F32)
        dr = wide_dy + norm_back(dn, hat, inv, vec_ref[steps(LN2_GAIN, 1), :])
        put(dn_acc, r, n, dr)
        n2[pl.ds(r, n), :] = dr.astype(BF)
        y_acc[pl.ds(r, n), :] += wide_r + vec_ref[steps(PROJ_BIAS, 1), :]
        for i, v in enumerate((dn * hat, dn, wide_dy, dr)):
            small_ref[steps(i, SUBLANE), :] += eights(v)

    @pl.when(after == 0)
    def _():
        r_copy.start()
        r_copy.wait()
        back(TAIL, IMAGES)

    @pl.when((after >= 0) & (after < 3))
    def _():
        back_part(back, after, 3)

    @pl.when(after == 2)
    def _():
        for cp in out_copies:
            cp.start()

    @pl.when(after == 3)
    def _():
        for cp in out_copies:
            cp.wait()
        from_image_order(y_acc, dn_acc)

        def narrow(r, n):
            dy[pl.ds(r, n), :] = joined(dn_acc, r, n).astype(BF)
        row_tiles(narrow)
        y_copy.start()

    @pl.when(after == QUAD)
    def _():
        y_copy.wait()


def mlp_call(r, n2, dy, vec, fc, proj, fcb):
    hbm = pl.BlockSpec(memory_space=pl.ANY)
    now = lambda i: jnp.minimum(i, MLP_STEPS - 1)
    done = lambda i: jnp.maximum(i - DRAIN, 0)
    return pl.pallas_call(
        mlp_kernel,
        grid=(MLP_STEPS + DRAIN,),
        in_specs=[hbm, hbm, hbm, whole(*vec.shape), by_cols(WIDTH, MLP_F, now),
                  pl.BlockSpec((PARTS, None, UNITS, WIDTH), lambda i: (0, now(i), 0, 0)),
                  by_cols(1, MLP_F, now)],
        out_specs=[hbm, hbm, hbm, by_cols(SHARD, MLP_F, done),
                   by_rows(UNITS, WIDTH, done),
                   by_cols(1, MLP_F, now), whole(32, WIDTH)],
        out_shape=[jax.ShapeDtypeStruct((TOKENS, WIDTH), BF), jax.ShapeDtypeStruct((LANES, TOKENS, LANE), F32),
                   jax.ShapeDtypeStruct((TOKENS, WIDTH), BF), jax.ShapeDtypeStruct((SHARD, FFN), F32),
                   jax.ShapeDtypeStruct((FFN // PARTS, WIDTH), F32),
                   jax.ShapeDtypeStruct((1, FFN), F32), jax.ShapeDtypeStruct((32, WIDTH), F32)],
        scratch_shapes=[pltpu.VMEM((TOKENS, WIDTH), BF), pltpu.VMEM((TOKENS, WIDTH), BF),
                        pltpu.VMEM((TOKENS, WIDTH), F32), pltpu.VMEM((LANES, TOKENS, LANE), F32),
                        pltpu.VMEM((TOKENS, MLP_F), BF), pltpu.VMEM((TOKENS, MLP_F), BF)]
                       + [pltpu.VMEM((MAIN + IMAGES, MLP_F), F32)] * QUAD + [pltpu.SemaphoreType.DMA]
                       + FC_SUM.scratch() + PROJ_SUM.scratch(),
        compiler_params=comm_params(0),
        cost_estimate=cost(12 * TOKENS * WIDTH * FFN, 150_000_000, TOKENS * FFN),
        name="mlp",
    )(r, n2, dy, vec, fc, proj.reshape(PARTS, MLP_STEPS, UNITS, WIDTH), fcb)


SCALE = HEAD ** -0.5
SCALE2 = SCALE * LOG2E
ATTN_COST = cost(40_000_000_000, 50_000_000, 8_400_000)


def window(h):
    first = min(HEAD * h // LANE * LANE, WIDTH - MAIN)
    wide = LANE if HEAD * h + HEAD <= first + LANE else MAIN
    return first, wide, HEAD * h - first


def lane_mask(h):
    first, wide, off = window(h)
    lane = lax.broadcasted_iota(jnp.int32, (MAIN, wide), 1)
    return (lane >= off) & (lane < off + HEAD)


def thirds(ref, rows=slice(None)):
    return [ref[rows, steps(i, WIDTH)] for i in range(3)]


def head_rows():
    lane = lax.broadcasted_iota(jnp.int32, (HEADS, WIDTH), 1)
    row = lax.broadcasted_iota(jnp.int32, (HEADS, WIDTH), 0)
    return (lane // HEAD == row).astype(F32)


def tail_softmax(s, s_self):
    m = jnp.maximum(jnp.max(s, axis=1, keepdims=True), s_self)
    e = jnp.exp((s - m) * SCALE)
    e_self = jnp.exp((s_self - m) * SCALE)
    inv = 1.0 / (row_sum(e) + e_self)
    return e * inv, e_self * inv


def attn_kernel(qkv_ref, qkvt_ref, x_ref, xt_ref, w_ref, vec_ref, proj_ref, o_hbm, r_hbm, n_hbm,
                max_ref, inv_ref, full,
                tails, o_tail, o_t, ptail, o_buf, r_buf, n_buf, sa, sb, sems, own, *comm):
    b, last = step_id(), pl.num_programs(0) - 1
    slot = b % 2
    gathers = []
    for i, kind in enumerate(PROJ_ALL):
        part = pl.ds(i * PROJ_FIRST, kind.rows)
        gathers.append(kind.bind(own.at[part], full.at[(*EVERY[1:], part)], comm[steps(i, 2)]))

    @pl.when(b == 0)
    def _():
        tails[ALL] = qkvt_ref[ALL].astype(F32)
        own[ALL] = proj_ref[ALL].astype(BF)
        gathers[0].meet()
        for gather in gathers:
            gather.begin()

    for turn, (stage, i) in enumerate(itertools.product((1, 2, 3), range(2))):
        @pl.when(b == turn + 1 + stage // 3)
        def _():
            gathers[i].turn(stage)

    heads = head_rows()
    q_t, k_t, v_t = (heads * z for z in thirds(tails, pl.ds(b, 1)))
    q, k, v = thirds(qkv_ref)

    p, p_self = tail_softmax(dot_nt(q_t.astype(BF), k), row_sum(q_t * k_t))
    mixed = dot(p.astype(BF), v) * heads + p_self.astype(BF).astype(F32) * v_t
    o_tail[pl.ds(b, 1), :] = col_sum(mixed)

    s_tail = dot_nt(k_t.astype(BF), q)
    v_turned = v.T
    scores = sa, sb

    def next_scores(h):
        first, wide, _ = window(h)
        q_h = jnp.where(lane_mask(h), qkv_ref[:, pl.ds(first, wide)], jnp.zeros((), BF))
        scores[h % 2][ALL] = dot_nt(qkv_ref[:, pl.ds(WIDTH + first, wide)], q_h)
    next_scores(0)
    for h in range(HEADS):
        if h + 1 < HEADS:
            next_scores(h + 1)
        s, mine = scores[h % 2], steps(h, 1)
        top = jnp.maximum(col_max(s[ALL]), s_tail[mine, :])
        e = jnp.exp((s[ALL] - top) * SCALE)
        e_tail = jnp.exp((s_tail[mine, :] - top) * SCALE)
        inv = 1.0 / (col_sum(e) + e_tail)
        max_ref[0, mine, :] = top
        inv_ref[0, mine, :] = inv
        ptail[mine, :] = e_tail * inv
        o_t[steps(h, HEAD), :] = dot(v_turned[steps(h, HEAD), :], (e * inv).astype(BF))

    outs = (o_buf, o_hbm), (r_buf, r_hbm), (n_buf, n_hbm)
    out_bias, gain, bias = (vec_ref[steps(i, 1), :] for i in (OUT_BIAS, LN2_GAIN, LN2_BIAS))

    def write(slot, rows, o, x):
        o_buf[slot, rows, :] = o
        r = (x.astype(F32) + dot(o, w_ref[ALL]) + out_bias).astype(BF)
        r_buf[slot, rows, :] = r
        hat, _ = norm_stats(r.astype(F32))
        n_buf[slot, rows, :] = (hat * gain + bias).astype(BF)

    @pl.when(b >= 2)
    def _():
        for n, (buf, hbm) in enumerate(outs):
            out_copy(buf, hbm, slot, b - 2, sems, n).wait()

    o = (o_t[ALL].T + dot_tn(ptail[ALL].astype(BF), v_t.astype(BF))).astype(BF)
    write(slot, slice(None), o, x_ref[ALL])
    for n, (buf, hbm) in enumerate(outs):
        out_copy(buf, hbm, slot, b, sems, n).start()

    @pl.when(b == last)
    def _():
        for n, (buf, hbm) in enumerate(outs):
            out_copy(buf, hbm, 1 - slot, b - 1, sems, n).wait()
        write(1 - slot, slice(IMAGES), o_tail[ALL].astype(BF), xt_ref[ALL])
        copies = [pltpu.make_async_copy(buf.at[1 - slot, pl.ds(0, IMAGES)], hbm.at[pl.ds(TAIL, IMAGES)], sems.at[n, 1 - slot])
                  for n, (buf, hbm) in enumerate(outs)]
        for cp in copies:
            cp.start()
        for cp in copies:
            cp.wait()
        for n, (buf, hbm) in enumerate(outs):
            out_copy(buf, hbm, slot, b, sems, n).wait()
        for gather in gathers:
            gather.end()


def out_copy(buf, hbm, slot, b, sems, n):
    return pltpu.make_async_copy(buf.at[slot], hbm.at[pl.ds(pl.multiple_of(b * MAIN, MAIN), MAIN)], sems.at[n, slot])


def attn_call(qkv, xim, w, vec, proj):
    hbm = pl.BlockSpec(memory_space=pl.ANY)
    main = lambda n: by_rows(MAIN, n)
    tail = lambda n: by_rows(IMAGES, n, lambda i: TAIL // IMAGES)
    stat = pl.BlockSpec((1, HEADS, MAIN), lambda i: (i, 0, 0))
    return pl.pallas_call(
        attn_kernel,
        grid=(IMAGES,),
        in_specs=[main(QKV), tail(QKV), main(WIDTH), tail(WIDTH),
                  whole(WIDTH, WIDTH), whole(*vec.shape), whole(*proj.shape)],
        out_specs=[hbm, hbm, hbm, stat, stat, hbm],
        out_shape=[*[jax.ShapeDtypeStruct((TOKENS, WIDTH), BF)] * 3,
                   jax.ShapeDtypeStruct((IMAGES, HEADS, MAIN), F32), jax.ShapeDtypeStruct((IMAGES, HEADS, MAIN), F32),
                   all_blocks(*proj.shape)],
        scratch_shapes=[pltpu.VMEM((IMAGES, QKV), F32), pltpu.VMEM((IMAGES, WIDTH), F32),
                        pltpu.VMEM((WIDTH, MAIN), F32), pltpu.VMEM((HEADS, MAIN), F32),
                        *[pltpu.VMEM((2, MAIN, WIDTH), BF)] * 3, *[pltpu.VMEM((MAIN, MAIN), F32)] * 2, pltpu.SemaphoreType.DMA((3, 2)),
                        pltpu.VMEM(proj.shape, BF)] + PROJ_ALL[0].scratch() * 2,
        compiler_params=comm_params(5),
        cost_estimate=ATTN_COST,
        name="attn",
    )(qkv, qkv, xim, xim, w, vec, proj)


def outb_kernel(dr_ref, o_ref, w_ref, dfc_ref, y_in, dproj_in, do_ref, dw_ref, dfc_out, y_out, dproj_out, y, dproj, sems):
    c, last = step_id(), pl.num_programs(0) - 1
    loads = [pltpu.make_async_copy(src, dst, sems.at[i]) for i, (src, dst) in enumerate(((y_in, y), (dproj_in, dproj)))]
    stores = [pltpu.make_async_copy(src, dst, sems.at[i]) for i, (src, dst) in enumerate(((y, y_out), (dproj, dproj_out)))]

    @pl.when(c == 0)
    def _():
        for cp in loads:
            cp.start()

    @pl.when(c == 1)
    def _():
        for cp in loads:
            cp.wait()
        for cp in stores:
            cp.start()

        def store_fc(tile, values):
            dfc_out[:, steps(tile, LANE)] = values
        regroup(SHARD, lambda n: n % MLP_STEPS * PARTS + n // MLP_STEPS, lambda tile: dfc_ref[:, steps(tile, LANE)], store_fc)
    do_ref[ALL] = dot_nt(dr_ref[ALL], w_ref[ALL]).astype(BF)
    dw_ref[ALL] = dot_tn(o_ref[ALL], dr_ref[:, pl.ds(pl.multiple_of(c * MAIN, MAIN), MAIN)])

    @pl.when(c == last)
    def _():
        for cp in stores:
            cp.wait()


def outb_call(dr, o, w, dfc, y, dproj):
    full, hbm = whole(TOKENS, WIDTH), pl.BlockSpec(memory_space=pl.ANY)
    like = lambda v: jax.ShapeDtypeStruct(v.shape, v.dtype)
    return pl.pallas_call(
        outb_kernel,
        grid=(WIDTH // MAIN,),
        in_specs=[full, full, by_rows(MAIN, WIDTH), whole(*dfc.shape), hbm, hbm],
        out_specs=[by_cols(TOKENS, MAIN), by_cols(WIDTH, MAIN), whole(*dfc.shape), hbm, hbm],
        out_shape=[like(dr), jax.ShapeDtypeStruct((WIDTH, WIDTH), F32), like(dfc), like(y), like(dproj)],
        scratch_shapes=[pltpu.VMEM(y.shape, BF), pltpu.VMEM(dproj.shape, F32), pltpu.SemaphoreType.DMA((2,))],
        compiler_params=pltpu.CompilerParams(dimension_semantics=("arbitrary",), vmem_limit_bytes=VMEM_MAX),
        cost_estimate=cost(QUAD * TOKENS * WIDTH * WIDTH, 50_000_000),
        name="outb",
    )(dr, o, w, dfc, y, dproj)


def attn_back_kernel(qkv_ref, qkvt_ref, do_ref, dot_ref, max_ref, inv_ref, dw_ref, dqkv_hbm, dwb_ref, dwout_ref,
                     tails, do_tails, grad_tails, dq_t, dk, dv, ds_tail, sa, da, sb, db, buf, sems, *comm):
    b = step_id()
    by_row = OUT_SUM.bind(comm)

    @pl.when(b == 0)
    def _():
        by_row.meet()

    @pl.when(b < OUT_STEPS)
    def _():
        by_row.put_local(b, dw_ref[ALL])
    advance((by_row,), b + 1, first_chunks(OUT_STEPS), lambda n, exchange, c: exchange.result(c, dwout_ref))

    @pl.when(b < IMAGES)
    def _():
        image_back(b, qkv_ref, qkvt_ref, do_ref, dot_ref, max_ref, inv_ref, dqkv_hbm, dwb_ref,
                   tails, do_tails, grad_tails, dq_t, dk, dv, ds_tail, ((sa, da), (sb, db)), buf, sems)


OUT_N = MAIN
OUT_STEPS = WIDTH // OUT_N
OUT_SUM = Exchange(SHARD, OUT_N, ROW_CUTS, 0)


def image_back(b, qkv_ref, qkvt_ref, do_ref, dot_ref, max_ref, inv_ref, dqkv_hbm, dwb_ref,
               tails, do_tails, grad_tails, dq_t, dk, dv, ds_tail, ahead, buf, sems):
    last = IMAGES - 1
    slot = b % 2

    @pl.when(b == 0)
    def _():
        tails[ALL] = qkvt_ref[ALL].astype(F32)
        do_tails[ALL] = dot_ref[ALL].astype(F32)
        clear(dwb_ref)

    heads = head_rows()
    q_t, k_t, v_t = (heads * z for z in thirds(tails, pl.ds(b, 1)))
    do_t = heads * do_tails[pl.ds(b, 1), :]
    q, k, v = thirds(qkv_ref)
    do = do_ref[ALL]
    q_t16, k_t16, v_t16, do_t16 = (z.astype(BF) for z in (q_t, k_t, v_t, do_t))

    p, p_self = tail_softmax(dot_nt(q_t16, k), row_sum(q_t * k_t))
    dp, dp_self = dot_nt(do_t16, v), row_sum(do_t * v_t)
    inner = row_sum(p * dp) + p_self * dp_self
    ds16 = (p * (dp - inner) * SCALE).astype(BF)
    ds_self = (p_self * (dp_self - inner) * SCALE).astype(BF).astype(F32)
    grad_q = col_sum(dot(ds16, k) * heads + ds_self * k_t)
    grad_k = ds_self * q_t
    grad_v = p_self.astype(BF).astype(F32) * do_t
    dk[ALL] = dot_tn(ds16, q_t16)
    dv[ALL] = dot_tn(p.astype(BF), do_t16)

    p_tail = jnp.exp2((dot_nt(k_t16, q) - max_ref[0]) * SCALE2) * inv_ref[0]
    dp_tail = dot_nt(v_t16, do)
    inner_tail = p_tail * dp_tail

    k_turned = k.T

    def masked(h):
        first, wide, _ = window(h)
        here, mask = pl.ds(first, wide), lane_mask(h)
        return here, jnp.where(mask, qkv_ref[:, here], jnp.zeros((), BF)), jnp.where(mask, do_ref[:, here], jnp.zeros((), BF))

    def next_products(h):
        first, wide, _ = window(h)
        _, q_h, do_h = masked(h)
        ahead[h % 2][0][ALL] = dot_nt(qkv_ref[:, pl.ds(WIDTH + first, wide)], q_h)
        ahead[h % 2][1][ALL] = dot_nt(qkv_ref[:, pl.ds(2 * WIDTH + first, wide)], do_h)
    next_products(0)
    for h in range(HEADS):
        if h + 1 < HEADS:
            next_products(h + 1)
        here, q_h, do_h = masked(h)
        mine = steps(h, 1)
        s, dp = (ref[ALL] for ref in ahead[h % 2])
        p = jnp.exp2((s - max_ref[0, mine, :]) * SCALE2) * inv_ref[0, mine, :]
        inner = col_sum(p * dp) + inner_tail[mine, :]
        ds = (p * (dp - inner) * SCALE).astype(BF)
        dv[:, here] += dot(p.astype(BF), do_h)
        dk[:, here] += dot(ds, q_h)
        dq_t[steps(h, HEAD), :] = dot(k_turned[steps(h, HEAD), :], ds)
        ds_tail[mine, :] = p_tail[mine, :] * (dp_tail[mine, :] - inner) * SCALE

    ds_tail16 = ds_tail[ALL].astype(BF)
    grad_k = col_sum(grad_k + dot(ds_tail16, q) * heads)
    grad_v = col_sum(grad_v + dot(p_tail.astype(BF), do) * heads)

    @pl.when(b >= 2)
    def _():
        out_copy(buf, dqkv_hbm, slot, b - 2, sems, 0).wait()

    grad = dq_t[ALL].T + dot_tn(ds_tail16, k_t16)
    for n, (main, tail) in enumerate(((grad, grad_q), (dk[ALL], grad_k), (dv[ALL], grad_v))):
        here = steps(n, WIDTH)
        buf[slot, :, here] = main.astype(BF)
        grad_tails[pl.ds(b, 1), here] = tail
        dwb_ref[:, here] += col_sum(main) + tail
    out_copy(buf, dqkv_hbm, slot, b, sems, 0).start()

    @pl.when(b == last)
    def _():
        out_copy(buf, dqkv_hbm, 1 - slot, b - 1, sems, 0).wait()
        buf[1 - slot, 0:IMAGES, :] = grad_tails[ALL].astype(BF)
        cp = pltpu.make_async_copy(buf.at[1 - slot, pl.ds(0, IMAGES)], dqkv_hbm.at[pl.ds(TAIL, IMAGES)], sems.at[0, 1 - slot])
        cp.start()
        cp.wait()
        out_copy(buf, dqkv_hbm, slot, b, sems, 0).wait()


def attn_back_call(qkv, do, top, inv, dw):
    hbm = pl.BlockSpec(memory_space=pl.ANY)
    image = lambda i: jnp.minimum(i, IMAGES - 1)
    main = lambda n: by_rows(MAIN, n, image)
    tail = lambda n: by_rows(IMAGES, n, lambda i: TAIL // IMAGES)
    stat = pl.BlockSpec((1, HEADS, MAIN), lambda i: (image(i), 0, 0))
    return pl.pallas_call(
        attn_back_kernel,
        grid=(OUT_STEPS + DRAIN - 1,),
        in_specs=[main(QKV), tail(QKV), main(WIDTH), tail(WIDTH), stat, stat,
                  by_cols(WIDTH, OUT_N, lambda i: jnp.minimum(i, OUT_STEPS - 1))],
        out_specs=[hbm, whole(1, QKV), by_cols(SHARD, OUT_N, lambda i: jnp.clip(i + 1 - DRAIN, 0, OUT_STEPS - 1))],
        out_shape=[jax.ShapeDtypeStruct((TOKENS, QKV), BF), jax.ShapeDtypeStruct((1, QKV), F32),
                   jax.ShapeDtypeStruct((SHARD, WIDTH), F32)],
        scratch_shapes=[pltpu.VMEM((IMAGES, QKV), F32), pltpu.VMEM((IMAGES, WIDTH), F32),
                        pltpu.VMEM((IMAGES, QKV), F32), pltpu.VMEM((WIDTH, MAIN), F32),
                        pltpu.VMEM((MAIN, WIDTH), F32), pltpu.VMEM((MAIN, WIDTH), F32), pltpu.VMEM((HEADS, MAIN), F32),
                        *[pltpu.VMEM((MAIN, MAIN), F32)] * QUAD, pltpu.VMEM((2, MAIN, QKV), BF), pltpu.SemaphoreType.DMA((1, 2))] + OUT_SUM.scratch(),
        compiler_params=comm_params(1),
        cost_estimate=ATTN_COST,
        name="attn_back",
    )(qkv, qkv, do, do, top, inv, dw)


QB_N = MAIN
QB_STEPS = QKV // QB_N
QKV_SUM = Exchange(SHARD, QB_N, ROW_CUTS, 0, 2)
VECTOR_SUM = Exchange(3 * SUBLANE, LANE, (0, SUBLANE, 2 * SUBLANE, 3 * SUBLANE), 0)
VECTOR_STEP = QB_STEPS + 2
QB_GRID = QB_STEPS + 1 + QUAD * QKV_SUM.stride


def qkvb_kernel(xim_hbm, dr_hbm, vec_ref, sums_ref, qb_ref, fb_ref, ht_ref, dqkv_ref, w_ref, dx_hbm, dw_ref, out_vec_ref,
                acc, dr, xd, sums, sems, *comm):
    t = step_id()
    by_row, by_vector = QKV_SUM.bind(comm[:Exchange.COUNT]), VECTOR_SUM.bind(comm[Exchange.COUNT:])
    loads = [pltpu.make_async_copy(dr_hbm, dr, sems.at[0]), pltpu.make_async_copy(xim_hbm, xd, sems.at[1])]
    store = pltpu.make_async_copy(xd, dx_hbm, sems.at[1])

    def put_row(place, row, lane, values):
        by_vector.local[(0, *place, pl.ds(row, len(values)), pl.ds(lane, values.shape[1]))] = values

    def share(row, values):
        for d, place in enumerate(DEVICES):
            put_row(place, row, 0, values[:, steps(d, SHARD)])

    @pl.when(t == 0)
    def _():
        by_row.meet()
        for cp in loads:
            cp.start()
        clear(acc, sums)
        by_vector.local[0] = jnp.zeros(by_vector.blocks, F32)
        share(0, jnp.concatenate([col_sum(sums_ref[steps(i, SUBLANE), :]) for i in range(QUAD)], axis=0))
        for d, place in enumerate(DEVICES):
            for i in range(3):
                put_row(place, QUAD + i, 0, qb_ref[:, pl.ds((3 * d + i) * SHARD, SHARD)])
            for n in range(MLP_STEPS):
                put_row(place, QUAD + 3 + n * UNITS // SHARD, n * UNITS % SHARD, fb_ref[:, pl.ds(n * MLP_F + d * UNITS, UNITS)])

    def emit_vectors(n, exchange, c):
        for part, (rows, _) in enumerate(exchange.parts[:2]):
            out_vec_ref[rows, :] = exchange.held[3][part][0, :, :SHARD]
    advance((by_row,), t, first_chunks(QB_STEPS), lambda n, exchange, c: exchange.result(c, dw_ref))
    advance((by_vector,), t - VECTOR_STEP, first_chunks(1), emit_vectors)

    @pl.when(t < QB_STEPS)
    def _():
        by_row.put_local(t, dot(ht_ref[ALL], dqkv_ref[ALL]))
        acc[ALL] += dot_nt(dqkv_ref[ALL], w_ref[ALL])

    @pl.when(t == QB_STEPS)
    def _():
        for cp in loads:
            cp.wait()

    def back(r, n):
        hat, inv = norm_stats(xd[pl.ds(r, n), :].astype(F32))
        dn = acc[pl.ds(r, n), :]
        for i, v in enumerate((dn * hat, dn)):
            sums[steps(i, SUBLANE), :] += eights(v)
        acc[pl.ds(r, n), :] = joined(dr, r, n) + norm_back(dn, hat, inv, vec_ref[steps(LN1_GAIN, 1), :])

    @pl.when((t >= QB_STEPS) & (t <= VECTOR_STEP))
    def _():
        back_part(back, t - QB_STEPS, 3)

    @pl.when(t == VECTOR_STEP)
    def _():
        back(TAIL, IMAGES)
        share(VECTOR_ROWS - 2, jnp.concatenate([col_sum(sums[steps(i, SUBLANE), :]) for i in range(2)], axis=0))

    @pl.when(t == VECTOR_STEP + 1)
    def _():
        from_image_order(acc, dr)

    @pl.when(t == VECTOR_STEP + 2)
    def _():
        def narrow(r, n):
            xd[pl.ds(r, n), :] = joined(dr, r, n).astype(BF)
        row_tiles(narrow)
        store.start()

    @pl.when(t == QB_GRID - 1)
    def _():
        store.wait()


DEVICES = list(itertools.product(range(2), repeat=QUAD))


def qkvb_call(xim, dr, vec, sums, qb, fb, ht, dqkv, w):
    hbm = pl.BlockSpec(memory_space=pl.ANY)
    now = lambda i: jnp.minimum(i, QB_STEPS - 1)
    return pl.pallas_call(
        qkvb_kernel,
        grid=(QB_GRID,),
        in_specs=[hbm, hbm, *(whole(*v.shape) for v in (vec, sums, qb, fb)),
                  whole(WIDTH, TOKENS, pipeline_mode=pl.Buffered(1)), by_cols(TOKENS, QB_N, now), by_cols(WIDTH, QB_N, now)],
        out_specs=[hbm, by_cols(SHARD, QB_N, lambda i: jnp.clip(i - 1 - QUAD * QKV_SUM.stride, 0, QB_STEPS - 1)),
                   whole(VECTOR_ROWS, SHARD)],
        out_shape=[jax.ShapeDtypeStruct((TOKENS, WIDTH), BF), jax.ShapeDtypeStruct((SHARD, QKV), F32),
                   jax.ShapeDtypeStruct((VECTOR_ROWS, SHARD), F32)],
        scratch_shapes=[pltpu.VMEM((TOKENS, WIDTH), F32), pltpu.VMEM((LANES, TOKENS, LANE), F32), pltpu.VMEM((TOKENS, WIDTH), BF),
                        pltpu.VMEM((2 * SUBLANE, WIDTH), F32), pltpu.SemaphoreType.DMA((2,))]
                       + QKV_SUM.scratch() + VECTOR_SUM.scratch(),
        compiler_params=comm_params(2),
        cost_estimate=cost(QUAD * TOKENS * WIDTH * QKV, 80_000_000),
        name="qkvb",
    )(xim, dr, vec, sums, qb, fb, ht, dqkv, w)


def solution(mesh):
    specs = (P("fsdp"),) * 14

    def device_step(resid_in, grad_out, ln1_gain, ln1_bias, qkv_weight, qkv_bias, out_weight, out_bias,
                    ln2_gain, ln2_bias, fc_weight, fc_bias, proj_weight, proj_bias):
        rows = jnp.concatenate([ln1_gain, ln1_bias, qkv_bias, out_bias, ln2_gain, ln2_bias, fc_bias, proj_bias]).reshape(-1, SHARD)
        rows = jnp.pad(rows, ((0, VECTOR_ROWS - len(rows)), (0, LANE - SHARD)))
        x = resid_in.swapaxes(0, 1).reshape(TOKENS, WIDTH)
        dy = grad_out.swapaxes(0, 1).reshape(TOKENS, WIDTH)
        xim, dyim, h, ht, rows, bq, bf, fc, wq, wo = open_call(x, dy, rows, fc_weight, qkv_weight, out_weight)
        wq, wo = wq.reshape(WIDTH, QKV), wo.reshape(WIDTH, WIDTH)
        qkv, wf = qkv_call(h, wq, bq, fc)
        o, r, n2, top, inv, wp = attn_call(qkv, xim, wo, rows, proj_weight)
        y, dr, dr16, dwf, dwp, dbf, small = mlp_call(r, n2, dyim, rows, wf.reshape(WIDTH, FFN), wp, bf)
        do, dwo, dwf, y, dwp = outb_call(dr16, o, wo, dwf, y, dwp)
        dqkv, dbq, dwo = attn_back_call(qkv, do, top, inv, dwo)
        dx, dwq, vec = qkvb_call(xim, dr, rows, small, dbq, dbf, ht, dqkv, wq)
        dg2, db2, dbp, dbo = vec[:4]
        dbq, dbf = vec[4:7].reshape(-1), vec[7:11].reshape(-1)
        dg1, db1 = vec[VECTOR_ROWS - 2:]
        unturn = lambda t: t.reshape(SEQ, IMAGES, WIDTH).swapaxes(0, 1)
        return (unturn(y), unturn(dx), dg1, db1, dwq, dbq, dwo, dbo, dg2, db2, dwf, dbf, dwp, dbp)

    return jax.shard_map(device_step, mesh=mesh, in_specs=specs, out_specs=specs, check_vma=False)
```
